32 devices in a mesh: ctx: 8 (over z, core), fsdp: 4 (over y, x).
Axes of the slice: x: 2, y: 2, z: 4, core: 2. Of those that a mesh axis runs over, the one named last changes fastest.
Arguments:
- tokens: bfloat16 [4, 1024, 1024], P('fsdp', 'ctx'), may hold values from -6 to 6
- norm_first: bfloat16 [1024], P(('ctx', 'fsdp')), may hold values from 0.099609375 to 1.8984375
- w_query: bfloat16 [1024, 1024], P(('ctx', 'fsdp')), may hold values from -0.65625 to 0.65625
- w_key: bfloat16 [1024, 512], P(('ctx', 'fsdp')), may hold values from -0.65625 to 0.65625
- w_value: bfloat16 [1024, 512], P(('ctx', 'fsdp')), may hold values from -0.1875 to 0.1875
- w_out: bfloat16 [1024, 1024], P(('ctx', 'fsdp')), may hold values from -6 to 6
- norm_second: bfloat16 [1024], P(('ctx', 'fsdp')), may hold values from 0.099609375 to 1.8984375
- w_router: bfloat16 [1024, 32], P(('ctx', 'fsdp')), may hold values from -0.375 to 0.375
- w_gate: bfloat16 [32, 1024, 512], P('fsdp', 'ctx'), may hold values from -0.1875 to 0.1875
- w_up: bfloat16 [32, 1024, 512], P('fsdp', 'ctx'), may hold values from -0.1875 to 0.1875
- w_down: bfloat16 [32, 512, 1024], P('fsdp', None, 'ctx'), may hold values from -2.390625 to 2.390625
- positions: int32 [4, 1024], P('fsdp', 'ctx'), may hold values from 0 to 1023, as said below
- routes: int32 [4, 1024, 8], P('fsdp', 'ctx'), may hold values from 0 to 31, all different within a row; in each aligned block of 128 rows (0 to 127, 128 to 255, ..., all dimensions but the last counted through in order) at most 48 rows name the same one
- cotangent: bfloat16 [4, 1024, 1024], P('fsdp', 'ctx'), may hold values from -6 to 6
Outputs:
- output: bfloat16 [4, 1024, 1024], P('fsdp', 'ctx')
- grad_tokens: float32 [4, 1024, 1024], P('fsdp', 'ctx')
- grad_norm_first: float32 [1024], P(('ctx', 'fsdp'))
- grad_query: float32 [1024, 1024], P(('ctx', 'fsdp'))
- grad_key: float32 [1024, 512], P(('ctx', 'fsdp'))
- grad_value: float32 [1024, 512], P(('ctx', 'fsdp'))
- grad_out: float32 [1024, 1024], P(('ctx', 'fsdp'))
- grad_norm_second: float32 [1024], P(('ctx', 'fsdp'))
- grad_router: float32 [1024, 32], P(('ctx', 'fsdp'))
- grad_gate: float32 [32, 1024, 512], P('fsdp', 'ctx')
- grad_up: float32 [32, 1024, 512], P('fsdp', 'ctx')
- grad_down: float32 [32, 512, 1024], P('fsdp', None, 'ctx')
The draws below stay inside these ranges and needn't reach their ends.
Inputs may be any that keep to these rules, and one draw needn't show every extreme that they name: Each sequence's positions are a permutation of 0 to 1023, made of runs of 64 consecutive increasing positions in an order drawn per sequence. `routes`: each row names 8 different experts; within the rows of one device (aligned blocks of 128 rows, sequences in order) no expert is named by more than 48 rows.
All inputs are finite; a program needn't handle non-finite values.
Results may differ from the reference program's by a relative error of at most 0.025.
The reference program's roundings to bfloat16 on the way count: a program that leaves them out, or rounds other values in their place, can miss the bound.
Values may be sent and summed in bfloat16 or wider, within the bound.
A program may use at most 192 MiB of HBM per device.

```python
import math
import jax
import jax.numpy as jnp
import numpy as np
from jax import lax

D = 1024
HEADS = 16
KV_HEADS = 8
HEAD = 64
EXPERTS = 32
FF = 512
TOP = 8
TOK_DEV = 128
RUN = 64
LEN = 1024
SEQS = 4
CAP = 48
N_CTX = 8


def draw_positions(key, part):
    run_count = LEN // RUN
    seq_keys = jax.random.split(key, SEQS)
    ordering = jax.vmap(lambda one_key: jax.random.permutation(one_key, run_count))(seq_keys)
    inside = jnp.arange(RUN, dtype=jnp.int32)
    layout = ordering.astype(jnp.int32)[:, :, None] * RUN + inside[None, None, :]
    return layout.reshape(SEQS, run_count * RUN).astype(jnp.int32)


def shard_levels(rng, extent, shards, low, high):
    factor_of, own = 1.0, jax.random.fold_in(rng, 6)
    for dim, parts in shards:
        heights = jnp.exp(jax.random.uniform(jax.random.fold_in(own, dim), (parts,), jnp.float32, low / len(shards), high / len(shards)))
        factor_of = factor_of * jnp.repeat(heights, extent[dim] // parts).reshape([-1 if axis == dim else 1 for axis in range(len(extent))])
    return factor_of


def deal_out(own_key, own, number, rows, amount, top, limit, slope):
    sequence = jax.random.permutation(own_key, amount)
    heavy_load, usual = load_shares(amount, rows * top, limit, slope, True), load_shares(amount, rows * top, limit, slope, False)
    places = jnp.arange(amount)

    def named(sizes, offset_by):
        used = int((sizes > 0).sum())
        fixed = max(1, used // 4)
        passed = fixed + (places - fixed + offset_by * (used - fixed)) % max(1, amount - fixed)
        return jnp.zeros((amount,), jnp.int32).at[sequence[jnp.where(places < fixed, places, passed)]].set(jnp.asarray(sizes, jnp.int32))

    sizes = jnp.where(number % 4 == 0, named(heavy_load, number // 4), named(usual, number - number // 4 - 1))
    mixed = jax.random.permutation(jax.random.fold_in(own, 3), amount)
    giver, receiver = mixed[0:amount // 2 * 2:2], mixed[1:amount // 2 * 2:2]
    room = jnp.minimum(sizes[giver] - 1, limit - sizes[receiver]) // 2
    room = jnp.where((giver == sequence[0]) | (receiver == sequence[0]) | (sizes[receiver] == 0), 0, jnp.maximum(room, 0))
    passed = jax.random.randint(jax.random.fold_in(own, 4), (amount // 2,), 0, 1 << 20) % (room + 1)
    sizes = sizes.at[giver].add(-passed).at[receiver].add(passed)
    members = jnp.searchsorted(jnp.cumsum(sizes), jnp.arange(rows * top), side="right").astype(jnp.int32)
    table = members.reshape(top, rows).T
    table = table[jax.random.permutation(jax.random.fold_in(own, 1), rows)]
    offset_by = jax.random.randint(jax.random.fold_in(own, 2), (rows, 1), 0, top)
    return jnp.take_along_axis(table, (jnp.arange(top)[None, :] + offset_by) % top, axis=1)


def load_shares(number_of, total, bound, lean, full):
    weights = [(1 << 20) // math.isqrt(grade ** lean) + 1 for grade in range(1, number_of + 1)]
    largest = bound if full else min(bound, max(-(-total // number_of), total * weights[0] // sum(weights)))
    least = 1 if total - largest >= number_of - 1 else 0
    counts, spare = [largest] + [least] * (number_of - 1), total - largest - least * (number_of - 1)
    while spare > 0:
        free = [i for i in range(1, number_of) if counts[i] < largest] or [i for i in range(1, number_of) if counts[i] < bound]
        whole, remaining = sum([weights[i] for i in free]), spare
        for i in free:
            more = min(bound - counts[i], max(1, remaining * weights[i] // whole), spare)
            counts[i] = counts[i] + more
            spare = spare - more
    return np.array(counts)


def centred(rng, extent, spread, bound, cuts=(), held_as=jnp.bfloat16):
    level = shard_levels(rng, extent, cuts, -0.22, 0.18) if cuts else 1.0
    array = jax.random.normal(rng, extent, jnp.float32) * spread * level
    return jnp.minimum(jnp.maximum(array, -bound), bound).astype(held_as)


def setup_inputs(seed: int = 0) -> dict:
    seeds = jax.random.split(jax.random.key(seed), 15)
    tokens = centred(seeds[0], (SEQS, LEN, D), 1.0, 6.0, ((0, 4), (1, 8)))
    norm_first = jnp.clip(1.0 + 0.18 * jax.random.normal(seeds[1], (D,), jnp.float32), 0.099609375, 1.8984375).astype(jnp.bfloat16)
    w_query = centred(seeds[2], (D, HEADS * HEAD), 0.11, 0.65625, ((0, 32),))
    w_key = centred(seeds[3], (D, KV_HEADS * HEAD), 0.11, 0.65625, ((0, 32),))
    w_value = centred(seeds[4], (D, KV_HEADS * HEAD), D ** -0.5, 0.1875, ((0, 32),))
    w_out = centred(seeds[5], (HEADS * HEAD, D), 1.0, 6.0, ((0, 32),))
    norm_second = jnp.clip(1.0 + 0.18 * jax.random.normal(seeds[6], (D,), jnp.float32), 0.099609375, 1.8984375).astype(jnp.bfloat16)
    w_router = centred(seeds[7], (D, EXPERTS), 0.0625, 0.375, ((0, 32),))
    w_gate = centred(seeds[8], (EXPERTS, D, FF), D ** -0.5, 0.1875, ((0, 4), (1, 8)))
    w_up = centred(seeds[9], (EXPERTS, D, FF), D ** -0.5, 0.1875, ((0, 4), (1, 8)))
    w_down = centred(seeds[10], (EXPERTS, FF, D), 0.4, 2.390625, ((0, 4), (2, 8)))
    positions = draw_positions(jax.random.fold_in(seeds[14], 71), 0)
    routes_keys = jax.random.split(jax.random.fold_in(seeds[12], 1), SEQS * LEN // TOK_DEV)
    routes_turns = jax.random.permutation(jax.random.fold_in(seeds[12], 3), SEQS * LEN // TOK_DEV)
    routes = jax.vmap(lambda own, number: deal_out(jax.random.fold_in(seeds[12], 2), own, number, TOK_DEV, EXPERTS, TOP, CAP, 1))(routes_keys, routes_turns).reshape((SEQS, LEN, TOP))
    cotangent = centred(seeds[13], (SEQS, LEN, D), 1.0, 6.0, ((0, 4), (1, 8)))
    return {"tokens": tokens, "norm_first": norm_first, "w_query": w_query, "w_key": w_key, "w_value": w_value, "w_out": w_out, "norm_second": norm_second, "w_router": w_router, "w_gate": w_gate, "w_up": w_up, "w_down": w_down, "positions": positions, "routes": routes, "cotangent": cotangent}


@jax.custom_vjp
def low(v):
    return lax.optimization_barrier(v.astype(jnp.bfloat16)).astype(jnp.float32)

@jax.custom_vjp
def low_back(v):
    return v

def low_keep(v):
    return (low(v), None)

def low_pass(kept, grad):
    return (grad,)

def back_keep(v):
    return (v, None)

def back_low(kept, grad):
    return (low(grad),)
low.defvjp(low_keep, low_pass)
low_back.defvjp(back_keep, back_low)
residual_scale = 0.22
score_scale = 0.015625
rope_base = 10000.0
norm_eps = 1e-06
masked_score = -1e+30

def product(left, right):
    return jnp.dot(left, right, precision=lax.Precision.HIGHEST, preferred_element_type=jnp.float32)

def rms_norm(values_in, gain_vector):
    inverse = lax.rsqrt(lax.optimization_barrier(jnp.mean(values_in * values_in, axis=-1, keepdims=True)) + norm_eps)
    return values_in * inverse * gain_vector

def rotate(values_in, position):
    head_size = values_in.shape[-1]
    half_size = head_size // 2
    frequency = rope_base ** (jnp.arange(half_size, dtype=jnp.float32) * (-2.0 / head_size))
    angles = position.astype(jnp.float32)[:, None] * frequency[None, :]
    cosine = jnp.cos(angles)[:, None, :]
    sine_part = jnp.sin(angles)[:, None, :]
    front_half = values_in[..., :half_size]
    back_half = values_in[..., half_size:]
    return jnp.concatenate([front_half * cosine - back_half * sine_part, back_half * cosine + front_half * sine_part], axis=-1)

def attend(queries, key_rows, value_rows, position):
    length = queries.shape[0]
    block_size = min(512, length)

    def one_block(block_index):
        begin_at = block_index * block_size
        query_block = lax.dynamic_slice_in_dim(queries, begin_at, block_size, 0)
        query_place = lax.dynamic_slice_in_dim(position, begin_at, block_size, 0)
        scores = low_back(jnp.einsum('tgrd,kgd->tgrk', query_block, key_rows, precision=lax.Precision.HIGHEST) * score_scale)
        allowed = jnp.broadcast_to((position[None, :] <= query_place[:, None])[:, None, None, :], scores.shape)
        probabilities = jax.nn.softmax(jnp.where(allowed, scores, masked_score), axis=-1, where=allowed)
        return jnp.einsum('tgrk,kgd->tgrd', low(probabilities), value_rows, precision=lax.Precision.HIGHEST)
    outputs = lax.map(jax.checkpoint(one_block), jnp.arange(length // block_size, dtype=jnp.int32))
    return outputs.reshape((length,) + outputs.shape[2:])

def experts(normed, gate_weights, route_ids, gate_w, up_w, down_w):
    flat_route = route_ids.reshape(-1)
    pair_count = flat_route.shape[0]
    ordering = jnp.arange(pair_count, dtype=jnp.int32)
    flat_gates = gate_weights.reshape(-1)
    capacity = N_CTX * CAP

    def one_expert(expert_id):
        picked = jnp.sort(jnp.where(flat_route == expert_id, ordering, pair_count))[:capacity]
        safe_pair = jnp.minimum(picked, pair_count - 1)
        member = normed[safe_pair // TOP]
        gate_value = low_back(product(member, gate_w[expert_id]))
        up_value = low_back(product(member, up_w[expert_id]))
        hidden = low(jax.nn.silu(gate_value) * up_value)
        result = low(low_back(product(hidden, down_w[expert_id])))
        weighting = jnp.where(picked < pair_count, flat_gates[safe_pair], 0.0)
        return (result * weighting[:, None], safe_pair // TOP)
    pieces, owners = lax.map(jax.checkpoint(one_expert), jnp.arange(EXPERTS, dtype=jnp.int32))
    return jnp.zeros(normed.shape, jnp.float32).at[owners.reshape(-1)].add(pieces.reshape(-1, normed.shape[1]))

def layer(seq_x, seq_place, seq_route, gain_one, query_w, key_w, value_w, out_w, gain_two, router_w, gate_w, up_w, down_w):
    length = seq_x.shape[0]
    normed_one = low(rms_norm(seq_x, gain_one))
    queries = low(rotate(low_back(product(normed_one, query_w)).reshape(length, HEADS, HEAD), seq_place))
    key_rows = low(rotate(low_back(product(normed_one, key_w)).reshape(length, KV_HEADS, HEAD), seq_place))
    value_rows = low(low_back(product(normed_one, value_w))).reshape(length, KV_HEADS, HEAD)
    attention_mix = attend(queries.reshape(length, KV_HEADS, HEADS // KV_HEADS, HEAD), key_rows, value_rows, seq_place)
    attended = low(low_back(attention_mix)).reshape(length, HEADS * HEAD)
    middle = seq_x + residual_scale * low_back(product(attended, out_w))
    normed_two = low(rms_norm(middle, gain_two))
    chosen = jnp.take_along_axis(product(normed_two, router_w), seq_route, axis=1)
    gate_weights = jax.nn.softmax(chosen, axis=-1)
    return middle + residual_scale * experts(normed_two, gate_weights, seq_route, gate_w, up_w, down_w)

def reference(tokens, norm_first, w_query, w_key, w_value, w_out, norm_second, w_router, w_gate, w_up, w_down, positions, routes, cotangent):
    params = tuple((weight.astype(jnp.float32) for weight in (norm_first, w_query, w_key, w_value, w_out, norm_second, w_router, w_gate, w_up, w_down)))
    inputs = tokens.astype(jnp.float32)

    def forward(inputs_f, *weights):

        def layer_step(running, sequence_item):
            seq_x, seq_place, seq_route = sequence_item
            return (running, layer(seq_x, seq_place, seq_route, *weights))
        return lax.scan(jax.checkpoint(layer_step), jnp.zeros((), jnp.float32), (inputs_f, positions, routes))[1]
    result, pullback = jax.vjp(forward, inputs, *params)
    gradients = pullback(cotangent.astype(jnp.float32))
    return (result.astype(jnp.bfloat16), gradients[0], gradients[1], gradients[2], gradients[3], gradients[4], gradients[5], gradients[6], gradients[7], gradients[8], gradients[9], gradients[10])
```

```python
import collections
import functools

import jax
import jax.numpy as jnp
from jax import lax
from jax.experimental import pallas as pl
from jax.experimental.pallas import tpu as pltpu
from jax.sharding import PartitionSpec as P

D = 1024
HEADS = 16
KV_HEADS = 8
HEAD = 64
EXPERTS = 32
TOP = 8
CAP = 48
OWN = 2

residual_scale = 0.22
score_scale = 0.015625
rope_base = 10000.0
norm_eps = 1e-06
masked_score = -1e30

MESH = pl.DeviceIdType.MESH
Place = collections.namedtuple("Place", ["c", "f", "m", "s", "q", "w"])
Flow = collections.namedtuple("Flow", ["group", "src", "dst", "src_of", "dst_of"])


class Sizes:
    def __init__(self, mesh):
        self.C = mesh.shape["ctx"]
        self.F = mesh.shape["fsdp"]
        self.N = self.C * self.F
        self.per_f = EXPERTS // self.F
        self.G = self.per_f // OWN
        self.S = self.C // self.G
        self.Q = self.F * self.G
        self.q_heads = HEADS // self.C
        self.q_width = self.q_heads * HEAD
        self.width = self.q_width + 2 * HEAD
        self.share = self.C // KV_HEADS
        self.rows_w = D // self.N

    def place(self, c, f):
        m = lax.rem(c, self.G)
        return Place(c, f, m, lax.div(c, self.G), f * self.G + m, c * self.F + f)

    def count(self, group):
        return {"ctx": self.C, "fsdp": self.F, "world": self.N, "cube": self.Q}[group]

    def peer(self, group, me, k):
        if group == "ctx":
            return self.place(lax.rem(me.c + k, self.C), me.f)
        if group == "fsdp":
            return self.place(me.c, lax.rem(me.f + k, self.F))
        if group == "world":
            w = lax.rem(me.w + k, self.N)
            return self.place(lax.div(w, self.F), lax.rem(w, self.F))
        q = lax.rem(me.q + k, self.Q)
        return self.place(me.s * self.G + lax.rem(q, self.G), lax.div(q, self.G))


def block(ref, index):
    return ref.at[index] if index is not None else ref


def exchange(sizes, name, collective_id, flows, ins, outs):
    groups = {"ctx", "fsdp", "world", "cube"} & {flow.group for flow in flows}
    widest = "world" if "world" in groups else ("cube" if "cube" in groups else None)
    meet = [widest] if widest else []
    meet += [g for g in ("ctx", "fsdp") if g in groups and widest != "world"]

    def body(*refs):
        in_refs = refs[: len(ins)]
        out_refs = refs[len(ins) : len(ins) + len(outs)]
        scratch = refs[len(ins) + len(outs) :]
        sends = scratch[0 : len(flows)]
        recvs = scratch[len(flows) : 2 * len(flows)]
        own_sem = scratch[2 * len(flows)]
        bounces = list(scratch[2 * len(flows) + 1 :])
        me = sizes.place(lax.axis_index("ctx"), lax.axis_index("fsdp"))

        barrier = pltpu.get_barrier_semaphore()
        total = 0
        for g in meet:
            def greet(k, carry, g=g):
                p = sizes.peer(g, me, k)
                pl.semaphore_signal(barrier, inc=1, device_id=(p.c, p.f), device_id_type=MESH)
                return carry
            lax.fori_loop(1, sizes.count(g), greet, 0)
            total += sizes.count(g) - 1
        pl.semaphore_wait(barrier, total)

        def copy_of(j, k, to):
            flow = flows[j]
            if isinstance(flow.src, tuple):
                source = flow.dst_of(out_refs[flow.src[1]], me)
            else:
                source = flow.src_of(in_refs[flow.src], to)
            return pltpu.make_async_remote_copy(
                src_ref=source,
                dst_ref=flow.dst_of(out_refs[flow.dst], me),
                send_sem=sends[j].at[k],
                recv_sem=recvs[j].at[k],
                device_id=(to.c, to.f),
                device_id_type=MESH,
            )

        def start(j):
            def one(k, carry):
                copy_of(j, k, sizes.peer(flows[j].group, me, k)).start()
                return carry
            lax.fori_loop(1, sizes.count(flows[j].group), one, 0)

        def finish(j):
            def one(k, carry):
                flow = flows[j]
                n = sizes.count(flow.group)
                to = sizes.peer(flow.group, me, k)
                copy_of(j, k, to).wait_send()
                sender = sizes.peer(flow.group, me, n - k)
                landed = flow.dst_of(out_refs[flow.dst], sender)
                pltpu.make_async_remote_copy(
                    src_ref=landed, dst_ref=landed, send_sem=sends[j].at[k], recv_sem=recvs[j].at[k],
                    device_id=(to.c, to.f), device_id_type=MESH,
                ).wait_recv()
                return carry
            lax.fori_loop(1, sizes.count(flows[j].group), one, 0)

        own_flows = [j for j in range(len(flows)) if not isinstance(flows[j].src, tuple)]
        bounce_of = dict(zip(own_flows, bounces))
        for j in own_flows:
            start(j)
        loads = {}
        for j in own_flows:
            loads[j] = pltpu.make_async_copy(
                flows[j].src_of(in_refs[flows[j].src], me), bounce_of[j], own_sem.at[j, 0])
            loads[j].start()
        stores = {}
        for j in own_flows:
            loads[j].wait()
            stores[j] = pltpu.make_async_copy(
                bounce_of[j], flows[j].dst_of(out_refs[flows[j].dst], me), own_sem.at[j, 1])
            stores[j].start()
        done = set()
        for j in range(len(flows)):
            if isinstance(flows[j].src, tuple):
                for i in range(j):
                    if i not in done and flows[i].dst == flows[j].src[1]:
                        finish(i)
                        stores[i].wait()
                        done.add(i)
                start(j)
        for j in range(len(flows)):
            if j not in done:
                finish(j)
                if j in stores:
                    stores[j].wait()

    me0 = Place(0, 0, 0, 0, 0, 0)
    bounce_shapes = []
    for flow in flows:
        if not isinstance(flow.src, tuple):
            shape = jax.eval_shape(lambda a, flow=flow: a, ins[flow.src])
            bounce_shapes.append(pltpu.VMEM(flow_shape(flow, shape.shape), shape.dtype))
    return pl.pallas_call(
        body,
        name=name,
        out_shape=outs,
        in_specs=[pl.BlockSpec(memory_space=pl.ANY)] * len(ins),
        out_specs=[pl.BlockSpec(memory_space=pl.ANY)] * len(outs),
        scratch_shapes=[pltpu.SemaphoreType.DMA((sizes.count(f.group),)) for f in flows] * 2
        + [pltpu.SemaphoreType.DMA((len(flows), 2))]
        + bounce_shapes,
        compiler_params=pltpu.CompilerParams(collective_id=collective_id, has_side_effects=True),
    )(*ins)


def flow_shape(flow, shape):
    return flow.src_of(ShapeProbe(shape), Place(0, 0, 0, 0, 0, 0)).shape


class ShapeProbe:
    def __init__(self, shape):
        self.shape = tuple(shape)

    @property
    def at(self):
        return self

    def __getitem__(self, index):
        index = index if isinstance(index, tuple) else (index,)
        kept = []
        for i, n in enumerate(self.shape):
            if i >= len(index) or (isinstance(index[i], slice) and index[i] == slice(None)):
                kept.append(n)
            elif hasattr(index[i], "size") and not isinstance(index[i], int) and hasattr(index[i], "start"):
                kept.append(index[i].size)
        return ShapeProbe(kept)


whole = lambda ref, p: ref
at_c = lambda ref, p: ref.at[p.c]
at_f = lambda ref, p: ref.at[p.f]
at_q = lambda ref, p: ref.at[p.q]
at_w = lambda ref, p: ref.at[p.w]


def bf(x):
    return x.astype(jnp.bfloat16)


def f32(x):
    return x.astype(jnp.float32)


def dot32(spec, a, b, **kw):
    return jnp.einsum(spec, a, b, preferred_element_type=jnp.float32, **kw)


def norm_parts(x):
    inverse = lax.rsqrt(jnp.mean(x * x, axis=-1, keepdims=True) + norm_eps)
    return x * inverse, inverse


def norm_back(d_output, normalized, inverse, gain):
    g = d_output * gain
    return inverse * (g - normalized * jnp.mean(g * normalized, axis=-1, keepdims=True))


def turn(x, cosine, sine):
    a, b = x[..., : HEAD // 2], x[..., HEAD // 2 :]
    return jnp.concatenate([a * cosine - b * sine, b * cosine + a * sine], axis=-1)


def shape_of(shape, dtype=jnp.bfloat16):
    return jax.ShapeDtypeStruct(shape, dtype)


def local(z, tokens, norm_first, w_query, w_key, w_value, w_out, norm_second, w_router,
          w_gate, w_up, w_down, positions, routes, cotangent):
    C, F, N, Q, S, G = z.C, z.F, z.N, z.Q, z.S, z.G
    R = tokens.shape[1]
    L = C * R
    rs = z.rows_w
    ff = w_gate.shape[2]
    dc = D // C
    my_c = lax.axis_index("ctx")

    expert_ids = jnp.arange(EXPERTS, dtype=jnp.int32)
    named = jnp.any(routes[0][:, :, None] == expert_ids[None, None, :], axis=1)
    before = (jnp.arange(R)[:, None] > jnp.arange(R)[None, :]).astype(jnp.bfloat16)
    slot = dot32("tu,ue->te", before, named.astype(jnp.bfloat16)).astype(jnp.int32)
    slot = jnp.where(named, slot, -1)
    pick = (slot.T[:, None, :] == jnp.arange(CAP, dtype=jnp.int32)[None, :, None]).astype(jnp.bfloat16)
    pick = pick.reshape(EXPERTS * CAP, R)

    heads_q = w_query.reshape(rs, C, z.q_width)
    heads_k = jnp.repeat(w_key.reshape(rs, KV_HEADS, HEAD), z.share, axis=1)
    heads_v = jnp.repeat(w_value.reshape(rs, KV_HEADS, HEAD), z.share, axis=1)
    w_pack = jnp.concatenate([heads_q, heads_k, heads_v], axis=2).transpose(1, 0, 2)
    small = jnp.concatenate(
        [w_router, norm_first[:, None], norm_second[:, None], jnp.zeros((rs, 128 - EXPERTS - 2), jnp.bfloat16)], axis=1)
    place_pack = jnp.broadcast_to(positions[0][None, :], (8, R))
    cot_rows = bf(dot32("st,td->sd", pick, cotangent[0])).reshape(Q, OWN * CAP, D)

    own_pair = lambda ref, p: ref.at[pl.ds(p.m * OWN, OWN)]
    tok_all, pos_all, w_c, small_all, wo, wg, wu, wd, cot_in = exchange(
        z, "first_exchange", 0,
        [
            Flow("ctx", 3, 4, whole, lambda ref, p: ref.at[p.c, p.f]),
            Flow("ctx", 0, 0, whole, at_c),
            Flow("ctx", 1, 1, whole, at_c),
            Flow("world", 2, 2, at_c, at_w),
            Flow("world", 4, 3, whole, at_w),
            Flow("fsdp", ("out", 4), 4, None, lambda ref, p: ref.at[:, p.f]),
            Flow("ctx", 5, 5, own_pair, lambda ref, p: ref.at[:, p.c]),
            Flow("ctx", 6, 6, own_pair, lambda ref, p: ref.at[:, p.c]),
            Flow("ctx", 7, 7, own_pair, lambda ref, p: ref.at[:, p.c]),
            Flow("cube", 8, 8, at_q, at_q),
        ],
        [tokens[0], place_pack, w_pack, w_out, small, w_gate, w_up, w_down, cot_rows],
        [
            shape_of((C, R, D)),
            shape_of((C, 8, R), jnp.int32),
            shape_of((N, rs, z.width)),
            shape_of((N, rs, 128)),
            shape_of((C, F, rs, D)),
            shape_of((OWN, C, dc, ff)),
            shape_of((OWN, C, dc, ff)),
            shape_of((OWN, C, ff, dc)),
            shape_of((Q, OWN * CAP, D)),
        ],
    )
    w_c = w_c.reshape(D, z.width)
    small_all = small_all.reshape(D, 128)
    router = small_all[:, :EXPERTS]
    gain_one = f32(small_all[:, EXPERTS])
    gain_two = f32(small_all[:, EXPERTS + 1])
    place = pos_all[:, 0, :].reshape(L)

    x_all = f32(tok_all.reshape(L, D))
    n1_all, r1_all = norm_parts(x_all)
    h1_all = bf(n1_all * gain_one)
    qkv = jnp.dot(h1_all, w_c, preferred_element_type=jnp.float32)
    frequency = rope_base ** (jnp.arange(HEAD // 2, dtype=jnp.float32) * (-2.0 / HEAD))
    angles = place.astype(jnp.float32)[:, None] * frequency[None, :]
    cosine, sine = jnp.cos(angles), jnp.sin(angles)
    queries = bf(turn(qkv[:, : z.q_width].reshape(L, z.q_heads, HEAD), cosine[:, None], sine[:, None]))
    keys = bf(turn(qkv[:, z.q_width : z.q_width + HEAD], cosine, sine))
    values = bf(qkv[:, z.q_width + HEAD :])
    allowed = (place[None, :] <= place[:, None])[None]
    scores = jnp.where(allowed, dot32("thd,kd->htk", queries, keys) * score_scale, masked_score)
    lse = jax.nn.logsumexp(scores, axis=-1)
    probs = jnp.where(allowed, jnp.exp(scores - lse[..., None]), 0.0)
    attended_f = dot32("htk,kd->thd", probs, f32(values), precision=lax.Precision.HIGHEST)
    attended = bf(dot32("htk,kd->thd", bf(probs), values)).reshape(L, z.q_width)

    (att_in,) = exchange(
        z, "attended_exchange", 1, [Flow("ctx", 0, 0, at_c, at_c)],
        [attended.reshape(C, R, z.q_width)], [shape_of((C, R, z.q_width))])
    attended_mine = att_in.transpose(1, 0, 2).reshape(R, D)
    w_out_all = wo.reshape(D, D)
    x = f32(tokens[0])
    middle = x + residual_scale * jnp.dot(attended_mine, w_out_all, preferred_element_type=jnp.float32)
    n2, r2 = norm_parts(middle)
    h2 = bf(n2 * gain_two)
    logits = jnp.where(named, jnp.dot(h2, router, preferred_element_type=jnp.float32), masked_score)
    top = jnp.max(logits, axis=-1, keepdims=True)
    raised = jnp.where(named, jnp.exp(logits - top), 0.0)
    gates = raised / jnp.sum(raised, axis=-1, keepdims=True)

    rows = bf(dot32("st,td->sd", pick, h2)).reshape(Q, OWN * CAP, D)
    gate_slots = jnp.sum(f32(pick).reshape(EXPERTS, CAP, R) * gates.T[:, None, :], axis=-1)
    gate_slots = gate_slots.reshape(Q, OWN * CAP)
    pad_slots = lambda a: jnp.broadcast_to(jnp.pad(a, ((0, 0), (0, 128 - OWN * CAP)))[:, None, :], (Q, 8, 128))
    rows_in, gates_in = exchange(
        z, "rows_exchange", 2,
        [Flow("cube", 0, 0, at_q, at_q), Flow("cube", 1, 1, at_q, at_q)],
        [rows, pad_slots(gate_slots)], [shape_of((Q, OWN * CAP, D)), shape_of((Q, 8, 128), jnp.float32)])

    by_expert = lambda a: a.reshape(Q, OWN, CAP, -1).transpose(1, 0, 2, 3).reshape(OWN, Q * CAP, -1)
    by_source = lambda a: a.reshape(OWN, Q, CAP, -1).transpose(1, 0, 2, 3).reshape(Q, OWN * CAP, -1)
    xin = by_expert(rows_in)
    cin = f32(by_expert(cot_in))
    gin = by_expert(gates_in[:, 0, : OWN * CAP])
    wg = wg.reshape(OWN, D, ff)
    wu = wu.reshape(OWN, D, ff)
    wd = wd.transpose(0, 2, 1, 3).reshape(OWN, ff, D)
    gate = dot32("esd,edf->esf", xin, wg)
    up = dot32("esd,edf->esf", xin, wu)
    sig = jax.nn.sigmoid(gate)
    act = gate * sig
    hidden = bf(act * up)
    result = bf(dot32("esf,efd->esd", hidden, wd))
    d_gate_slots = residual_scale * jnp.sum(cin * f32(result), axis=-1, keepdims=True)
    d_result = bf(residual_scale * gin * cin)
    d_hidden = dot32("esd,efd->esf", d_result, wd)
    g_down = bf(dot32("esf,esd->efd", hidden, d_result))
    d_gate = bf(d_hidden * up * sig * (1.0 + gate * (1.0 - sig)))
    d_up = bf(d_hidden * act)
    g_gate = bf(dot32("esd,esf->edf", xin, d_gate))
    g_up = bf(dot32("esd,esf->edf", xin, d_up))
    d_rows = bf(dot32("esf,edf->esd", d_gate, wg) + dot32("esf,edf->esd", d_up, wu))

    out_in, d_in, dg_in = exchange(
        z, "return_exchange", 3,
        [Flow("cube", 0, 0, at_q, at_q), Flow("cube", 1, 1, at_q, at_q), Flow("cube", 2, 2, at_q, at_q)],
        [by_source(d_rows), by_source(result), pad_slots(by_source(d_gate_slots)[:, :, 0])],
        [shape_of((Q, OWN * CAP, D)), shape_of((Q, OWN * CAP, D)), shape_of((Q, 8, 128), jnp.float32)])
    d_in, out_in = out_in, d_in
    d_gates = jnp.sum(
        f32(pick).reshape(EXPERTS, CAP, R) * dg_in[:, 0, : OWN * CAP].reshape(EXPERTS, CAP, 1), axis=1).T
    weights = f32(pick).reshape(EXPERTS, CAP, R) * gates.T[:, None, :]
    mixture = dot32("st,sd->td", weights.reshape(EXPERTS * CAP, R), f32(out_in.reshape(EXPERTS * CAP, D)),
                    precision=lax.Precision.HIGHEST)
    output = bf(middle + residual_scale * mixture)
    d_h2 = dot32("st,sd->td", pick, d_in.reshape(EXPERTS * CAP, D))
    d_logits = gates * (d_gates - jnp.sum(gates * d_gates, axis=-1, keepdims=True))
    g_router = jnp.dot(f32(h2).T, d_logits, precision=lax.Precision.HIGHEST)
    d_h2 = d_h2 + jnp.dot(d_logits, f32(router).T, precision=lax.Precision.HIGHEST)
    g_gain_two = jnp.sum(d_h2 * n2, axis=0)
    d_middle = f32(cotangent[0]) + norm_back(d_h2, n2, r2, gain_two)
    d_attn = bf(residual_scale * d_middle)

    (d_attn_all,) = exchange(
        z, "upstream_exchange", 4, [Flow("ctx", 0, 0, whole, at_c)], [d_attn], [shape_of((C, R, D))])
    d_attn_all = d_attn_all.reshape(L, D)
    w_out_c = lax.dynamic_index_in_dim(wo, my_c, 0, keepdims=False).reshape(z.q_width, D)
    g_out = bf(dot32("ti,td->id", attended, d_attn_all))
    d_mix = bf(dot32("td,id->ti", d_attn_all, w_out_c)).reshape(L, z.q_heads, HEAD)
    delta = jnp.sum(f32(d_mix) * attended_f, axis=-1)
    d_probs = dot32("thd,kd->htk", d_mix, values)
    d_scores = bf(probs * (d_probs - delta.T[..., None]))
    d_q = dot32("htk,kd->thd", d_scores, keys) * score_scale
    d_k = dot32("htk,thd->kd", d_scores, queries) * score_scale
    d_v = dot32("htk,thd->kd", bf(probs), d_mix)
    d_qkv = jnp.concatenate(
        [bf(turn(d_q, cosine[:, None], -sine[:, None])).reshape(L, z.q_width), bf(turn(d_k, cosine, -sine)), bf(d_v)], axis=1)
    g_c = bf(dot32("td,tf->df", h1_all, d_qkv))
    d_h1_part = dot32("tf,df->td", d_qkv, w_c)
    g_gain_one = jnp.sum(d_h1_part * n1_all, axis=0)
    g_small = jnp.concatenate(
        [g_router, g_gain_one[:, None], g_gain_two[:, None], jnp.zeros((D, 128 - EXPERTS - 2), jnp.float32)], axis=1)

    to_set = lambda ref, p: ref.at[p.s, pl.ds(p.m * OWN, OWN)]
    from_c = lambda ref, p: ref.at[:, p.c]
    dh_in, gc_in, go_in, gs_in, gg_in, gu_in, gd_in = exchange(
        z, "last_exchange", 5,
        [
            Flow("ctx", 0, 0, at_c, at_c),
            Flow("world", 1, 1, at_w, at_w),
            Flow("fsdp", 2, 2, at_f, at_f),
            Flow("world", 3, 3, at_w, at_w),
            Flow("ctx", 4, 4, from_c, to_set),
            Flow("ctx", 5, 5, from_c, to_set),
            Flow("ctx", 6, 6, from_c, to_set),
        ],
        [
            bf(d_h1_part).reshape(C, R, D),
            g_c.reshape(N, rs, z.width),
            g_out.reshape(F, rs, D),
            g_small.reshape(N, rs, 128),
            g_gate.reshape(OWN, C, dc, ff),
            g_up.reshape(OWN, C, dc, ff),
            g_down.reshape(OWN, ff, C, dc).transpose(0, 2, 1, 3),
        ],
        [
            shape_of((C, R, D)),
            shape_of((N, rs, z.width)),
            shape_of((F, rs, D)),
            shape_of((N, rs, 128), jnp.float32),
            shape_of((S, z.per_f, dc, ff)),
            shape_of((S, z.per_f, dc, ff)),
            shape_of((S, z.per_f, ff, dc)),
        ],
    )
    d_h1 = jnp.sum(f32(dh_in), axis=0)
    n1, r1 = norm_parts(x)
    grad_tokens = d_middle + norm_back(d_h1, n1, r1, gain_one)
    gc = jnp.sum(f32(gc_in).reshape(C, F, rs, z.width), axis=1)
    join = lambda a: a.reshape(KV_HEADS, z.share, rs, HEAD).sum(axis=1).transpose(1, 0, 2).reshape(rs, KV_HEADS * HEAD)
    gs = jnp.sum(gs_in, axis=0)
    return (
        output[None],
        grad_tokens[None],
        gs[:, EXPERTS],
        gc[:, :, : z.q_width].transpose(1, 0, 2).reshape(rs, D),
        join(gc[:, :, z.q_width : z.q_width + HEAD]),
        join(gc[:, :, z.q_width + HEAD :]),
        jnp.sum(f32(go_in), axis=0),
        gs[:, EXPERTS + 1],
        gs[:, :EXPERTS],
        jnp.sum(f32(gg_in), axis=0),
        jnp.sum(f32(gu_in), axis=0),
        jnp.sum(f32(gd_in), axis=0),
    )


def solution(mesh):
    row = P(("ctx", "fsdp"), None)
    vec = P(("ctx", "fsdp"))
    seq = P("fsdp", "ctx", None)
    down = P("fsdp", None, "ctx")
    return jax.shard_map(
        functools.partial(local, Sizes(mesh)),
        mesh=mesh,
        in_specs=(seq, vec, row, row, row, row, vec, row, seq, seq, down, P("fsdp", "ctx"), seq, seq),
        out_specs=(seq, seq, vec, row, row, row, row, vec, row, seq, seq, down),
        check_vma=False,
    )
```

```python
import collections
import functools

import jax
import jax.numpy as jnp
import numpy as np
from jax import lax
from jax.experimental import pallas as pl
from jax.experimental.pallas import tpu as pltpu
from jax.sharding import PartitionSpec as P

D = 1024
HEADS = 16
KV_HEADS = 8
HEAD = 64
EXPERTS = 32
TOP = 8
CAP = 48
LANES = 128
OWN = 2

residual_scale = 0.22
score_scale = 0.015625
rope_base = 10000.0
norm_eps = 1e-06
masked_score = -1e30

MESH = pl.DeviceIdType.MESH
Place = collections.namedtuple("Place", ["c", "f", "m", "s", "q", "w"])
Flow = collections.namedtuple("Flow", ["group", "src", "dst", "src_of", "dst_of"])


class Sizes:
    def __init__(self, mesh):
        self.C = mesh.shape["ctx"]
        self.F = mesh.shape["fsdp"]
        self.N = self.C * self.F
        self.per_f = EXPERTS // self.F
        self.G = self.per_f // OWN
        self.S = self.C // self.G
        self.Q = self.F * self.G
        self.q_heads = HEADS // self.C
        self.q_width = self.q_heads * HEAD
        self.share = self.C // KV_HEADS
        self.rows_w = D // self.N

    def place(self, c, f):
        m = lax.rem(c, self.G)
        return Place(c, f, m, lax.div(c, self.G), f * self.G + m, c * self.F + f)

    def count(self, group):
        return {"ctx": self.C, "fsdp": self.F, "world": self.N, "cube": self.Q}[group]

    def peer(self, group, me, k):
        if group == "ctx":
            return self.place(lax.rem(me.c + k, self.C), me.f)
        if group == "fsdp":
            return self.place(me.c, lax.rem(me.f + k, self.F))
        if group == "world":
            w = lax.rem(me.w + k, self.N)
            return self.place(lax.div(w, self.F), lax.rem(w, self.F))
        q = lax.rem(me.q + k, self.Q)
        return self.place(me.s * self.G + lax.rem(q, self.G), lax.div(q, self.G))


def block(ref, index):
    return ref.at[index] if index is not None else ref


def exchange(sizes, name, collective_id, flows, ins, outs):
    groups = {"ctx", "fsdp", "world", "cube"} & {flow.group for flow in flows}
    widest = "world" if "world" in groups else ("cube" if "cube" in groups else None)
    meet = [widest] if widest else []
    meet += [g for g in ("ctx", "fsdp") if g in groups and widest != "world"]

    def body(*refs):
        in_refs = refs[: len(ins)]
        out_refs = refs[len(ins) : len(ins) + len(outs)]
        scratch = refs[len(ins) + len(outs) :]
        sends = scratch[0 : len(flows)]
        recvs = scratch[len(flows) : 2 * len(flows)]
        own_sem = scratch[2 * len(flows)]
        bounces = list(scratch[2 * len(flows) + 1 :])
        me = sizes.place(lax.axis_index("ctx"), lax.axis_index("fsdp"))

        barrier = pltpu.get_barrier_semaphore()
        total = 0
        for g in meet:
            def greet(k, carry, g=g):
                p = sizes.peer(g, me, k)
                pl.semaphore_signal(barrier, inc=1, device_id=(p.c, p.f), device_id_type=MESH)
                return carry
            lax.fori_loop(1, sizes.count(g), greet, 0)
            total += sizes.count(g) - 1
        pl.semaphore_wait(barrier, total)

        def copy_of(j, k, to):
            flow = flows[j]
            if isinstance(flow.src, tuple):
                source = flow.dst_of(out_refs[flow.src[1]], me)
            else:
                source = flow.src_of(in_refs[flow.src], to)
            return pltpu.make_async_remote_copy(
                src_ref=source,
                dst_ref=flow.dst_of(out_refs[flow.dst], me),
                send_sem=sends[j].at[k],
                recv_sem=recvs[j].at[k],
                device_id=(to.c, to.f),
                device_id_type=MESH,
            )

        def start(j):
            def one(k, carry):
                copy_of(j, k, sizes.peer(flows[j].group, me, k)).start()
                return carry
            lax.fori_loop(1, sizes.count(flows[j].group), one, 0)

        def finish(j):
            def one(k, carry):
                flow = flows[j]
                n = sizes.count(flow.group)
                to = sizes.peer(flow.group, me, k)
                copy_of(j, k, to).wait_send()
                sender = sizes.peer(flow.group, me, n - k)
                landed = flow.dst_of(out_refs[flow.dst], sender)
                pltpu.make_async_remote_copy(
                    src_ref=landed, dst_ref=landed, send_sem=sends[j].at[k], recv_sem=recvs[j].at[k],
                    device_id=(to.c, to.f), device_id_type=MESH,
                ).wait_recv()
                return carry
            lax.fori_loop(1, sizes.count(flows[j].group), one, 0)

        own_flows = [j for j in range(len(flows)) if not isinstance(flows[j].src, tuple)]
        bounce_of = dict(zip(own_flows, bounces))
        for j in own_flows:
            start(j)
        loads = {}
        for j in own_flows:
            loads[j] = pltpu.make_async_copy(
                flows[j].src_of(in_refs[flows[j].src], me), bounce_of[j], own_sem.at[j, 0])
            loads[j].start()
        stores = {}
        for j in own_flows:
            loads[j].wait()
            stores[j] = pltpu.make_async_copy(
                bounce_of[j], flows[j].dst_of(out_refs[flows[j].dst], me), own_sem.at[j, 1])
            stores[j].start()
        done = set()
        for j in range(len(flows)):
            if isinstance(flows[j].src, tuple):
                for i in range(j):
                    if i not in done and flows[i].dst == flows[j].src[1]:
                        finish(i)
                        stores[i].wait()
                        done.add(i)
                start(j)
        for j in range(len(flows)):
            if j not in done:
                finish(j)
                if j in stores:
                    stores[j].wait()

    me0 = Place(0, 0, 0, 0, 0, 0)
    bounce_shapes = []
    for flow in flows:
        if not isinstance(flow.src, tuple):
            shape = jax.eval_shape(lambda a, flow=flow: a, ins[flow.src])
            bounce_shapes.append(pltpu.VMEM(flow_shape(flow, shape.shape), shape.dtype))
    return pl.pallas_call(
        body,
        name=name,
        out_shape=outs,
        in_specs=[pl.BlockSpec(memory_space=pl.ANY)] * len(ins),
        out_specs=[pl.BlockSpec(memory_space=pl.ANY)] * len(outs),
        scratch_shapes=[pltpu.SemaphoreType.DMA((sizes.count(f.group),)) for f in flows] * 2
        + [pltpu.SemaphoreType.DMA((len(flows), 2))]
        + bounce_shapes,
        compiler_params=pltpu.CompilerParams(collective_id=collective_id, has_side_effects=True),
    )(*ins)


def flow_shape(flow, shape):
    return flow.src_of(ShapeProbe(shape), Place(0, 0, 0, 0, 0, 0)).shape


class ShapeProbe:
    def __init__(self, shape):
        self.shape = tuple(shape)

    @property
    def at(self):
        return self

    def __getitem__(self, index):
        index = index if isinstance(index, tuple) else (index,)
        kept = []
        for i, n in enumerate(self.shape):
            if i >= len(index) or (isinstance(index[i], slice) and index[i] == slice(None)):
                kept.append(n)
            elif hasattr(index[i], "size") and not isinstance(index[i], int) and hasattr(index[i], "start"):
                kept.append(index[i].size)
        return ShapeProbe(kept)


whole = lambda ref, p: ref
at_c = lambda ref, p: ref.at[p.c]
at_f = lambda ref, p: ref.at[p.f]
at_q = lambda ref, p: ref.at[p.q]
at_w = lambda ref, p: ref.at[p.w]


def bf(x):
    return x.astype(jnp.bfloat16)


def f32(x):
    return x.astype(jnp.float32)


def dot32(spec, a, b, **kw):
    return jnp.einsum(spec, a, b, preferred_element_type=jnp.float32, **kw)


def norm_parts(x):
    inverse = lax.rsqrt(jnp.mean(x * x, axis=-1, keepdims=True) + norm_eps)
    return x * inverse, inverse


def norm_back(d_output, normalized, inverse, gain):
    g = d_output * gain
    return inverse * (g - normalized * jnp.mean(g * normalized, axis=-1, keepdims=True))


def turn(x, cosine, sine):
    a, b = x[..., : HEAD // 2], x[..., HEAD // 2 :]
    return jnp.concatenate([a * cosine - b * sine, b * cosine + a * sine], axis=-1)


def shape_of(shape, dtype=jnp.bfloat16):
    return jax.ShapeDtypeStruct(shape, dtype)


class Lane:
    def __init__(self, sizes, me, group, src, dst, sends, recvs):
        self.sizes, self.me, self.group, self.src, self.dst = sizes, me, group, src, dst
        self.sends, self.recvs, self.n = sends, recvs, sizes.count(group)

    def copy(self, k, to, source, landing):
        return pltpu.make_async_remote_copy(
            src_ref=source, dst_ref=landing, send_sem=self.sends.at[k], recv_sem=self.recvs.at[k],
            device_id=(to.c, to.f), device_id_type=MESH)

    def to(self, k):
        return self.sizes.peer(self.group, self.me, k)

    def start_one(self, k):
        to = self.to(k)
        self.copy(k, to, self.src(to), self.dst(self.me)).start()

    def wait_recv_one(self, k):
        landed = self.dst(self.sizes.peer(self.group, self.me, self.n - k))
        self.copy(k, self.to(k), landed, landed).wait_recv()

    def wait_send_one(self, k):
        to = self.to(k)
        self.copy(k, to, self.src(to), self.dst(self.me)).wait_send()

    def each(self, step):
        def one(k, carry):
            step(k)
            return carry
        lax.fori_loop(1, self.n, one, 0)

    def start(self):
        self.each(self.start_one)

    def wait_recv(self):
        self.each(self.wait_recv_one)

    def wait_send(self):
        self.each(self.wait_send_one)


def meet(sizes, me, groups):
    barrier = pltpu.get_barrier_semaphore()
    total = 0
    for group in groups:
        def greet(k, carry, group=group):
            p = sizes.peer(group, me, k)
            pl.semaphore_signal(barrier, inc=1, device_id=(p.c, p.f), device_id_type=MESH)
            return carry
        lax.fori_loop(1, sizes.count(group), greet, 0)
        total += sizes.count(group) - 1
    pl.semaphore_wait(barrier, total)


def times(n, step):
    def one(i, carry):
        step(i)
        return carry
    lax.fori_loop(0, n, one, 0)


def nn(a, b):
    return lax.dot_general(a, b, (((1,), (0,)), ((), ())), preferred_element_type=jnp.float32)


def nt(a, b):
    return lax.dot_general(a, b, (((1,), (1,)), ((), ())), preferred_element_type=jnp.float32)


def tn(a, b):
    return lax.dot_general(a, b, (((0,), (0,)), ((), ())), preferred_element_type=jnp.float32)


def lane_of(shape):
    return lax.broadcasted_iota(jnp.int32, shape, 1)


def rope_tables(place_columns, frequency):
    angles = place_columns.astype(jnp.float32) * frequency
    return jnp.cos(angles), jnp.sin(angles)


def rope(x, cosine, sine):
    half = HEAD // 2
    mixed = jnp.where(lax.rem(lane_of(x.shape), HEAD) < half, -pltpu.roll(x, LANES - half, 1), pltpu.roll(x, half, 1))
    return x * cosine + mixed * sine


def sem_pairs(sizes, groups):
    return [pltpu.SemaphoreType.DMA((sizes.count(g),)) for g in groups for _ in range(2)]


FIRST_GROUPS = ["ctx", "ctx", "world", "world", "ctx", "cube", "ctx", "ctx", "ctx", "ctx"]


def first_kernel(z, R, dc, tok, place, routes, cot, freq, w_pack, small, w_out, w_gate, w_up, w_downt,
                 tok_out, wc_out, small_out, wo_out, wt, cot_in, h1, q_all, k2, v2, lse, att_f, middle, h2, gates, pick,
                 tok_all, place_all, wc_v, small_v, wo_v, cot_stage, att_stage, att_in, own_w, place_col, place_row,
                 slot_t, own_sem, col_send, col_recv, *sems):
    me = z.place(lax.axis_index("ctx"), lax.axis_index("fsdp"))
    C, F, Q, rs, qw = z.C, z.F, z.Q, z.rows_w, z.q_width
    L = C * R
    pair = lambda i: (sems[2 * i], sems[2 * i + 1])
    tok_lane = Lane(z, me, "ctx", lambda to: tok, lambda p: tok_all.at[p.c], *pair(0))
    place_lane = Lane(z, me, "ctx", lambda to: place, lambda p: place_all.at[p.c], *pair(1))
    wc_lane = Lane(z, me, "world", lambda to: w_pack.at[to.c], lambda p: rows_at(wc_v, p.w, rs), *pair(2))
    small_lane = Lane(z, me, "world", lambda to: small, lambda p: rows_at(small_v, p.w, rs), *pair(3))
    wo_lane = Lane(z, me, "ctx", lambda to: w_out, lambda p: rows_at(wo_v, p.w, rs), *pair(4))
    cot_lane = Lane(z, me, "cube", lambda to: cot_stage.at[to.q], lambda p: cot_in.at[:, p.q], *pair(5))
    weights = [w_gate, w_up, w_downt]
    weight_lanes = [
        Lane(z, me, "ctx", lambda to, j=j: weights[j].at[to.m * OWN],
             lambda p, j=j: rows_at(wt.at[j], p.c, dc), *pair(6 + j))
        for j in range(3)
    ]
    att_lane = Lane(z, me, "ctx", lambda to: att_stage.at[to.c], lambda p: att_in.at[p.c], *pair(9))
    col_lanes = [
        Lane(z, me, "fsdp", lambda to, c=c: rows_at(wo_v, c * F + me.f, rs), lambda p, c=c: rows_at(wo_v, c * F + p.f, rs),
             col_send.at[c], col_recv.at[c])
        for c in range(C)
    ]

    meet(z, me, ["world"])
    tok_lane.start()
    place_lane.start()
    wc_lane.start()
    small_lane.start()
    wo_lane.start()

    own = [
        pltpu.make_async_copy(w_pack.at[me.c], rows_at(wc_v, me.w, rs), own_sem.at[0]),
        pltpu.make_async_copy(small, rows_at(small_v, me.w, rs), own_sem.at[1]),
        pltpu.make_async_copy(w_out, rows_at(wo_v, me.w, rs), own_sem.at[2]),
    ]
    own_loads = [pltpu.make_async_copy(weights[j].at[me.m * OWN], own_w.at[j], own_sem.at[3 + j]) for j in range(3)]
    for copy in own + own_loads:
        copy.start()
    tok_all[me.c] = tok[...]
    place_all[me.c] = place[...]

    named = jnp.zeros((R, LANES), jnp.float32)
    for j in range(TOP):
        named = jnp.where(routes[:, j : j + 1] == lane_of((R, LANES)), 1.0, named)
    row_id = lax.broadcasted_iota(jnp.int32, (R, R), 0)
    before = jnp.where(row_id > lane_of((R, R)), 1.0, 0.0).astype(jnp.bfloat16)
    slot = nn(before, named.astype(jnp.bfloat16))
    slot_t[...] = jnp.where(named > 0.5, slot, -1.0).T
    slot_id = lax.broadcasted_iota(jnp.int32, (CAP, R), 0).astype(jnp.float32)

    def dispatch(q):
        for i in range(OWN):
            hot = jnp.where(slot_t[pl.ds(q * OWN + i, 1), :] == slot_id, 1.0, 0.0).astype(jnp.bfloat16)
            pick[q, i * CAP : (i + 1) * CAP, :] = hot
            cot_stage[q, i] = nn(hot, cot[...]).astype(jnp.bfloat16)
    times(Q, dispatch)
    weight_lanes[0].start()
    cot_lane.start()
    own_cot = pltpu.make_async_copy(cot_stage.at[me.q], cot_in.at[:, me.q], own_sem.at[6])
    own_cot.start()
    own_stores = []
    for j in range(3):
        own_loads[j].wait()
        own_stores.append(pltpu.make_async_copy(own_w.at[j], rows_at(wt.at[j], me.c, dc), own_sem.at[7 + j]))
        own_stores[j].start()

    for copy in own:
        copy.wait()
    place_lane.wait_recv()
    small_lane.wait_recv()
    wc_lane.wait_recv()
    gain_one = small_v[...].astype(jnp.float32).T[EXPERTS : EXPERTS + 1, :]
    gain_two = small_v[...].astype(jnp.float32).T[EXPERTS + 1 : EXPERTS + 2, :]
    head_of = lax.div(lane_of((R, LANES)), HEAD)

    def project(k):
        c = lax.rem(me.c + C - k, C)
        @pl.when(k > 0)
        def _():
            tok_lane.wait_recv_one(k)
        x = tok_all[c].astype(jnp.float32)
        inverse = lax.rsqrt(jnp.mean(x * x, axis=-1, keepdims=True) + norm_eps)
        h = (x * inverse * gain_one).astype(jnp.bfloat16)
        part = pl.ds(pl.multiple_of(c * R, R), R)
        h1[part, :] = h
        qkv = nn(h, wc_v[...])
        row = place_all[c][0:1, :].astype(jnp.float32)
        place_row[c] = jnp.broadcast_to(row, (8, R))
        column = jnp.broadcast_to(row, (R, R)).T
        place_col[part, :] = column
        q_all[part, :] = rope(qkv[:, :LANES], *rope_tables(column, freq[0:1, :])).astype(jnp.bfloat16)
        kv = rope(qkv[:, LANES:], *rope_tables(column, freq[1:2, :]))
        swapped = pltpu.roll(kv, HEAD, 1)
        k2[part, :] = jnp.where(head_of == 0, kv, swapped).astype(jnp.bfloat16)
        v2[part, :] = jnp.where(head_of == 0, swapped, kv).astype(jnp.bfloat16)
    times(C, project)
    wo_lane.wait_recv()
    for lane in col_lanes:
        lane.start()
    weight_lanes[1].start()

    def attend(c):
        part = pl.ds(pl.multiple_of(c * R, R), R)
        q = q_all[part, :]
        row = jnp.concatenate([place_row[i, 0:1, :] for i in range(C)], axis=1)
        allowed = row <= place_col[part, 0:1]
        total = jnp.zeros((R, LANES), jnp.float32)
        for h in range(z.q_heads):
            mine = head_of == h
            s = nt(jnp.where(mine, q, jnp.zeros_like(q)), k2[...]) * score_scale
            s = jnp.where(allowed, s, masked_score)
            top = jnp.max(s, axis=-1, keepdims=True)
            e = jnp.exp(s - top)
            weight = jnp.sum(e, axis=-1, keepdims=True)
            lse[h, part, :] = jnp.broadcast_to(top + jnp.log(weight), (R, LANES))
            total = jnp.where(mine, nn(e.astype(jnp.bfloat16), v2[...]) / weight, total)
        att_f[part, :] = total
        att_stage[c] = total.astype(jnp.bfloat16)
    times(C, attend)
    att_lane.start()
    weight_lanes[2].start()
    att_in[me.c] = att_stage[me.c]
    for lane in col_lanes:
        lane.wait_recv()
    att_lane.wait_recv()
    x = tok[...].astype(jnp.float32)
    mixed = jnp.zeros((R, D), jnp.float32)
    for c in range(C):
        mixed = mixed + nn(att_in[c][:, :qw], wo_v[c * qw : (c + 1) * qw, :])
    mid = x + residual_scale * mixed
    middle[...] = mid
    inverse = lax.rsqrt(jnp.mean(mid * mid, axis=-1, keepdims=True) + norm_eps)
    hidden = (mid * inverse * gain_two).astype(jnp.bfloat16)
    h2[...] = hidden
    chosen = slot_t[...].T > -0.5
    logits = jnp.where(chosen, nn(hidden, small_v[...]), masked_score)
    raised = jnp.where(chosen, jnp.exp(logits - jnp.max(logits, axis=-1, keepdims=True)), 0.0)
    gates[...] = raised / jnp.sum(raised, axis=-1, keepdims=True)

    outs = [
        pltpu.make_async_copy(source, out, own_sem.at[10 + i])
        for i, (source, out) in enumerate([(tok_all, tok_out), (wc_v, wc_out), (small_v, small_out), (wo_v, wo_out)])
    ]
    for copy in outs:
        copy.start()
    for lane in [tok_lane, place_lane, wc_lane, small_lane, wo_lane, att_lane] + col_lanes:
        lane.wait_send()
    for lane in [cot_lane] + weight_lanes:
        lane.wait_recv()
        lane.wait_send()
    for copy in outs + own_stores + [own_cot]:
        copy.wait()


def rows_at(ref, i, n):
    return ref.at[pl.ds(pl.multiple_of(i * n, n), n), :]


def vmem(shape, dtype=jnp.bfloat16):
    return pltpu.VMEM(shape, dtype)


def call(z, kernel, name, collective_id, ins, outs, scratch, **kw):
    space = lambda fast: pl.BlockSpec(memory_space=pltpu.VMEM if fast else pl.ANY)
    return pl.pallas_call(
        kernel, name=name,
        out_shape=[o for o, _ in outs], in_specs=[space(f) for _, f in ins], out_specs=[space(f) for _, f in outs],
        scratch_shapes=scratch,
        compiler_params=pltpu.CompilerParams(
            collective_id=collective_id, has_side_effects=True, vmem_limit_bytes=60000 * 1024),
    )(*[a for a, _ in ins])


def first_call(z, R, ff, dc, tok, place, routes, cot, w_pack, small, w_out, w_gate, w_up, w_downt):
    C, F, Q, rs = z.C, z.F, z.Q, z.rows_w
    L = C * R
    half = HEAD // 2
    lanes = np.arange(LANES)
    steps = rope_base ** ((lanes % half) * (-2.0 / HEAD))
    freq = jnp.asarray(np.stack([steps, np.where(lanes < HEAD, steps, 0.0)] + [steps] * 6), jnp.float32)
    ins = [(tok, 1), (place, 1), (routes, 1), (cot, 1), (freq, 1), (w_pack, 0), (small, 0), (w_out, 0),
           (w_gate, 0), (w_up, 0), (w_downt, 0)]
    f = jnp.float32
    outs = [
        (shape_of((C, R, D)), 0), (shape_of((D, 2 * LANES)), 0), (shape_of((D, LANES)), 0), (shape_of((D, D)), 0),
        (shape_of((3, D, ff)), 0), (shape_of((OWN, Q, CAP, D)), 0),
        (shape_of((L, D)), 1), (shape_of((L, LANES)), 1), (shape_of((L, LANES)), 1), (shape_of((L, LANES)), 1),
        (shape_of((z.q_heads, L, LANES), f), 1), (shape_of((L, LANES), f), 1), (shape_of((R, D), f), 1),
        (shape_of((R, D)), 1), (shape_of((R, LANES), f), 1), (shape_of((Q, OWN * CAP, R)), 1),
    ]
    scratch = [
        vmem((C, R, D)), vmem((C, 8, R), jnp.int32), vmem((D, 2 * LANES)), vmem((D, LANES)), vmem((D, D)),
        vmem((Q, OWN, CAP, D)), vmem((C, R, LANES)), vmem((C, R, LANES)), vmem((3, dc, ff)), vmem((L, R), f),
        vmem((C, 8, R), f), vmem((LANES, R), f), pltpu.SemaphoreType.DMA((16,)),
        pltpu.SemaphoreType.DMA((C, F)), pltpu.SemaphoreType.DMA((C, F)),
    ] + sem_pairs(z, FIRST_GROUPS)
    return call(z, functools.partial(first_kernel, z, R, dc), "first", 0, ins, outs, scratch)


def local(z, tokens, norm_first, w_query, w_key, w_value, w_out, norm_second, w_router,
          w_gate, w_up, w_down, positions, routes, cotangent):
    C, F, N, Q, S, G = z.C, z.F, z.N, z.Q, z.S, z.G
    R = tokens.shape[1]
    L = C * R
    rs = z.rows_w
    ff = w_gate.shape[2]
    dc = D // C
    my_c = lax.axis_index("ctx")

    expert_ids = jnp.arange(EXPERTS, dtype=jnp.int32)
    named = jnp.any(routes[0][:, :, None] == expert_ids[None, None, :], axis=1)
    before = (jnp.arange(R)[:, None] > jnp.arange(R)[None, :]).astype(jnp.bfloat16)
    slot = dot32("tu,ue->te", before, named.astype(jnp.bfloat16)).astype(jnp.int32)
    slot = jnp.where(named, slot, -1)
    pick = (slot.T[:, None, :] == jnp.arange(CAP, dtype=jnp.int32)[None, :, None]).astype(jnp.bfloat16)
    pick = pick.reshape(EXPERTS * CAP, R)

    heads_q = jnp.pad(w_query.reshape(rs, C, z.q_width), ((0, 0), (0, 0), (0, LANES - z.q_width)))
    heads_k = jnp.repeat(w_key.reshape(rs, KV_HEADS, HEAD), z.share, axis=1)
    heads_v = jnp.repeat(w_value.reshape(rs, KV_HEADS, HEAD), z.share, axis=1)
    w_pack = jnp.concatenate([heads_q, heads_k, heads_v], axis=2).transpose(1, 0, 2)
    small = jnp.concatenate(
        [w_router, norm_first[:, None], norm_second[:, None], jnp.zeros((rs, 128 - EXPERTS - 2), jnp.bfloat16)], axis=1)
    place_pack = jnp.broadcast_to(positions[0][None, :], (8, R))
    w_downt = w_down.transpose(0, 2, 1)
    (tok_all, w_c, small_all, wo, wt, cot_in, h1_all, q_all, k2, v2, lse, att_f, middle, h2, gates, pick) = first_call(
        z, R, ff, dc, tokens[0], place_pack, routes[0], cotangent[0], w_pack, small, w_out, w_gate, w_up, w_downt)
    own_pair = lambda ref, p: ref.at[p.m * OWN + 1]
    (wt2,) = exchange(
        z, "second_weights", 1,
        [Flow("ctx", j, 0, own_pair, lambda ref, p, j=j: ref.at[j, pl.ds(pl.multiple_of(p.c * dc, dc), dc), :])
         for j in range(3)],
        [w_gate, w_up, w_downt], [shape_of((3, D, ff))])
    router = small_all[:, :EXPERTS]
    gain_one = f32(small_all[:, EXPERTS])
    gain_two = f32(small_all[:, EXPERTS + 1])
    n1_all, r1_all = norm_parts(f32(tok_all.reshape(L, D)))
    x = f32(tokens[0])
    n2, r2 = norm_parts(middle)
    gates = gates[:, :EXPERTS]
    pick = pick.reshape(EXPERTS * CAP, R)
    rows = bf(dot32("st,td->sd", pick, h2)).reshape(Q, OWN * CAP, D)
    gate_slots = jnp.sum(f32(pick).reshape(EXPERTS, CAP, R) * gates.T[:, None, :], axis=-1)
    gate_slots = gate_slots.reshape(Q, OWN * CAP)
    pad_slots = lambda a: jnp.broadcast_to(jnp.pad(a, ((0, 0), (0, 128 - OWN * CAP)))[:, None, :], (Q, 8, 128))
    rows_in, gates_in = exchange(
        z, "rows_exchange", 2,
        [Flow("cube", 0, 0, at_q, at_q), Flow("cube", 1, 1, at_q, at_q)],
        [rows, pad_slots(gate_slots)], [shape_of((Q, OWN * CAP, D)), shape_of((Q, 8, 128), jnp.float32)])

    by_expert = lambda a: a.reshape(Q, OWN, CAP, -1).transpose(1, 0, 2, 3).reshape(OWN, Q * CAP, -1)
    by_source = lambda a: a.reshape(OWN, Q, CAP, -1).transpose(1, 0, 2, 3).reshape(Q, OWN * CAP, -1)
    xin = by_expert(rows_in)
    cin = f32(cot_in.reshape(OWN, Q * CAP, D))
    gin = by_expert(gates_in[:, 0, : OWN * CAP])
    wg, wu, wd = [jnp.stack([wt[j], wt2[j]]) for j in range(3)]
    wd = wd.transpose(0, 2, 1)
    gate = dot32("esd,edf->esf", xin, wg)
    up = dot32("esd,edf->esf", xin, wu)
    sig = jax.nn.sigmoid(gate)
    act = gate * sig
    hidden = bf(act * up)
    result = bf(dot32("esf,efd->esd", hidden, wd))
    d_gate_slots = residual_scale * jnp.sum(cin * f32(result), axis=-1, keepdims=True)
    d_result = bf(residual_scale * gin * cin)
    d_hidden = dot32("esd,efd->esf", d_result, wd)
    g_down = bf(dot32("esf,esd->efd", hidden, d_result))
    d_gate = bf(d_hidden * up * sig * (1.0 + gate * (1.0 - sig)))
    d_up = bf(d_hidden * act)
    g_gate = bf(dot32("esd,esf->edf", xin, d_gate))
    g_up = bf(dot32("esd,esf->edf", xin, d_up))
    d_rows = bf(dot32("esf,edf->esd", d_gate, wg) + dot32("esf,edf->esd", d_up, wu))

    out_in, d_in, dg_in = exchange(
        z, "return_exchange", 3,
        [Flow("cube", 0, 0, at_q, at_q), Flow("cube", 1, 1, at_q, at_q), Flow("cube", 2, 2, at_q, at_q)],
        [by_source(d_rows), by_source(result), pad_slots(by_source(d_gate_slots)[:, :, 0])],
        [shape_of((Q, OWN * CAP, D)), shape_of((Q, OWN * CAP, D)), shape_of((Q, 8, 128), jnp.float32)])
    d_in, out_in = out_in, d_in
    d_gates = jnp.sum(
        f32(pick).reshape(EXPERTS, CAP, R) * dg_in[:, 0, : OWN * CAP].reshape(EXPERTS, CAP, 1), axis=1).T
    weights = f32(pick).reshape(EXPERTS, CAP, R) * gates.T[:, None, :]
    mixture = dot32("st,sd->td", weights.reshape(EXPERTS * CAP, R), f32(out_in.reshape(EXPERTS * CAP, D)),
                    precision=lax.Precision.HIGHEST)
    output = bf(middle + residual_scale * mixture)
    d_h2 = dot32("st,sd->td", pick, d_in.reshape(EXPERTS * CAP, D))
    d_logits = gates * (d_gates - jnp.sum(gates * d_gates, axis=-1, keepdims=True))
    g_router = jnp.dot(f32(h2).T, d_logits, precision=lax.Precision.HIGHEST)
    d_h2 = d_h2 + jnp.dot(d_logits, f32(router).T, precision=lax.Precision.HIGHEST)
    g_gain_two = jnp.sum(d_h2 * n2, axis=0)
    d_middle = f32(cotangent[0]) + norm_back(d_h2, n2, r2, gain_two)
    d_attn = bf(residual_scale * d_middle)

    (d_attn_all,) = exchange(
        z, "upstream_exchange", 4, [Flow("ctx", 0, 0, whole, at_c)], [d_attn], [shape_of((C, R, D))])
    d_attn_all = d_attn_all.reshape(L, D)
    w_out_c = lax.dynamic_slice_in_dim(wo, my_c * z.q_width, z.q_width, 0)
    place = lax.all_gather(positions[0], "ctx", axis=0, tiled=True)
    attended = bf(att_f[:, : z.q_width])
    attended_f = att_f[:, : z.q_width].reshape(L, z.q_heads, HEAD)
    queries = q_all[:, : z.q_width].reshape(L, z.q_heads, HEAD)
    keys, values = k2[:, :HEAD], v2[:, :HEAD]
    frequency = rope_base ** (jnp.arange(HEAD // 2, dtype=jnp.float32) * (-2.0 / HEAD))
    angles = place.astype(jnp.float32)[:, None] * frequency[None, :]
    cosine, sine = jnp.cos(angles), jnp.sin(angles)
    allowed = (place[None, :] <= place[:, None])[None]
    scores = jnp.where(allowed, dot32("thd,kd->htk", queries, keys) * score_scale, masked_score)
    probs = jnp.where(allowed, jnp.exp(scores - lse[..., :1]), 0.0)
    g_out = bf(dot32("ti,td->id", attended, d_attn_all))
    d_mix = bf(dot32("td,id->ti", d_attn_all, w_out_c)).reshape(L, z.q_heads, HEAD)
    delta = jnp.sum(f32(d_mix) * attended_f, axis=-1)
    d_probs = dot32("thd,kd->htk", d_mix, values)
    d_scores = bf(probs * (d_probs - delta.T[..., None]))
    d_q = dot32("htk,kd->thd", d_scores, keys) * score_scale
    d_k = dot32("htk,thd->kd", d_scores, queries) * score_scale
    d_v = dot32("htk,thd->kd", bf(probs), d_mix)
    d_qkv = jnp.concatenate(
        [bf(turn(d_q, cosine[:, None], -sine[:, None])).reshape(L, z.q_width), jnp.zeros((L, LANES - z.q_width), jnp.bfloat16),
         bf(turn(d_k, cosine, -sine)), bf(d_v)], axis=1)
    g_c = bf(dot32("td,tf->df", h1_all, d_qkv))
    d_h1_part = dot32("tf,df->td", d_qkv, w_c)
    g_gain_one = jnp.sum(d_h1_part * n1_all, axis=0)
    g_small = jnp.concatenate(
        [g_router, g_gain_one[:, None], g_gain_two[:, None], jnp.zeros((D, 128 - EXPERTS - 2), jnp.float32)], axis=1)

    to_set = lambda ref, p: ref.at[p.s, pl.ds(p.m * OWN, OWN)]
    from_c = lambda ref, p: ref.at[:, p.c]
    dh_in, gc_in, go_in, gs_in, gg_in, gu_in, gd_in = exchange(
        z, "last_exchange", 5,
        [
            Flow("ctx", 0, 0, at_c, at_c),
            Flow("world", 1, 1, at_w, at_w),
            Flow("fsdp", 2, 2, at_f, at_f),
            Flow("world", 3, 3, at_w, at_w),
            Flow("ctx", 4, 4, from_c, to_set),
            Flow("ctx", 5, 5, from_c, to_set),
            Flow("ctx", 6, 6, from_c, to_set),
        ],
        [
            bf(d_h1_part).reshape(C, R, D),
            g_c.reshape(N, rs, 2 * LANES),
            g_out.reshape(F, rs, D),
            g_small.reshape(N, rs, 128),
            g_gate.reshape(OWN, C, dc, ff),
            g_up.reshape(OWN, C, dc, ff),
            g_down.reshape(OWN, ff, C, dc).transpose(0, 2, 1, 3),
        ],
        [
            shape_of((C, R, D)),
            shape_of((N, rs, 2 * LANES)),
            shape_of((F, rs, D)),
            shape_of((N, rs, 128), jnp.float32),
            shape_of((S, z.per_f, dc, ff)),
            shape_of((S, z.per_f, dc, ff)),
            shape_of((S, z.per_f, ff, dc)),
        ],
    )
    d_h1 = jnp.sum(f32(dh_in), axis=0)
    n1, r1 = norm_parts(x)
    grad_tokens = d_middle + norm_back(d_h1, n1, r1, gain_one)
    gc = jnp.sum(f32(gc_in).reshape(C, F, rs, 2 * LANES), axis=1)
    join = lambda a: a.reshape(KV_HEADS, z.share, rs, HEAD).sum(axis=1).transpose(1, 0, 2).reshape(rs, KV_HEADS * HEAD)
    gs = jnp.sum(gs_in, axis=0)
    return (
        output[None],
        grad_tokens[None],
        gs[:, EXPERTS],
        gc[:, :, : z.q_width].transpose(1, 0, 2).reshape(rs, D),
        join(gc[:, :, LANES : LANES + HEAD]),
        join(gc[:, :, LANES + HEAD :]),
        jnp.sum(f32(go_in), axis=0),
        gs[:, EXPERTS + 1],
        gs[:, :EXPERTS],
        jnp.sum(f32(gg_in), axis=0),
        jnp.sum(f32(gu_in), axis=0),
        jnp.sum(f32(gd_in), axis=0),
    )


def solution(mesh):
    row = P(("ctx", "fsdp"), None)
    vec = P(("ctx", "fsdp"))
    seq = P("fsdp", "ctx", None)
    down = P("fsdp", None, "ctx")
    return jax.shard_map(
        functools.partial(local, Sizes(mesh)),
        mesh=mesh,
        in_specs=(seq, vec, row, row, row, row, vec, row, seq, seq, down, P("fsdp", "ctx"), seq, seq),
        out_specs=(seq, seq, vec, row, row, row, row, vec, row, seq, seq, down),
        check_vma=False,
    )
```

```python
import collections
import functools

import jax
import jax.numpy as jnp
import numpy as np
from jax import lax
from jax.experimental import pallas as pl
from jax.experimental.pallas import tpu as pltpu
from jax.sharding import PartitionSpec as P

D = 1024
HEADS = 16
KV_HEADS = 8
HEAD = 64
EXPERTS = 32
TOP = 8
CAP = 48
LANES = 128
OWN = 2

residual_scale = 0.22
score_scale = 0.015625
rope_base = 10000.0
norm_eps = 1e-06
masked_score = -1e30

MESH = pl.DeviceIdType.MESH
Place = collections.namedtuple("Place", ["c", "f", "m", "s", "q", "w"])


class Sizes:
    def __init__(self, mesh):
        self.C = mesh.shape["ctx"]
        self.F = mesh.shape["fsdp"]
        self.N = self.C * self.F
        self.per_f = EXPERTS // self.F
        self.G = self.per_f // OWN
        self.S = self.C // self.G
        self.Q = self.F * self.G
        self.q_heads = HEADS // self.C
        self.q_width = self.q_heads * HEAD
        self.share = self.C // KV_HEADS
        self.rows_w = D // self.N

    def place(self, c, f):
        m = lax.rem(c, self.G)
        return Place(c, f, m, lax.div(c, self.G), f * self.G + m, c * self.F + f)

    def count(self, group):
        return {"ctx": self.C, "fsdp": self.F, "world": self.N, "cube": self.Q}[group]

    def peer(self, group, me, k):
        if group == "ctx":
            return self.place(lax.rem(me.c + k, self.C), me.f)
        if group == "fsdp":
            return self.place(me.c, lax.rem(me.f + k, self.F))
        if group == "world":
            w = lax.rem(me.w + k, self.N)
            return self.place(lax.div(w, self.F), lax.rem(w, self.F))
        q = lax.rem(me.q + k, self.Q)
        return self.place(me.s * self.G + lax.rem(q, self.G), lax.div(q, self.G))


def bf(x):
    return x.astype(jnp.bfloat16)


def f32(x):
    return x.astype(jnp.float32)


def shape_of(shape, dtype=jnp.bfloat16):
    return jax.ShapeDtypeStruct(shape, dtype)


class Lane:
    def __init__(self, sizes, me, group, src, dst, sends, recvs):
        self.sizes, self.me, self.group, self.src, self.dst = sizes, me, group, src, dst
        self.sends, self.recvs, self.n = sends, recvs, sizes.count(group)

    def copy(self, k, to, source, landing):
        return pltpu.make_async_remote_copy(
            src_ref=source, dst_ref=landing, send_sem=self.sends.at[k], recv_sem=self.recvs.at[k],
            device_id=(to.c, to.f), device_id_type=MESH)

    def to(self, k):
        return self.sizes.peer(self.group, self.me, k)

    def start_one(self, k):
        to = self.to(k)
        self.copy(k, to, self.src(to), self.dst(self.me)).start()

    def wait_recv_one(self, k):
        landed = self.dst(self.sizes.peer(self.group, self.me, self.n - k))
        self.copy(k, self.to(k), landed, landed).wait_recv()

    def wait_send_one(self, k):
        to = self.to(k)
        self.copy(k, to, self.src(to), self.dst(self.me)).wait_send()

    def each(self, step):
        def one(k, carry):
            step(k)
            return carry
        lax.fori_loop(1, self.n, one, 0)

    def start(self):
        self.each(self.start_one)

    def wait_recv(self):
        self.each(self.wait_recv_one)

    def wait_send(self):
        self.each(self.wait_send_one)


def meet(sizes, me, groups):
    barrier = pltpu.get_barrier_semaphore()
    total = 0
    for group in groups:
        def greet(k, carry, group=group):
            p = sizes.peer(group, me, k)
            pl.semaphore_signal(barrier, inc=1, device_id=(p.c, p.f), device_id_type=MESH)
            return carry
        lax.fori_loop(1, sizes.count(group), greet, 0)
        total += sizes.count(group) - 1
    pl.semaphore_wait(barrier, total)


def times(n, step):
    def one(i, carry):
        step(i)
        return carry
    lax.fori_loop(0, n, one, 0)


def nn(a, b):
    return lax.dot_general(a, b, (((1,), (0,)), ((), ())), preferred_element_type=jnp.float32)


def nt(a, b):
    return lax.dot_general(a, b, (((1,), (1,)), ((), ())), preferred_element_type=jnp.float32)


def tn(a, b):
    return lax.dot_general(a, b, (((0,), (0,)), ((), ())), preferred_element_type=jnp.float32)


def lane_of(shape):
    return lax.broadcasted_iota(jnp.int32, shape, 1)


def rope_tables(place_columns, frequency):
    angles = place_columns.astype(jnp.float32) * frequency
    return jnp.cos(angles), jnp.sin(angles)


def rope(x, cosine, sine):
    half = HEAD // 2
    mixed = jnp.where(lax.rem(lane_of(x.shape), HEAD) < half, -pltpu.roll(x, LANES - half, 1), pltpu.roll(x, half, 1))
    return x * cosine + mixed * sine


def sem_pairs(sizes, groups):
    return [pltpu.SemaphoreType.DMA((sizes.count(g),)) for g in groups for _ in range(2)]


FIRST_GROUPS = ["ctx", "ctx", "world", "world", "ctx", "cube", "ctx", "ctx", "ctx", "ctx"]


def first_kernel(z, R, dc, tok, place, routes, cot, freq, w_pack, small, w_out, w_gate, w_up, w_downt,
                 tok_out, wc_out, small_out, wo_out, place_out, wt, cot_in, h1, q_all, k2, v2, lse, att_f, middle, h2, gates, pick,
                 tok_all, place_all, wc_v, small_v, wo_v, cot_stage, att_stage, att_in, own_w, place_col, place_row,
                 slot_t, own_sem, col_send, col_recv, *sems):
    me = z.place(lax.axis_index("ctx"), lax.axis_index("fsdp"))
    C, F, Q, rs, qw = z.C, z.F, z.Q, z.rows_w, z.q_width
    L = C * R
    pair = lambda i: (sems[2 * i], sems[2 * i + 1])
    tok_lane = Lane(z, me, "ctx", lambda to: tok, lambda p: tok_all.at[p.c], *pair(0))
    place_lane = Lane(z, me, "ctx", lambda to: place, lambda p: place_all.at[p.c], *pair(1))
    wc_lane = Lane(z, me, "world", lambda to: w_pack.at[to.c], lambda p: rows_at(wc_v, p.w, rs), *pair(2))
    small_lane = Lane(z, me, "world", lambda to: small, lambda p: rows_at(small_v, p.w, rs), *pair(3))
    wo_lane = Lane(z, me, "ctx", lambda to: w_out, lambda p: rows_at(wo_v, p.w, rs), *pair(4))
    cot_lane = Lane(z, me, "cube", lambda to: cot_stage.at[to.q], lambda p: cot_in.at[:, p.q], *pair(5))
    weights = [w_gate, w_up, w_downt]
    weight_lanes = [
        Lane(z, me, "ctx", lambda to, j=j: weights[j].at[to.m * OWN],
             lambda p, j=j: rows_at(wt.at[j], p.c, dc), *pair(6 + j))
        for j in range(3)
    ]
    att_lane = Lane(z, me, "ctx", lambda to: att_stage.at[to.c], lambda p: att_in.at[p.c], *pair(9))
    col_lanes = [
        Lane(z, me, "fsdp", lambda to, c=c: rows_at(wo_v, c * F + me.f, rs), lambda p, c=c: rows_at(wo_v, c * F + p.f, rs),
             col_send.at[c], col_recv.at[c])
        for c in range(C)
    ]

    meet(z, me, ["world"])
    tok_lane.start()
    place_lane.start()
    wc_lane.start()
    small_lane.start()
    wo_lane.start()

    own = [
        pltpu.make_async_copy(w_pack.at[me.c], rows_at(wc_v, me.w, rs), own_sem.at[0]),
        pltpu.make_async_copy(small, rows_at(small_v, me.w, rs), own_sem.at[1]),
        pltpu.make_async_copy(w_out, rows_at(wo_v, me.w, rs), own_sem.at[2]),
    ]
    own_loads = [pltpu.make_async_copy(weights[j].at[me.m * OWN], own_w.at[j], own_sem.at[3 + j]) for j in range(3)]
    for copy in own + own_loads:
        copy.start()
    tok_all[me.c] = tok[...]
    place_all[me.c] = place[...]

    named = jnp.zeros((R, LANES), jnp.float32)
    for j in range(TOP):
        named = jnp.where(routes[:, j : j + 1] == lane_of((R, LANES)), 1.0, named)
    row_id = lax.broadcasted_iota(jnp.int32, (R, R), 0)
    before = jnp.where(row_id > lane_of((R, R)), 1.0, 0.0).astype(jnp.bfloat16)
    slot = nn(before, named.astype(jnp.bfloat16))
    slot_t[...] = jnp.where(named > 0.5, slot, -1.0).T
    slot_id = lax.broadcasted_iota(jnp.int32, (CAP, R), 0).astype(jnp.float32)

    def dispatch(q):
        for i in range(OWN):
            hot = jnp.where(slot_t[pl.ds(q * OWN + i, 1), :] == slot_id, 1.0, 0.0).astype(jnp.bfloat16)
            pick[q, i * CAP : (i + 1) * CAP, :] = hot
            cot_stage[q, i] = nn(hot, cot[...]).astype(jnp.bfloat16)
    times(Q, dispatch)
    weight_lanes[0].start()
    cot_lane.start()
    own_cot = pltpu.make_async_copy(cot_stage.at[me.q], cot_in.at[:, me.q], own_sem.at[6])
    own_cot.start()
    own_stores = []
    for j in range(3):
        own_loads[j].wait()
        own_stores.append(pltpu.make_async_copy(own_w.at[j], rows_at(wt.at[j], me.c, dc), own_sem.at[7 + j]))
        own_stores[j].start()

    for copy in own:
        copy.wait()
    place_lane.wait_recv()
    small_lane.wait_recv()
    wc_lane.wait_recv()
    gain_one = small_v[...].astype(jnp.float32).T[EXPERTS : EXPERTS + 1, :]
    gain_two = small_v[...].astype(jnp.float32).T[EXPERTS + 1 : EXPERTS + 2, :]
    head_of = lax.div(lane_of((R, LANES)), HEAD)

    def project(k):
        c = lax.rem(me.c + C - k, C)
        @pl.when(k > 0)
        def _():
            tok_lane.wait_recv_one(k)
        x = tok_all[c].astype(jnp.float32)
        inverse = lax.rsqrt(jnp.mean(x * x, axis=-1, keepdims=True) + norm_eps)
        h = (x * inverse * gain_one).astype(jnp.bfloat16)
        part = pl.ds(pl.multiple_of(c * R, R), R)
        h1[part, :] = h
        qkv = nn(h, wc_v[...])
        row = place_all[c][0:1, :].astype(jnp.float32)
        place_row[c] = jnp.broadcast_to(row, (8, R))
        column = jnp.broadcast_to(row, (R, R)).T
        place_col[part, :] = column
        q_all[part, :] = rope(qkv[:, :LANES], *rope_tables(column, freq[0:1, :])).astype(jnp.bfloat16)
        kv = rope(qkv[:, LANES:], *rope_tables(column, freq[1:2, :]))
        swapped = pltpu.roll(kv, HEAD, 1)
        k2[part, :] = jnp.where(head_of == 0, kv, swapped).astype(jnp.bfloat16)
        v2[part, :] = jnp.where(head_of == 0, swapped, kv).astype(jnp.bfloat16)
    times(C, project)
    wo_lane.wait_recv()
    for lane in col_lanes:
        lane.start()
    weight_lanes[1].start()

    def attend(c):
        part = pl.ds(pl.multiple_of(c * R, R), R)
        q = q_all[part, :]
        row = jnp.concatenate([place_row[i, 0:1, :] for i in range(C)], axis=1)
        allowed = row <= place_col[part, 0:1]
        total = jnp.zeros((R, LANES), jnp.float32)
        for h in range(z.q_heads):
            mine = head_of == h
            s = nt(jnp.where(mine, q, jnp.zeros_like(q)), k2[...]) * score_scale
            s = jnp.where(allowed, s, masked_score)
            top = jnp.max(s, axis=-1, keepdims=True)
            e = jnp.exp(s - top)
            weight = jnp.sum(e, axis=-1, keepdims=True)
            lse[h, part, :] = jnp.broadcast_to(top + jnp.log(weight), (R, LANES))
            total = jnp.where(mine, nn(e.astype(jnp.bfloat16), v2[...]) / weight, total)
        att_f[part, :] = total
        att_stage[c] = total.astype(jnp.bfloat16)
    times(C, attend)
    att_lane.start()
    weight_lanes[2].start()
    att_in[me.c] = att_stage[me.c]
    for lane in col_lanes:
        lane.wait_recv()
    att_lane.wait_recv()
    x = tok[...].astype(jnp.float32)
    mixed = jnp.zeros((R, D), jnp.float32)
    for c in range(C):
        mixed = mixed + nn(att_in[c][:, :qw], wo_v[c * qw : (c + 1) * qw, :])
    mid = x + residual_scale * mixed
    middle[...] = mid
    inverse = lax.rsqrt(jnp.mean(mid * mid, axis=-1, keepdims=True) + norm_eps)
    hidden = (mid * inverse * gain_two).astype(jnp.bfloat16)
    h2[...] = hidden
    chosen = slot_t[...].T > -0.5
    logits = jnp.where(chosen, nn(hidden, small_v[...]), masked_score)
    raised = jnp.where(chosen, jnp.exp(logits - jnp.max(logits, axis=-1, keepdims=True)), 0.0)
    gates[...] = raised / jnp.sum(raised, axis=-1, keepdims=True)

    outs = [
        pltpu.make_async_copy(source, out, own_sem.at[10 + i])
        for i, (source, out) in enumerate([(tok_all, tok_out), (wc_v, wc_out), (small_v, small_out), (wo_v, wo_out), (place_all, place_out)])
    ]
    for copy in outs:
        copy.start()
    for lane in [tok_lane, place_lane, wc_lane, small_lane, wo_lane, att_lane] + col_lanes:
        lane.wait_send()
    for lane in [cot_lane] + weight_lanes:
        lane.wait_recv()
        lane.wait_send()
    for copy in outs + own_stores + [own_cot]:
        copy.wait()


def rows_at(ref, i, n):
    return ref.at[pl.ds(pl.multiple_of(i * n, n), n), :]


def vmem(shape, dtype=jnp.bfloat16):
    return pltpu.VMEM(shape, dtype)


def call(z, kernel, name, collective_id, ins, outs, scratch, **kw):
    space = lambda fast: pl.BlockSpec(memory_space=pltpu.VMEM if fast else pl.ANY)
    return pl.pallas_call(
        kernel, name=name,
        out_shape=[o for o, _ in outs], in_specs=[space(f) for _, f in ins], out_specs=[space(f) for _, f in outs],
        scratch_shapes=scratch,
        compiler_params=pltpu.CompilerParams(
            collective_id=collective_id, has_side_effects=True, vmem_limit_bytes=60000 * 1024),
    )(*[a for a, _ in ins])


def first_call(z, R, ff, dc, tok, place, routes, cot, w_pack, small, w_out, w_gate, w_up, w_downt):
    C, F, Q, rs = z.C, z.F, z.Q, z.rows_w
    L = C * R
    freq = frequencies()
    ins = [(tok, 1), (place, 1), (routes, 1), (cot, 1), (freq, 1), (w_pack, 0), (small, 0), (w_out, 0),
           (w_gate, 0), (w_up, 0), (w_downt, 0)]
    f = jnp.float32
    outs = [
        (shape_of((C, R, D)), 0), (shape_of((D, 2 * LANES)), 0), (shape_of((D, LANES)), 0), (shape_of((D, D)), 0),
        (shape_of((C, 8, R), jnp.int32), 0), (shape_of((3, D, ff)), 0), (shape_of((OWN, Q, CAP, D)), 0),
        (shape_of((L, D)), 1), (shape_of((L, LANES)), 1), (shape_of((L, LANES)), 1), (shape_of((L, LANES)), 1),
        (shape_of((z.q_heads, L, LANES), f), 1), (shape_of((L, LANES), f), 1), (shape_of((R, D), f), 1),
        (shape_of((R, D)), 1), (shape_of((R, LANES), f), 1), (shape_of((Q, OWN * CAP, R)), 1),
    ]
    scratch = [
        vmem((C, R, D)), vmem((C, 8, R), jnp.int32), vmem((D, 2 * LANES)), vmem((D, LANES)), vmem((D, D)),
        vmem((Q, OWN, CAP, D)), vmem((C, R, LANES)), vmem((C, R, LANES)), vmem((3, dc, ff)), vmem((L, R), f),
        vmem((C, 8, R), f), vmem((LANES, R), f), pltpu.SemaphoreType.DMA((16,)),
        pltpu.SemaphoreType.DMA((C, F)), pltpu.SemaphoreType.DMA((C, F)),
    ] + sem_pairs(z, FIRST_GROUPS)
    return call(z, functools.partial(first_kernel, z, R, dc), "first", 0, ins, outs, scratch)


SECOND_GROUPS = ["cube", "cube", "ctx", "ctx", "ctx", "cube", "cube"]


def exact(kind, a, b):
    dims = {"nn": ((1,), (0,)), "nt": ((1,), (1,)), "tn": ((0,), (0,))}[kind]
    return lax.dot_general(a, b, (dims, ((), ())), precision=lax.Precision.HIGHEST, preferred_element_type=jnp.float32)


def second_kernel(z, R, ff, dc, tile, pick, h2, gates, middle, cot, small, w_gate, w_up, w_downt, wt, cot_in,
                  d_mid, d_attn, g_small, gain_out, result, grads,
                  stage, xin, g_stage, gin, wv, cot_v, d_rows, d_in, dg_stage, dg_in, hid, d_gate, d_up, d_res,
                  g_col, d_col, turn_v, own_w, own_sem, *sems):
    me = z.place(lax.axis_index("ctx"), lax.axis_index("fsdp"))
    C, F, Q = z.C, z.F, z.Q
    pair = lambda i: (sems[2 * i], sems[2 * i + 1])
    slots = lambda ref, q: ref.at[:, pl.ds(pl.multiple_of(q * CAP, CAP), CAP), :]
    row_lane = Lane(z, me, "cube", lambda to: stage.at[to.q], lambda p: slots(xin, p.q), *pair(0))
    g_lane = Lane(z, me, "cube", lambda to: g_stage.at[to.q], lambda p: gin.at[p.q], *pair(1))
    weights = [w_gate, w_up, w_downt]
    weight_lanes = [
        Lane(z, me, "ctx", lambda to, j=j: weights[j].at[to.m * OWN + 1],
             lambda p, j=j: rows_at(wv.at[1, j], p.c, dc), *pair(2 + j))
        for j in range(3)
    ]
    back_lane = Lane(z, me, "cube", lambda to: slots(d_rows, to.q), lambda p: d_in.at[:, p.q], *pair(5))
    dg_lane = Lane(z, me, "cube", lambda to: dg_stage.at[to.q], lambda p: dg_in.at[p.q], *pair(6))
    first_load = pltpu.make_async_copy(wt, wv.at[0], own_sem.at[0])
    cot_load = pltpu.make_async_copy(cot_in, cot_v, own_sem.at[1])
    own_loads = [
        pltpu.make_async_copy(weights[j].at[me.m * OWN + 1], rows_at(wv.at[1, j], me.c, dc), own_sem.at[2 + j])
        for j in range(3)
    ]
    for copy in [first_load, cot_load] + own_loads:
        copy.start()
    meet(z, me, ["cube", "ctx"])

    turn_v[...] = gates[...].T
    slot_lane = lane_of((8, LANES))

    def send_rows(k):
        to = z.peer("cube", me, k)
        q = to.q
        for i in range(OWN):
            stage[q, i] = nn(pick[q, i * CAP : (i + 1) * CAP, :], h2[...]).astype(jnp.bfloat16)
        hot = jnp.concatenate([pick[q].astype(jnp.float32), jnp.zeros((LANES - OWN * CAP, R), jnp.float32)], axis=0)
        row = jnp.zeros((8, LANES), jnp.float32)
        for i in range(OWN):
            g = jnp.broadcast_to(turn_v[pl.ds(q * OWN + i, 1), :], (8, R))
            row = jnp.where(lax.div(slot_lane, CAP) == i, exact("nt", g, hot), row)
        g_stage[q] = row
        @pl.when(k > 0)
        def _():
            row_lane.start_one(k)
            g_lane.start_one(k)
    times(Q, send_rows)
    for lane in weight_lanes:
        lane.start()
    for i in range(OWN):
        xin[i, pl.ds(pl.multiple_of(me.q * CAP, CAP), CAP), :] = stage[me.q, i]
    gin[me.q] = g_stage[me.q]
    g_lane.wait_recv()

    def columns(q):
        column = jnp.broadcast_to(gin[q][0:1, :], (LANES, LANES)).T
        for i in range(OWN):
            g_col[i, pl.ds(pl.multiple_of(q * CAP, CAP), CAP), :] = column[i * CAP : (i + 1) * CAP, :]
    times(Q, columns)
    first_load.wait()
    cot_load.wait()
    row_lane.wait_recv()

    def expert(i):
        @pl.when(i == 1)
        def _():
            for copy in own_loads:
                copy.wait()
            for lane in weight_lanes:
                lane.wait_recv()

        def rows(r):
            part = pl.ds(pl.multiple_of(r * tile, tile), tile)
            x = xin[i, part, :]
            gate = nn(x, wv[i, 0])
            up = nn(x, wv[i, 1])
            sig = jax.nn.sigmoid(gate)
            act = gate * sig
            hidden = (act * up).astype(jnp.bfloat16)
            hid[part, :] = hidden
            out = nt(hidden, wv[i, 2]).astype(jnp.bfloat16)
            result[i, part, :] = out
            upstream = cot_v[i, part, :].astype(jnp.float32)
            d_gates = residual_scale * jnp.sum(upstream * out.astype(jnp.float32), axis=-1, keepdims=True)
            d_col[i, part, :] = jnp.broadcast_to(d_gates, (tile, LANES))
            d_out = (residual_scale * g_col[i, part, 0:1] * upstream).astype(jnp.bfloat16)
            d_res[part, :] = d_out
            d_hidden = nn(d_out, wv[i, 2])
            dg = (d_hidden * up * sig * (1.0 + gate * (1.0 - sig))).astype(jnp.bfloat16)
            du = (d_hidden * act).astype(jnp.bfloat16)
            d_gate[part, :] = dg
            d_up[part, :] = du
            d_rows[i, part, :] = (nt(dg, wv[i, 0]) + nt(du, wv[i, 1])).astype(jnp.bfloat16)
        times(Q * CAP // tile, rows)

        @pl.when(i == OWN - 1)
        def _():
            times(Q, send_back)

        def cut(d):
            part = pl.ds(pl.multiple_of(d * 256, 256), 256)
            grads[i, 0, part, :] = tn(xin[i, :, part], d_gate[...]).astype(jnp.bfloat16)
            grads[i, 1, part, :] = tn(xin[i, :, part], d_up[...]).astype(jnp.bfloat16)
            grads[i, 2, part, :] = tn(d_res[:, part], hid[...]).astype(jnp.bfloat16)
        times(D // 256, cut)

    def send_back(k):
        to = z.peer("cube", me, k)
        q = to.q
        parts = [d_col[i, pl.ds(pl.multiple_of(q * CAP, CAP), CAP), :] for i in range(OWN)]
        column = jnp.concatenate(parts + [jnp.zeros((LANES - OWN * CAP, LANES), jnp.float32)], axis=0)
        dg_stage[q] = column.T[0:8, :]
        @pl.when(k > 0)
        def _():
            back_lane.start_one(k)
            dg_lane.start_one(k)
    times(OWN, expert)
    for i in range(OWN):
        d_in[i, me.q] = d_rows[i, pl.ds(pl.multiple_of(me.q * CAP, CAP), CAP), :]
    dg_in[me.q] = dg_stage[me.q]

    back_lane.wait_recv()
    dg_lane.wait_recv()
    turn_v[...] = jnp.zeros((LANES, R), jnp.float32)

    def collect(q):
        hot = pick[q].astype(jnp.float32)
        row = jnp.broadcast_to(dg_in[q][0:1, : OWN * CAP], (8, OWN * CAP))
        slot = lax.div(lane_of((8, OWN * CAP)), CAP)
        for i in range(OWN):
            turn_v[pl.ds(q * OWN + i, 1), :] = exact("nn", jnp.where(slot == i, row, 0.0), hot)[0:1, :]
    times(Q, collect)
    gts = gates[...]
    dgs = turn_v[...].T
    d_log = gts * (dgs - jnp.sum(gts * dgs, axis=-1, keepdims=True))
    g_small[...] = exact("tn", h2[...].astype(jnp.float32), d_log)
    d_h2 = exact("nt", d_log, small[...].astype(jnp.float32))
    for i in range(OWN):
        hot = pick[:, i * CAP : (i + 1) * CAP, :].reshape(Q * CAP, R)
        d_h2 = d_h2 + tn(hot, d_in[i].reshape(Q * CAP, D))
    mid = middle[...]
    inverse = lax.rsqrt(jnp.mean(mid * mid, axis=-1, keepdims=True) + norm_eps)
    n2 = mid * inverse
    gain_out[...] = jnp.broadcast_to(jnp.sum(d_h2 * n2, axis=0, keepdims=True), (8, D))
    gain_two = small[...].astype(jnp.float32).T[EXPERTS + 1 : EXPERTS + 2, :]
    g = d_h2 * gain_two
    dm = cot[...].astype(jnp.float32) + inverse * (g - n2 * jnp.mean(g * n2, axis=-1, keepdims=True))
    d_mid[...] = dm
    d_attn[...] = (residual_scale * dm).astype(jnp.bfloat16)
    for lane in [row_lane, g_lane, back_lane, dg_lane] + weight_lanes:
        lane.wait_send()


def second_call(z, R, ff, dc, pick, h2, gates, middle, cot, small, w_gate, w_up, w_downt, wt, cot_in):
    Q = z.Q
    rows = Q * CAP
    tile = 256
    f = jnp.float32
    ins = [(pick, 1), (h2, 1), (gates, 1), (middle, 1), (cot, 1), (small, 1), (w_gate, 0), (w_up, 0), (w_downt, 0),
           (wt, 0), (cot_in, 0)]
    outs = [
        (shape_of((R, D), f), 1), (shape_of((R, D)), 1), (shape_of((D, LANES), f), 1), (shape_of((8, D), f), 1),
        (shape_of((OWN, rows, D)), 1), (shape_of((OWN, 3, D, ff)), 1),
    ]
    scratch = [
        vmem((Q, OWN, CAP, D)), vmem((OWN, rows, D)), vmem((Q, 8, LANES), f), vmem((Q, 8, LANES), f),
        vmem((OWN, 3, D, ff)), vmem((OWN, rows, D)), vmem((OWN, rows, D)), vmem((OWN, Q, CAP, D)),
        vmem((Q, 8, LANES), f), vmem((Q, 8, LANES), f), vmem((rows, ff)), vmem((rows, ff)), vmem((rows, ff)),
        vmem((rows, D)), vmem((OWN, rows, LANES), f), vmem((OWN, rows, LANES), f), vmem((LANES, R), f),
        vmem((8, LANES)), pltpu.SemaphoreType.DMA((8,)),
    ] + sem_pairs(z, SECOND_GROUPS)
    return call(z, functools.partial(second_kernel, z, R, ff, dc, tile), "second", 1, ins, outs, scratch)


def frequencies():
    lanes = np.arange(LANES)
    steps = rope_base ** ((lanes % (HEAD // 2)) * (-2.0 / HEAD))
    return jnp.asarray(np.stack([steps, np.where(lanes < HEAD, steps, 0.0)] + [steps] * 6), jnp.float32)


THIRD_GROUPS = ["ctx", "cube", "ctx", "world", "world", "fsdp"] + ["ctx"] * (3 * OWN)


def third_kernel(z, R, dc, d_attn, h1, q_all, k2, v2, lse, att_f, wc, place, freq, g_small, gain_two, middle, d_mid, tok,
                 small, pick, gates, tok_all, wo, result, grads,
                 output, grad_tokens, gc_in, gs_in, go_in, gw_in,
                 d_all, wo_c, tok_v, d_qkv, ds_v, p_v, q_v, dm_v, dk_acc, dv_acc, place_col, place_row, dn_stage, dn_in,
                 gc_stage, go_stage, gs_stage, gain_v, out_in, mix_hi, mix_lo, own_w, own_sem, *sems):
    me = z.place(lax.axis_index("ctx"), lax.axis_index("fsdp"))
    C, F, Q, rs, qw = z.C, z.F, z.Q, z.rows_w, z.q_width
    L = C * R
    pair = lambda i: (sems[2 * i], sems[2 * i + 1])
    up_lane = Lane(z, me, "ctx", lambda to: d_attn, lambda p: d_all.at[p.c], *pair(0))
    out_lane = Lane(z, me, "cube", lambda to: result.at[:, to.q], lambda p: out_in.at[:, p.q], *pair(1))
    dn_lane = Lane(z, me, "ctx", lambda to: dn_stage.at[to.c], lambda p: dn_in.at[p.c], *pair(2))
    gc_lane = Lane(z, me, "world", lambda to: rows_at(gc_stage, to.w, rs), lambda p: gc_in.at[p.w], *pair(3))
    gs_lane = Lane(z, me, "world", lambda to: rows_at(gs_stage, to.w, rs), lambda p: gs_in.at[p.w], *pair(4))
    go_lane = Lane(z, me, "fsdp", lambda to: rows_at(go_stage, to.f, rs), lambda p: go_in.at[p.f], *pair(5))
    grad_src = lambda e, j, c: rows_at(grads.at[e, j], c, dc)
    grad_dst = lambda e, j, p: gw_in.at[j, p.s, p.m * OWN + e]
    grad_lanes = [
        Lane(z, me, "ctx", lambda to, e=e, j=j: grad_src(e, j, to.c), lambda p, e=e, j=j: grad_dst(e, j, p),
             *pair(6 + 3 * e + j))
        for e in range(OWN) for j in range(3)
    ]
    wo_load = pltpu.make_async_copy(rows_at(wo, me.c, qw), wo_c, own_sem.at[0])
    tok_load = pltpu.make_async_copy(tok_all, tok_v, own_sem.at[1])
    out_load = pltpu.make_async_copy(result.at[:, me.q], out_in.at[:, me.q], own_sem.at[2])
    own_loads = [
        pltpu.make_async_copy(grad_src(e, j, me.c), own_w.at[3 * e + j], own_sem.at[3 + 3 * e + j])
        for e in range(OWN) for j in range(3)
    ]
    for copy in [wo_load, tok_load, out_load] + own_loads:
        copy.start()
    meet(z, me, ["world"])
    up_lane.start()
    out_lane.start()
    for lane in grad_lanes:
        lane.start()

    own_stores = []
    for e in range(OWN):
        for j in range(3):
            own_loads[3 * e + j].wait()
            own_stores.append(pltpu.make_async_copy(own_w.at[3 * e + j], grad_dst(e, j, me), own_sem.at[9 + 3 * e + j]))
            own_stores[-1].start()
    d_all[me.c] = d_attn[...]
    dk_acc[...] = jnp.zeros((L, LANES), jnp.float32)
    dv_acc[...] = jnp.zeros((L, LANES), jnp.float32)

    def columns(c):
        row = place[c][0:1, :].astype(jnp.float32)
        place_row[c] = jnp.broadcast_to(row, (8, R))
        place_col[pl.ds(pl.multiple_of(c * R, R), R), :] = jnp.broadcast_to(row, (R, R)).T
    times(C, columns)
    wo_load.wait()
    head_of = lax.div(lane_of((R, LANES)), HEAD)

    def attend(k):
        c = lax.rem(me.c + C - k, C)
        @pl.when(k > 0)
        def _():
            up_lane.wait_recv_one(k)
        part = pl.ds(pl.multiple_of(c * R, R), R)
        q = q_all[part, :]
        d_mix = nt(d_all[c], wo_c[...])
        if qw < LANES:
            d_mix = jnp.concatenate([d_mix, jnp.zeros((R, LANES - qw), jnp.float32)], axis=1)
        d_mix = d_mix.astype(jnp.bfloat16)
        row = jnp.concatenate([place_row[i, 0:1, :] for i in range(C)], axis=1)
        column = place_col[part, :]
        allowed = row <= column[:, 0:1]
        dq = jnp.zeros((R, LANES), jnp.float32)
        for h in range(z.q_heads):
            mine = head_of == h
            rows = pl.ds(h * R, R)
            q_h = jnp.where(mine, q, jnp.zeros_like(q))
            dm_h = jnp.where(mine, d_mix, jnp.zeros_like(d_mix))
            q_v[rows, :] = q_h
            dm_v[rows, :] = dm_h
            s = jnp.where(allowed, nt(q_h, k2[...]) * score_scale, masked_score)
            p = jnp.exp(s - lse[h, part, 0:1])
            p_v[rows, :] = p.astype(jnp.bfloat16)
            delta = jnp.sum(dm_h.astype(jnp.float32) * att_f[part, :], axis=-1, keepdims=True)
            ds = (p * (nt(dm_h, v2[...]) - delta)).astype(jnp.bfloat16)
            ds_v[rows, :] = ds
            dq = jnp.where(mine, nn(ds, k2[...]) * score_scale, dq)
        dk_acc[...] += tn(ds_v[...], q_v[...])
        dv_acc[...] += tn(p_v[...], dm_v[...])
        cosine, sine = rope_tables(column, freq[0:1, :])
        d_qkv[part, 0:LANES] = rope(dq, cosine, -sine).astype(jnp.bfloat16)
    times(C, attend)

    def finish_kv(c):
        part = pl.ds(pl.multiple_of(c * R, R), R)
        dk = dk_acc[part, :] * score_scale
        dv = dv_acc[part, :]
        dk = dk + pltpu.roll(dk, HEAD, 1)
        dv = dv + pltpu.roll(dv, HEAD, 1)
        cosine, sine = rope_tables(place_col[part, :], freq[1:2, :])
        d_qkv[part, LANES : 2 * LANES] = rope(jnp.where(head_of == 0, dk, dv), cosine, -sine).astype(jnp.bfloat16)
    times(C, finish_kv)
    tok_load.wait()
    gain_v[...] = jnp.zeros((LANES, D), jnp.float32)

    def down(k):
        c = lax.rem(me.c + k, C)
        part = pl.ds(pl.multiple_of(c * R, R), R)
        dn = nt(d_qkv[part, :], wc[...])
        x = tok_v[c].astype(jnp.float32)
        n1 = x * lax.rsqrt(jnp.mean(x * x, axis=-1, keepdims=True) + norm_eps)
        gain_v[EXPERTS : EXPERTS + 1, :] += jnp.sum(dn * n1, axis=0, keepdims=True)
        dn_stage[c] = dn.astype(jnp.bfloat16)
        @pl.when(k > 0)
        def _():
            dn_lane.start_one(k)
    times(C, down)
    dn_in[me.c] = dn_stage[me.c]

    def weights(d):
        part = pl.ds(pl.multiple_of(d * 256, 256), 256)
        gc_stage[part, :] = tn(h1[:, part], d_qkv[...]).astype(jnp.bfloat16)
    times(D // 256, weights)
    gc_lane.start()
    go_stage[...] = tn(att_f[...].astype(jnp.bfloat16), d_all[...].reshape(L, D)).astype(jnp.bfloat16)
    go_lane.start()
    gain_v[EXPERTS + 1 : EXPERTS + 2, :] = gain_two[0:1, :]
    gs_stage[...] = g_small[...] + gain_v[...].T
    gs_lane.start()
    own_last = [
        pltpu.make_async_copy(rows_at(gc_stage, me.w, rs), gc_in.at[me.w], own_sem.at[15]),
        pltpu.make_async_copy(rows_at(gs_stage, me.w, rs), gs_in.at[me.w], own_sem.at[16]),
        pltpu.make_async_copy(rows_at(go_stage, me.f, rs), go_in.at[me.f], own_sem.at[17]),
    ]
    for copy in own_last:
        copy.start()

    place_col[0:LANES, :] = gates[...].T

    def mix(q):
        for i in range(OWN):
            g = place_col[pl.ds(q * OWN + i, 1), :] * pick[q, i * CAP : (i + 1) * CAP, :].astype(jnp.float32)
            high = g.astype(jnp.bfloat16)
            part = pl.ds(pl.multiple_of(q * CAP, CAP), CAP)
            mix_hi[i, part, :] = high
            mix_lo[i, part, :] = (g - high.astype(jnp.float32)).astype(jnp.bfloat16)
    times(Q, mix)
    out_load.wait()
    out_lane.wait_recv()
    mixed = jnp.zeros((R, D), jnp.float32)
    for i in range(OWN):
        rows = out_in[i].reshape(Q * CAP, D)
        mixed = mixed + tn(mix_hi[i], rows) + tn(mix_lo[i], rows)
    output[...] = (middle[...] + residual_scale * mixed).astype(jnp.bfloat16)

    dn_lane.wait_recv()
    d_h1 = dn_in[0].astype(jnp.float32)
    for c in range(1, C):
        d_h1 = d_h1 + dn_in[c].astype(jnp.float32)
    x = tok[...].astype(jnp.float32)
    inverse = lax.rsqrt(jnp.mean(x * x, axis=-1, keepdims=True) + norm_eps)
    n1 = x * inverse
    g = d_h1 * small[...].astype(jnp.float32).T[EXPERTS : EXPERTS + 1, :]
    grad_tokens[...] = d_mid[...] + inverse * (g - n1 * jnp.mean(g * n1, axis=-1, keepdims=True))
    for lane in [gc_lane, gs_lane, go_lane] + grad_lanes:
        lane.wait_recv()
    for lane in [up_lane, out_lane, dn_lane, gc_lane, gs_lane, go_lane] + grad_lanes:
        lane.wait_send()
    for copy in own_stores + own_last:
        copy.wait()


def third_call(z, R, ff, dc, *arrays):
    C, F, N, Q, S, rs, qw = z.C, z.F, z.N, z.Q, z.S, z.rows_w, z.q_width
    L, rows, f = C * R, z.Q * CAP, jnp.float32
    heads = z.q_heads * R
    ins = [(a, 1) for a in arrays[:-4]] + [(a, 0) for a in arrays[-4:]]
    outs = [
        (shape_of((R, D)), 1), (shape_of((R, D), f), 1), (shape_of((N, rs, 2 * LANES)), 0), (shape_of((N, rs, LANES), f), 0),
        (shape_of((F, rs, D)), 0), (shape_of((3, S, z.per_f, dc, ff)), 0),
    ]
    scratch = [
        vmem((C, R, D)), vmem((qw, D)), vmem((C, R, D)), vmem((L, 2 * LANES)), vmem((heads, L)), vmem((heads, L)),
        vmem((heads, LANES)), vmem((heads, LANES)), vmem((L, LANES), f), vmem((L, LANES), f), vmem((L, R), f),
        vmem((C, 8, R), f), vmem((C, R, D)), vmem((C, R, D)), vmem((D, 2 * LANES)), vmem((LANES, D)), vmem((D, LANES), f),
        vmem((LANES, D), f), vmem((OWN, Q, CAP, D)), vmem((OWN, rows, R)), vmem((OWN, rows, R)), vmem((3 * OWN, dc, ff)),
        pltpu.SemaphoreType.DMA((18,)),
    ] + sem_pairs(z, THIRD_GROUPS)
    return call(z, functools.partial(third_kernel, z, R, dc), "third", 2, ins, outs, scratch)


def local(z, tokens, norm_first, w_query, w_key, w_value, w_out, norm_second, w_router,
          w_gate, w_up, w_down, positions, routes, cotangent):
    C, F, N, Q, S, G = z.C, z.F, z.N, z.Q, z.S, z.G
    R = tokens.shape[1]
    rs = z.rows_w
    ff = w_gate.shape[2]
    dc = D // C

    heads_q = jnp.pad(w_query.reshape(rs, C, z.q_width), ((0, 0), (0, 0), (0, LANES - z.q_width)))
    heads_k = jnp.repeat(w_key.reshape(rs, KV_HEADS, HEAD), z.share, axis=1)
    heads_v = jnp.repeat(w_value.reshape(rs, KV_HEADS, HEAD), z.share, axis=1)
    w_pack = jnp.concatenate([heads_q, heads_k, heads_v], axis=2).transpose(1, 0, 2)
    small = jnp.concatenate(
        [w_router, norm_first[:, None], norm_second[:, None], jnp.zeros((rs, 128 - EXPERTS - 2), jnp.bfloat16)], axis=1)
    place_pack = jnp.broadcast_to(positions[0][None, :], (8, R))
    w_downt = w_down.transpose(0, 2, 1)
    (tok_all, w_c, small_all, wo, place_all, wt, cot_in, h1, q_all, k2, v2, lse, att_f, middle, h2, gates, pick) = first_call(
        z, R, ff, dc, tokens[0], place_pack, routes[0], cotangent[0], w_pack, small, w_out, w_gate, w_up, w_downt)
    d_mid, d_attn, g_small, g_gain_two, result, grads = second_call(
        z, R, ff, dc, pick, h2, gates, middle, cotangent[0], small_all, w_gate, w_up, w_downt, wt,
        cot_in.reshape(OWN, Q * CAP, D))
    output, grad_tokens, gc_in, gs_in, go_in, gw_in = third_call(
        z, R, ff, dc, d_attn, h1, q_all, k2, v2, lse, att_f, w_c, place_all, frequencies(), g_small, g_gain_two, middle, d_mid,
        tokens[0], small_all, pick, gates, tok_all, wo, result.reshape(OWN, Q, CAP, D), grads)
    gc = jnp.sum(f32(gc_in).reshape(C, F, rs, 2 * LANES), axis=1)
    join = lambda a: a.reshape(KV_HEADS, z.share, rs, HEAD).sum(axis=1).transpose(1, 0, 2).reshape(rs, KV_HEADS * HEAD)
    gs = jnp.sum(gs_in, axis=0)
    return (
        output[None],
        grad_tokens[None],
        gs[:, EXPERTS],
        gc[:, :, : z.q_width].transpose(1, 0, 2).reshape(rs, D),
        join(gc[:, :, LANES : LANES + HEAD]),
        join(gc[:, :, LANES + HEAD :]),
        jnp.sum(f32(go_in), axis=0),
        gs[:, EXPERTS + 1],
        gs[:, :EXPERTS],
        jnp.sum(f32(gw_in[0]), axis=0),
        jnp.sum(f32(gw_in[1]), axis=0),
        jnp.sum(f32(gw_in[2]), axis=0).transpose(0, 2, 1),
    )


def solution(mesh):
    row = P(("ctx", "fsdp"), None)
    vec = P(("ctx", "fsdp"))
    seq = P("fsdp", "ctx", None)
    down = P("fsdp", None, "ctx")
    return jax.shard_map(
        functools.partial(local, Sizes(mesh)),
        mesh=mesh,
        in_specs=(seq, vec, row, row, row, row, vec, row, seq, seq, down, P("fsdp", "ctx"), seq, seq),
        out_specs=(seq, seq, vec, row, row, row, row, vec, row, seq, seq, down),
        check_vma=False,
    )
```

```python
import collections
import functools

import jax
import jax.numpy as jnp
import numpy as np
from jax import lax
from jax.experimental import pallas as pl
from jax.experimental.pallas import tpu as pltpu
from jax.sharding import PartitionSpec as P

D = 1024
HEADS = 16
KV_HEADS = 8
HEAD = 64
EXPERTS = 32
TOP = 8
CAP = 48
LANES = 128

residual_scale = 0.22
score_scale = 0.015625
rope_base = 10000.0
norm_eps = 1e-06
masked_score = -1e30

MESH = pl.DeviceIdType.MESH
Place = collections.namedtuple("Place", ["c", "f", "m", "s", "h", "k", "p", "w"])


class Sizes:
    def __init__(self, mesh):
        self.C = mesh.shape["ctx"]
        self.F = mesh.shape["fsdp"]
        self.N = self.C * self.F
        self.G = EXPERTS // self.F
        self.S = self.C // self.G
        self.H = self.G // 2
        self.P = 2 * self.F
        self.J = self.C // 2
        self.q_heads = HEADS // self.C
        self.q_width = self.q_heads * HEAD
        self.share = self.C // KV_HEADS
        self.rows_w = D // self.N

    def place(self, c, f):
        k = lax.rem(c, 2)
        return Place(c, f, lax.rem(c, self.G), lax.div(c, self.G), lax.rem(lax.div(c, 2), self.H), k, f * 2 + k, c * self.F + f)

    def count(self, group):
        return {"ctx": self.C, "fsdp": self.F, "world": self.N, "col": self.H, "line": self.J, "plane": self.P}[group]

    def peer(self, group, me, n):
        if group == "ctx":
            return self.place(lax.rem(me.c + n, self.C), me.f)
        if group == "fsdp":
            return self.place(me.c, lax.rem(me.f + n, self.F))
        if group == "world":
            w = lax.rem(me.w + n, self.N)
            return self.place(lax.div(w, self.F), lax.rem(w, self.F))
        if group == "col":
            return self.place(me.s * self.G + 2 * lax.rem(me.h + n, self.H) + me.k, me.f)
        if group == "line":
            return self.place(2 * lax.rem(lax.div(me.c, 2) + n, self.J) + me.k, me.f)
        p = lax.rem(me.p + n, self.P)
        return self.place(me.s * self.G + 2 * me.h + lax.rem(p, 2), lax.div(p, 2))

    def expert(self, me, p):
        return lax.div(p, 2) * self.G + 2 * me.h + lax.rem(p, 2)


def bf(x):
    return x.astype(jnp.bfloat16)


def f32(x):
    return x.astype(jnp.float32)


def shape_of(shape, dtype=jnp.bfloat16):
    return jax.ShapeDtypeStruct(shape, dtype)


class Lane:
    def __init__(self, sizes, me, group, src, dst, sends, recvs):
        self.sizes, self.me, self.group, self.src, self.dst = sizes, me, group, src, dst
        self.sends, self.recvs, self.n = sends, recvs, sizes.count(group)

    def copy(self, k, to, source, landing):
        return pltpu.make_async_remote_copy(
            src_ref=source, dst_ref=landing, send_sem=self.sends.at[k], recv_sem=self.recvs.at[k],
            device_id=(to.c, to.f), device_id_type=MESH)

    def to(self, k):
        return self.sizes.peer(self.group, self.me, k)

    def start_one(self, k):
        to = self.to(k)
        self.copy(k, to, self.src(to), self.dst(self.me)).start()

    def wait_recv_one(self, k):
        landed = self.dst(self.sizes.peer(self.group, self.me, self.n - k))
        self.copy(k, self.to(k), landed, landed).wait_recv()

    def wait_send_one(self, k):
        to = self.to(k)
        self.copy(k, to, self.src(to), self.dst(self.me)).wait_send()

    def each(self, step):
        def one(k, carry):
            step(k)
            return carry
        lax.fori_loop(1, self.n, one, 0)

    def start(self):
        self.each(self.start_one)

    def wait_recv(self):
        self.each(self.wait_recv_one)

    def wait_send(self):
        self.each(self.wait_send_one)


class Relay:
    def __init__(self, sizes, me, own, landing, sends, recvs):
        self.sizes, self.me, self.own, self.landing, self.sends, self.recvs = sizes, me, own, landing, sends, recvs

    def member(self, n, core):
        J = self.sizes.J
        return 2 * lax.rem(lax.div(self.me.c, 2) + J - n, J) + core

    def copy(self, n, source, landing):
        return pltpu.make_async_remote_copy(
            src_ref=source, dst_ref=landing, send_sem=self.sends.at[n], recv_sem=self.recvs.at[n],
            device_id=(self.me.c + 1 - 2 * self.me.k, self.me.f), device_id_type=MESH)

    def start_own(self):
        self.copy(0, self.own, self.landing(self.me.c)).start()

    def start_one(self, n):
        here = self.landing(self.member(n, self.me.k))
        self.copy(n, here, here).start()

    def wait_recv_one(self, n):
        there = self.landing(self.member(n, 1 - self.me.k))
        self.copy(n, there, there).wait_recv()

    def wait_send(self):
        def one(n, carry):
            here = self.landing(self.member(n, self.me.k))
            self.copy(n, here, here).wait_send()
            return carry
        lax.fori_loop(0, self.sizes.J, one, 0)


def meet(sizes, me, groups):
    barrier = pltpu.get_barrier_semaphore()
    total = 0
    for group in groups:
        def greet(k, carry, group=group):
            p = sizes.peer(group, me, k)
            pl.semaphore_signal(barrier, inc=1, device_id=(p.c, p.f), device_id_type=MESH)
            return carry
        lax.fori_loop(1, sizes.count(group), greet, 0)
        total += sizes.count(group) - 1
    pl.semaphore_wait(barrier, total)


def times(n, step):
    def one(i, carry):
        step(i)
        return carry
    lax.fori_loop(0, n, one, 0)


def nn(a, b):
    return lax.dot_general(a, b, (((1,), (0,)), ((), ())), preferred_element_type=jnp.float32)


def nt(a, b):
    return lax.dot_general(a, b, (((1,), (1,)), ((), ())), preferred_element_type=jnp.float32)


def tn(a, b):
    return lax.dot_general(a, b, (((0,), (0,)), ((), ())), preferred_element_type=jnp.float32)


def lane_of(shape):
    return lax.broadcasted_iota(jnp.int32, shape, 1)


def rope_tables(place_columns, frequency):
    angles = place_columns.astype(jnp.float32) * frequency
    return jnp.cos(angles), jnp.sin(angles)


def rope(x, cosine, sine):
    half = HEAD // 2
    mixed = jnp.where(lax.rem(lane_of(x.shape), HEAD) < half, -pltpu.roll(x, LANES - half, 1), pltpu.roll(x, half, 1))
    return x * cosine + mixed * sine


def sem_pairs(sizes, groups):
    return [pltpu.SemaphoreType.DMA((sizes.count(g),)) for g in groups for _ in range(2)]


FIRST_GROUPS = ["line", "ctx", "world", "world", "ctx", "col", "col", "ctx", "ctx", "ctx"]


def first_kernel(z, R, dc, tok, place, routes, cot, freq, w_pack, small, w_out, w_gate, w_up,
                 tok_out, wc_out, small_out, wo_out, place_out, wt, cot_in, h1, q_all, k2, v2, lse, att_f, middle, h2, gates_t,
                 pick, tok_all, place_all, wc_v, small_v, wo_v, cot_all, slot_all, cot_stage, att_stage, att_in, own_w,
                 place_col, place_row, slot_t, own_sem, fwd_send, fwd_recv, cot_send, cot_recv, col_send, col_recv, *sems):
    me = z.place(lax.axis_index("ctx"), lax.axis_index("fsdp"))
    C, F, H, P, J, rs, qw = z.C, z.F, z.H, z.P, z.J, z.rows_w, z.q_width
    L = C * R
    pair = lambda i: (sems[2 * i], sems[2 * i + 1])
    tok_lane = Lane(z, me, "line", lambda to: tok, lambda p: tok_all.at[p.c], *pair(0))
    tok_relay = Relay(z, me, tok, lambda c: tok_all.at[c], fwd_send, fwd_recv)
    place_lane = Lane(z, me, "ctx", lambda to: place, lambda p: place_all.at[p.c], *pair(1))
    wc_lane = Lane(z, me, "world", lambda to: w_pack.at[to.c], lambda p: rows_at(wc_v, p.w, rs), *pair(2))
    small_lane = Lane(z, me, "world", lambda to: small, lambda p: rows_at(small_v, p.w, rs), *pair(3))
    wo_lane = Lane(z, me, "ctx", lambda to: w_out, lambda p: rows_at(wo_v, p.w, rs), *pair(4))
    cot_lane = Lane(z, me, "col", lambda to: cot, lambda p: cot_all.at[p.h], *pair(5))
    slot_lane = Lane(z, me, "col", lambda to: slot_t.at[pl.ds(0, EXPERTS), :], lambda p: slot_all.at[p.h], *pair(6))
    weights = [w_gate, w_up]
    weight_lanes = [
        Lane(z, me, "ctx", lambda to, j=j: weights[j].at[to.m], lambda p, j=j: rows_at(wt.at[j], p.c, dc), *pair(7 + j))
        for j in range(2)
    ]
    att_lane = Lane(z, me, "ctx", lambda to: att_stage.at[to.c], lambda p: att_in.at[p.c], *pair(9))

    def rows_lane(h):
        return Lane(z, me, "plane", lambda to: cot_stage.at[h, to.p], lambda p: cot_in.at[h, p.p], cot_send.at[h], cot_recv.at[h])
    col_lanes = [
        Lane(z, me, "fsdp", lambda to, c=c: rows_at(wo_v, c * F + me.f, rs), lambda p, c=c: rows_at(wo_v, c * F + p.f, rs),
             col_send.at[c], col_recv.at[c])
        for c in range(C)
    ]

    meet(z, me, ["world"])
    tok_relay.start_own()
    tok_lane.start()
    place_lane.start()
    wc_lane.start()
    small_lane.start()
    wo_lane.start()
    cot_lane.start()

    own = [
        pltpu.make_async_copy(w_pack.at[me.c], rows_at(wc_v, me.w, rs), own_sem.at[0]),
        pltpu.make_async_copy(small, rows_at(small_v, me.w, rs), own_sem.at[1]),
        pltpu.make_async_copy(w_out, rows_at(wo_v, me.w, rs), own_sem.at[2]),
    ]
    own_loads = [pltpu.make_async_copy(weights[j].at[me.m], own_w.at[j], own_sem.at[3 + j]) for j in range(2)]
    for copy in own + own_loads:
        copy.start()
    tok_all[me.c] = tok[...]
    place_all[me.c] = place[...]
    cot_all[me.h] = cot[...]

    named = jnp.zeros((R, LANES), jnp.float32)
    for j in range(TOP):
        named = jnp.where(routes[:, j : j + 1] == lane_of((R, LANES)), 1.0, named)
    row_id = lax.broadcasted_iota(jnp.int32, (R, R), 0)
    before = jnp.where(row_id > lane_of((R, R)), 1.0, 0.0).astype(jnp.bfloat16)
    slot = nn(before, named.astype(jnp.bfloat16))
    slot_t[...] = jnp.where(named > 0.5, slot, -1.0).T
    slot_all[me.h] = slot_t[0:EXPERTS, :]
    slot_lane.start()
    slot_id = lax.broadcasted_iota(jnp.int32, (CAP, R), 0).astype(jnp.float32)

    def dispatch(j):
        h = lax.rem(me.h + H - j, H)
        lane = rows_lane(h)
        @pl.when(j > 0)
        def _():
            cot_lane.wait_recv_one(j)
            slot_lane.wait_recv_one(j)

        def to_expert(n):
            p = lax.rem(me.p + n, P)
            row = slot_all[h, pl.ds(z.expert(me, p), 1), :]
            hot = jnp.where(row == slot_id, 1.0, 0.0).astype(jnp.bfloat16)
            pick[h, p] = hot
            cot_stage[h, p] = nn(hot, cot_all[h]).astype(jnp.bfloat16)
            @pl.when(n > 0)
            def _():
                lane.start_one(n)
        times(P, to_expert)
    dispatch(0)
    weight_lanes[0].start()
    own_stores = []
    for j in range(2):
        own_loads[j].wait()
        own_stores.append(pltpu.make_async_copy(own_w.at[j], rows_at(wt.at[j], me.c, dc), own_sem.at[7 + j]))
        own_stores[j].start()

    for copy in own:
        copy.wait()
    place_lane.wait_recv()
    small_lane.wait_recv()
    wc_lane.wait_recv()
    gain_one = small_v[...].astype(jnp.float32).T[EXPERTS : EXPERTS + 1, :]
    gain_two = small_v[...].astype(jnp.float32).T[EXPERTS + 1 : EXPERTS + 2, :]
    head_of = lax.div(lane_of((R, LANES)), HEAD)

    def project(i):
        n = lax.rem(i, J)
        c = tok_relay.member(n, jnp.where(i < J, me.k, 1 - me.k))
        @pl.when(jnp.logical_and(i > 0, i < J))
        def _():
            tok_lane.wait_recv_one(n)
            tok_relay.start_one(n)
        @pl.when(i >= J)
        def _():
            tok_relay.wait_recv_one(n)
        x = tok_all[c].astype(jnp.float32)
        inverse = lax.rsqrt(jnp.mean(x * x, axis=-1, keepdims=True) + norm_eps)
        h = (x * inverse * gain_one).astype(jnp.bfloat16)
        part = pl.ds(pl.multiple_of(c * R, R), R)
        h1[part, :] = h
        qkv = nn(h, wc_v[...])
        row = place_all[c][0:1, :].astype(jnp.float32)
        place_row[c] = jnp.broadcast_to(row, (8, R))
        column = jnp.broadcast_to(row, (R, R)).T
        place_col[part, :] = column
        q_all[part, :] = rope(qkv[:, :LANES], *rope_tables(column, freq[0:1, :])).astype(jnp.bfloat16)
        kv = rope(qkv[:, LANES:], *rope_tables(column, freq[1:2, :]))
        swapped = pltpu.roll(kv, HEAD, 1)
        k2[part, :] = jnp.where(head_of == 0, kv, swapped).astype(jnp.bfloat16)
        v2[part, :] = jnp.where(head_of == 0, swapped, kv).astype(jnp.bfloat16)
    times(C, project)
    for j in range(1, H):
        dispatch(j)
    own_cot = pltpu.make_async_copy(cot_stage.at[:, me.p], cot_in.at[:, me.p], own_sem.at[6])
    own_cot.start()
    wo_lane.wait_recv()
    for lane in col_lanes:
        lane.start()
    weight_lanes[1].start()

    def attend(c):
        part = pl.ds(pl.multiple_of(c * R, R), R)
        q = q_all[part, :]
        row = jnp.concatenate([place_row[i, 0:1, :] for i in range(C)], axis=1)
        allowed = row <= place_col[part, 0:1]
        total = jnp.zeros((R, LANES), jnp.float32)
        for h in range(z.q_heads):
            mine = head_of == h
            s = nt(jnp.where(mine, q, jnp.zeros_like(q)), k2[...]) * score_scale
            s = jnp.where(allowed, s, masked_score)
            top = jnp.max(s, axis=-1, keepdims=True)
            e = jnp.exp(s - top)
            weight = jnp.sum(e, axis=-1, keepdims=True)
            lse[h, part, :] = jnp.broadcast_to(top + jnp.log(weight), (R, LANES))
            total = jnp.where(mine, nn(e.astype(jnp.bfloat16), v2[...]) / weight, total)
        att_f[part, :] = total
        att_stage[c] = total.astype(jnp.bfloat16)
    times(C, attend)
    att_lane.start()
    att_in[me.c] = att_stage[me.c]
    for lane in col_lanes:
        lane.wait_recv()
    att_lane.wait_recv()
    x = tok[...].astype(jnp.float32)
    mixed = jnp.zeros((R, D), jnp.float32)
    for c in range(C):
        mixed = mixed + nn(att_in[c][:, :qw], wo_v[c * qw : (c + 1) * qw, :])
    mid = x + residual_scale * mixed
    middle[...] = mid
    inverse = lax.rsqrt(jnp.mean(mid * mid, axis=-1, keepdims=True) + norm_eps)
    hidden = (mid * inverse * gain_two).astype(jnp.bfloat16)
    h2[...] = hidden
    chosen = slot_t[...].T > -0.5
    logits = jnp.where(chosen, nn(hidden, small_v[...]), masked_score)
    raised = jnp.where(chosen, jnp.exp(logits - jnp.max(logits, axis=-1, keepdims=True)), 0.0)
    gates_t[...] = (raised / jnp.sum(raised, axis=-1, keepdims=True)).T

    outs = [
        pltpu.make_async_copy(source, out, own_sem.at[10 + i])
        for i, (source, out) in enumerate([(tok_all, tok_out), (wc_v, wc_out), (small_v, small_out), (wo_v, wo_out), (place_all, place_out)])
    ]
    for copy in outs:
        copy.start()
    tok_relay.wait_send()
    for lane in [tok_lane, place_lane, wc_lane, small_lane, wo_lane, cot_lane, slot_lane, att_lane] + col_lanes:
        lane.wait_send()
    for h in range(H):
        rows_lane(h).wait_recv()
        rows_lane(h).wait_send()
    for lane in weight_lanes:
        lane.wait_recv()
        lane.wait_send()
    for copy in outs + own_stores + [own_cot]:
        copy.wait()


def rows_at(ref, i, n):
    return ref.at[pl.ds(pl.multiple_of(i * n, n), n), :]


def vmem(shape, dtype=jnp.bfloat16):
    return pltpu.VMEM(shape, dtype)


def call(z, kernel, name, collective_id, ins, outs, scratch, **kw):
    space = lambda fast: pl.BlockSpec(memory_space=pltpu.VMEM if fast else pl.ANY)
    return pl.pallas_call(
        kernel, name=name,
        out_shape=[o for o, _ in outs], in_specs=[space(f) for _, f in ins], out_specs=[space(f) for _, f in outs],
        scratch_shapes=scratch,
        compiler_params=pltpu.CompilerParams(
            collective_id=collective_id, has_side_effects=True, vmem_limit_bytes=60000 * 1024),
    )(*[a for a, _ in ins])


def first_call(z, R, ff, dc, tok, place, routes, cot, w_pack, small, w_out, w_gate, w_up):
    C, F, H, P = z.C, z.F, z.H, z.P
    L = C * R
    ins = [(tok, 1), (place, 1), (routes, 1), (cot, 1), (frequencies(), 1), (w_pack, 0), (small, 0), (w_out, 0),
           (w_gate, 0), (w_up, 0)]
    f = jnp.float32
    outs = [
        (shape_of((C, R, D)), 0), (shape_of((D, 2 * LANES)), 0), (shape_of((D, LANES)), 0), (shape_of((D, D)), 0),
        (shape_of((C, 8, R), jnp.int32), 0), (shape_of((2, D, ff)), 0), (shape_of((H, P, CAP, D)), 0),
        (shape_of((L, D)), 1), (shape_of((L, LANES)), 1), (shape_of((L, LANES)), 1), (shape_of((L, LANES)), 1),
        (shape_of((z.q_heads, L, LANES), f), 1), (shape_of((L, LANES), f), 1), (shape_of((R, D), f), 1),
        (shape_of((R, D)), 1), (shape_of((LANES, R), f), 1), (shape_of((H, P, CAP, R)), 1),
    ]
    sem = lambda a, b: [pltpu.SemaphoreType.DMA((a, b)), pltpu.SemaphoreType.DMA((a, b))]
    scratch = [
        vmem((C, R, D)), vmem((C, 8, R), jnp.int32), vmem((D, 2 * LANES)), vmem((D, LANES)), vmem((D, D)),
        vmem((H, R, D)), vmem((H, EXPERTS, R), f), vmem((H, P, CAP, D)), vmem((C, R, LANES)), vmem((C, R, LANES)),
        vmem((2, dc, ff)), vmem((L, R), f), vmem((C, 8, R), f), vmem((LANES, R), f), pltpu.SemaphoreType.DMA((16,)),
        pltpu.SemaphoreType.DMA((z.J,)), pltpu.SemaphoreType.DMA((z.J,)),
    ] + sem(H, P) + sem(C, F) + sem_pairs(z, FIRST_GROUPS)
    return call(z, functools.partial(first_kernel, z, R, dc), "first", 0, ins, outs, scratch)


def frequencies():
    lanes = np.arange(LANES)
    steps = rope_base ** ((lanes % (HEAD // 2)) * (-2.0 / HEAD))
    return jnp.asarray(np.stack([steps, np.where(lanes < HEAD, steps, 0.0)] + [steps] * 6), jnp.float32)


SECOND_GROUPS = ["col", "col", "ctx", "col", "col"]
SECOND_GRIDS = 4


def exact(kind, a, b):
    dims = {"nn": ((1,), (0,)), "nt": ((1,), (1,)), "tn": ((0,), (0,))}[kind]
    return lax.dot_general(a, b, (dims, ((), ())), precision=lax.Precision.HIGHEST, preferred_element_type=jnp.float32)


def second_kernel(z, R, dc, tile, pick, h2, gates_t, middle, cot, small, w_downt, wt, cot_in,
                  d_mid, d_attn, g_small, gain_out, result, grads, gate_all,
                  h_all, stage, xin, g_stage, gin, wv, cot_v, d_rows, d_in, dg_stage, dg_in, hid, d_gate, d_up, d_res,
                  g_col, part_stage, part_in, turn_stage, turn_in, turn_v, own_sem, *sems):
    me = z.place(lax.axis_index("ctx"), lax.axis_index("fsdp"))
    C, F, H, P = z.C, z.F, z.H, z.P
    pair = lambda i: (sems[2 * i], sems[2 * i + 1])
    grid = lambda i, h: (sems[2 * len(SECOND_GROUPS) + 2 * i].at[h], sems[2 * len(SECOND_GROUPS) + 2 * i + 1].at[h])
    h_lane = Lane(z, me, "col", lambda to: h2, lambda p: h_all.at[p.h], *pair(0))
    gate_lane = Lane(z, me, "col", lambda to: gates_t.at[pl.ds(0, EXPERTS), :], lambda p: gate_all.at[p.h], *pair(1))
    down_lane = Lane(z, me, "ctx", lambda to: w_downt.at[to.m], lambda p: rows_at(wv.at[2], p.c, dc), *pair(2))
    part_lane = Lane(z, me, "col", lambda to: part_stage.at[to.h], lambda p: part_in.at[p.h], *pair(3))
    turn_lane = Lane(z, me, "col", lambda to: turn_stage.at[to.h], lambda p: turn_in.at[p.h], *pair(4))
    plane = lambda i, h, source, landing: Lane(
        z, me, "plane", lambda to: source.at[h, to.p], lambda p: landing.at[h, p.p], *grid(i, h))
    row_lane = lambda h: plane(0, h, stage, xin)
    g_lane = lambda h: plane(1, h, g_stage, gin)
    back_lane = lambda h: plane(2, h, d_rows, d_in)
    dg_lane = lambda h: plane(3, h, dg_stage, dg_in)
    loads = [
        pltpu.make_async_copy(wt.at[0], wv.at[0], own_sem.at[0]),
        pltpu.make_async_copy(wt.at[1], wv.at[1], own_sem.at[1]),
        pltpu.make_async_copy(cot_in, cot_v, own_sem.at[2]),
        pltpu.make_async_copy(w_downt.at[me.m], rows_at(wv.at[2], me.c, dc), own_sem.at[3]),
    ]
    for copy in loads:
        copy.start()
    meet(z, me, ["ctx", "plane"])
    h_lane.start()
    gate_lane.start()
    down_lane.start()
    h_all[me.h] = h2[...]
    gate_all[me.h] = gates_t[0:EXPERTS, :]

    def dispatch(j):
        h = lax.rem(me.h + H - j, H)
        @pl.when(j > 0)
        def _():
            h_lane.wait_recv_one(j)
            gate_lane.wait_recv_one(j)

        def to_expert(n):
            p = lax.rem(me.p + n, P)
            hot = pick[h, p]
            stage[h, p] = nn(hot, h_all[h]).astype(jnp.bfloat16)
            g = jnp.broadcast_to(gate_all[h, pl.ds(z.expert(me, p), 1), :], (8, R))
            wide = jnp.concatenate([hot.astype(jnp.float32), jnp.zeros((LANES - CAP, R), jnp.float32)], axis=0)
            g_stage[h, p] = exact("nt", g, wide)
            @pl.when(n > 0)
            def _():
                row_lane(h).start_one(n)
                g_lane(h).start_one(n)
        times(P, to_expert)
        xin[h, me.p] = stage[h, me.p]
        gin[h, me.p] = g_stage[h, me.p]
    times(H, dispatch)
    for copy in loads:
        copy.wait()
    down_lane.wait_recv()
    per = tile // CAP

    def chunk(j):
        h = lax.rem(me.h + H - lax.rem(j + 1, H), H)
        row_lane(h).wait_recv()
        g_lane(h).wait_recv()

        def rows(r):
            some = pl.ds(pl.multiple_of(r * per, per), per)
            part = pl.ds(pl.multiple_of((h * P + r * per) * CAP, CAP), tile)
            for p in range(per):
                column = jnp.broadcast_to(gin[h, r * per + p, 0:1, :], (LANES, LANES)).T
                g_col[p * CAP : (p + 1) * CAP, :] = column[0:CAP, :]
            x = xin[h, some].reshape(tile, D)
            gate = nn(x, wv[0])
            up = nn(x, wv[1])
            sig = jax.nn.sigmoid(gate)
            act = gate * sig
            hidden = (act * up).astype(jnp.bfloat16)
            hid[part, :] = hidden
            out = nt(hidden, wv[2]).astype(jnp.bfloat16)
            result[h, some] = out.reshape(per, CAP, D)
            upstream = cot_v[h, some].reshape(tile, D).astype(jnp.float32)
            d_gates = residual_scale * jnp.sum(upstream * out.astype(jnp.float32), axis=-1, keepdims=True)
            d_out = (residual_scale * g_col[:, 0:1] * upstream).astype(jnp.bfloat16)
            d_res[part, :] = d_out
            d_hidden = nn(d_out, wv[2])
            dg = (d_hidden * up * sig * (1.0 + gate * (1.0 - sig))).astype(jnp.bfloat16)
            du = (d_hidden * act).astype(jnp.bfloat16)
            d_gate[part, :] = dg
            d_up[part, :] = du
            d_rows[h, some] = (nt(dg, wv[0]) + nt(du, wv[1])).astype(jnp.bfloat16).reshape(per, CAP, D)
            g_col[...] = jnp.broadcast_to(d_gates, (tile, LANES))
            for p in range(per):
                column = jnp.concatenate(
                    [g_col[p * CAP : (p + 1) * CAP, :], jnp.zeros((LANES - CAP, LANES), jnp.float32)], axis=0)
                dg_stage[h, r * per + p] = column.T[0:8, :]
        times(P // per, rows)
        back_lane(h).start()
        dg_lane(h).start()
        d_in[h, me.p] = d_rows[h, me.p]
        dg_in[h, me.p] = dg_stage[h, me.p]
    times(H, chunk)

    def cut(d):
        part = pl.ds(pl.multiple_of(d * 256, 256), 256)
        x = xin[:, :, :, part].reshape(H * P * CAP, 256)
        grads[0, part, :] = tn(x, d_gate[...]).astype(jnp.bfloat16)
        grads[1, part, :] = tn(x, d_up[...]).astype(jnp.bfloat16)
        grads[2, part, :] = tn(d_res[:, part], hid[...]).astype(jnp.bfloat16)
    times(D // 256, cut)

    def collect(j):
        n = lax.rem(j + 1, H)
        h = lax.rem(me.h + H - n, H)
        back_lane(h).wait_recv()
        dg_lane(h).wait_recv()
        part = tn(pick[h].reshape(P * CAP, R), d_in[h].reshape(P * CAP, D))
        turn_stage[h] = jnp.zeros((EXPERTS, R), jnp.float32)

        def gates_of(p):
            row = jnp.broadcast_to(dg_in[h, p, 0:1, 0:CAP], (8, CAP))
            turn_stage[h, pl.ds(z.expert(me, p), 1), :] = exact("nn", row, pick[h, p].astype(jnp.float32))[0:1, :]
        times(P, gates_of)
        @pl.when(n > 0)
        def _():
            part_stage[h] = part.astype(jnp.bfloat16)
            part_lane.start_one(H - n)
            turn_lane.start_one(H - n)
        @pl.when(n == 0)
        def _():
            d_mid[...] = part
            turn_v[...] = jnp.zeros((LANES, R), jnp.float32)
            turn_v[0:EXPERTS, :] = turn_stage[h]
    times(H, collect)
    part_lane.wait_recv()
    turn_lane.wait_recv()

    def add(n):
        h = lax.rem(me.h + n + 1, H)
        d_mid[...] += part_in[h].astype(jnp.float32)
        turn_v[0:EXPERTS, :] += turn_in[h]
    times(H - 1, add)
    gts = gates_t[...].T
    dgs = turn_v[...].T
    d_log = gts * (dgs - jnp.sum(gts * dgs, axis=-1, keepdims=True))
    g_small[...] = exact("tn", h2[...].astype(jnp.float32), d_log)
    d_h2 = d_mid[...] + exact("nt", d_log, small[...].astype(jnp.float32))
    mid = middle[...]
    inverse = lax.rsqrt(jnp.mean(mid * mid, axis=-1, keepdims=True) + norm_eps)
    n2 = mid * inverse
    gain_out[...] = jnp.broadcast_to(jnp.sum(d_h2 * n2, axis=0, keepdims=True), (8, D))
    gain_two = small[...].astype(jnp.float32).T[EXPERTS + 1 : EXPERTS + 2, :]
    g = d_h2 * gain_two
    dm = cot[...].astype(jnp.float32) + inverse * (g - n2 * jnp.mean(g * n2, axis=-1, keepdims=True))
    d_mid[...] = dm
    d_attn[...] = (residual_scale * dm).astype(jnp.bfloat16)
    for lane in [h_lane, gate_lane, down_lane, part_lane, turn_lane]:
        lane.wait_send()

    def drain(h):
        for lane in [row_lane, g_lane, back_lane, dg_lane]:
            lane(h).wait_send()
    times(H, drain)


def second_call(z, R, ff, dc, pick, h2, gates_t, middle, cot, small, w_downt, wt, cot_in):
    H, P = z.H, z.P
    rows = H * P * CAP
    tile = 8 * CAP
    f = jnp.float32
    ins = [(pick, 1), (h2, 1), (gates_t, 1), (middle, 1), (cot, 1), (small, 1), (w_downt, 0), (wt, 0), (cot_in, 0)]
    outs = [
        (shape_of((R, D), f), 1), (shape_of((R, D)), 1), (shape_of((D, LANES), f), 1), (shape_of((8, D), f), 1),
        (shape_of((H, P, CAP, D)), 1), (shape_of((3, D, ff)), 1), (shape_of((H, EXPERTS, R), f), 1),
    ]
    scratch = [
        vmem((H, R, D)), vmem((H, P, CAP, D)), vmem((H, P, CAP, D)), vmem((H, P, 8, LANES), f), vmem((H, P, 8, LANES), f),
        vmem((3, D, ff)), vmem((H, P, CAP, D)), vmem((H, P, CAP, D)), vmem((H, P, CAP, D)), vmem((H, P, 8, LANES), f),
        vmem((H, P, 8, LANES), f), vmem((rows, ff)), vmem((rows, ff)), vmem((rows, ff)), vmem((rows, D)),
        vmem((tile, LANES), f), vmem((H, R, D)), vmem((H, R, D)), vmem((H, EXPERTS, R), f), vmem((H, EXPERTS, R), f),
        vmem((LANES, R), f), pltpu.SemaphoreType.DMA((4,)),
    ] + sem_pairs(z, SECOND_GROUPS) + [pltpu.SemaphoreType.DMA((H, P)) for _ in range(2 * SECOND_GRIDS)]
    return call(z, functools.partial(second_kernel, z, R, dc, tile), "second", 1, ins, outs, scratch)


THIRD_GROUPS = ["line", "col", "line", "world", "world", "fsdp", "ctx", "ctx", "ctx"]


def third_kernel(z, R, dc, d_attn, h1, q_all, k2, v2, lse, att_f, wc, place, freq, g_small, gain_two, middle, d_mid, tok,
                 small, pick, gate_all, tok_all, wo, result, grads,
                 output, grad_tokens, gc_in, gs_in, go_in, gw_in,
                 d_all, wo_c, tok_v, d_qkv, ds_v, p_v, q_v, dm_v, dk_acc, dv_acc, place_col, place_row, dn_stage, dn_in,
                 sib_in, gc_stage, go_stage, gs_stage, gain_v, out_in, mix_hi, mix_lo, mix_stage, mix_in, own_w, own_sem,
                 fwd_send, fwd_recv, sib_send, sib_recv, out_send, out_recv, *sems):
    me = z.place(lax.axis_index("ctx"), lax.axis_index("fsdp"))
    C, F, H, P, J, rs, qw = z.C, z.F, z.H, z.P, z.J, z.rows_w, z.q_width
    L = C * R
    pair = lambda i: (sems[2 * i], sems[2 * i + 1])
    up_lane = Lane(z, me, "line", lambda to: d_attn, lambda p: d_all.at[p.c], *pair(0))
    up_relay = Relay(z, me, d_attn, lambda c: d_all.at[c], fwd_send, fwd_recv)
    mix_lane = Lane(z, me, "col", lambda to: mix_stage.at[to.h], lambda p: mix_in.at[p.h], *pair(1))
    dn_lane = Lane(z, me, "line", lambda to: dn_stage.at[to.c], lambda p: dn_in.at[lax.div(p.c, 2)], *pair(2))
    gc_lane = Lane(z, me, "world", lambda to: rows_at(gc_stage, to.w, rs), lambda p: gc_in.at[p.w], *pair(3))
    gs_lane = Lane(z, me, "world", lambda to: rows_at(gs_stage, to.w, rs), lambda p: gs_in.at[p.w], *pair(4))
    go_lane = Lane(z, me, "fsdp", lambda to: rows_at(go_stage, to.f, rs), lambda p: go_in.at[p.f], *pair(5))
    grad_lanes = [
        Lane(z, me, "ctx", lambda to, j=j: rows_at(grads.at[j], to.c, dc), lambda p, j=j: gw_in.at[j, p.s, p.m], *pair(6 + j))
        for j in range(3)
    ]

    def out_lane(h):
        return Lane(z, me, "plane", lambda to: result.at[h, to.p], lambda p: out_in.at[h, p.p], out_send.at[h], out_recv.at[h])

    def sib_copy(j):
        block = dn_stage.at[2 * j + 1 - me.k]
        return pltpu.make_async_remote_copy(
            src_ref=block, dst_ref=sib_in.at[j], send_sem=sib_send.at[j], recv_sem=sib_recv.at[j],
            device_id=(me.c + 1 - 2 * me.k, me.f), device_id_type=MESH)
    wo_load = pltpu.make_async_copy(rows_at(wo, me.c, qw), wo_c, own_sem.at[0])
    tok_load = pltpu.make_async_copy(tok_all, tok_v, own_sem.at[1])
    out_load = pltpu.make_async_copy(result.at[:, me.p], out_in.at[:, me.p], own_sem.at[2])
    own_loads = [
        pltpu.make_async_copy(rows_at(grads.at[j], me.c, dc), own_w.at[j], own_sem.at[3 + j]) for j in range(3)
    ]
    for copy in [wo_load, tok_load, out_load] + own_loads:
        copy.start()
    meet(z, me, ["world"])
    up_relay.start_own()
    up_lane.start()
    for h in range(H):
        out_lane(h).start()
    for lane in grad_lanes:
        lane.start()

    own_stores = []
    for j in range(3):
        own_loads[j].wait()
        own_stores.append(pltpu.make_async_copy(own_w.at[j], gw_in.at[j, me.s, me.m], own_sem.at[9 + j]))
        own_stores[-1].start()
    d_all[me.c] = d_attn[...]
    dk_acc[...] = jnp.zeros((L, LANES), jnp.float32)
    dv_acc[...] = jnp.zeros((L, LANES), jnp.float32)

    def columns(c):
        row = place[c][0:1, :].astype(jnp.float32)
        place_row[c] = jnp.broadcast_to(row, (8, R))
        place_col[pl.ds(pl.multiple_of(c * R, R), R), :] = jnp.broadcast_to(row, (R, R)).T
    times(C, columns)
    wo_load.wait()
    head_of = lax.div(lane_of((R, LANES)), HEAD)

    def attend(i):
        n = lax.rem(i, J)
        c = up_relay.member(n, jnp.where(i < J, me.k, 1 - me.k))
        @pl.when(jnp.logical_and(i > 0, i < J))
        def _():
            up_lane.wait_recv_one(n)
            up_relay.start_one(n)
        @pl.when(i >= J)
        def _():
            up_relay.wait_recv_one(n)
        part = pl.ds(pl.multiple_of(c * R, R), R)
        q = q_all[part, :]
        d_mix = nt(d_all[c], wo_c[...])
        if qw < LANES:
            d_mix = jnp.concatenate([d_mix, jnp.zeros((R, LANES - qw), jnp.float32)], axis=1)
        d_mix = d_mix.astype(jnp.bfloat16)
        row = jnp.concatenate([place_row[i, 0:1, :] for i in range(C)], axis=1)
        column = place_col[part, :]
        allowed = row <= column[:, 0:1]
        dq = jnp.zeros((R, LANES), jnp.float32)
        for h in range(z.q_heads):
            mine = head_of == h
            rows = pl.ds(h * R, R)
            q_h = jnp.where(mine, q, jnp.zeros_like(q))
            dm_h = jnp.where(mine, d_mix, jnp.zeros_like(d_mix))
            q_v[rows, :] = q_h
            dm_v[rows, :] = dm_h
            s = jnp.where(allowed, nt(q_h, k2[...]) * score_scale, masked_score)
            p = jnp.exp(s - lse[h, part, 0:1])
            p_v[rows, :] = p.astype(jnp.bfloat16)
            delta = jnp.sum(dm_h.astype(jnp.float32) * att_f[part, :], axis=-1, keepdims=True)
            ds = (p * (nt(dm_h, v2[...]) - delta)).astype(jnp.bfloat16)
            ds_v[rows, :] = ds
            dq = jnp.where(mine, nn(ds, k2[...]) * score_scale, dq)
        dk_acc[...] += tn(ds_v[...], q_v[...])
        dv_acc[...] += tn(p_v[...], dm_v[...])
        cosine, sine = rope_tables(column, freq[0:1, :])
        d_qkv[part, 0:LANES] = rope(dq, cosine, -sine).astype(jnp.bfloat16)
    times(C, attend)

    def finish_kv(c):
        part = pl.ds(pl.multiple_of(c * R, R), R)
        dk = dk_acc[part, :] * score_scale
        dv = dv_acc[part, :]
        dk = dk + pltpu.roll(dk, HEAD, 1)
        dv = dv + pltpu.roll(dv, HEAD, 1)
        cosine, sine = rope_tables(place_col[part, :], freq[1:2, :])
        d_qkv[part, LANES : 2 * LANES] = rope(jnp.where(head_of == 0, dk, dv), cosine, -sine).astype(jnp.bfloat16)
    times(C, finish_kv)
    tok_load.wait()
    gain_v[...] = jnp.zeros((LANES, D), jnp.float32)

    def down(c):
        dn = nt(d_qkv[pl.ds(pl.multiple_of(c * R, R), R), :], wc[...])
        x = tok_v[c].astype(jnp.float32)
        n1 = x * lax.rsqrt(jnp.mean(x * x, axis=-1, keepdims=True) + norm_eps)
        gain_v[EXPERTS : EXPERTS + 1, :] += jnp.sum(dn * n1, axis=0, keepdims=True)
        return dn

    def for_sibling(j):
        c = 2 * j + 1 - me.k
        dn_stage[c] = down(c).astype(jnp.bfloat16)
        sib_copy(j).start()
    times(J, for_sibling)

    def for_line(i):
        n = lax.rem(i + 1, J)
        to = z.peer("line", me, n)
        dn = down(to.c)
        j = lax.div(to.c, 2)
        sib_copy(j).wait_recv()
        dn_stage[to.c] = (dn + sib_in[j].astype(jnp.float32)).astype(jnp.bfloat16)
        @pl.when(n > 0)
        def _():
            dn_lane.start_one(n)
    times(J, for_line)
    dn_in[lax.div(me.c, 2)] = dn_stage[me.c]

    def weights(d):
        part = pl.ds(pl.multiple_of(d * 256, 256), 256)
        gc_stage[part, :] = tn(h1[:, part], d_qkv[...]).astype(jnp.bfloat16)
    times(D // 256, weights)
    gc_lane.start()
    go_stage[...] = tn(att_f[...].astype(jnp.bfloat16), d_all[...].reshape(L, D)).astype(jnp.bfloat16)
    go_lane.start()
    gain_v[EXPERTS + 1 : EXPERTS + 2, :] = gain_two[0:1, :]
    gs_stage[...] = (g_small[...] + gain_v[...].T).astype(jnp.bfloat16)
    gs_lane.start()
    own_last = [
        pltpu.make_async_copy(rows_at(gc_stage, me.w, rs), gc_in.at[me.w], own_sem.at[15]),
        pltpu.make_async_copy(rows_at(gs_stage, me.w, rs), gs_in.at[me.w], own_sem.at[16]),
        pltpu.make_async_copy(rows_at(go_stage, me.f, rs), go_in.at[me.f], own_sem.at[17]),
    ]
    for copy in own_last:
        copy.start()

    out_load.wait()

    def mix(i):
        n = lax.rem(i + 1, H)
        h = lax.rem(me.h + H - n, H)

        def weigh(p):
            g = gate_all[h, pl.ds(z.expert(me, p), 1), :] * pick[h, p].astype(jnp.float32)
            high = g.astype(jnp.bfloat16)
            mix_hi[p] = high
            mix_lo[p] = (g - high.astype(jnp.float32)).astype(jnp.bfloat16)
        times(P, weigh)
        out_lane(h).wait_recv()
        rows = out_in[h].reshape(P * CAP, D)
        total = tn(mix_hi[...].reshape(P * CAP, R), rows) + tn(mix_lo[...].reshape(P * CAP, R), rows)
        mix_stage[h] = total.astype(jnp.bfloat16)
        @pl.when(n > 0)
        def _():
            mix_lane.start_one(H - n)
        @pl.when(n == 0)
        def _():
            grad_tokens[...] = total
    times(H, mix)
    mix_lane.wait_recv()

    def add(n):
        grad_tokens[...] += mix_in[lax.rem(me.h + n + 1, H)].astype(jnp.float32)
    times(H - 1, add)
    output[...] = (middle[...] + residual_scale * grad_tokens[...]).astype(jnp.bfloat16)

    dn_lane.wait_recv()
    d_h1 = dn_in[0].astype(jnp.float32)
    for c in range(1, J):
        d_h1 = d_h1 + dn_in[c].astype(jnp.float32)
    x = tok[...].astype(jnp.float32)
    inverse = lax.rsqrt(jnp.mean(x * x, axis=-1, keepdims=True) + norm_eps)
    n1 = x * inverse
    g = d_h1 * small[...].astype(jnp.float32).T[EXPERTS : EXPERTS + 1, :]
    grad_tokens[...] = d_mid[...] + inverse * (g - n1 * jnp.mean(g * n1, axis=-1, keepdims=True))
    for lane in [gc_lane, gs_lane, go_lane] + grad_lanes:
        lane.wait_recv()
    for lane in [up_lane, mix_lane, dn_lane, gc_lane, gs_lane, go_lane] + grad_lanes:
        lane.wait_send()
    up_relay.wait_send()
    times(J, lambda j: sib_copy(j).wait_send())
    for h in range(H):
        out_lane(h).wait_send()
    for copy in own_stores + own_last:
        copy.wait()


def third_call(z, R, ff, dc, *arrays):
    C, F, N, H, P, J, S, rs, qw = z.C, z.F, z.N, z.H, z.P, z.J, z.S, z.rows_w, z.q_width
    L, f = C * R, jnp.float32
    heads = z.q_heads * R
    ins = [(a, 1) for a in arrays[:-4]] + [(a, 0) for a in arrays[-4:]]
    outs = [
        (shape_of((R, D)), 1), (shape_of((R, D), f), 1), (shape_of((N, rs, 2 * LANES)), 0), (shape_of((N, rs, LANES)), 0),
        (shape_of((F, rs, D)), 0), (shape_of((3, S, z.G, dc, ff)), 0),
    ]
    scratch = [
        vmem((C, R, D)), vmem((qw, D)), vmem((C, R, D)), vmem((L, 2 * LANES)), vmem((heads, L)), vmem((heads, L)),
        vmem((heads, LANES)), vmem((heads, LANES)), vmem((L, LANES), f), vmem((L, LANES), f), vmem((L, R), f),
        vmem((C, 8, R), f), vmem((C, R, D)), vmem((J, R, D)), vmem((J, R, D)), vmem((D, 2 * LANES)), vmem((LANES, D)),
        vmem((D, LANES)), vmem((LANES, D), f), vmem((H, P, CAP, D)), vmem((P, CAP, R)), vmem((P, CAP, R)), vmem((H, R, D)),
        vmem((H, R, D)), vmem((3, dc, ff)), pltpu.SemaphoreType.DMA((18,)),
    ] + [pltpu.SemaphoreType.DMA((J,)) for _ in range(4)] + [pltpu.SemaphoreType.DMA((H, P)) for _ in range(2)] + sem_pairs(z, THIRD_GROUPS)
    return call(z, functools.partial(third_kernel, z, R, dc), "third", 2, ins, outs, scratch)


def local(z, tokens, norm_first, w_query, w_key, w_value, w_out, norm_second, w_router,
          w_gate, w_up, w_down, positions, routes, cotangent):
    C, F = z.C, z.F
    R = tokens.shape[1]
    rs = z.rows_w
    ff = w_gate.shape[2]
    dc = D // C

    heads_q = jnp.pad(w_query.reshape(rs, C, z.q_width), ((0, 0), (0, 0), (0, LANES - z.q_width)))
    heads_k = jnp.repeat(w_key.reshape(rs, KV_HEADS, HEAD), z.share, axis=1)
    heads_v = jnp.repeat(w_value.reshape(rs, KV_HEADS, HEAD), z.share, axis=1)
    w_pack = jnp.concatenate([heads_q, heads_k, heads_v], axis=2).transpose(1, 0, 2)
    small = jnp.concatenate(
        [w_router, norm_first[:, None], norm_second[:, None], jnp.zeros((rs, 128 - EXPERTS - 2), jnp.bfloat16)], axis=1)
    place_pack = jnp.broadcast_to(positions[0][None, :], (8, R))
    w_downt = w_down.transpose(0, 2, 1)
    (tok_all, w_c, small_all, wo, place_all, wt, cot_in, h1, q_all, k2, v2, lse, att_f, middle, h2, gates_t, pick) = first_call(
        z, R, ff, dc, tokens[0], place_pack, routes[0], cotangent[0], w_pack, small, w_out, w_gate, w_up)
    d_mid, d_attn, g_small, g_gain_two, result, grads, gate_all = second_call(
        z, R, ff, dc, pick, h2, gates_t, middle, cotangent[0], small_all, w_downt, wt, cot_in)
    output, grad_tokens, gc_in, gs_in, go_in, gw_in = third_call(
        z, R, ff, dc, d_attn, h1, q_all, k2, v2, lse, att_f, w_c, place_all, frequencies(), g_small, g_gain_two, middle, d_mid,
        tokens[0], small_all, pick, gate_all, tok_all, wo, result, grads)
    gc = jnp.sum(f32(gc_in).reshape(C, F, rs, 2 * LANES), axis=1)
    join = lambda a: a.reshape(KV_HEADS, z.share, rs, HEAD).sum(axis=1).transpose(1, 0, 2).reshape(rs, KV_HEADS * HEAD)
    gs = jnp.sum(f32(gs_in), axis=0)
    return (
        output[None],
        grad_tokens[None],
        gs[:, EXPERTS],
        gc[:, :, : z.q_width].transpose(1, 0, 2).reshape(rs, D),
        join(gc[:, :, LANES : LANES + HEAD]),
        join(gc[:, :, LANES + HEAD :]),
        jnp.sum(f32(go_in), axis=0),
        gs[:, EXPERTS + 1],
        gs[:, :EXPERTS],
        jnp.sum(f32(gw_in[0]), axis=0),
        jnp.sum(f32(gw_in[1]), axis=0),
        jnp.sum(f32(gw_in[2]), axis=0).transpose(0, 2, 1),
    )


def solution(mesh):
    row = P(("ctx", "fsdp"), None)
    vec = P(("ctx", "fsdp"))
    seq = P("fsdp", "ctx", None)
    down = P("fsdp", None, "ctx")
    return jax.shard_map(
        functools.partial(local, Sizes(mesh)),
        mesh=mesh,
        in_specs=(seq, vec, row, row, row, row, vec, row, seq, seq, down, P("fsdp", "ctx"), seq, seq),
        out_specs=(seq, seq, vec, row, row, row, row, vec, row, seq, seq, down),
        check_vma=False,
    )
```

```python
import collections
import functools

import jax
import jax.numpy as jnp
import numpy as np
from jax import lax
from jax.experimental import pallas as pl
from jax.experimental.pallas import tpu as pltpu
from jax.sharding import PartitionSpec as P

D = 1024
HEADS = 16
KV_HEADS = 8
HEAD = 64
EXPERTS = 32
TOP = 8
CAP = 48
LANES = 128

residual_scale = 0.22
score_scale = 0.015625
rope_base = 10000.0
norm_eps = 1e-06
masked_score = -1e30

MESH = pl.DeviceIdType.MESH
Place = collections.namedtuple("Place", ["c", "f", "m", "s", "h", "k", "p", "w"])


class Sizes:
    def __init__(self, mesh):
        self.C = mesh.shape["ctx"]
        self.F = mesh.shape["fsdp"]
        self.N = self.C * self.F
        self.G = EXPERTS // self.F
        self.S = self.C // self.G
        self.H = self.G // 2
        self.P = 2 * self.F
        self.J = self.C // 2
        self.q_heads = HEADS // self.C
        self.q_width = self.q_heads * HEAD
        self.share = self.C // KV_HEADS
        self.rows_w = D // self.N

    def place(self, c, f):
        k = lax.rem(c, 2)
        return Place(c, f, lax.rem(c, self.G), lax.div(c, self.G), lax.rem(lax.div(c, 2), self.H), k, f * 2 + k, c * self.F + f)

    def count(self, group):
        return {"ctx": self.C, "fsdp": self.F, "world": self.N, "col": self.H, "line": self.J, "plane": self.P}[group]

    def peer(self, group, me, n):
        if group == "ctx":
            return self.place(lax.rem(me.c + n, self.C), me.f)
        if group == "fsdp":
            return self.place(me.c, lax.rem(me.f + n, self.F))
        if group == "world":
            w = lax.rem(me.w + n, self.N)
            return self.place(lax.div(w, self.F), lax.rem(w, self.F))
        if group == "col":
            return self.place(me.s * self.G + 2 * lax.rem(me.h + n, self.H) + me.k, me.f)
        if group == "line":
            return self.place(2 * lax.rem(lax.div(me.c, 2) + n, self.J) + me.k, me.f)
        p = lax.rem(me.p + n, self.P)
        return self.place(me.s * self.G + 2 * me.h + lax.rem(p, 2), lax.div(p, 2))

    def expert(self, me, p):
        return lax.div(p, 2) * self.G + 2 * me.h + lax.rem(p, 2)


def bf(x):
    return x.astype(jnp.bfloat16)


def f32(x):
    return x.astype(jnp.float32)


def shape_of(shape, dtype=jnp.bfloat16):
    return jax.ShapeDtypeStruct(shape, dtype)


class Lane:
    def __init__(self, sizes, me, group, src, dst, sends, recvs):
        self.sizes, self.me, self.group, self.src, self.dst = sizes, me, group, src, dst
        self.sends, self.recvs, self.n = sends, recvs, sizes.count(group)

    def copy(self, k, to, source, landing):
        return pltpu.make_async_remote_copy(
            src_ref=source, dst_ref=landing, send_sem=self.sends.at[k], recv_sem=self.recvs.at[k],
            device_id=(to.c, to.f), device_id_type=MESH)

    def to(self, k):
        return self.sizes.peer(self.group, self.me, k)

    def start_one(self, k):
        to = self.to(k)
        self.copy(k, to, self.src(to), self.dst(self.me)).start()

    def wait_recv_one(self, k):
        landed = self.dst(self.sizes.peer(self.group, self.me, self.n - k))
        self.copy(k, self.to(k), landed, landed).wait_recv()

    def wait_send_one(self, k):
        to = self.to(k)
        self.copy(k, to, self.src(to), self.dst(self.me)).wait_send()

    def each(self, step):
        def one(k, carry):
            step(k)
            return carry
        lax.fori_loop(1, self.n, one, 0)

    def start(self):
        self.each(self.start_one)

    def wait_recv(self):
        self.each(self.wait_recv_one)

    def wait_send(self):
        self.each(self.wait_send_one)


class Relay:
    def __init__(self, sizes, me, own, landing, sends, recvs):
        self.sizes, self.me, self.own, self.landing, self.sends, self.recvs = sizes, me, own, landing, sends, recvs

    def member(self, n, core):
        J = self.sizes.J
        return 2 * lax.rem(lax.div(self.me.c, 2) + J - n, J) + core

    def copy(self, n, source, landing):
        return pltpu.make_async_remote_copy(
            src_ref=source, dst_ref=landing, send_sem=self.sends.at[n], recv_sem=self.recvs.at[n],
            device_id=(self.me.c + 1 - 2 * self.me.k, self.me.f), device_id_type=MESH)

    def start_own(self):
        self.copy(0, self.own, self.landing(self.me.c)).start()

    def start_one(self, n):
        here = self.landing(self.member(n, self.me.k))
        self.copy(n, here, here).start()

    def wait_recv_one(self, n):
        there = self.landing(self.member(n, 1 - self.me.k))
        self.copy(n, there, there).wait_recv()

    def wait_send(self):
        def one(n, carry):
            here = self.landing(self.member(n, self.me.k))
            self.copy(n, here, here).wait_send()
            return carry
        lax.fori_loop(0, self.sizes.J, one, 0)


def meet(sizes, me, groups):
    barrier = pltpu.get_barrier_semaphore()
    total = 0
    for group in groups:
        def greet(k, carry, group=group):
            p = sizes.peer(group, me, k)
            pl.semaphore_signal(barrier, inc=1, device_id=(p.c, p.f), device_id_type=MESH)
            return carry
        lax.fori_loop(1, sizes.count(group), greet, 0)
        total += sizes.count(group) - 1
    pl.semaphore_wait(barrier, total)


def times(n, step, first=0):
    def one(i, carry):
        step(i)
        return carry
    lax.fori_loop(first, n, one, 0)


def column_lane(z, me, c, source, landing, sends, recvs):
    return Lane(z, me, "fsdp", lambda to: source(c, to), lambda p: landing(c, p), sends.at[c], recvs.at[c])


def nn(a, b):
    return lax.dot_general(a, b, (((1,), (0,)), ((), ())), preferred_element_type=jnp.float32)


def nt(a, b):
    return lax.dot_general(a, b, (((1,), (1,)), ((), ())), preferred_element_type=jnp.float32)


def tn(a, b):
    return lax.dot_general(a, b, (((0,), (0,)), ((), ())), preferred_element_type=jnp.float32)


def lane_of(shape):
    return lax.broadcasted_iota(jnp.int32, shape, 1)


def rope_tables(place_columns, frequency):
    angles = place_columns.astype(jnp.float32) * frequency
    return jnp.cos(angles), jnp.sin(angles)


def rope(x, cosine, sine):
    half = HEAD // 2
    mixed = jnp.where(lax.rem(lane_of(x.shape), HEAD) < half, -pltpu.roll(x, LANES - half, 1), pltpu.roll(x, half, 1))
    return x * cosine + mixed * sine


def sem_pairs(sizes, groups):
    return [pltpu.SemaphoreType.DMA((sizes.count(g),)) for g in groups for _ in range(2)]


FIRST_GROUPS = ["line", "ctx", "ctx", "ctx", "line", "col", "col", "ctx", "ctx", "ctx"]


def first_kernel(z, R, dc, tok, place, routes, cot, freq, w_pack, small, w_out, w_gate, w_up,
                 tok_out, wc_out, small_out, wo_out, place_out, wt, cot_in, h1, q_all, k2, v2, lse, att_f, middle, h2, gates_t,
                 pick, tok_all, place_all, wc_v, small_v, wo_v, cot_all, slot_all, cot_stage, att_stage, att_in, own_w,
                 place_col, place_row, slot_t, own_sem, fwd_send, fwd_recv, wo_send, wo_recv, cot_send, cot_recv, *sems):
    me = z.place(lax.axis_index("ctx"), lax.axis_index("fsdp"))
    C, F, H, P, J, rs, qw = z.C, z.F, z.H, z.P, z.J, z.rows_w, z.q_width
    L = C * R
    pair = lambda i: (sems[2 * i], sems[2 * i + 1])
    tok_lane = Lane(z, me, "line", lambda to: tok, lambda p: tok_all.at[p.c], *pair(0))
    tok_relay = Relay(z, me, tok, lambda c: tok_all.at[c], fwd_send, fwd_recv)
    place_lane = Lane(z, me, "ctx", lambda to: place, lambda p: place_all.at[p.c], *pair(1))
    wc_lane = Lane(z, me, "ctx", lambda to: w_pack.at[to.c], lambda p: rows_at(wc_v, p.w, rs), *pair(2))
    small_lane = Lane(z, me, "ctx", lambda to: small, lambda p: rows_at(small_v, p.w, rs), *pair(3))
    wo_lane = Lane(z, me, "line", lambda to: w_out, lambda p: rows_at(wo_v, p.w, rs), *pair(4))
    wo_relay = Relay(z, me, w_out, lambda c: rows_at(wo_v, c * F + me.f, rs), wo_send, wo_recv)
    cols = sems[2 * len(FIRST_GROUPS) :]

    def column(i, c):
        ref = (wc_v, small_v, wo_v)[i]
        return column_lane(z, me, c, lambda c, to: rows_at(ref, c * F + me.f, rs), lambda c, p: rows_at(ref, c * F + p.f, rs),
                           cols[2 * i], cols[2 * i + 1])
    cot_lane = Lane(z, me, "col", lambda to: cot, lambda p: cot_all.at[p.h], *pair(5))
    slot_lane = Lane(z, me, "col", lambda to: slot_t.at[pl.ds(0, EXPERTS), :], lambda p: slot_all.at[p.h], *pair(6))
    weights = [w_gate, w_up]
    cut = [pl.ds(0, dc), pl.ds(0, dc // 2)]
    weight_lanes = [
        Lane(z, me, "ctx", lambda to, j=j: weights[j].at[to.m, cut[j]], lambda p, j=j: wt.at[j, p.c, cut[j]], *pair(7 + j))
        for j in range(2)
    ]
    att_lane = Lane(z, me, "ctx", lambda to: att_stage.at[to.c], lambda p: att_in.at[p.c], *pair(9))

    def rows_lane(h):
        return Lane(z, me, "plane", lambda to: cot_stage.at[h, to.p], lambda p: cot_in.at[h, p.p], cot_send.at[h], cot_recv.at[h])
    meet(z, me, ["ctx", "plane", "fsdp"])
    wc_lane.start()
    small_lane.start()
    place_lane.start()
    tok_relay.start_own()
    tok_lane.start()
    wo_relay.start_own()
    wo_lane.start()
    cot_lane.start()

    own = [
        pltpu.make_async_copy(w_pack.at[me.c], rows_at(wc_v, me.w, rs), own_sem.at[0]),
        pltpu.make_async_copy(small, rows_at(small_v, me.w, rs), own_sem.at[1]),
        pltpu.make_async_copy(w_out, rows_at(wo_v, me.w, rs), own_sem.at[2]),
    ]
    own_loads = [pltpu.make_async_copy(weights[j].at[me.m], own_w.at[j], own_sem.at[3 + j]) for j in range(2)]
    for copy in own + own_loads:
        copy.start()
    tok_all[me.c] = tok[...]
    place_all[me.c] = place[...]
    cot_all[me.h] = cot[...]

    named = jnp.zeros((R, LANES), jnp.float32)
    for j in range(TOP):
        named = jnp.where(routes[:, j : j + 1] == lane_of((R, LANES)), 1.0, named)
    row_id = lax.broadcasted_iota(jnp.int32, (R, R), 0)
    before = jnp.where(row_id > lane_of((R, R)), 1.0, 0.0).astype(jnp.bfloat16)
    slot = nn(before, named.astype(jnp.bfloat16))
    slot_t[...] = jnp.where(named > 0.5, slot, -1.0).T
    slot_all[me.h] = slot_t[0:EXPERTS, :]
    slot_lane.start()
    slot_id = lax.broadcasted_iota(jnp.int32, (CAP, R), 0).astype(jnp.float32)

    def dispatch(j):
        h = lax.rem(me.h + H - j, H)
        lane = rows_lane(h)
        @pl.when(j > 0)
        def _():
            cot_lane.wait_recv_one(j)
            slot_lane.wait_recv_one(j)

        def to_expert(n):
            p = lax.rem(me.p + n, P)
            row = slot_all[h, pl.ds(z.expert(me, p), 1), :]
            hot = jnp.where(row == slot_id, 1.0, 0.0).astype(jnp.bfloat16)
            pick[h, p] = hot
            cot_stage[h, p] = nn(hot, cot_all[h]).astype(jnp.bfloat16)
            @pl.when(n > 0)
            def _():
                lane.start_one(n)
        times(P, to_expert)
    dispatch(0)
    weight_lanes[0].start()
    own_stores = []
    for j in range(2):
        own_loads[j].wait()
        own_stores.append(pltpu.make_async_copy(own_w.at[j, cut[j]], wt.at[j, me.c, cut[j]], own_sem.at[7 + j]))
        own_stores[j].start()

    for copy in own:
        copy.wait()
    for i, lane in enumerate([wc_lane, small_lane]):
        lane.wait_recv()
        times(C, lambda c, i=i: column(i, c).start())
    place_lane.wait_recv()
    for i in range(2):
        times(C, lambda c, i=i: column(i, c).wait_recv())
    gain_one = small_v[...].astype(jnp.float32).T[EXPERTS : EXPERTS + 1, :]
    gain_two = small_v[...].astype(jnp.float32).T[EXPERTS + 1 : EXPERTS + 2, :]
    head_of = lax.div(lane_of((R, LANES)), HEAD)

    def project(i):
        n = lax.rem(i, J)
        c = tok_relay.member(n, jnp.where(i < J, me.k, 1 - me.k))
        @pl.when(jnp.logical_and(i > 0, i < J))
        def _():
            tok_lane.wait_recv_one(n)
            tok_relay.start_one(n)
        @pl.when(i >= J)
        def _():
            tok_relay.wait_recv_one(n)
        x = tok_all[c].astype(jnp.float32)
        inverse = lax.rsqrt(jnp.mean(x * x, axis=-1, keepdims=True) + norm_eps)
        h = (x * inverse * gain_one).astype(jnp.bfloat16)
        part = pl.ds(pl.multiple_of(c * R, R), R)
        h1[part, :] = h
        qkv = nn(h, wc_v[...])
        row = place_all[c][0:1, :].astype(jnp.float32)
        place_row[c] = jnp.broadcast_to(row, (8, R))
        column = jnp.broadcast_to(row, (R, R)).T
        place_col[part, :] = column
        q_all[part, :] = rope(qkv[:, :LANES], *rope_tables(column, freq[0:1, :])).astype(jnp.bfloat16)
        kv = rope(qkv[:, LANES:], *rope_tables(column, freq[1:2, :]))
        swapped = pltpu.roll(kv, HEAD, 1)
        k2[part, :] = jnp.where(head_of == 0, kv, swapped).astype(jnp.bfloat16)
        v2[part, :] = jnp.where(head_of == 0, swapped, kv).astype(jnp.bfloat16)
    times(C, project)
    wo_lane.wait_recv()
    times(J, wo_relay.start_one, 1)

    def attend(c):
        part = pl.ds(pl.multiple_of(c * R, R), R)
        q = q_all[part, :]
        row = jnp.concatenate([place_row[i, 0:1, :] for i in range(C)], axis=1)
        allowed = row <= place_col[part, 0:1]
        total = jnp.zeros((R, LANES), jnp.float32)
        for h in range(z.q_heads):
            mine = head_of == h
            s = nt(jnp.where(mine, q, jnp.zeros_like(q)), k2[...]) * score_scale
            s = jnp.where(allowed, s, masked_score)
            top = jnp.max(s, axis=-1, keepdims=True)
            e = jnp.exp(s - top)
            weight = jnp.sum(e, axis=-1, keepdims=True)
            lse[h, part, :] = jnp.broadcast_to(top + jnp.log(weight), (R, LANES))
            total = jnp.where(mine, nn(e.astype(jnp.bfloat16), v2[...]) / weight, total)
        att_f[part, :] = total
        att_stage[c] = total.astype(jnp.bfloat16)
    times(C // 2, attend)
    times(J, wo_relay.wait_recv_one)
    times(C, lambda c: column(2, c).start())
    times(C, attend, C // 2)
    att_lane.start()
    weight_lanes[1].start()
    att_in[me.c] = att_stage[me.c]
    times(H, dispatch, 1)
    own_cot = pltpu.make_async_copy(cot_stage.at[:, me.p], cot_in.at[:, me.p], own_sem.at[6])
    own_cot.start()
    times(C, lambda c: column(2, c).wait_recv())
    att_lane.wait_recv()
    x = tok[...].astype(jnp.float32)
    mixed = jnp.zeros((R, D), jnp.float32)
    for c in range(C):
        mixed = mixed + nn(att_in[c][:, :qw], wo_v[c * qw : (c + 1) * qw, :])
    mid = x + residual_scale * mixed
    middle[...] = mid
    inverse = lax.rsqrt(jnp.mean(mid * mid, axis=-1, keepdims=True) + norm_eps)
    hidden = (mid * inverse * gain_two).astype(jnp.bfloat16)
    h2[...] = hidden
    chosen = slot_t[...].T > -0.5
    logits = jnp.where(chosen, nn(hidden, small_v[...]), masked_score)
    raised = jnp.where(chosen, jnp.exp(logits - jnp.max(logits, axis=-1, keepdims=True)), 0.0)
    gates_t[...] = (raised / jnp.sum(raised, axis=-1, keepdims=True)).T

    outs = [
        pltpu.make_async_copy(source, out, own_sem.at[10 + i])
        for i, (source, out) in enumerate([(tok_all, tok_out), (wc_v, wc_out), (small_v, small_out), (wo_v, wo_out), (place_all, place_out)])
    ]
    for copy in outs:
        copy.start()
    tok_relay.wait_send()
    wo_relay.wait_send()
    for lane in [tok_lane, place_lane, wc_lane, small_lane, wo_lane, cot_lane, slot_lane, att_lane]:
        lane.wait_send()
    for i in range(3):
        times(C, lambda c, i=i: column(i, c).wait_send())
    for h in range(H):
        rows_lane(h).wait_recv()
        rows_lane(h).wait_send()
    for lane in weight_lanes:
        lane.wait_recv()
        lane.wait_send()
    for copy in outs + own_stores + [own_cot]:
        copy.wait()


def rows_at(ref, i, n):
    return ref.at[pl.ds(pl.multiple_of(i * n, n), n), :]


def vmem(shape, dtype=jnp.bfloat16):
    return pltpu.VMEM(shape, dtype)


def call(z, kernel, name, collective_id, ins, outs, scratch, **kw):
    space = lambda fast: pl.BlockSpec(memory_space=pltpu.VMEM if fast else pl.ANY)
    return pl.pallas_call(
        kernel, name=name,
        out_shape=[o for o, _ in outs], in_specs=[space(f) for _, f in ins], out_specs=[space(f) for _, f in outs],
        scratch_shapes=scratch,
        compiler_params=pltpu.CompilerParams(
            collective_id=collective_id, has_side_effects=True, vmem_limit_bytes=60000 * 1024),
    )(*[a for a, _ in ins])


def first_call(z, R, ff, dc, tok, place, routes, cot, w_pack, small, w_out, w_gate, w_up):
    C, F, H, P = z.C, z.F, z.H, z.P
    L = C * R
    ins = [(tok, 1), (place, 1), (routes, 1), (cot, 1), (frequencies(), 1), (w_pack, 0), (small, 0), (w_out, 0),
           (w_gate, 0), (w_up, 0)]
    f = jnp.float32
    outs = [
        (shape_of((C, R, D)), 0), (shape_of((D, 2 * LANES)), 0), (shape_of((D, LANES)), 0), (shape_of((D, D)), 0),
        (shape_of((C, 8, R), jnp.int32), 0), (shape_of((2, C, dc, ff)), 0), (shape_of((H, P, CAP, D)), 0),
        (shape_of((L, D)), 1), (shape_of((L, LANES)), 1), (shape_of((L, LANES)), 1), (shape_of((L, LANES)), 1),
        (shape_of((z.q_heads, L, LANES), f), 1), (shape_of((L, LANES), f), 1), (shape_of((R, D), f), 1),
        (shape_of((R, D)), 1), (shape_of((LANES, R), f), 1), (shape_of((H, P, CAP, R)), 1),
    ]
    sem = lambda a, b: [pltpu.SemaphoreType.DMA((a, b)), pltpu.SemaphoreType.DMA((a, b))]
    scratch = [
        vmem((C, R, D)), vmem((C, 8, R), jnp.int32), vmem((D, 2 * LANES)), vmem((D, LANES)), vmem((D, D)),
        vmem((H, R, D)), vmem((H, EXPERTS, R), f), vmem((H, P, CAP, D)), vmem((C, R, LANES)), vmem((C, R, LANES)),
        vmem((2, dc, ff)), vmem((L, R), f), vmem((C, 8, R), f), vmem((LANES, R), f), pltpu.SemaphoreType.DMA((16,)),
    ] + [pltpu.SemaphoreType.DMA((z.J,)) for _ in range(4)] + sem(H, P) + sem_pairs(z, FIRST_GROUPS) + sem(C, F) * 3
    return call(z, functools.partial(first_kernel, z, R, dc), "first", 0, ins, outs, scratch)


def frequencies():
    lanes = np.arange(LANES)
    steps = rope_base ** ((lanes % (HEAD // 2)) * (-2.0 / HEAD))
    return jnp.asarray(np.stack([steps, np.where(lanes < HEAD, steps, 0.0)] + [steps] * 6), jnp.float32)


SECOND_GROUPS = ["col", "col", "ctx", "col", "col", "ctx"]
SECOND_GRIDS = 4


def exact(kind, a, b):
    dims = {"nn": ((1,), (0,)), "nt": ((1,), (1,)), "tn": ((0,), (0,))}[kind]
    return lax.dot_general(a, b, (dims, ((), ())), precision=lax.Precision.HIGHEST, preferred_element_type=jnp.float32)


def second_kernel(z, R, dc, tile, pick, h2, gates_t, middle, cot, small, w_up, w_downt, wt, cot_in,
                  d_mid, d_attn, g_small, gain_out, result, grads, gate_all,
                  h_all, stage, xin, g_stage, gin, wv, cot_v, d_rows, d_in, dg_stage, dg_in, hid, d_gate, d_up, d_res,
                  g_col, part_stage, part_in, turn_stage, turn_in, turn_v, own_sem, *sems):
    me = z.place(lax.axis_index("ctx"), lax.axis_index("fsdp"))
    C, F, H, P = z.C, z.F, z.H, z.P
    pair = lambda i: (sems[2 * i], sems[2 * i + 1])
    grid = lambda i, h: (sems[2 * len(SECOND_GROUPS) + 2 * i].at[h], sems[2 * len(SECOND_GROUPS) + 2 * i + 1].at[h])
    h_lane = Lane(z, me, "col", lambda to: h2, lambda p: h_all.at[p.h], *pair(0))
    gate_lane = Lane(z, me, "col", lambda to: gates_t.at[pl.ds(0, EXPERTS), :], lambda p: gate_all.at[p.h], *pair(1))
    down_lane = Lane(z, me, "ctx", lambda to: w_downt.at[to.m], lambda p: wv.at[2, p.c], *pair(2))
    rest, have = pl.ds(dc // 2, dc // 2), pl.ds(0, dc // 2)
    up_lane = Lane(z, me, "ctx", lambda to: w_up.at[to.m, rest], lambda p: wv.at[1, p.c, rest], *pair(5))
    part_lane = Lane(z, me, "col", lambda to: part_stage.at[to.h], lambda p: part_in.at[p.h], *pair(3))
    turn_lane = Lane(z, me, "col", lambda to: turn_stage.at[to.h], lambda p: turn_in.at[p.h], *pair(4))
    plane = lambda i, h, source, landing: Lane(
        z, me, "plane", lambda to: source.at[h, to.p], lambda p: landing.at[h, p.p], *grid(i, h))
    row_lane = lambda h: plane(0, h, stage, xin)
    g_lane = lambda h: plane(1, h, g_stage, gin)
    back_lane = lambda h: plane(2, h, d_rows, d_in)
    dg_lane = lambda h: plane(3, h, dg_stage, dg_in)
    loads = [
        pltpu.make_async_copy(wt.at[0], wv.at[0], own_sem.at[0]),
        pltpu.make_async_copy(wt.at[1, :, have], wv.at[1, :, have], own_sem.at[1]),
        pltpu.make_async_copy(cot_in, cot_v, own_sem.at[2]),
        pltpu.make_async_copy(w_downt.at[me.m], wv.at[2, me.c], own_sem.at[3]),
        pltpu.make_async_copy(w_up.at[me.m, rest], wv.at[1, me.c, rest], own_sem.at[4]),
    ]
    for copy in loads:
        copy.start()
    meet(z, me, ["ctx", "plane"])
    h_lane.start()
    gate_lane.start()
    up_lane.start()
    down_lane.start()
    h_all[me.h] = h2[...]
    gate_all[me.h] = gates_t[0:EXPERTS, :]

    def dispatch(j):
        h = lax.rem(me.h + H - j, H)
        @pl.when(j > 0)
        def _():
            h_lane.wait_recv_one(j)
            gate_lane.wait_recv_one(j)

        def to_expert(n):
            p = lax.rem(me.p + n, P)
            hot = pick[h, p]
            stage[h, p] = nn(hot, h_all[h]).astype(jnp.bfloat16)
            g = jnp.broadcast_to(gate_all[h, pl.ds(z.expert(me, p), 1), :], (8, R))
            wide = jnp.concatenate([hot.astype(jnp.float32), jnp.zeros((LANES - CAP, R), jnp.float32)], axis=0)
            g_stage[h, p] = exact("nt", g, wide)
            @pl.when(n > 0)
            def _():
                row_lane(h).start_one(n)
                g_lane(h).start_one(n)
        times(P, to_expert)
        xin[h, me.p] = stage[h, me.p]
        gin[h, me.p] = g_stage[h, me.p]
    times(H, dispatch)
    for copy in loads:
        copy.wait()
    up_lane.wait_recv()
    down_lane.wait_recv()
    wg, wu, wd = [wv.at[j].reshape(D, wv.shape[3]) for j in range(3)]
    per = tile // CAP

    def chunk(j):
        h = lax.rem(me.h + H - lax.rem(j + 1, H), H)
        row_lane(h).wait_recv()
        g_lane(h).wait_recv()

        def rows(r):
            some = pl.ds(pl.multiple_of(r * per, per), per)
            part = pl.ds(pl.multiple_of((h * P + r * per) * CAP, CAP), tile)
            for p in range(per):
                column = jnp.broadcast_to(gin[h, r * per + p, 0:1, :], (LANES, LANES)).T
                g_col[p * CAP : (p + 1) * CAP, :] = column[0:CAP, :]
            x = xin[h, some].reshape(tile, D)
            gate = nn(x, wg[...])
            up = nn(x, wu[...])
            sig = jax.nn.sigmoid(gate)
            act = gate * sig
            hidden = (act * up).astype(jnp.bfloat16)
            hid[part, :] = hidden
            out = nt(hidden, wd[...]).astype(jnp.bfloat16)
            result[h, some] = out.reshape(per, CAP, D)
            upstream = cot_v[h, some].reshape(tile, D).astype(jnp.float32)
            d_gates = residual_scale * jnp.sum(upstream * out.astype(jnp.float32), axis=-1, keepdims=True)
            d_out = (residual_scale * g_col[:, 0:1] * upstream).astype(jnp.bfloat16)
            d_res[part, :] = d_out
            d_hidden = nn(d_out, wd[...])
            dg = (d_hidden * up * sig * (1.0 + gate * (1.0 - sig))).astype(jnp.bfloat16)
            du = (d_hidden * act).astype(jnp.bfloat16)
            d_gate[part, :] = dg
            d_up[part, :] = du
            d_rows[h, some] = (nt(dg, wg[...]) + nt(du, wu[...])).astype(jnp.bfloat16).reshape(per, CAP, D)
            g_col[...] = jnp.broadcast_to(d_gates, (tile, LANES))
            for p in range(per):
                column = jnp.concatenate(
                    [g_col[p * CAP : (p + 1) * CAP, :], jnp.zeros((LANES - CAP, LANES), jnp.float32)], axis=0)
                dg_stage[h, r * per + p] = column.T[0:8, :]
        times(P // per, rows)
        back_lane(h).start()
        dg_lane(h).start()
        d_in[h, me.p] = d_rows[h, me.p]
        dg_in[h, me.p] = dg_stage[h, me.p]
    times(H, chunk)

    def cut(d):
        part = pl.ds(pl.multiple_of(d * 256, 256), 256)
        x = xin[:, :, :, part].reshape(H * P * CAP, 256)
        grads[0, part, :] = tn(x, d_gate[...]).astype(jnp.bfloat16)
        grads[1, part, :] = tn(x, d_up[...]).astype(jnp.bfloat16)
        grads[2, part, :] = tn(d_res[:, part], hid[...]).astype(jnp.bfloat16)
    times(D // 256, cut)

    def collect(j):
        n = lax.rem(j + 1, H)
        h = lax.rem(me.h + H - n, H)
        back_lane(h).wait_recv()
        dg_lane(h).wait_recv()
        part = tn(pick[h].reshape(P * CAP, R), d_in[h].reshape(P * CAP, D))
        turn_stage[h] = jnp.zeros((EXPERTS, R), jnp.float32)

        def gates_of(p):
            row = jnp.broadcast_to(dg_in[h, p, 0:1, 0:CAP], (8, CAP))
            turn_stage[h, pl.ds(z.expert(me, p), 1), :] = exact("nn", row, pick[h, p].astype(jnp.float32))[0:1, :]
        times(P, gates_of)
        @pl.when(n > 0)
        def _():
            part_stage[h] = part.astype(jnp.bfloat16)
            part_lane.start_one(H - n)
            turn_lane.start_one(H - n)
        @pl.when(n == 0)
        def _():
            d_mid[...] = part
            turn_v[...] = jnp.zeros((LANES, R), jnp.float32)
            turn_v[0:EXPERTS, :] = turn_stage[h]
    times(H, collect)
    part_lane.wait_recv()
    turn_lane.wait_recv()

    def add(n):
        h = lax.rem(me.h + n + 1, H)
        d_mid[...] += part_in[h].astype(jnp.float32)
        turn_v[0:EXPERTS, :] += turn_in[h]
    times(H - 1, add)
    gts = gates_t[...].T
    dgs = turn_v[...].T
    d_log = gts * (dgs - jnp.sum(gts * dgs, axis=-1, keepdims=True))
    g_small[...] = exact("tn", h2[...].astype(jnp.float32), d_log)
    d_h2 = d_mid[...] + exact("nt", d_log, small[...].astype(jnp.float32))
    mid = middle[...]
    inverse = lax.rsqrt(jnp.mean(mid * mid, axis=-1, keepdims=True) + norm_eps)
    n2 = mid * inverse
    gain_out[...] = jnp.broadcast_to(jnp.sum(d_h2 * n2, axis=0, keepdims=True), (8, D))
    gain_two = small[...].astype(jnp.float32).T[EXPERTS + 1 : EXPERTS + 2, :]
    g = d_h2 * gain_two
    dm = cot[...].astype(jnp.float32) + inverse * (g - n2 * jnp.mean(g * n2, axis=-1, keepdims=True))
    d_mid[...] = dm
    d_attn[...] = (residual_scale * dm).astype(jnp.bfloat16)
    for lane in [h_lane, gate_lane, up_lane, down_lane, part_lane, turn_lane]:
        lane.wait_send()

    def drain(h):
        for lane in [row_lane, g_lane, back_lane, dg_lane]:
            lane(h).wait_send()
    times(H, drain)


def second_call(z, R, ff, dc, pick, h2, gates_t, middle, cot, small, w_up, w_downt, wt, cot_in):
    H, P = z.H, z.P
    rows = H * P * CAP
    tile = 8 * CAP
    f = jnp.float32
    ins = [(pick, 1), (h2, 1), (gates_t, 1), (middle, 1), (cot, 1), (small, 1), (w_up, 0), (w_downt, 0), (wt, 0), (cot_in, 0)]
    outs = [
        (shape_of((R, D), f), 1), (shape_of((R, D)), 1), (shape_of((D, LANES), f), 1), (shape_of((8, D), f), 1),
        (shape_of((H, P, CAP, D)), 1), (shape_of((3, D, ff)), 1), (shape_of((H, EXPERTS, R), f), 1),
    ]
    scratch = [
        vmem((H, R, D)), vmem((H, P, CAP, D)), vmem((H, P, CAP, D)), vmem((H, P, 8, LANES), f), vmem((H, P, 8, LANES), f),
        vmem((3, z.C, dc, ff)), vmem((H, P, CAP, D)), vmem((H, P, CAP, D)), vmem((H, P, CAP, D)), vmem((H, P, 8, LANES), f),
        vmem((H, P, 8, LANES), f), vmem((rows, ff)), vmem((rows, ff)), vmem((rows, ff)), vmem((rows, D)),
        vmem((tile, LANES), f), vmem((H, R, D)), vmem((H, R, D)), vmem((H, EXPERTS, R), f), vmem((H, EXPERTS, R), f),
        vmem((LANES, R), f), pltpu.SemaphoreType.DMA((5,)),
    ] + sem_pairs(z, SECOND_GROUPS) + [pltpu.SemaphoreType.DMA((H, P)) for _ in range(2 * SECOND_GRIDS)]
    return call(z, functools.partial(second_kernel, z, R, dc, tile), "second", 1, ins, outs, scratch)


THIRD_GROUPS = ["line", "col", "line", "ctx", "ctx", "fsdp", "ctx", "ctx", "ctx"]


def third_kernel(z, R, dc, d_attn, h1, q_all, k2, v2, lse, att_f, wc, place, freq, g_small, gain_two, middle, d_mid, tok,
                 small, pick, gate_all, tok_all, wo, result, grads,
                 output, grad_tokens, gc_in, gs_in, go_in, gw_in,
                 d_all, wo_c, tok_v, d_qkv, ds_v, p_v, q_v, dm_v, dk_acc, dv_acc, place_col, place_row, dn_stage, dn_in,
                 sib_in, gc_stage, go_stage, gs_stage, gc_x, gs_x, gc_sum, gs_sum, gain_v, out_in, mix_hi, mix_lo, mix_stage, mix_in, own_w, own_sem,
                 own_cols, fwd_send, fwd_recv, sib_send, sib_recv, out_send, out_recv, *sems):
    me = z.place(lax.axis_index("ctx"), lax.axis_index("fsdp"))
    C, F, H, P, J, rs, qw = z.C, z.F, z.H, z.P, z.J, z.rows_w, z.q_width
    L = C * R
    pair = lambda i: (sems[2 * i], sems[2 * i + 1])
    up_lane = Lane(z, me, "line", lambda to: d_attn, lambda p: d_all.at[p.c], *pair(0))
    up_relay = Relay(z, me, d_attn, lambda c: d_all.at[c], fwd_send, fwd_recv)
    mix_lane = Lane(z, me, "col", lambda to: mix_stage.at[to.h], lambda p: mix_in.at[p.h], *pair(1))
    dn_lane = Lane(z, me, "line", lambda to: dn_stage.at[to.c], lambda p: dn_in.at[lax.div(p.c, 2)], *pair(2))
    gc_lane = Lane(z, me, "ctx", lambda to: gc_sum.at[to.c], lambda p: gc_in.at[p.c], *pair(3))
    gs_lane = Lane(z, me, "ctx", lambda to: gs_sum.at[to.c], lambda p: gs_in.at[p.c], *pair(4))
    cols = sems[2 * len(THIRD_GROUPS) :]

    def column(i, c):
        source, landing = ((gc_stage, gc_x), (gs_stage, gs_x))[i]
        return column_lane(z, me, c, lambda c, to: rows_at(source, c * F + to.f, rs), lambda c, p: landing.at[p.f, c],
                           cols[2 * i], cols[2 * i + 1])
    go_lane = Lane(z, me, "fsdp", lambda to: rows_at(go_stage, to.f, rs), lambda p: go_in.at[p.f], *pair(5))
    grad_lanes = [
        Lane(z, me, "ctx", lambda to, j=j: rows_at(grads.at[j], to.c, dc), lambda p, j=j: gw_in.at[j, p.s, p.m], *pair(6 + j))
        for j in range(3)
    ]

    def out_lane(h):
        return Lane(z, me, "plane", lambda to: result.at[h, to.p], lambda p: out_in.at[h, p.p], out_send.at[h], out_recv.at[h])

    def sib_copy(j):
        block = dn_stage.at[2 * j + 1 - me.k]
        return pltpu.make_async_remote_copy(
            src_ref=block, dst_ref=sib_in.at[j], send_sem=sib_send.at[j], recv_sem=sib_recv.at[j],
            device_id=(me.c + 1 - 2 * me.k, me.f), device_id_type=MESH)
    wo_load = pltpu.make_async_copy(rows_at(wo, me.c, qw), wo_c, own_sem.at[0])
    tok_load = pltpu.make_async_copy(tok_all, tok_v, own_sem.at[1])
    out_load = pltpu.make_async_copy(result.at[:, me.p], out_in.at[:, me.p], own_sem.at[2])
    own_loads = [
        pltpu.make_async_copy(rows_at(grads.at[j], me.c, dc), own_w.at[j], own_sem.at[3 + j]) for j in range(3)
    ]
    for copy in [wo_load, tok_load, out_load] + own_loads:
        copy.start()
    meet(z, me, ["ctx", "plane", "fsdp"])
    up_relay.start_own()
    up_lane.start()
    for h in range(H):
        out_lane(h).start()
    for lane in grad_lanes:
        lane.start()

    own_stores = []
    for j in range(3):
        own_loads[j].wait()
        own_stores.append(pltpu.make_async_copy(own_w.at[j], gw_in.at[j, me.s, me.m], own_sem.at[9 + j]))
        own_stores[-1].start()
    d_all[me.c] = d_attn[...]
    dk_acc[...] = jnp.zeros((L, LANES), jnp.float32)
    dv_acc[...] = jnp.zeros((L, LANES), jnp.float32)

    def columns(c):
        row = place[c][0:1, :].astype(jnp.float32)
        place_row[c] = jnp.broadcast_to(row, (8, R))
        place_col[pl.ds(pl.multiple_of(c * R, R), R), :] = jnp.broadcast_to(row, (R, R)).T
    times(C, columns)
    wo_load.wait()
    head_of = lax.div(lane_of((R, LANES)), HEAD)

    def attend(i):
        n = lax.rem(i, J)
        c = up_relay.member(n, jnp.where(i < J, me.k, 1 - me.k))
        @pl.when(jnp.logical_and(i > 0, i < J))
        def _():
            up_lane.wait_recv_one(n)
            up_relay.start_one(n)
        @pl.when(i >= J)
        def _():
            up_relay.wait_recv_one(n)
        part = pl.ds(pl.multiple_of(c * R, R), R)
        q = q_all[part, :]
        d_mix = nt(d_all[c], wo_c[...])
        if qw < LANES:
            d_mix = jnp.concatenate([d_mix, jnp.zeros((R, LANES - qw), jnp.float32)], axis=1)
        d_mix = d_mix.astype(jnp.bfloat16)
        row = jnp.concatenate([place_row[i, 0:1, :] for i in range(C)], axis=1)
        column = place_col[part, :]
        allowed = row <= column[:, 0:1]
        dq = jnp.zeros((R, LANES), jnp.float32)
        for h in range(z.q_heads):
            mine = head_of == h
            rows = pl.ds(h * R, R)
            q_h = jnp.where(mine, q, jnp.zeros_like(q))
            dm_h = jnp.where(mine, d_mix, jnp.zeros_like(d_mix))
            q_v[rows, :] = q_h
            dm_v[rows, :] = dm_h
            s = jnp.where(allowed, nt(q_h, k2[...]) * score_scale, masked_score)
            p = jnp.exp(s - lse[h, part, 0:1])
            p_v[rows, :] = p.astype(jnp.bfloat16)
            delta = jnp.sum(dm_h.astype(jnp.float32) * att_f[part, :], axis=-1, keepdims=True)
            ds = (p * (nt(dm_h, v2[...]) - delta)).astype(jnp.bfloat16)
            ds_v[rows, :] = ds
            dq = jnp.where(mine, nn(ds, k2[...]) * score_scale, dq)
        dk_acc[...] += tn(ds_v[...], q_v[...])
        dv_acc[...] += tn(p_v[...], dm_v[...])
        cosine, sine = rope_tables(column, freq[0:1, :])
        d_qkv[part, 0:LANES] = rope(dq, cosine, -sine).astype(jnp.bfloat16)
    times(C, attend)

    def finish_kv(c):
        part = pl.ds(pl.multiple_of(c * R, R), R)
        dk = dk_acc[part, :] * score_scale
        dv = dv_acc[part, :]
        dk = dk + pltpu.roll(dk, HEAD, 1)
        dv = dv + pltpu.roll(dv, HEAD, 1)
        cosine, sine = rope_tables(place_col[part, :], freq[1:2, :])
        d_qkv[part, LANES : 2 * LANES] = rope(jnp.where(head_of == 0, dk, dv), cosine, -sine).astype(jnp.bfloat16)
    times(C, finish_kv)
    tok_load.wait()
    gain_v[...] = jnp.zeros((LANES, D), jnp.float32)

    def down(c):
        dn = nt(d_qkv[pl.ds(pl.multiple_of(c * R, R), R), :], wc[...])
        x = tok_v[c].astype(jnp.float32)
        n1 = x * lax.rsqrt(jnp.mean(x * x, axis=-1, keepdims=True) + norm_eps)
        gain_v[EXPERTS : EXPERTS + 1, :] += jnp.sum(dn * n1, axis=0, keepdims=True)
        return dn

    def for_sibling(j):
        c = 2 * j + 1 - me.k
        dn_stage[c] = down(c).astype(jnp.bfloat16)
        sib_copy(j).start()
    times(J, for_sibling)

    def for_line(i):
        n = lax.rem(i + 1, J)
        to = z.peer("line", me, n)
        dn = down(to.c)
        j = lax.div(to.c, 2)
        sib_copy(j).wait_recv()
        dn_stage[to.c] = (dn + sib_in[j].astype(jnp.float32)).astype(jnp.bfloat16)
        @pl.when(n > 0)
        def _():
            dn_lane.start_one(n)
    times(J, for_line)
    dn_in[lax.div(me.c, 2)] = dn_stage[me.c]

    def weights(d):
        part = pl.ds(pl.multiple_of(d * 256, 256), 256)
        gc_stage[part, :] = tn(h1[:, part], d_qkv[...]).astype(jnp.bfloat16)
    times(D // 256, weights)
    times(C, lambda c: column(0, c).start())
    gain_v[EXPERTS + 1 : EXPERTS + 2, :] = gain_two[0:1, :]
    gs_stage[...] = (g_small[...] + gain_v[...].T).astype(jnp.bfloat16)
    times(C, lambda c: column(1, c).start())
    own_last = [
        pltpu.make_async_copy(rows_at(gc_stage, c * F + me.f, rs), gc_x.at[me.f, c], own_cols.at[0, c]) for c in range(C)
    ] + [
        pltpu.make_async_copy(rows_at(gs_stage, c * F + me.f, rs), gs_x.at[me.f, c], own_cols.at[1, c]) for c in range(C)
    ]
    for copy in own_last:
        copy.start()
    go_stage[...] = tn(att_f[...].astype(jnp.bfloat16), d_all[...].reshape(L, D)).astype(jnp.bfloat16)
    go_lane.start()
    own_go = pltpu.make_async_copy(rows_at(go_stage, me.f, rs), go_in.at[me.f], own_sem.at[17])
    own_go.start()
    for copy in own_last:
        copy.wait()
    for i in range(2):
        times(C, lambda c, i=i: column(i, c).wait_recv())
    gc_total = gc_x[0].astype(jnp.float32)
    gs_total = gs_x[0].astype(jnp.float32)
    for f in range(1, F):
        gc_total = gc_total + gc_x[f].astype(jnp.float32)
        gs_total = gs_total + gs_x[f].astype(jnp.float32)
    gc_sum[...] = gc_total.astype(jnp.bfloat16)
    gs_sum[...] = gs_total.astype(jnp.bfloat16)
    gc_lane.start()
    gs_lane.start()
    own_sums = [
        pltpu.make_async_copy(gc_sum.at[me.c], gc_in.at[me.c], own_sem.at[15]),
        pltpu.make_async_copy(gs_sum.at[me.c], gs_in.at[me.c], own_sem.at[16]),
    ]
    for copy in own_sums:
        copy.start()

    out_load.wait()

    def mix(i):
        n = lax.rem(i + 1, H)
        h = lax.rem(me.h + H - n, H)

        def weigh(p):
            g = gate_all[h, pl.ds(z.expert(me, p), 1), :] * pick[h, p].astype(jnp.float32)
            high = g.astype(jnp.bfloat16)
            mix_hi[p] = high
            mix_lo[p] = (g - high.astype(jnp.float32)).astype(jnp.bfloat16)
        times(P, weigh)
        out_lane(h).wait_recv()
        rows = out_in[h].reshape(P * CAP, D)
        total = tn(mix_hi[...].reshape(P * CAP, R), rows) + tn(mix_lo[...].reshape(P * CAP, R), rows)
        mix_stage[h] = total.astype(jnp.bfloat16)
        @pl.when(n > 0)
        def _():
            mix_lane.start_one(H - n)
        @pl.when(n == 0)
        def _():
            grad_tokens[...] = total
    times(H, mix)
    mix_lane.wait_recv()

    def add(n):
        grad_tokens[...] += mix_in[lax.rem(me.h + n + 1, H)].astype(jnp.float32)
    times(H - 1, add)
    output[...] = (middle[...] + residual_scale * grad_tokens[...]).astype(jnp.bfloat16)

    dn_lane.wait_recv()
    d_h1 = dn_in[0].astype(jnp.float32)
    for c in range(1, J):
        d_h1 = d_h1 + dn_in[c].astype(jnp.float32)
    x = tok[...].astype(jnp.float32)
    inverse = lax.rsqrt(jnp.mean(x * x, axis=-1, keepdims=True) + norm_eps)
    n1 = x * inverse
    g = d_h1 * small[...].astype(jnp.float32).T[EXPERTS : EXPERTS + 1, :]
    grad_tokens[...] = d_mid[...] + inverse * (g - n1 * jnp.mean(g * n1, axis=-1, keepdims=True))
    for lane in [gc_lane, gs_lane, go_lane] + grad_lanes:
        lane.wait_recv()
    for lane in [up_lane, mix_lane, dn_lane, gc_lane, gs_lane, go_lane] + grad_lanes:
        lane.wait_send()
    up_relay.wait_send()
    times(J, lambda j: sib_copy(j).wait_send())
    for h in range(H):
        out_lane(h).wait_send()
    for i in range(2):
        times(C, lambda c, i=i: column(i, c).wait_send())
    for copy in own_stores + own_sums + [own_go]:
        copy.wait()


def third_call(z, R, ff, dc, *arrays):
    C, F, N, H, P, J, S, rs, qw = z.C, z.F, z.N, z.H, z.P, z.J, z.S, z.rows_w, z.q_width
    L, f = C * R, jnp.float32
    heads = z.q_heads * R
    ins = [(a, 1) for a in arrays[:-4]] + [(a, 0) for a in arrays[-4:]]
    outs = [
        (shape_of((R, D)), 1), (shape_of((R, D), f), 1), (shape_of((C, rs, 2 * LANES)), 0), (shape_of((C, rs, LANES)), 0),
        (shape_of((F, rs, D)), 0), (shape_of((3, S, z.G, dc, ff)), 0),
    ]
    scratch = [
        vmem((C, R, D)), vmem((qw, D)), vmem((C, R, D)), vmem((L, 2 * LANES)), vmem((heads, L)), vmem((heads, L)),
        vmem((heads, LANES)), vmem((heads, LANES)), vmem((L, LANES), f), vmem((L, LANES), f), vmem((L, R), f),
        vmem((C, 8, R), f), vmem((C, R, D)), vmem((J, R, D)), vmem((J, R, D)), vmem((D, 2 * LANES)), vmem((LANES, D)),
        vmem((D, LANES)), vmem((F, C, rs, 2 * LANES)), vmem((F, C, rs, LANES)), vmem((C, rs, 2 * LANES)), vmem((C, rs, LANES)),
        vmem((LANES, D), f), vmem((H, P, CAP, D)), vmem((P, CAP, R)), vmem((P, CAP, R)), vmem((H, R, D)),
        vmem((H, R, D)), vmem((3, dc, ff)), pltpu.SemaphoreType.DMA((18,)), pltpu.SemaphoreType.DMA((2, C)),
    ] + [pltpu.SemaphoreType.DMA((J,)) for _ in range(4)] + [pltpu.SemaphoreType.DMA((H, P)) for _ in range(2)] + sem_pairs(z, THIRD_GROUPS) + [pltpu.SemaphoreType.DMA((C, F)) for _ in range(4)]
    return call(z, functools.partial(third_kernel, z, R, dc), "third", 2, ins, outs, scratch)


def local(z, tokens, norm_first, w_query, w_key, w_value, w_out, norm_second, w_router,
          w_gate, w_up, w_down, positions, routes, cotangent):
    C, F = z.C, z.F
    R = tokens.shape[1]
    rs = z.rows_w
    ff = w_gate.shape[2]
    dc = D // C

    heads_q = jnp.pad(w_query.reshape(rs, C, z.q_width), ((0, 0), (0, 0), (0, LANES - z.q_width)))
    heads_k = jnp.repeat(w_key.reshape(rs, KV_HEADS, HEAD), z.share, axis=1)
    heads_v = jnp.repeat(w_value.reshape(rs, KV_HEADS, HEAD), z.share, axis=1)
    w_pack = jnp.concatenate([heads_q, heads_k, heads_v], axis=2).transpose(1, 0, 2)
    small = jnp.concatenate(
        [w_router, norm_first[:, None], norm_second[:, None], jnp.zeros((rs, 128 - EXPERTS - 2), jnp.bfloat16)], axis=1)
    place_pack = jnp.broadcast_to(positions[0][None, :], (8, R))
    w_downt = w_down.transpose(0, 2, 1)
    (tok_all, w_c, small_all, wo, place_all, wt, cot_in, h1, q_all, k2, v2, lse, att_f, middle, h2, gates_t, pick) = first_call(
        z, R, ff, dc, tokens[0], place_pack, routes[0], cotangent[0], w_pack, small, w_out, w_gate, w_up)
    d_mid, d_attn, g_small, g_gain_two, result, grads, gate_all = second_call(
        z, R, ff, dc, pick, h2, gates_t, middle, cotangent[0], small_all, w_up, w_downt, wt, cot_in)
    output, grad_tokens, gc_in, gs_in, go_in, gw_in = third_call(
        z, R, ff, dc, d_attn, h1, q_all, k2, v2, lse, att_f, w_c, place_all, frequencies(), g_small, g_gain_two, middle, d_mid,
        tokens[0], small_all, pick, gate_all, tok_all, wo, result, grads)
    gc = f32(gc_in)
    join = lambda a: a.reshape(KV_HEADS, z.share, rs, HEAD).sum(axis=1).transpose(1, 0, 2).reshape(rs, KV_HEADS * HEAD)
    gs = jnp.sum(f32(gs_in), axis=0)
    return (
        output[None],
        grad_tokens[None],
        gs[:, EXPERTS],
        gc[:, :, : z.q_width].transpose(1, 0, 2).reshape(rs, D),
        join(gc[:, :, LANES : LANES + HEAD]),
        join(gc[:, :, LANES + HEAD :]),
        jnp.sum(f32(go_in), axis=0),
        gs[:, EXPERTS + 1],
        gs[:, :EXPERTS],
        jnp.sum(f32(gw_in[0]), axis=0),
        jnp.sum(f32(gw_in[1]), axis=0),
        jnp.sum(f32(gw_in[2]), axis=0).transpose(0, 2, 1),
    )


def solution(mesh):
    row = P(("ctx", "fsdp"), None)
    vec = P(("ctx", "fsdp"))
    seq = P("fsdp", "ctx", None)
    down = P("fsdp", None, "ctx")
    return jax.shard_map(
        functools.partial(local, Sizes(mesh)),
        mesh=mesh,
        in_specs=(seq, vec, row, row, row, row, vec, row, seq, seq, down, P("fsdp", "ctx"), seq, seq),
        out_specs=(seq, seq, vec, row, row, row, row, vec, row, seq, seq, down),
        check_vma=False,
    )
```

```python
import collections
import functools
import types

import jax
import jax.numpy as jnp
import numpy as np
from jax import lax
from jax.experimental import pallas as pl
from jax.experimental.pallas import tpu as pltpu
from jax.sharding import PartitionSpec as P

D = 1024
HEADS = 16
KV_HEADS = 8
HEAD = 64
EXPERTS = 32
TOP = 8
CAP = 48
LANES = 128

residual_scale = 0.22
score_scale = 0.015625
rope_base = 10000.0
norm_eps = 1e-06
masked_score = -1e30

MESH = pl.DeviceIdType.MESH
Place = collections.namedtuple("Place", ["c", "f", "m", "s", "h", "k", "p", "w"])


class Sizes:
    def __init__(self, mesh):
        self.C = mesh.shape["ctx"]
        self.F = mesh.shape["fsdp"]
        self.N = self.C * self.F
        self.G = EXPERTS // self.F
        self.S = self.C // self.G
        self.H = self.G // 2
        self.P = 2 * self.F
        self.J = self.C // 2
        self.q_heads = HEADS // self.C
        self.q_width = self.q_heads * HEAD
        self.share = self.C // KV_HEADS
        self.rows_w = D // self.N

    def place(self, c, f):
        k = lax.rem(c, 2)
        return Place(c, f, lax.rem(c, self.G), lax.div(c, self.G), lax.rem(lax.div(c, 2), self.H), k, f * 2 + k, c * self.F + f)

    def count(self, group):
        return {"ctx": self.C, "fsdp": self.F, "world": self.N, "col": self.H, "line": self.J, "plane": self.P}[group]

    def peer(self, group, me, n):
        if group == "ctx":
            return self.place(lax.rem(me.c + n, self.C), me.f)
        if group == "fsdp":
            return self.place(me.c, lax.rem(me.f + n, self.F))
        if group == "world":
            w = lax.rem(me.w + n, self.N)
            return self.place(lax.div(w, self.F), lax.rem(w, self.F))
        if group == "col":
            return self.place(me.s * self.G + 2 * lax.rem(me.h + n, self.H) + me.k, me.f)
        if group == "line":
            return self.place(2 * lax.rem(lax.div(me.c, 2) + n, self.J) + me.k, me.f)
        p = lax.rem(me.p + n, self.P)
        return self.place(me.s * self.G + 2 * me.h + lax.rem(p, 2), lax.div(p, 2))

    def expert(self, me, p):
        return lax.div(p, 2) * self.G + 2 * me.h + lax.rem(p, 2)


def bf(x):
    return x.astype(jnp.bfloat16)


def f32(x):
    return x.astype(jnp.float32)


def shape_of(shape, dtype=jnp.bfloat16):
    return jax.ShapeDtypeStruct(shape, dtype)


class Lane:
    def __init__(self, sizes, me, group, src, dst, sends, recvs):
        self.sizes, self.me, self.group, self.src, self.dst = sizes, me, group, src, dst
        self.sends, self.recvs, self.n = sends, recvs, sizes.count(group)

    def copy(self, k, to, source, landing):
        return pltpu.make_async_remote_copy(
            src_ref=source, dst_ref=landing, send_sem=self.sends.at[k], recv_sem=self.recvs.at[k],
            device_id=(to.c, to.f), device_id_type=MESH)

    def to(self, k):
        return self.sizes.peer(self.group, self.me, k)

    def start_one(self, k):
        to = self.to(k)
        self.copy(k, to, self.src(to), self.dst(self.me)).start()

    def wait_recv_one(self, k):
        landed = self.dst(self.sizes.peer(self.group, self.me, self.n - k))
        self.copy(k, self.to(k), landed, landed).wait_recv()

    def wait_send_one(self, k):
        to = self.to(k)
        self.copy(k, to, self.src(to), self.dst(self.me)).wait_send()

    def each(self, step):
        def one(k, carry):
            step(k)
            return carry
        lax.fori_loop(1, self.n, one, 0)

    def start(self):
        self.each(self.start_one)

    def wait_recv(self):
        self.each(self.wait_recv_one)

    def wait_send(self):
        self.each(self.wait_send_one)


class Relay:
    def __init__(self, sizes, me, own, landing, sends, recvs):
        self.sizes, self.me, self.own, self.landing, self.sends, self.recvs = sizes, me, own, landing, sends, recvs

    def member(self, n, core):
        J = self.sizes.J
        return 2 * lax.rem(lax.div(self.me.c, 2) + J - n, J) + core

    def copy(self, n, source, landing):
        return pltpu.make_async_remote_copy(
            src_ref=source, dst_ref=landing, send_sem=self.sends.at[n], recv_sem=self.recvs.at[n],
            device_id=(self.me.c + 1 - 2 * self.me.k, self.me.f), device_id_type=MESH)

    def start_own(self):
        self.copy(0, self.own, self.landing(self.me.c)).start()

    def start_one(self, n):
        here = self.landing(self.member(n, self.me.k))
        self.copy(n, here, here).start()

    def wait_recv_one(self, n):
        there = self.landing(self.member(n, 1 - self.me.k))
        self.copy(n, there, there).wait_recv()

    def wait_send(self):
        def one(n, carry):
            here = self.landing(self.member(n, self.me.k))
            self.copy(n, here, here).wait_send()
            return carry
        lax.fori_loop(0, self.sizes.J, one, 0)


def meet(sizes, me, groups):
    barrier = pltpu.get_barrier_semaphore()
    total = 0
    for group in groups:
        def greet(k, carry, group=group):
            p = sizes.peer(group, me, k)
            pl.semaphore_signal(barrier, inc=1, device_id=(p.c, p.f), device_id_type=MESH)
            return carry
        lax.fori_loop(1, sizes.count(group), greet, 0)
        total += sizes.count(group) - 1
    pl.semaphore_wait(barrier, total)


def times(n, step, first=0):
    def one(i, carry):
        step(i)
        return carry
    lax.fori_loop(first, n, one, 0)


def column_lane(z, me, c, source, landing, sends, recvs):
    return Lane(z, me, "fsdp", lambda to: source(c, to), lambda p: landing(c, p), sends.at[c], recvs.at[c])


def nn(a, b):
    return lax.dot_general(a, b, (((1,), (0,)), ((), ())), preferred_element_type=jnp.float32)


def nt(a, b):
    return lax.dot_general(a, b, (((1,), (1,)), ((), ())), preferred_element_type=jnp.float32)


def tn(a, b):
    return lax.dot_general(a, b, (((0,), (0,)), ((), ())), preferred_element_type=jnp.float32)


def lane_of(shape):
    return lax.broadcasted_iota(jnp.int32, shape, 1)


def rope_tables(place_columns, frequency):
    angles = place_columns.astype(jnp.float32) * frequency
    return jnp.cos(angles), jnp.sin(angles)


def rope(x, cosine, sine):
    half = HEAD // 2
    mixed = jnp.where(lax.rem(lane_of(x.shape), HEAD) < half, -pltpu.roll(x, LANES - half, 1), pltpu.roll(x, half, 1))
    return x * cosine + mixed * sine


def rows_at(ref, i, n):
    return ref.at[pl.ds(pl.multiple_of(i * n, n), n), :]


def vmem(shape, dtype=jnp.bfloat16):
    return pltpu.VMEM(shape, dtype)


def frequencies():
    lanes = np.arange(LANES)
    steps = rope_base ** ((lanes % (HEAD // 2)) * (-2.0 / HEAD))
    return jnp.asarray(np.stack([steps, np.where(lanes < HEAD, steps, 0.0)] + [steps] * 6), jnp.float32)


def exact(kind, a, b):
    dims = {"nn": ((1,), (0,)), "nt": ((1,), (1,)), "tn": ((0,), (0,))}[kind]
    return lax.dot_general(a, b, (dims, ((), ())), precision=lax.Precision.HIGHEST, preferred_element_type=jnp.float32)


LANE_GROUPS = dict(
    tok="line", place="ctx", wc="ctx", small="ctx", wo="line", cot="col", slot="col", gate_a="ctx", gate_b="ctx", up="ctx",
    down="ctx", att="ctx", rows="col", gates="col", part="col", turn="col", d_attn="line", mix="col", dn="line", gc="ctx",
    gs="ctx", go="fsdp", grad0="ctx", grad1="ctx", grad2="ctx", grad3="ctx", grad4="ctx", grad5="ctx")
PLANE_LANES = ["cot", "row", "g", "back", "dg", "out"]
COLUMN_LANES = ["wc", "small", "wo", "gc", "gs"]
RELAYS = ["tok", "wo", "d_attn", "sib"]


def layer_kernel(z, R, dc, tile, names, *refs):
    r = types.SimpleNamespace(**dict(zip(names, refs)))
    me = z.place(lax.axis_index("ctx"), lax.axis_index("fsdp"))
    C, F, H, P, J, rs, qw = z.C, z.F, z.H, z.P, z.J, z.rows_w, z.q_width
    L = C * R
    half = dc // 2
    low, high = pl.ds(0, half), pl.ds(half, half)
    sems = lambda kind, name: (getattr(r, kind + name + "_send"), getattr(r, kind + name + "_recv"))

    def at_slot(ref, h, p):
        return rows_at(ref, h * P + p, CAP)

    def lane(name, source, landing):
        return Lane(z, me, LANE_GROUPS[name], source, landing, *sems("lane_", name))

    def plane(name, source, landing):
        def at(h):
            send, recv = sems("plane_", name)
            land = lambda p: at_slot(landing, h, p.p) if len(landing.shape) == 2 else landing.at[h, p.p]
            return Lane(z, me, "plane", lambda to: source.at[h, to.p], land, send.at[h], recv.at[h])
        return at

    def column(name, source, landing):
        return lambda c: column_lane(z, me, c, source, landing, *sems("column_", name))

    def relay(name, own, landing):
        return Relay(z, me, own, landing, *sems("relay_", name))

    tok_lane = lane("tok", lambda to: r.tok, lambda p: r.blocks.at[p.c])
    tok_relay = relay("tok", r.tok, lambda c: r.blocks.at[c])
    place_lane = lane("place", lambda to: r.place, lambda p: r.place_all.at[p.c])
    wc_lane = lane("wc", lambda to: r.w_pack.at[to.c], lambda p: rows_at(r.wc_v, p.w, rs))
    small_lane = lane("small", lambda to: r.small, lambda p: rows_at(r.small_v, p.w, rs))
    wo_lane = lane("wo", lambda to: r.w_out, lambda p: rows_at(r.wo_v, p.w, rs))
    wo_relay = relay("wo", r.w_out, lambda c: rows_at(r.wo_v, c * F + me.f, rs))
    spread = lambda name, ref: column(
        name, lambda c, to: rows_at(ref, c * F + me.f, rs), lambda c, p: rows_at(ref, c * F + p.f, rs))
    wc_column, small_column, wo_column = spread("wc", r.wc_v), spread("small", r.small_v), spread("wo", r.wo_v)
    cot_lane = lane("cot", lambda to: r.cot, lambda p: r.cot_all.at[p.h])
    slot_lane = lane("slot", lambda to: r.slot_t.at[pl.ds(0, EXPERTS), :], lambda p: r.slot_all.at[p.h])
    gate_a_lane = lane("gate_a", lambda to: r.w_gate.at[to.m, low], lambda p: r.wv.at[0, p.c, low])
    gate_b_lane = lane("gate_b", lambda to: r.w_gate.at[to.m, high], lambda p: r.wv.at[0, p.c, high])
    up_lane = lane("up", lambda to: r.w_up.at[to.m], lambda p: r.wv.at[1, p.c])
    down_lane = lane("down", lambda to: r.w_downt.at[to.m], lambda p: r.wv.at[2, p.c])
    att_lane = lane("att", lambda to: r.att_stage.at[to.c], lambda p: r.att_in.at[p.c])
    rows_lane = lane("rows", lambda to: r.h2, lambda p: r.h_all.at[p.h])
    gates_lane = lane("gates", lambda to: r.gates_t.at[pl.ds(0, EXPERTS), :], lambda p: r.gate_all.at[p.h])
    part_lane = lane("part", lambda to: r.part_stage.at[to.h], lambda p: r.part_in.at[p.h])
    turn_lane = lane("turn", lambda to: r.turn_stage.at[to.h], lambda p: r.turn_in.at[p.h])
    up_attn_lane = lane("d_attn", lambda to: r.d_attn, lambda p: r.blocks.at[p.c])
    up_attn_relay = relay("d_attn", r.d_attn, lambda c: r.blocks.at[c])
    mix_lane = lane("mix", lambda to: r.part_stage.at[to.h], lambda p: r.mix_in.at[p.h])
    dn_block = lambda c: rows_at(r.pool, c, R)
    dn_in = lambda j: rows_at(r.xin, j, R)
    sib_in = lambda j: rows_at(r.cot_v, j, R)
    dn_lane = lane("dn", lambda to: dn_block(to.c), lambda p: dn_in(lax.div(p.c, 2)))
    gc_lane = lane("gc", lambda to: r.gc_sum.at[to.c], lambda p: r.gc_in.at[p.c])
    gs_lane = lane("gs", lambda to: r.gs_sum.at[to.c], lambda p: r.gs_in.at[p.c])
    go_lane = lane("go", lambda to: rows_at(r.go_stage, to.f, rs), lambda p: r.go_in.at[p.f])
    gather = lambda name, stage, landing: column(
        name, lambda c, to: rows_at(stage, c * F + to.f, rs), lambda c, p: landing.at[p.f, c])
    gc_column, gs_column = gather("gc", r.gc_stage, r.gc_x), gather("gs", r.gs_stage, r.gs_x)
    grad_lanes = [
        lane("grad" + str(2 * j + i),
             lambda to, j=j, i=i: r.wv.at[j, to.c, (low, high)[i]],
             lambda p, j=j, i=i: r.gw_in.at[j, p.s, p.m, (low, high)[i]])
        for j in range(3) for i in range(2)
    ]
    cot_plane = plane("cot", r.d_rows, r.cot_v)
    row_plane = plane("row", r.stage, r.xin)
    g_plane = plane("g", r.g_stage, r.gin)
    back_plane = plane("back", r.d_rows, r.stage)
    dg_plane = plane("dg", r.dg_stage, r.dg_in)
    out_plane = plane("out", r.result, r.out_in)

    def sib_copy(j):
        send, recv = sems("relay_", "sib")
        return pltpu.make_async_remote_copy(
            src_ref=dn_block(2 * j + 1 - me.k), dst_ref=sib_in(j), send_sem=send.at[j], recv_sem=recv.at[j],
            device_id=(me.c + 1 - 2 * me.k, me.f), device_id_type=MESH)

    meet(z, me, ["ctx", "plane", "fsdp"])
    wc_lane.start()
    small_lane.start()
    place_lane.start()
    tok_relay.start_own()
    tok_lane.start()

    own = [
        pltpu.make_async_copy(r.w_pack.at[me.c], rows_at(r.wc_v, me.w, rs), r.own_sem.at[0]),
        pltpu.make_async_copy(r.small, rows_at(r.small_v, me.w, rs), r.own_sem.at[1]),
        pltpu.make_async_copy(r.w_out, rows_at(r.wo_v, me.w, rs), r.own_sem.at[2]),
    ]
    own_weights = [
        pltpu.make_async_copy(source.at[me.m], r.wv.at[j, me.c], r.own_sem.at[3 + j])
        for j, source in enumerate([r.w_gate, r.w_up, r.w_downt])
    ]
    for copy in own + own_weights:
        copy.start()
    r.blocks[me.c] = r.tok[...]
    r.place_all[me.c] = r.place[...]
    r.cot_all[me.h] = r.cot[...]

    named = jnp.zeros((R, LANES), jnp.float32)
    for j in range(TOP):
        named = jnp.where(r.routes[:, j : j + 1] == lane_of((R, LANES)), 1.0, named)
    row_id = lax.broadcasted_iota(jnp.int32, (R, R), 0)
    before = jnp.where(row_id > lane_of((R, R)), 1.0, 0.0).astype(jnp.bfloat16)
    slot = nn(before, named.astype(jnp.bfloat16))
    r.slot_t[...] = jnp.where(named > 0.5, slot, -1.0).T
    r.slot_all[me.h] = r.slot_t[0:EXPERTS, :]
    slot_lane.start()
    slot_id = lax.broadcasted_iota(jnp.int32, (CAP, R), 0).astype(jnp.float32)

    for copy in own:
        copy.wait()
    wc_lane.wait_recv()
    times(C, lambda c: wc_column(c).start())
    small_lane.wait_recv()
    times(C, lambda c: small_column(c).start())

    def dispatch_cot(j):
        h = lax.rem(me.h + H - j, H)
        @pl.when(j > 0)
        def _():
            cot_lane.wait_recv_one(j)
            slot_lane.wait_recv_one(j)

        def to_expert(n):
            p = lax.rem(me.p + n, P)
            row = r.slot_all[h, pl.ds(z.expert(me, p), 1), :]
            hot = jnp.where(row == slot_id, 1.0, 0.0).astype(jnp.bfloat16)
            r.pick[h, p] = hot
            r.d_rows[h, p] = nn(hot, r.cot_all[h]).astype(jnp.bfloat16)
            @pl.when(n > 0)
            def _():
                cot_plane(h).start_one(n)
        times(P, to_expert)
        at_slot(r.cot_v, h, me.p)[...] = r.d_rows[h, me.p]
    dispatch_cot(0)
    place_lane.wait_recv()
    times(C, lambda c: wc_column(c).wait_recv())
    times(C, lambda c: small_column(c).wait_recv())
    gain_one = r.small_v[...].astype(jnp.float32).T[EXPERTS : EXPERTS + 1, :]
    gain_two = r.small_v[...].astype(jnp.float32).T[EXPERTS + 1 : EXPERTS + 2, :]
    head_of = lax.div(lane_of((R, LANES)), HEAD)

    def project(i):
        n = lax.rem(i, J)
        c = tok_relay.member(n, jnp.where(i < J, me.k, 1 - me.k))
        @pl.when(jnp.logical_and(i > 0, i < J))
        def _():
            tok_lane.wait_recv_one(n)
            tok_relay.start_one(n)
        @pl.when(i >= J)
        def _():
            tok_relay.wait_recv_one(n)
        x = r.blocks[c].astype(jnp.float32)
        inverse = lax.rsqrt(jnp.mean(x * x, axis=-1, keepdims=True) + norm_eps)
        h = (x * inverse * gain_one).astype(jnp.bfloat16)
        part = pl.ds(pl.multiple_of(c * R, R), R)
        r.h1[part, :] = h
        qkv = nn(h, r.wc_v[...])
        row = r.place_all[c][0:1, :].astype(jnp.float32)
        r.place_row[c] = jnp.broadcast_to(row, (8, R))
        places = jnp.broadcast_to(row, (R, R)).T
        r.place_col[part, :] = places
        r.q_all[part, :] = rope(qkv[:, :LANES], *rope_tables(places, r.freq[0:1, :])).astype(jnp.bfloat16)
        kv = rope(qkv[:, LANES:], *rope_tables(places, r.freq[1:2, :]))
        swapped = pltpu.roll(kv, HEAD, 1)
        r.k2[part, :] = jnp.where(head_of == 0, kv, swapped).astype(jnp.bfloat16)
        r.v2[part, :] = jnp.where(head_of == 0, swapped, kv).astype(jnp.bfloat16)
    times(C, project)
    wo_relay.start_own()
    wo_lane.start()
    cot_lane.start()
    tok_relay.wait_send()

    def attend(c):
        part = pl.ds(pl.multiple_of(c * R, R), R)
        q = r.q_all[part, :]
        row = jnp.concatenate([r.place_row[i, 0:1, :] for i in range(C)], axis=1)
        allowed = row <= r.place_col[part, 0:1]
        total = jnp.zeros((R, LANES), jnp.float32)
        for h in range(z.q_heads):
            mine = head_of == h
            s = nt(jnp.where(mine, q, jnp.zeros_like(q)), r.k2[...]) * score_scale
            s = jnp.where(allowed, s, masked_score)
            top = jnp.max(s, axis=-1, keepdims=True)
            e = jnp.exp(s - top)
            weight = jnp.sum(e, axis=-1, keepdims=True)
            r.lse[h, part, :] = jnp.broadcast_to(top + jnp.log(weight), (R, LANES))
            total = jnp.where(mine, nn(e.astype(jnp.bfloat16), r.v2[...]) / weight, total)
        r.att_f[part, :] = total
        r.att_stage[c] = total.astype(jnp.bfloat16)
    times(C // 2, attend)
    wo_lane.wait_recv()
    times(J, wo_relay.start_one, 1)
    times(C, attend, C // 2)
    att_lane.start()
    gate_a_lane.start()
    r.att_in[me.c] = r.att_stage[me.c]
    times(J, wo_relay.wait_recv_one)
    times(C, lambda c: wo_column(c).start())
    times(H, dispatch_cot, 1)
    att_lane.wait_recv()
    times(C, lambda c: wo_column(c).wait_recv())
    x = r.tok[...].astype(jnp.float32)
    mixed = jnp.zeros((R, D), jnp.float32)
    for c in range(C):
        mixed = mixed + nn(r.att_in[c][:, :qw], r.wo_v[c * qw : (c + 1) * qw, :])
    mid = x + residual_scale * mixed
    r.middle[...] = mid
    inverse = lax.rsqrt(jnp.mean(mid * mid, axis=-1, keepdims=True) + norm_eps)
    hidden = (mid * inverse * gain_two).astype(jnp.bfloat16)
    r.h2[...] = hidden
    rows_lane.start()
    chosen = r.slot_t[...].T > -0.5
    logits = jnp.where(chosen, nn(hidden, r.small_v[...]), masked_score)
    raised = jnp.where(chosen, jnp.exp(logits - jnp.max(logits, axis=-1, keepdims=True)), 0.0)
    r.gates_t[...] = (raised / jnp.sum(raised, axis=-1, keepdims=True)).T
    gates_lane.start()
    gate_b_lane.start()
    up_lane.start()
    down_lane.start()
    r.h_all[me.h] = r.h2[...]
    r.gate_all[me.h] = r.gates_t[0:EXPERTS, :]

    def dispatch_rows(j):
        h = lax.rem(me.h + H - j, H)
        @pl.when(j > 0)
        def _():
            rows_lane.wait_recv_one(j)
            gates_lane.wait_recv_one(j)

        def to_expert(n):
            p = lax.rem(me.p + n, P)
            hot = r.pick[h, p]
            r.stage[h, p] = nn(hot, r.h_all[h]).astype(jnp.bfloat16)
            g = jnp.broadcast_to(r.gate_all[h, pl.ds(z.expert(me, p), 1), :], (8, R))
            wide = jnp.concatenate([hot.astype(jnp.float32), jnp.zeros((LANES - CAP, R), jnp.float32)], axis=0)
            r.g_stage[h, p] = exact("nt", g, wide)
            @pl.when(n > 0)
            def _():
                row_plane(h).start_one(n)
        times(P, to_expert)
        at_slot(r.xin, h, me.p)[...] = r.stage[h, me.p]
        r.gin[h, me.p] = r.g_stage[h, me.p]
    times(H, dispatch_rows)

    def send_gates(j):
        h = lax.rem(me.h + H - j, H)

        def to_expert(n):
            row_plane(h).wait_send_one(n)
            g_plane(h).start_one(n)
        times(P, to_expert, 1)
    times(H, send_gates)
    times(H, lambda h: cot_plane(h).wait_send())
    for copy in own_weights:
        copy.wait()
    for bulk in [gate_a_lane, gate_b_lane, up_lane, down_lane]:
        bulk.wait_recv()
    times(H, lambda h: cot_plane(h).wait_recv())
    wg, wu, wd = [r.wv.at[j].reshape(D, r.wv.shape[3]) for j in range(3)]
    per = tile // CAP

    def chunk(j):
        h = lax.rem(me.h + H - lax.rem(j + 1, H), H)
        row_plane(h).wait_recv()
        g_plane(h).wait_recv()

        def rows(t):
            some = pl.ds(pl.multiple_of(t * per, per), per)
            part = pl.ds(pl.multiple_of((h * P + t * per) * CAP, CAP), tile)
            for p in range(per):
                turned = jnp.broadcast_to(r.gin[h, t * per + p, 0:1, :], (LANES, LANES)).T
                r.g_col[p * CAP : (p + 1) * CAP, :] = turned[0:CAP, :]
            x = r.xin[part, :]
            gate = nn(x, wg[...])
            up = nn(x, wu[...])
            sig = jax.nn.sigmoid(gate)
            act = gate * sig
            hidden = (act * up).astype(jnp.bfloat16)
            r.hid[part, :] = hidden
            out = nt(hidden, wd[...]).astype(jnp.bfloat16)
            r.result[h, some] = out.reshape(per, CAP, D)
            upstream = r.cot_v[part, :].astype(jnp.float32)
            d_gates = residual_scale * jnp.sum(upstream * out.astype(jnp.float32), axis=-1, keepdims=True)
            d_out = (residual_scale * r.g_col[:, 0:1] * upstream).astype(jnp.bfloat16)
            r.pool[part, :] = d_out
            d_hidden = nn(d_out, wd[...])
            dg = (d_hidden * up * sig * (1.0 + gate * (1.0 - sig))).astype(jnp.bfloat16)
            du = (d_hidden * act).astype(jnp.bfloat16)
            r.d_gate[part, :] = dg
            r.d_up[part, :] = du
            r.d_rows[h, some] = (nt(dg, wg[...]) + nt(du, wu[...])).astype(jnp.bfloat16).reshape(per, CAP, D)
            r.g_col[...] = jnp.broadcast_to(d_gates, (tile, LANES))
            for p in range(per):
                turned = jnp.concatenate(
                    [r.g_col[p * CAP : (p + 1) * CAP, :], jnp.zeros((LANES - CAP, LANES), jnp.float32)], axis=0)
                r.dg_stage[h, t * per + p] = turned.T[0:8, :]
        times(P // per, rows)
        back_plane(h).start()
        dg_plane(h).start()
        r.stage[h, me.p] = r.d_rows[h, me.p]
        r.dg_in[h, me.p] = r.dg_stage[h, me.p]
    times(H, chunk)
    times(H, lambda h: out_plane(h).start())
    own_out = pltpu.make_async_copy(r.result.at[:, me.p], r.out_in.at[:, me.p], r.own_sem.at[7])
    own_out.start()

    def cut(d):
        part = pl.ds(pl.multiple_of(d * 256, 256), 256)
        x = r.xin[:, part]
        wg[part, :] = tn(x, r.d_gate[...]).astype(jnp.bfloat16)
        wu[part, :] = tn(x, r.d_up[...]).astype(jnp.bfloat16)
        wd[part, :] = tn(r.pool[pl.ds(0, H * P * CAP), part], r.hid[...]).astype(jnp.bfloat16)
    times(D // 256, cut)
    grad_lanes[0].start()
    own_grads = [
        pltpu.make_async_copy(r.wv.at[j, me.c], r.gw_in.at[j, me.s, me.m], r.own_sem.at[8 + j]) for j in range(3)
    ]
    for copy in own_grads:
        copy.start()

    def collect(j):
        n = lax.rem(j + 1, H)
        h = lax.rem(me.h + H - n, H)
        back_plane(h).wait_recv()
        dg_plane(h).wait_recv()
        part = tn(r.pick[h].reshape(P * CAP, R), r.stage[h].reshape(P * CAP, D))
        r.turn_stage[h] = jnp.zeros((EXPERTS, R), jnp.float32)

        def gates_of(p):
            row = jnp.broadcast_to(r.dg_in[h, p, 0:1, 0:CAP], (8, CAP))
            r.turn_stage[h, pl.ds(z.expert(me, p), 1), :] = exact("nn", row, r.pick[h, p].astype(jnp.float32))[0:1, :]
        times(P, gates_of)
        @pl.when(n > 0)
        def _():
            r.part_stage[h] = part.astype(jnp.bfloat16)
            part_lane.start_one(H - n)
            turn_lane.start_one(H - n)
        @pl.when(n == 0)
        def _():
            r.d_mid[...] = part
            r.turn_v[...] = jnp.zeros((LANES, R), jnp.float32)
            r.turn_v[0:EXPERTS, :] = r.turn_stage[h]
    times(H, collect)
    grad_lanes[1].start()
    part_lane.wait_recv()
    turn_lane.wait_recv()

    def add_part(n):
        h = lax.rem(me.h + n + 1, H)
        r.d_mid[...] += r.part_in[h].astype(jnp.float32)
        r.turn_v[0:EXPERTS, :] += r.turn_in[h]
    times(H - 1, add_part)
    gts = r.gates_t[...].T
    dgs = r.turn_v[...].T
    d_log = gts * (dgs - jnp.sum(gts * dgs, axis=-1, keepdims=True))
    d_h2 = r.d_mid[...] + exact("nt", d_log, r.small_v[...].astype(jnp.float32))
    mid = r.middle[...]
    inverse = lax.rsqrt(jnp.mean(mid * mid, axis=-1, keepdims=True) + norm_eps)
    n2 = mid * inverse
    g = d_h2 * gain_two
    dm = r.cot[...].astype(jnp.float32) + inverse * (g - n2 * jnp.mean(g * n2, axis=-1, keepdims=True))
    r.d_mid[...] = dm
    r.d_attn[...] = (residual_scale * dm).astype(jnp.bfloat16)
    up_attn_relay.start_own()
    up_attn_lane.start()
    grad_lanes[2].start()
    r.gain_v[...] = jnp.zeros((LANES, D), jnp.float32)
    r.gain_v[EXPERTS + 1 : EXPERTS + 2, :] = jnp.sum(d_h2 * n2, axis=0, keepdims=True)
    r.g_small[...] = exact("tn", r.h2[...].astype(jnp.float32), d_log)

    r.blocks[me.c] = r.d_attn[...]
    r.dk_acc[...] = jnp.zeros((L, LANES), jnp.float32)
    r.dv_acc[...] = jnp.zeros((L, LANES), jnp.float32)
    wo_c = rows_at(r.wo_v, me.c, qw)

    def attend_back(i):
        n = lax.rem(i, J)
        c = up_attn_relay.member(n, jnp.where(i < J, me.k, 1 - me.k))
        @pl.when(jnp.logical_and(i > 0, i < J))
        def _():
            up_attn_lane.wait_recv_one(n)
            up_attn_relay.start_one(n)
        @pl.when(i >= J)
        def _():
            up_attn_relay.wait_recv_one(n)
        part = pl.ds(pl.multiple_of(c * R, R), R)
        q = r.q_all[part, :]
        d_mix = nt(r.blocks[c], wo_c[...])
        if qw < LANES:
            d_mix = jnp.concatenate([d_mix, jnp.zeros((R, LANES - qw), jnp.float32)], axis=1)
        d_mix = d_mix.astype(jnp.bfloat16)
        row = jnp.concatenate([r.place_row[i, 0:1, :] for i in range(C)], axis=1)
        places = r.place_col[part, :]
        allowed = row <= places[:, 0:1]
        dq = jnp.zeros((R, LANES), jnp.float32)
        for h in range(z.q_heads):
            mine = head_of == h
            rows = pl.ds(h * R, R)
            q_h = jnp.where(mine, q, jnp.zeros_like(q))
            dm_h = jnp.where(mine, d_mix, jnp.zeros_like(d_mix))
            r.q_v[rows, :] = q_h
            r.dm_v[rows, :] = dm_h
            s = jnp.where(allowed, nt(q_h, r.k2[...]) * score_scale, masked_score)
            p = jnp.exp(s - r.lse[h, part, 0:1])
            r.p_v[rows, :] = p.astype(jnp.bfloat16)
            delta = jnp.sum(dm_h.astype(jnp.float32) * r.att_f[part, :], axis=-1, keepdims=True)
            ds = (p * (nt(dm_h, r.v2[...]) - delta)).astype(jnp.bfloat16)
            r.ds_v[rows, :] = ds
            dq = jnp.where(mine, nn(ds, r.k2[...]) * score_scale, dq)
        r.dk_acc[...] += tn(r.ds_v[...], r.q_v[...])
        r.dv_acc[...] += tn(r.p_v[...], r.dm_v[...])
        cosine, sine = rope_tables(places, r.freq[0:1, :])
        r.d_qkv[part, 0:LANES] = rope(dq, cosine, -sine).astype(jnp.bfloat16)
    times(C, attend_back)

    def finish_kv(c):
        part = pl.ds(pl.multiple_of(c * R, R), R)
        dk = r.dk_acc[part, :] * score_scale
        dv = r.dv_acc[part, :]
        dk = dk + pltpu.roll(dk, HEAD, 1)
        dv = dv + pltpu.roll(dv, HEAD, 1)
        cosine, sine = rope_tables(r.place_col[part, :], r.freq[1:2, :])
        r.d_qkv[part, LANES : 2 * LANES] = rope(jnp.where(head_of == 0, dk, dv), cosine, -sine).astype(jnp.bfloat16)
    times(C, finish_kv)

    def down_tokens(c):
        return nt(r.d_qkv[pl.ds(pl.multiple_of(c * R, R), R), :], r.wc_v[...])

    def for_sibling(j):
        c = 2 * j + 1 - me.k
        dn_block(c)[...] = down_tokens(c).astype(jnp.bfloat16)
        sib_copy(j).start()
    times(J, for_sibling)

    def for_line(i):
        n = lax.rem(i + 1, J)
        to = z.peer("line", me, n)
        dn = down_tokens(to.c)
        j = lax.div(to.c, 2)
        sib_copy(j).wait_recv()
        dn_block(to.c)[...] = (dn + sib_in(j)[...].astype(jnp.float32)).astype(jnp.bfloat16)
        @pl.when(n > 0)
        def _():
            dn_lane.start_one(n)
    times(J, for_line)
    dn_in(lax.div(me.c, 2))[...] = dn_block(me.c)[...]

    own_out.wait()
    part_lane.wait_send()

    def mix(i):
        n = lax.rem(i + 1, H)
        h = lax.rem(me.h + H - n, H)
        out_plane(h).wait_recv()
        load = pltpu.make_async_copy(r.out_in.at[h], r.stage.at[h], r.own_sem.at[12])
        load.start()

        def weigh(p):
            g = r.gate_all[h, pl.ds(z.expert(me, p), 1), :] * r.pick[h, p].astype(jnp.float32)
            high = g.astype(jnp.bfloat16)
            r.mix_hi[p] = high
            r.mix_lo[p] = (g - high.astype(jnp.float32)).astype(jnp.bfloat16)
        times(P, weigh)
        load.wait()
        rows = r.stage[h].reshape(P * CAP, D)
        total = tn(r.mix_hi[...].reshape(P * CAP, R), rows) + tn(r.mix_lo[...].reshape(P * CAP, R), rows)
        r.part_stage[h] = total.astype(jnp.bfloat16)
        @pl.when(n > 0)
        def _():
            mix_lane.start_one(H - n)
        @pl.when(n == 0)
        def _():
            r.grad_tokens[...] = total
    times(H, mix)

    def weights(d):
        part = pl.ds(pl.multiple_of(d * 256, 256), 256)
        total = tn(r.h1[:, part], r.d_qkv[...])
        r.gc_stage[part, :] = total.astype(jnp.bfloat16)
        gain = jnp.sum(total * r.wc_v[part, :].astype(jnp.float32), axis=-1, keepdims=True)
        gain = gain / r.small_v[part, EXPERTS : EXPERTS + 1].astype(jnp.float32)
        r.g_small[part, :] = jnp.where(lane_of((256, LANES)) == EXPERTS, gain, r.g_small[part, :])
    times(D // 256, weights)
    times(C, lambda c: gc_column(c).start())
    r.gs_stage[...] = (r.g_small[...] + r.gain_v[...].T).astype(jnp.bfloat16)
    times(C, lambda c: gs_column(c).start())
    own_last = [
        pltpu.make_async_copy(rows_at(stage, c * F + me.f, rs), landing.at[me.f, c], r.own_cols.at[i, c])
        for i, (stage, landing) in enumerate([(r.gc_stage, r.gc_x), (r.gs_stage, r.gs_x)]) for c in range(C)
    ]
    for copy in own_last:
        copy.start()
    for bulk in grad_lanes[3:]:
        bulk.start()
    r.go_stage[...] = tn(r.att_f[...].astype(jnp.bfloat16), r.blocks[...].reshape(L, D)).astype(jnp.bfloat16)
    go_lane.start()
    own_go = pltpu.make_async_copy(rows_at(r.go_stage, me.f, rs), r.go_in.at[me.f], r.own_sem.at[13])
    own_go.start()
    for copy in own_last:
        copy.wait()
    times(C, lambda c: gc_column(c).wait_recv())
    times(C, lambda c: gs_column(c).wait_recv())
    gc_total = r.gc_x[0].astype(jnp.float32)
    gs_total = r.gs_x[0].astype(jnp.float32)
    for f in range(1, F):
        gc_total = gc_total + r.gc_x[f].astype(jnp.float32)
        gs_total = gs_total + r.gs_x[f].astype(jnp.float32)
    r.gc_sum[...] = gc_total.astype(jnp.bfloat16)
    r.gs_sum[...] = gs_total.astype(jnp.bfloat16)
    gc_lane.start()
    gs_lane.start()
    own_sums = [
        pltpu.make_async_copy(r.gc_sum.at[me.c], r.gc_in.at[me.c], r.own_sem.at[14]),
        pltpu.make_async_copy(r.gs_sum.at[me.c], r.gs_in.at[me.c], r.own_sem.at[15]),
    ]
    for copy in own_sums:
        copy.start()
    mix_lane.wait_recv()

    def add_mix(n):
        r.grad_tokens[...] += r.mix_in[lax.rem(me.h + n + 1, H)].astype(jnp.float32)
    times(H - 1, add_mix)
    r.output[...] = (r.middle[...] + residual_scale * r.grad_tokens[...]).astype(jnp.bfloat16)

    dn_lane.wait_recv()
    d_h1 = dn_in(0)[...].astype(jnp.float32)
    for c in range(1, J):
        d_h1 = d_h1 + dn_in(c)[...].astype(jnp.float32)
    x = r.tok[...].astype(jnp.float32)
    inverse = lax.rsqrt(jnp.mean(x * x, axis=-1, keepdims=True) + norm_eps)
    n1 = x * inverse
    g = d_h1 * gain_one
    r.grad_tokens[...] = r.d_mid[...] + inverse * (g - n1 * jnp.mean(g * n1, axis=-1, keepdims=True))
    for last in [gc_lane, gs_lane, go_lane]:
        last.wait_recv()
    for last in grad_lanes:
        last.wait_recv()
    for last in [tok_lane, place_lane, wc_lane, small_lane, wo_lane, cot_lane, slot_lane, gate_a_lane, gate_b_lane, up_lane,
                 down_lane, att_lane, rows_lane, gates_lane, turn_lane, up_attn_lane, mix_lane, dn_lane, gc_lane,
                 gs_lane, go_lane] + grad_lanes:
        last.wait_send()
    for last in [wo_relay, up_attn_relay]:
        last.wait_send()
    times(J, lambda j: sib_copy(j).wait_send())
    for last in [g_plane, back_plane, dg_plane, out_plane]:
        times(H, lambda h, last=last: last(h).wait_send())
    for last in [wc_column, small_column, wo_column, gc_column, gs_column]:
        times(C, lambda c, last=last: last(c).wait_send())
    for copy in own_grads + own_sums + [own_go]:
        copy.wait()


def layer_call(z, R, ff, dc, tok, place, routes, cot, w_pack, small, w_out, w_gate, w_up, w_downt):
    C, F, N, H, P, J, S, rs = z.C, z.F, z.N, z.H, z.P, z.J, z.S, z.rows_w
    L, f, f16 = C * R, jnp.float32, jnp.bfloat16
    rows, heads, tile = H * P * CAP, z.q_heads * R, 8 * CAP
    ins = dict(tok=(tok, 1), place=(place, 1), routes=(routes, 1), cot=(cot, 1), freq=(frequencies(), 1), w_pack=(w_pack, 0),
               small=(small, 0), w_out=(w_out, 0), w_gate=(w_gate, 0), w_up=(w_up, 0), w_downt=(w_downt, 0))
    outs = dict(
        output=(shape_of((R, D)), 1), grad_tokens=(shape_of((R, D), f), 1), gc_in=(shape_of((C, rs, 2 * LANES)), 0),
        gs_in=(shape_of((C, rs, LANES)), 0), go_in=(shape_of((F, rs, D)), 0), gw_in=(shape_of((3, S, z.G, dc, ff)), 0),
        out_in=(shape_of((H, P, CAP, D)), 0))
    scratch = dict(
        blocks=vmem((C, R, D)), place_all=vmem((C, 8, R), jnp.int32), wc_v=vmem((D, 2 * LANES)), small_v=vmem((D, LANES)),
        wo_v=vmem((D, D)), cot_all=vmem((H, R, D)), slot_all=vmem((H, EXPERTS, R), f), slot_t=vmem((LANES, R), f),
        place_col=vmem((L, R), f), place_row=vmem((C, 8, R), f), h1=vmem((L, D)), q_all=vmem((L, LANES)), k2=vmem((L, LANES)),
        v2=vmem((L, LANES)), lse=vmem((z.q_heads, L, LANES), f), att_f=vmem((L, LANES), f), att_stage=vmem((C, R, LANES)),
        att_in=vmem((C, R, LANES)), middle=vmem((R, D), f), h2=vmem((R, D)), gates_t=vmem((LANES, R), f),
        gate_all=vmem((H, EXPERTS, R), f), h_all=vmem((H, R, D)), pick=vmem((H, P, CAP, R)), stage=vmem((H, P, CAP, D)),
        xin=vmem((rows, D)), g_stage=vmem((H, P, 8, LANES), f), gin=vmem((H, P, 8, LANES), f), wv=vmem((3, C, dc, ff)),
        cot_v=vmem((rows, D)), d_rows=vmem((H, P, CAP, D)), dg_stage=vmem((H, P, 8, LANES), f),
        dg_in=vmem((H, P, 8, LANES), f), hid=vmem((rows, ff)), d_gate=vmem((rows, ff)), d_up=vmem((rows, ff)),
        pool=vmem((max(rows, L), D)), g_col=vmem((tile, LANES), f), result=vmem((H, P, CAP, D)),
        part_stage=vmem((H, R, D)), part_in=vmem((H, R, D)), turn_stage=vmem((H, EXPERTS, R), f),
        turn_in=vmem((H, EXPERTS, R), f), turn_v=vmem((LANES, R), f), d_mid=vmem((R, D), f), d_attn=vmem((R, D)),
        g_small=vmem((D, LANES), f), gain_v=vmem((LANES, D), f), ds_v=vmem((heads, L)), p_v=vmem((heads, L)),
        q_v=vmem((heads, LANES)), dm_v=vmem((heads, LANES)), dk_acc=vmem((L, LANES), f), dv_acc=vmem((L, LANES), f),
        d_qkv=vmem((L, 2 * LANES)),
        gc_stage=vmem((D, 2 * LANES)), go_stage=vmem((LANES, D)), gs_stage=vmem((D, LANES)), gc_x=vmem((F, C, rs, 2 * LANES)),
        gs_x=vmem((F, C, rs, LANES)), gc_sum=vmem((C, rs, 2 * LANES)), gs_sum=vmem((C, rs, LANES)), mix_hi=vmem((P, CAP, R)),
        mix_lo=vmem((P, CAP, R)), mix_in=vmem((H, R, D)), own_sem=pltpu.SemaphoreType.DMA((16,)),
        own_cols=pltpu.SemaphoreType.DMA((2, C)))
    both = ("_send", "_recv")
    scratch |= {"lane_" + n + b: pltpu.SemaphoreType.DMA((z.count(g),)) for n, g in LANE_GROUPS.items() for b in both}
    scratch |= {"plane_" + n + b: pltpu.SemaphoreType.DMA((H, P)) for n in PLANE_LANES for b in both}
    scratch |= {"column_" + n + b: pltpu.SemaphoreType.DMA((C, F)) for n in COLUMN_LANES for b in both}
    scratch |= {"relay_" + n + b: pltpu.SemaphoreType.DMA((J,)) for n in RELAYS for b in both}
    names = list(ins) + list(outs) + list(scratch)
    space = lambda fast: pl.BlockSpec(memory_space=pltpu.VMEM if fast else pl.ANY)
    results = pl.pallas_call(
        functools.partial(layer_kernel, z, R, dc, tile, names), name="layer",
        out_shape=[o for o, _ in outs.values()], in_specs=[space(fast) for _, fast in ins.values()],
        out_specs=[space(fast) for _, fast in outs.values()], scratch_shapes=list(scratch.values()),
        compiler_params=pltpu.CompilerParams(collective_id=0, has_side_effects=True, vmem_limit_bytes=67043328),
    )(*[a for a, _ in ins.values()])
    return results[:6]


def local(z, tokens, norm_first, w_query, w_key, w_value, w_out, norm_second, w_router,
          w_gate, w_up, w_down, positions, routes, cotangent):
    C, F = z.C, z.F
    R = tokens.shape[1]
    rs = z.rows_w
    ff = w_gate.shape[2]
    dc = D // C

    heads_q = jnp.pad(w_query.reshape(rs, C, z.q_width), ((0, 0), (0, 0), (0, LANES - z.q_width)))
    heads_k = jnp.repeat(w_key.reshape(rs, KV_HEADS, HEAD), z.share, axis=1)
    heads_v = jnp.repeat(w_value.reshape(rs, KV_HEADS, HEAD), z.share, axis=1)
    w_pack = jnp.concatenate([heads_q, heads_k, heads_v], axis=2).transpose(1, 0, 2)
    small = jnp.concatenate(
        [w_router, norm_first[:, None], norm_second[:, None], jnp.zeros((rs, 128 - EXPERTS - 2), jnp.bfloat16)], axis=1)
    place_pack = jnp.broadcast_to(positions[0][None, :], (8, R))
    w_downt = w_down.transpose(0, 2, 1)
    output, grad_tokens, gc_in, gs_in, go_in, gw_in = layer_call(
        z, R, ff, dc, tokens[0], place_pack, routes[0], cotangent[0], w_pack, small, w_out, w_gate, w_up, w_downt)
    gc = f32(gc_in)
    join = lambda a: a.reshape(KV_HEADS, z.share, rs, HEAD).sum(axis=1).transpose(1, 0, 2).reshape(rs, KV_HEADS * HEAD)
    gs = jnp.sum(f32(gs_in), axis=0)
    return (
        output[None],
        grad_tokens[None],
        gs[:, EXPERTS],
        gc[:, :, : z.q_width].transpose(1, 0, 2).reshape(rs, D),
        join(gc[:, :, LANES : LANES + HEAD]),
        join(gc[:, :, LANES + HEAD :]),
        jnp.sum(f32(go_in), axis=0),
        gs[:, EXPERTS + 1],
        gs[:, :EXPERTS],
        jnp.sum(f32(gw_in[0]), axis=0),
        jnp.sum(f32(gw_in[1]), axis=0),
        jnp.sum(f32(gw_in[2]), axis=0).transpose(0, 2, 1),
    )


def solution(mesh):
    row = P(("ctx", "fsdp"), None)
    vec = P(("ctx", "fsdp"))
    seq = P("fsdp", "ctx", None)
    down = P("fsdp", None, "ctx")
    return jax.shard_map(
        functools.partial(local, Sizes(mesh)),
        mesh=mesh,
        in_specs=(seq, vec, row, row, row, row, vec, row, seq, seq, down, P("fsdp", "ctx"), seq, seq),
        out_specs=(seq, seq, vec, row, row, row, row, vec, row, seq, seq, down),
        check_vma=False,
    )
```

```python
import collections
import functools
import types

import jax
import jax.numpy as jnp
import numpy as np
from jax import lax
from jax.experimental import pallas as pl
from jax.experimental.pallas import tpu as pltpu
from jax.sharding import PartitionSpec as P

D = 1024
HEADS = 16
KV_HEADS = 8
HEAD = 64
EXPERTS = 32
TOP = 8
CAP = 48
LANES = 128

residual_scale = 0.22
score_scale = 0.015625
rope_base = 10000.0
norm_eps = 1e-06
masked_score = -1e30

MESH = pl.DeviceIdType.MESH
Place = collections.namedtuple("Place", ["c", "f", "m", "s", "h", "k", "p", "w"])


class Sizes:
    def __init__(self, mesh):
        self.C = mesh.shape["ctx"]
        self.F = mesh.shape["fsdp"]
        self.N = self.C * self.F
        self.G = EXPERTS // self.F
        self.S = self.C // self.G
        self.H = self.G // 2
        self.P = 2 * self.F
        self.J = self.C // 2
        self.q_heads = HEADS // self.C
        self.q_width = self.q_heads * HEAD
        self.share = self.C // KV_HEADS
        self.rows_w = D // self.N

    def place(self, c, f):
        k = lax.rem(c, 2)
        return Place(c, f, lax.rem(c, self.G), lax.div(c, self.G), lax.rem(lax.div(c, 2), self.H), k, f * 2 + k, c * self.F + f)

    def count(self, group):
        return {"ctx": self.C, "fsdp": self.F, "world": self.N, "col": self.H, "line": self.J, "plane": self.P}[group]

    def peer(self, group, me, n):
        if group == "ctx":
            return self.place(lax.rem(me.c + n, self.C), me.f)
        if group == "fsdp":
            return self.place(me.c, lax.rem(me.f + n, self.F))
        if group == "world":
            w = lax.rem(me.w + n, self.N)
            return self.place(lax.div(w, self.F), lax.rem(w, self.F))
        if group == "col":
            return self.place(me.s * self.G + 2 * lax.rem(me.h + n, self.H) + me.k, me.f)
        if group == "line":
            return self.place(2 * lax.rem(lax.div(me.c, 2) + n, self.J) + me.k, me.f)
        p = lax.rem(me.p + n, self.P)
        return self.place(me.s * self.G + 2 * me.h + lax.rem(p, 2), lax.div(p, 2))

    def expert(self, me, p):
        return lax.div(p, 2) * self.G + 2 * me.h + lax.rem(p, 2)


def bf(x):
    return x.astype(jnp.bfloat16)


def f32(x):
    return x.astype(jnp.float32)


def shape_of(shape, dtype=jnp.bfloat16):
    return jax.ShapeDtypeStruct(shape, dtype)


class Lane:
    def __init__(self, sizes, me, group, src, dst, sends, recvs):
        self.sizes, self.me, self.group, self.src, self.dst = sizes, me, group, src, dst
        self.sends, self.recvs, self.n = sends, recvs, sizes.count(group)

    def copy(self, k, to, source, landing):
        return pltpu.make_async_remote_copy(
            src_ref=source, dst_ref=landing, send_sem=self.sends.at[k], recv_sem=self.recvs.at[k],
            device_id=(to.c, to.f), device_id_type=MESH)

    def to(self, k):
        return self.sizes.peer(self.group, self.me, k)

    def start_one(self, k):
        to = self.to(k)
        self.copy(k, to, self.src(to), self.dst(self.me)).start()

    def wait_recv_one(self, k):
        landed = self.dst(self.sizes.peer(self.group, self.me, self.n - k))
        self.copy(k, self.to(k), landed, landed).wait_recv()

    def wait_send_one(self, k):
        to = self.to(k)
        self.copy(k, to, self.src(to), self.dst(self.me)).wait_send()

    def each(self, step):
        def one(k, carry):
            step(k)
            return carry
        lax.fori_loop(1, self.n, one, 0)

    def start(self):
        self.each(self.start_one)

    def wait_recv(self):
        self.each(self.wait_recv_one)

    def wait_send(self):
        self.each(self.wait_send_one)


class Chain:
    def __init__(self, sizes, me, group, own, landing, sends, recvs):
        self.col = group == "col"
        self.place, self.n = (me.h, sizes.H) if self.col else (lax.div(me.c, 2), sizes.J)
        self.sizes, self.me, self.own, self.landing, self.sends, self.recvs = sizes, me, own, landing, sends, recvs

    def copy(self, t, to, source, landing):
        c = self.me.s * self.sizes.G + 2 * to + self.me.k if self.col else 2 * to + self.me.k
        return pltpu.make_async_remote_copy(
            src_ref=source, dst_ref=landing, send_sem=self.sends.at[t], recv_sem=self.recvs.at[t],
            device_id=(c, self.me.f), device_id_type=MESH)

    def inside(self, place):
        return jnp.logical_and(place >= 0, place < self.n)

    def origin(self, t):
        return self.place - (1 - 2 * lax.rem(t, 2)) * (lax.div(t, 2) + 1)

    def start(self):
        for t, to in ((0, self.place + 1), (1, self.place - 1)):
            @pl.when(self.inside(to))
            def _(t=t, to=to):
                self.copy(t, to, self.own, self.landing(self.place)).start()

    def take(self, t):
        sign = 1 - 2 * lax.rem(t, 2)
        here = self.landing(self.origin(t))
        self.copy(t, self.place - sign, here, here).wait_recv()
        @pl.when(self.inside(self.place + sign))
        def _():
            self.copy(t + 2, self.place + sign, here, here).start()

    def wait_send(self):
        def one(t, carry):
            to = self.place + 1 - 2 * lax.rem(t, 2)
            origin = to - (1 - 2 * lax.rem(t, 2)) * (lax.div(t, 2) + 1)
            @pl.when(jnp.logical_and(self.inside(to), self.inside(origin)))
            def _():
                self.copy(t, to, self.landing(self.place), self.landing(self.place)).wait_send()
            return carry
        lax.fori_loop(0, 2 * (self.n - 1), one, 0)

    def visit(self, step, relay=None):
        each = 2 * self.n - 1

        def one(i):
            u = lax.rem(i, each)
            origin = jnp.where(u == 0, self.place, self.origin(jnp.maximum(u - 1, 0)))
            @pl.when(self.inside(origin))
            def _():
                @pl.when(jnp.logical_and(u > 0, i < each))
                def _():
                    self.take(u - 1)
                    if relay is not None:
                        relay.start(origin)
                if relay is None:
                    step(origin)
                else:
                    @pl.when(i >= each)
                    def _():
                        relay.wait_recv(origin)
                    step(origin, jnp.where(i < each, self.me.k, 1 - self.me.k))
        times(each if relay is None else 2 * each, one)


class Relay:
    def __init__(self, sizes, me, own, landing, sends, recvs):
        self.J, self.me, self.own, self.landing, self.sends, self.recvs = sizes.J, me, own, landing, sends, recvs
        self.place = lax.div(me.c, 2)

    def copy(self, place, source, landing):
        return pltpu.make_async_remote_copy(
            src_ref=source, dst_ref=landing, send_sem=self.sends.at[place], recv_sem=self.recvs.at[place],
            device_id=(self.me.c + 1 - 2 * self.me.k, self.me.f), device_id_type=MESH)

    def start_own(self):
        self.copy(self.place, self.own, self.landing(self.me.c)).start()

    def start(self, place):
        here = self.landing(2 * place + self.me.k)
        self.copy(place, here, here).start()

    def wait_recv(self, place):
        there = self.landing(2 * place + 1 - self.me.k)
        self.copy(place, there, there).wait_recv()

    def wait_send(self):
        def one(place, carry):
            here = self.landing(2 * place + self.me.k)
            self.copy(place, here, here).wait_send()
            return carry
        lax.fori_loop(0, self.J, one, 0)


def meet(sizes, me, groups):
    barrier = pltpu.get_barrier_semaphore()
    total = 0
    for group in groups:
        def greet(k, carry, group=group):
            p = sizes.peer(group, me, k)
            pl.semaphore_signal(barrier, inc=1, device_id=(p.c, p.f), device_id_type=MESH)
            return carry
        lax.fori_loop(1, sizes.count(group), greet, 0)
        total += sizes.count(group) - 1
    pl.semaphore_wait(barrier, total)


def times(n, step, first=0):
    def one(i, carry):
        step(i)
        return carry
    lax.fori_loop(first, n, one, 0)


def column_lane(z, me, c, source, landing, sends, recvs):
    return Lane(z, me, "fsdp", lambda to: source(c, to), lambda p: landing(c, p), sends.at[c], recvs.at[c])


def nn(a, b):
    return lax.dot_general(a, b, (((1,), (0,)), ((), ())), preferred_element_type=jnp.float32)


def nt(a, b):
    return lax.dot_general(a, b, (((1,), (1,)), ((), ())), preferred_element_type=jnp.float32)


def tn(a, b):
    return lax.dot_general(a, b, (((0,), (0,)), ((), ())), preferred_element_type=jnp.float32)


def lane_of(shape):
    return lax.broadcasted_iota(jnp.int32, shape, 1)


def rope_tables(place_columns, frequency):
    angles = place_columns.astype(jnp.float32) * frequency
    return jnp.cos(angles), jnp.sin(angles)


def rope(x, cosine, sine):
    half = HEAD // 2
    mixed = jnp.where(lax.rem(lane_of(x.shape), HEAD) < half, -pltpu.roll(x, LANES - half, 1), pltpu.roll(x, half, 1))
    return x * cosine + mixed * sine


def rows_at(ref, i, n):
    return ref.at[pl.ds(pl.multiple_of(i * n, n), n), :]


def vmem(shape, dtype=jnp.bfloat16):
    return pltpu.VMEM(shape, dtype)


def frequencies():
    lanes = np.arange(LANES)
    steps = rope_base ** ((lanes % (HEAD // 2)) * (-2.0 / HEAD))
    return jnp.asarray(np.stack([steps, np.where(lanes < HEAD, steps, 0.0)] + [steps] * 6), jnp.float32)


def exact(kind, a, b):
    dims = {"nn": ((1,), (0,)), "nt": ((1,), (1,)), "tn": ((0,), (0,))}[kind]
    return lax.dot_general(a, b, (dims, ((), ())), precision=lax.Precision.HIGHEST, preferred_element_type=jnp.float32)


CHAIN_GROUPS = dict(tok="line", wo="line", cot="col", rows="col", d_attn="line")
LANE_GROUPS = dict(
    place="ctx", wc="ctx", small="ctx", slot="col", gate_a="ctx", gate_b="ctx", up="ctx",
    down="ctx", att="ctx", gates="col", part="col", turn="col", mix="col", dn="line", gc="ctx",
    gs="ctx", go="fsdp", grad0="ctx", grad1="ctx", grad2="ctx", grad3="ctx", grad4="ctx", grad5="ctx")
PLANE_LANES = ["cot", "row", "g", "back", "dg", "out"]
COLUMN_LANES = ["wc", "small", "wo", "gc", "gs"]
RELAYS = ["tok", "wo", "d_attn", "sib"]


def layer_kernel(z, R, dc, tile, names, *refs):
    r = types.SimpleNamespace(**dict(zip(names, refs)))
    me = z.place(lax.axis_index("ctx"), lax.axis_index("fsdp"))
    C, F, H, P, J, rs, qw = z.C, z.F, z.H, z.P, z.J, z.rows_w, z.q_width
    L = C * R
    half = dc // 2
    low, high = pl.ds(0, half), pl.ds(half, half)
    sems = lambda kind, name: (getattr(r, kind + name + "_send"), getattr(r, kind + name + "_recv"))

    def at_slot(ref, h, p):
        return rows_at(ref, h * P + p, CAP)

    def lane(name, source, landing):
        return Lane(z, me, LANE_GROUPS[name], source, landing, *sems("lane_", name))

    def chain(name, own, landing):
        return Chain(z, me, CHAIN_GROUPS[name], own, landing, *sems("chain_", name))

    def plane(name, source, landing):
        def at(h):
            send, recv = sems("plane_", name)
            land = lambda p: at_slot(landing, h, p.p) if len(landing.shape) == 2 else landing.at[h, p.p]
            return Lane(z, me, "plane", lambda to: source.at[h, to.p], land, send.at[h], recv.at[h])
        return at

    def column(name, source, landing):
        return lambda c: column_lane(z, me, c, source, landing, *sems("column_", name))

    def relay(name, own, landing):
        return Relay(z, me, own, landing, *sems("relay_", name))

    tok_chain = chain("tok", r.tok, lambda place: r.blocks.at[2 * place + me.k])
    tok_relay = relay("tok", r.tok, lambda c: r.blocks.at[c])
    place_lane = lane("place", lambda to: r.place, lambda p: r.place_all.at[p.c])
    wc_lane = lane("wc", lambda to: r.w_pack.at[to.c], lambda p: rows_at(r.wc_v, p.w, rs))
    small_lane = lane("small", lambda to: r.small, lambda p: rows_at(r.small_v, p.w, rs))
    wo_chain = chain("wo", r.w_out, lambda place: rows_at(r.wo_v, (2 * place + me.k) * F + me.f, rs))
    wo_relay = relay("wo", r.w_out, lambda c: rows_at(r.wo_v, c * F + me.f, rs))
    spread = lambda name, ref: column(
        name, lambda c, to: rows_at(ref, c * F + me.f, rs), lambda c, p: rows_at(ref, c * F + p.f, rs))
    wc_column, small_column, wo_column = spread("wc", r.wc_v), spread("small", r.small_v), spread("wo", r.wo_v)
    cot_chain = chain("cot", r.cot, lambda h: r.cot_all.at[h])
    slot_lane = lane("slot", lambda to: r.slot_t.at[pl.ds(0, EXPERTS), :], lambda p: r.slot_all.at[p.h])
    gate_a_lane = lane("gate_a", lambda to: r.w_gate.at[to.m, low], lambda p: r.wv.at[0, p.c, low])
    gate_b_lane = lane("gate_b", lambda to: r.w_gate.at[to.m, high], lambda p: r.wv.at[0, p.c, high])
    up_lane = lane("up", lambda to: r.w_up.at[to.m], lambda p: r.wv.at[1, p.c])
    down_lane = lane("down", lambda to: r.w_downt.at[to.m], lambda p: r.wv.at[2, p.c])
    att_lane = lane("att", lambda to: r.att_stage.at[to.c], lambda p: r.att_in.at[p.c])
    rows_chain = chain("rows", r.h2, lambda h: r.h_all.at[h])
    gates_lane = lane("gates", lambda to: r.gates_t.at[pl.ds(0, EXPERTS), :], lambda p: r.gate_all.at[p.h])
    part_lane = lane("part", lambda to: r.part_stage.at[to.h], lambda p: r.part_in.at[p.h])
    turn_lane = lane("turn", lambda to: r.turn_stage.at[to.h], lambda p: r.turn_in.at[p.h])
    up_attn_chain = chain("d_attn", r.d_attn, lambda place: r.blocks.at[2 * place + me.k])
    up_attn_relay = relay("d_attn", r.d_attn, lambda c: r.blocks.at[c])
    mix_lane = lane("mix", lambda to: r.part_stage.at[to.h], lambda p: r.mix_in.at[p.h])
    dn_block = lambda c: rows_at(r.pool, c, R)
    dn_in = lambda j: rows_at(r.xin, j, R)
    sib_in = lambda j: rows_at(r.cot_v, j, R)
    dn_lane = lane("dn", lambda to: dn_block(to.c), lambda p: dn_in(lax.div(p.c, 2)))
    gc_lane = lane("gc", lambda to: r.gc_sum.at[to.c], lambda p: r.gc_in.at[p.c])
    gs_lane = lane("gs", lambda to: r.gs_sum.at[to.c], lambda p: r.gs_in.at[p.c])
    go_lane = lane("go", lambda to: rows_at(r.go_stage, to.f, rs), lambda p: r.go_in.at[p.f])
    gather = lambda name, stage, landing: column(
        name, lambda c, to: rows_at(stage, c * F + to.f, rs), lambda c, p: landing.at[p.f, c])
    gc_column, gs_column = gather("gc", r.gc_stage, r.gc_x), gather("gs", r.gs_stage, r.gs_x)
    grad_of = lambda j, c: rows_at(r.g_down, c, dc) if j == 2 else r.wv.at[j, c]
    grad_lanes = [
        lane("grad" + str(2 * j + i),
             lambda to, j=j, i=i: grad_of(j, to.c).at[(low, high)[i]],
             lambda p, j=j, i=i: r.gw_in.at[j, p.s, p.m, (low, high)[i]])
        for j in range(3) for i in range(2)
    ]
    cot_plane = plane("cot", r.d_rows, r.cot_v)
    row_plane = plane("row", r.stage, r.xin)
    g_plane = plane("g", r.g_stage, r.gin)
    back_plane = plane("back", r.d_rows, r.stage)
    dg_plane = plane("dg", r.dg_stage, r.dg_in)
    out_plane = plane("out", r.result, r.out_in)

    def sib_copy(j):
        send, recv = sems("relay_", "sib")
        return pltpu.make_async_remote_copy(
            src_ref=dn_block(2 * j + 1 - me.k), dst_ref=sib_in(j), send_sem=send.at[j], recv_sem=recv.at[j],
            device_id=(me.c + 1 - 2 * me.k, me.f), device_id_type=MESH)

    meet(z, me, ["ctx", "plane", "fsdp"])
    wc_lane.start()
    small_lane.start()
    place_lane.start()

    own = [
        pltpu.make_async_copy(r.w_pack.at[me.c], rows_at(r.wc_v, me.w, rs), r.own_sem.at[0]),
        pltpu.make_async_copy(r.small, rows_at(r.small_v, me.w, rs), r.own_sem.at[1]),
        pltpu.make_async_copy(r.w_out, rows_at(r.wo_v, me.w, rs), r.own_sem.at[2]),
    ]
    own_weights = [
        pltpu.make_async_copy(source.at[me.m], r.wv.at[j, me.c], r.own_sem.at[3 + j])
        for j, source in enumerate([r.w_gate, r.w_up, r.w_downt])
    ]
    for copy in own + own_weights:
        copy.start()
    r.blocks[me.c] = r.tok[...]
    r.place_all[me.c] = r.place[...]
    r.cot_all[me.h] = r.cot[...]

    named = jnp.zeros((R, LANES), jnp.float32)
    for j in range(TOP):
        named = jnp.where(r.routes[:, j : j + 1] == lane_of((R, LANES)), 1.0, named)
    row_id = lax.broadcasted_iota(jnp.int32, (R, R), 0)
    before = jnp.where(row_id > lane_of((R, R)), 1.0, 0.0).astype(jnp.bfloat16)
    slot = nn(before, named.astype(jnp.bfloat16))
    r.slot_t[...] = jnp.where(named > 0.5, slot, -1.0).T
    r.slot_all[me.h] = r.slot_t[0:EXPERTS, :]
    slot_lane.start()
    slot_id = lax.broadcasted_iota(jnp.int32, (CAP, R), 0).astype(jnp.float32)

    wc_lane.wait_recv()
    small_lane.wait_recv()
    wo_relay.start_own()
    wo_chain.start()
    tok_relay.start_own()
    tok_chain.start()
    cot_chain.start()
    for copy in own:
        copy.wait()
    times(C, lambda c: wc_column(c).start())
    times(C, lambda c: small_column(c).start())

    def choose(j):
        h = lax.rem(me.h + H - j, H)
        @pl.when(j > 0)
        def _():
            slot_lane.wait_recv_one(j)

        def for_expert(p):
            row = r.slot_all[h, pl.ds(z.expert(me, p), 1), :]
            r.pick[h, p] = jnp.where(row == slot_id, 1.0, 0.0).astype(jnp.bfloat16)
        times(P, for_expert)

    def dispatch_cot(h):
        def to_expert(n):
            p = lax.rem(me.p + n, P)
            r.d_rows[h, p] = nn(r.pick[h, p], r.cot_all[h]).astype(jnp.bfloat16)
            @pl.when(n > 0)
            def _():
                cot_plane(h).start_one(n)
        times(P, to_expert)
        at_slot(r.cot_v, h, me.p)[...] = r.d_rows[h, me.p]
    place_lane.wait_recv()
    times(C, lambda c: wc_column(c).wait_recv())
    times(C, lambda c: small_column(c).wait_recv())
    times(H, choose)
    wo_chain.visit(lambda place, core: wo_column(2 * place + core).start(), wo_relay)
    gain_one = r.small_v[...].astype(jnp.float32).T[EXPERTS : EXPERTS + 1, :]
    gain_two = r.small_v[...].astype(jnp.float32).T[EXPERTS + 1 : EXPERTS + 2, :]
    head_of = lax.div(lane_of((R, LANES)), HEAD)

    def project(place, core):
        c = 2 * place + core
        x = r.blocks[c].astype(jnp.float32)
        inverse = lax.rsqrt(jnp.mean(x * x, axis=-1, keepdims=True) + norm_eps)
        h = (x * inverse * gain_one).astype(jnp.bfloat16)
        part = pl.ds(pl.multiple_of(c * R, R), R)
        r.h1[part, :] = h
        qkv = nn(h, r.wc_v[...])
        row = r.place_all[c][0:1, :].astype(jnp.float32)
        r.place_row[c] = jnp.broadcast_to(row, (8, R))
        places = jnp.broadcast_to(row, (R, R)).T
        r.place_col[part, :] = places
        r.q_all[part, :] = rope(qkv[:, :LANES], *rope_tables(places, r.freq[0:1, :])).astype(jnp.bfloat16)
        kv = rope(qkv[:, LANES:], *rope_tables(places, r.freq[1:2, :]))
        swapped = pltpu.roll(kv, HEAD, 1)
        r.k2[part, :] = jnp.where(head_of == 0, kv, swapped).astype(jnp.bfloat16)
        r.v2[part, :] = jnp.where(head_of == 0, swapped, kv).astype(jnp.bfloat16)
    tok_chain.visit(project, tok_relay)
    gate_a_lane.start()
    tok_relay.wait_send()

    def attend(c):
        part = pl.ds(pl.multiple_of(c * R, R), R)
        q = r.q_all[part, :]
        row = jnp.concatenate([r.place_row[i, 0:1, :] for i in range(C)], axis=1)
        allowed = row <= r.place_col[part, 0:1]
        total = jnp.zeros((R, LANES), jnp.float32)
        for h in range(z.q_heads):
            mine = head_of == h
            s = nt(jnp.where(mine, q, jnp.zeros_like(q)), r.k2[...]) * score_scale
            s = jnp.where(allowed, s, masked_score)
            top = jnp.max(s, axis=-1, keepdims=True)
            e = jnp.exp(s - top)
            weight = jnp.sum(e, axis=-1, keepdims=True)
            r.lse[h, part, :] = jnp.broadcast_to(top + jnp.log(weight), (R, LANES))
            total = jnp.where(mine, nn(e.astype(jnp.bfloat16), r.v2[...]) / weight, total)
        r.att_f[part, :] = total
        r.att_stage[c] = total.astype(jnp.bfloat16)
    times(C, attend)
    tok_chain.wait_send()
    att_lane.start()
    r.att_in[me.c] = r.att_stage[me.c]
    cot_chain.visit(dispatch_cot)
    att_lane.wait_recv()
    times(C, lambda c: wo_column(c).wait_recv())
    x = r.tok[...].astype(jnp.float32)
    mixed = jnp.zeros((R, D), jnp.float32)
    for c in range(C):
        mixed = mixed + nn(r.att_in[c][:, :qw], r.wo_v[c * qw : (c + 1) * qw, :])
    mid = x + residual_scale * mixed
    r.middle[...] = mid
    inverse = lax.rsqrt(jnp.mean(mid * mid, axis=-1, keepdims=True) + norm_eps)
    hidden = (mid * inverse * gain_two).astype(jnp.bfloat16)
    r.h2[...] = hidden
    rows_chain.start()
    chosen = r.slot_t[...].T > -0.5
    logits = jnp.where(chosen, nn(hidden, r.small_v[...]), masked_score)
    raised = jnp.where(chosen, jnp.exp(logits - jnp.max(logits, axis=-1, keepdims=True)), 0.0)
    r.gates_t[...] = (raised / jnp.sum(raised, axis=-1, keepdims=True)).T
    gates_lane.start()
    r.h_all[me.h] = r.h2[...]
    r.gate_all[me.h] = r.gates_t[0:EXPERTS, :]

    def dispatch_rows(h):
        @pl.when(h != me.h)
        def _():
            gates_lane.wait_recv_one(lax.rem(me.h + H - h, H))

        def to_expert(n):
            p = lax.rem(me.p + n, P)
            hot = r.pick[h, p]
            r.stage[h, p] = nn(hot, r.h_all[h]).astype(jnp.bfloat16)
            g = jnp.broadcast_to(r.gate_all[h, pl.ds(z.expert(me, p), 1), :], (8, R))
            wide = jnp.concatenate([hot.astype(jnp.float32), jnp.zeros((LANES - CAP, R), jnp.float32)], axis=0)
            r.g_stage[h, p] = exact("nt", g, wide)
            @pl.when(n > 0)
            def _():
                row_plane(h).start_one(n)
        times(P, to_expert)
        at_slot(r.xin, h, me.p)[...] = r.stage[h, me.p]
        r.gin[h, me.p] = r.g_stage[h, me.p]
    rows_chain.visit(dispatch_rows)
    gate_b_lane.start()
    up_lane.start()
    down_lane.start()

    def send_gates(j):
        h = lax.rem(me.h + H - j, H)

        def to_expert(n):
            row_plane(h).wait_send_one(n)
            g_plane(h).start_one(n)
        times(P, to_expert, 1)
    times(H, send_gates)
    times(H, lambda h: cot_plane(h).wait_send())
    for copy in own_weights:
        copy.wait()
    for bulk in [gate_a_lane, gate_b_lane, up_lane]:
        bulk.wait_recv()
    times(H, lambda h: cot_plane(h).wait_recv())
    wg, wu, wd = [r.wv.at[j].reshape(D, r.wv.shape[3]) for j in range(3)]
    per = tile // CAP

    def forward(j):
        h = lax.rem(me.h + H - lax.rem(j + 1, H), H)
        row_plane(h).wait_recv()
        g_plane(h).wait_recv()

        def rows(t):
            part = pl.ds(pl.multiple_of((h * P + t * per) * CAP, CAP), tile)
            for p in range(per):
                turned = jnp.broadcast_to(r.gin[h, t * per + p, 0:1, :], (LANES, LANES)).T
                r.g_col[p * CAP : (p + 1) * CAP, :] = turned[0:CAP, :]
            x = r.xin[part, :]
            r.hid[part, :] = (jax.nn.silu(nn(x, wg[...])) * nn(x, wu[...])).astype(jnp.bfloat16)
            r.pool[part, :] = (residual_scale * r.g_col[:, 0:1] * r.cot_v[part, :].astype(jnp.float32)).astype(jnp.bfloat16)
        times(P // per, rows)
    times(H, forward)

    def cut_down(d):
        part = pl.ds(pl.multiple_of(d * 256, 256), 256)
        r.g_down[part, :] = tn(r.pool[pl.ds(0, H * P * CAP), part], r.hid[...]).astype(jnp.bfloat16)
    times(D // 256, cut_down)
    grad_lanes[4].start()
    grad_lanes[5].start()
    down_lane.wait_recv()

    def chunk(j):
        h = lax.rem(me.h + H - lax.rem(j + 1, H), H)

        def rows(t):
            some = pl.ds(pl.multiple_of(t * per, per), per)
            part = pl.ds(pl.multiple_of((h * P + t * per) * CAP, CAP), tile)
            x = r.xin[part, :]
            gate = nn(x, wg[...])
            up = nn(x, wu[...])
            sig = jax.nn.sigmoid(gate)
            act = gate * sig
            out = nt(r.hid[part, :], wd[...]).astype(jnp.bfloat16)
            r.result[h, some] = out.reshape(per, CAP, D)
            upstream = r.cot_v[part, :].astype(jnp.float32)
            d_gates = residual_scale * jnp.sum(upstream * out.astype(jnp.float32), axis=-1, keepdims=True)
            d_hidden = nn(r.pool[part, :], wd[...])
            dg = (d_hidden * up * sig * (1.0 + gate * (1.0 - sig))).astype(jnp.bfloat16)
            du = (d_hidden * act).astype(jnp.bfloat16)
            r.d_gate[part, :] = dg
            r.d_up[part, :] = du
            r.d_rows[h, some] = (nt(dg, wg[...]) + nt(du, wu[...])).astype(jnp.bfloat16).reshape(per, CAP, D)
            r.g_col[...] = jnp.broadcast_to(d_gates, (tile, LANES))
            for p in range(per):
                turned = jnp.concatenate(
                    [r.g_col[p * CAP : (p + 1) * CAP, :], jnp.zeros((LANES - CAP, LANES), jnp.float32)], axis=0)
                r.dg_stage[h, t * per + p] = turned.T[0:8, :]
        times(P // per, rows)
        back_plane(h).start()
        dg_plane(h).start()
        r.stage[h, me.p] = r.d_rows[h, me.p]
        r.dg_in[h, me.p] = r.dg_stage[h, me.p]
    times(H, chunk)

    def cut(d):
        part = pl.ds(pl.multiple_of(d * 256, 256), 256)
        x = r.xin[:, part]
        wg[part, :] = tn(x, r.d_gate[...]).astype(jnp.bfloat16)
        wu[part, :] = tn(x, r.d_up[...]).astype(jnp.bfloat16)
    times(D // 256, cut)
    grad_lanes[0].start()
    own_grads = [
        pltpu.make_async_copy(grad_of(j, me.c), r.gw_in.at[j, me.s, me.m], r.own_sem.at[8 + j]) for j in range(3)
    ]
    for copy in own_grads:
        copy.start()

    def collect(j):
        n = lax.rem(j + 1, H)
        h = lax.rem(me.h + H - n, H)
        back_plane(h).wait_recv()
        dg_plane(h).wait_recv()
        part = tn(r.pick[h].reshape(P * CAP, R), r.stage[h].reshape(P * CAP, D))
        r.turn_stage[h] = jnp.zeros((EXPERTS, R), jnp.float32)

        def gates_of(p):
            row = jnp.broadcast_to(r.dg_in[h, p, 0:1, 0:CAP], (8, CAP))
            r.turn_stage[h, pl.ds(z.expert(me, p), 1), :] = exact("nn", row, r.pick[h, p].astype(jnp.float32))[0:1, :]
        times(P, gates_of)
        @pl.when(n > 0)
        def _():
            r.part_stage[h] = part.astype(jnp.bfloat16)
            part_lane.start_one(H - n)
            turn_lane.start_one(H - n)
        @pl.when(n == 0)
        def _():
            r.d_mid[...] = part
            r.turn_v[...] = jnp.zeros((LANES, R), jnp.float32)
            r.turn_v[0:EXPERTS, :] = r.turn_stage[h]
    times(H, collect)
    times(H, lambda h: out_plane(h).start())
    own_out = pltpu.make_async_copy(r.result.at[:, me.p], r.out_in.at[:, me.p], r.own_sem.at[7])
    own_out.start()
    part_lane.wait_recv()
    turn_lane.wait_recv()

    def add_part(n):
        h = lax.rem(me.h + n + 1, H)
        r.d_mid[...] += r.part_in[h].astype(jnp.float32)
        r.turn_v[0:EXPERTS, :] += r.turn_in[h]
    times(H - 1, add_part)
    gts = r.gates_t[...].T
    dgs = r.turn_v[...].T
    d_log = gts * (dgs - jnp.sum(gts * dgs, axis=-1, keepdims=True))
    d_h2 = r.d_mid[...] + exact("nt", d_log, r.small_v[...].astype(jnp.float32))
    mid = r.middle[...]
    inverse = lax.rsqrt(jnp.mean(mid * mid, axis=-1, keepdims=True) + norm_eps)
    n2 = mid * inverse
    g = d_h2 * gain_two
    dm = r.cot[...].astype(jnp.float32) + inverse * (g - n2 * jnp.mean(g * n2, axis=-1, keepdims=True))
    r.d_mid[...] = dm
    r.d_attn[...] = (residual_scale * dm).astype(jnp.bfloat16)
    up_attn_relay.start_own()
    up_attn_chain.start()
    r.gain_v[...] = jnp.zeros((LANES, D), jnp.float32)
    r.gain_v[EXPERTS + 1 : EXPERTS + 2, :] = jnp.sum(d_h2 * n2, axis=0, keepdims=True)
    r.g_small[...] = exact("tn", r.h2[...].astype(jnp.float32), d_log)

    r.blocks[me.c] = r.d_attn[...]
    r.dk_acc[...] = jnp.zeros((L, LANES), jnp.float32)
    r.dv_acc[...] = jnp.zeros((L, LANES), jnp.float32)
    wo_c = rows_at(r.wo_v, me.c, qw)

    def attend_back(place, core):
        c = 2 * place + core
        part = pl.ds(pl.multiple_of(c * R, R), R)
        q = r.q_all[part, :]
        d_mix = nt(r.blocks[c], wo_c[...])
        if qw < LANES:
            d_mix = jnp.concatenate([d_mix, jnp.zeros((R, LANES - qw), jnp.float32)], axis=1)
        d_mix = d_mix.astype(jnp.bfloat16)
        row = jnp.concatenate([r.place_row[i, 0:1, :] for i in range(C)], axis=1)
        places = r.place_col[part, :]
        allowed = row <= places[:, 0:1]
        dq = jnp.zeros((R, LANES), jnp.float32)
        for h in range(z.q_heads):
            mine = head_of == h
            rows = pl.ds(h * R, R)
            q_h = jnp.where(mine, q, jnp.zeros_like(q))
            dm_h = jnp.where(mine, d_mix, jnp.zeros_like(d_mix))
            r.q_v[rows, :] = q_h
            r.dm_v[rows, :] = dm_h
            s = jnp.where(allowed, nt(q_h, r.k2[...]) * score_scale, masked_score)
            p = jnp.exp(s - r.lse[h, part, 0:1])
            r.p_v[rows, :] = p.astype(jnp.bfloat16)
            delta = jnp.sum(dm_h.astype(jnp.float32) * r.att_f[part, :], axis=-1, keepdims=True)
            ds = (p * (nt(dm_h, r.v2[...]) - delta)).astype(jnp.bfloat16)
            r.ds_v[rows, :] = ds
            dq = jnp.where(mine, nn(ds, r.k2[...]) * score_scale, dq)
        r.dk_acc[...] += tn(r.ds_v[...], r.q_v[...])
        r.dv_acc[...] += tn(r.p_v[...], r.dm_v[...])
        cosine, sine = rope_tables(places, r.freq[0:1, :])
        r.d_qkv[part, 0:LANES] = rope(dq, cosine, -sine).astype(jnp.bfloat16)
    up_attn_chain.visit(attend_back, up_attn_relay)
    grad_lanes[1].start()

    def finish_kv(c):
        part = pl.ds(pl.multiple_of(c * R, R), R)
        dk = r.dk_acc[part, :] * score_scale
        dv = r.dv_acc[part, :]
        dk = dk + pltpu.roll(dk, HEAD, 1)
        dv = dv + pltpu.roll(dv, HEAD, 1)
        cosine, sine = rope_tables(r.place_col[part, :], r.freq[1:2, :])
        r.d_qkv[part, LANES : 2 * LANES] = rope(jnp.where(head_of == 0, dk, dv), cosine, -sine).astype(jnp.bfloat16)
    times(C, finish_kv)

    def down_tokens(c):
        return nt(r.d_qkv[pl.ds(pl.multiple_of(c * R, R), R), :], r.wc_v[...])

    def for_sibling(j):
        c = 2 * j + 1 - me.k
        dn_block(c)[...] = down_tokens(c).astype(jnp.bfloat16)
        sib_copy(j).start()
    times(J, for_sibling)

    def for_line(i):
        n = lax.rem(i + 1, J)
        to = z.peer("line", me, n)
        dn = down_tokens(to.c)
        j = lax.div(to.c, 2)
        sib_copy(j).wait_recv()
        dn_block(to.c)[...] = (dn + sib_in(j)[...].astype(jnp.float32)).astype(jnp.bfloat16)
        @pl.when(n > 0)
        def _():
            dn_lane.start_one(n)
    times(J, for_line)
    dn_in(lax.div(me.c, 2))[...] = dn_block(me.c)[...]

    own_out.wait()
    part_lane.wait_send()

    def mix(i):
        n = lax.rem(i + 1, H)
        h = lax.rem(me.h + H - n, H)
        out_plane(h).wait_recv()
        load = pltpu.make_async_copy(r.out_in.at[h], r.stage.at[h], r.own_sem.at[12])
        load.start()

        def weigh(p):
            g = r.gate_all[h, pl.ds(z.expert(me, p), 1), :] * r.pick[h, p].astype(jnp.float32)
            high = g.astype(jnp.bfloat16)
            r.mix_hi[p] = high
            r.mix_lo[p] = (g - high.astype(jnp.float32)).astype(jnp.bfloat16)
        times(P, weigh)
        load.wait()
        rows = r.stage[h].reshape(P * CAP, D)
        total = tn(r.mix_hi[...].reshape(P * CAP, R), rows) + tn(r.mix_lo[...].reshape(P * CAP, R), rows)
        r.part_stage[h] = total.astype(jnp.bfloat16)
        @pl.when(n > 0)
        def _():
            mix_lane.start_one(H - n)
        @pl.when(n == 0)
        def _():
            r.grad_tokens[...] = total
    times(H, mix)
    grad_lanes[2].start()
    grad_lanes[3].start()

    def weights(d):
        part = pl.ds(pl.multiple_of(d * 256, 256), 256)
        total = tn(r.h1[:, part], r.d_qkv[...])
        r.gc_stage[part, :] = total.astype(jnp.bfloat16)
        gain = jnp.sum(total * r.wc_v[part, :].astype(jnp.float32), axis=-1, keepdims=True)
        gain = gain / r.small_v[part, EXPERTS : EXPERTS + 1].astype(jnp.float32)
        r.g_small[part, :] = jnp.where(lane_of((256, LANES)) == EXPERTS, gain, r.g_small[part, :])
    times(D // 256, weights)
    times(C, lambda c: gc_column(c).start())
    r.gs_stage[...] = (r.g_small[...] + r.gain_v[...].T).astype(jnp.bfloat16)
    times(C, lambda c: gs_column(c).start())
    own_last = [
        pltpu.make_async_copy(rows_at(stage, c * F + me.f, rs), landing.at[me.f, c], r.own_cols.at[i, c])
        for i, (stage, landing) in enumerate([(r.gc_stage, r.gc_x), (r.gs_stage, r.gs_x)]) for c in range(C)
    ]
    for copy in own_last:
        copy.start()
    r.go_stage[...] = tn(r.att_f[...].astype(jnp.bfloat16), r.blocks[...].reshape(L, D)).astype(jnp.bfloat16)
    go_lane.start()
    own_go = pltpu.make_async_copy(rows_at(r.go_stage, me.f, rs), r.go_in.at[me.f], r.own_sem.at[13])
    own_go.start()
    for copy in own_last:
        copy.wait()
    times(C, lambda c: gc_column(c).wait_recv())
    times(C, lambda c: gs_column(c).wait_recv())
    gc_total = r.gc_x[0].astype(jnp.float32)
    gs_total = r.gs_x[0].astype(jnp.float32)
    for f in range(1, F):
        gc_total = gc_total + r.gc_x[f].astype(jnp.float32)
        gs_total = gs_total + r.gs_x[f].astype(jnp.float32)
    r.gc_sum[...] = gc_total.astype(jnp.bfloat16)
    r.gs_sum[...] = gs_total.astype(jnp.bfloat16)
    gc_lane.start()
    gs_lane.start()
    own_sums = [
        pltpu.make_async_copy(r.gc_sum.at[me.c], r.gc_in.at[me.c], r.own_sem.at[14]),
        pltpu.make_async_copy(r.gs_sum.at[me.c], r.gs_in.at[me.c], r.own_sem.at[15]),
    ]
    for copy in own_sums:
        copy.start()
    mix_lane.wait_recv()

    def add_mix(n):
        r.grad_tokens[...] += r.mix_in[lax.rem(me.h + n + 1, H)].astype(jnp.float32)
    times(H - 1, add_mix)
    r.output[...] = (r.middle[...] + residual_scale * r.grad_tokens[...]).astype(jnp.bfloat16)

    dn_lane.wait_recv()
    d_h1 = dn_in(0)[...].astype(jnp.float32)
    for c in range(1, J):
        d_h1 = d_h1 + dn_in(c)[...].astype(jnp.float32)
    x = r.tok[...].astype(jnp.float32)
    inverse = lax.rsqrt(jnp.mean(x * x, axis=-1, keepdims=True) + norm_eps)
    n1 = x * inverse
    g = d_h1 * gain_one
    r.grad_tokens[...] = r.d_mid[...] + inverse * (g - n1 * jnp.mean(g * n1, axis=-1, keepdims=True))
    for last in [gc_lane, gs_lane, go_lane]:
        last.wait_recv()
    for last in grad_lanes:
        last.wait_recv()
    for last in [place_lane, wc_lane, small_lane, slot_lane, gate_a_lane, gate_b_lane, up_lane, down_lane, att_lane, gates_lane,
                 turn_lane, mix_lane, dn_lane, gc_lane, gs_lane, go_lane] + grad_lanes:
        last.wait_send()
    for last in [wo_chain, cot_chain, rows_chain, up_attn_chain]:
        last.wait_send()
    for last in [wo_relay, up_attn_relay]:
        last.wait_send()
    times(J, lambda j: sib_copy(j).wait_send())
    for last in [g_plane, back_plane, dg_plane, out_plane]:
        times(H, lambda h, last=last: last(h).wait_send())
    for last in [wc_column, small_column, wo_column, gc_column, gs_column]:
        times(C, lambda c, last=last: last(c).wait_send())
    for copy in own_grads + own_sums + [own_go]:
        copy.wait()


def layer_call(z, R, ff, dc, tok, place, routes, cot, w_pack, small, w_out, w_gate, w_up, w_downt):
    C, F, N, H, P, J, S, rs = z.C, z.F, z.N, z.H, z.P, z.J, z.S, z.rows_w
    L, f, f16 = C * R, jnp.float32, jnp.bfloat16
    rows, heads, tile = H * P * CAP, z.q_heads * R, 8 * CAP
    ins = dict(tok=(tok, 1), place=(place, 1), routes=(routes, 1), cot=(cot, 1), freq=(frequencies(), 1), w_pack=(w_pack, 0),
               small=(small, 0), w_out=(w_out, 0), w_gate=(w_gate, 0), w_up=(w_up, 0), w_downt=(w_downt, 0))
    outs = dict(
        output=(shape_of((R, D)), 1), grad_tokens=(shape_of((R, D), f), 1), gc_in=(shape_of((C, rs, 2 * LANES)), 0),
        gs_in=(shape_of((C, rs, LANES)), 0), go_in=(shape_of((F, rs, D)), 0), gw_in=(shape_of((3, S, z.G, dc, ff)), 0),
        out_in=(shape_of((H, P, CAP, D)), 0))
    scratch = dict(
        blocks=vmem((C, R, D)), place_all=vmem((C, 8, R), jnp.int32), wc_v=vmem((D, 2 * LANES)), small_v=vmem((D, LANES)),
        wo_v=vmem((D, D)), cot_all=vmem((H, R, D)), slot_all=vmem((H, EXPERTS, R), f), slot_t=vmem((LANES, R), f),
        place_col=vmem((L, R), f), place_row=vmem((C, 8, R), f), h1=vmem((L, D)), q_all=vmem((L, LANES)), k2=vmem((L, LANES)),
        v2=vmem((L, LANES)), lse=vmem((z.q_heads, L, LANES), f), att_f=vmem((L, LANES), f), att_stage=vmem((C, R, LANES)),
        att_in=vmem((C, R, LANES)), middle=vmem((R, D), f), h2=vmem((R, D)), gates_t=vmem((LANES, R), f),
        gate_all=vmem((H, EXPERTS, R), f), h_all=vmem((H, R, D)), pick=vmem((H, P, CAP, R)), stage=vmem((H, P, CAP, D)),
        xin=vmem((rows, D)), g_stage=vmem((H, P, 8, LANES), f), gin=vmem((H, P, 8, LANES), f), wv=vmem((3, C, dc, ff)),
        cot_v=vmem((rows, D)), d_rows=vmem((H, P, CAP, D)), dg_stage=vmem((H, P, 8, LANES), f),
        dg_in=vmem((H, P, 8, LANES), f), hid=vmem((rows, ff)), d_gate=vmem((rows, ff)), d_up=vmem((rows, ff)),
        pool=vmem((max(rows, L), D)), g_col=vmem((tile, LANES), f), result=vmem((H, P, CAP, D)),
        part_stage=vmem((H, R, D)), part_in=vmem((H, R, D)), turn_stage=vmem((H, EXPERTS, R), f),
        turn_in=vmem((H, EXPERTS, R), f), turn_v=vmem((LANES, R), f), d_mid=vmem((R, D), f), d_attn=vmem((R, D)),
        g_small=vmem((D, LANES), f), g_down=vmem((D, ff)), gain_v=vmem((LANES, D), f), ds_v=vmem((heads, L)), p_v=vmem((heads, L)),
        q_v=vmem((heads, LANES)), dm_v=vmem((heads, LANES)), dk_acc=vmem((L, LANES), f), dv_acc=vmem((L, LANES), f),
        d_qkv=vmem((L, 2 * LANES)),
        gc_stage=vmem((D, 2 * LANES)), go_stage=vmem((LANES, D)), gs_stage=vmem((D, LANES)), gc_x=vmem((F, C, rs, 2 * LANES)),
        gs_x=vmem((F, C, rs, LANES)), gc_sum=vmem((C, rs, 2 * LANES)), gs_sum=vmem((C, rs, LANES)), mix_hi=vmem((P, CAP, R)),
        mix_lo=vmem((P, CAP, R)), mix_in=vmem((H, R, D)), own_sem=pltpu.SemaphoreType.DMA((16,)),
        own_cols=pltpu.SemaphoreType.DMA((2, C)))
    both = ("_send", "_recv")
    scratch |= {"lane_" + n + b: pltpu.SemaphoreType.DMA((z.count(g),)) for n, g in LANE_GROUPS.items() for b in both}
    steps = {"col": 2 * H, "line": 2 * J}
    scratch |= {"chain_" + n + b: pltpu.SemaphoreType.DMA((steps[g],)) for n, g in CHAIN_GROUPS.items() for b in both}
    scratch |= {"plane_" + n + b: pltpu.SemaphoreType.DMA((H, P)) for n in PLANE_LANES for b in both}
    scratch |= {"column_" + n + b: pltpu.SemaphoreType.DMA((C, F)) for n in COLUMN_LANES for b in both}
    scratch |= {"relay_" + n + b: pltpu.SemaphoreType.DMA((J,)) for n in RELAYS for b in both}
    names = list(ins) + list(outs) + list(scratch)
    space = lambda fast: pl.BlockSpec(memory_space=pltpu.VMEM if fast else pl.ANY)
    results = pl.pallas_call(
        functools.partial(layer_kernel, z, R, dc, tile, names), name="layer",
        out_shape=[o for o, _ in outs.values()], in_specs=[space(fast) for _, fast in ins.values()],
        out_specs=[space(fast) for _, fast in outs.values()], scratch_shapes=list(scratch.values()),
        compiler_params=pltpu.CompilerParams(collective_id=0, has_side_effects=True, vmem_limit_bytes=67043328),
    )(*[a for a, _ in ins.values()])
    return results[:6]


def local(z, tokens, norm_first, w_query, w_key, w_value, w_out, norm_second, w_router,
          w_gate, w_up, w_down, positions, routes, cotangent):
    C, F = z.C, z.F
    R = tokens.shape[1]
    rs = z.rows_w
    ff = w_gate.shape[2]
    dc = D // C

    heads_q = jnp.pad(w_query.reshape(rs, C, z.q_width), ((0, 0), (0, 0), (0, LANES - z.q_width)))
    heads_k = jnp.repeat(w_key.reshape(rs, KV_HEADS, HEAD), z.share, axis=1)
    heads_v = jnp.repeat(w_value.reshape(rs, KV_HEADS, HEAD), z.share, axis=1)
    w_pack = jnp.concatenate([heads_q, heads_k, heads_v], axis=2).transpose(1, 0, 2)
    small = jnp.concatenate(
        [w_router, norm_first[:, None], norm_second[:, None], jnp.zeros((rs, 128 - EXPERTS - 2), jnp.bfloat16)], axis=1)
    place_pack = jnp.broadcast_to(positions[0][None, :], (8, R))
    w_downt = w_down.transpose(0, 2, 1)
    output, grad_tokens, gc_in, gs_in, go_in, gw_in = layer_call(
        z, R, ff, dc, tokens[0], place_pack, routes[0], cotangent[0], w_pack, small, w_out, w_gate, w_up, w_downt)
    gc = f32(gc_in)
    join = lambda a: a.reshape(KV_HEADS, z.share, rs, HEAD).sum(axis=1).transpose(1, 0, 2).reshape(rs, KV_HEADS * HEAD)
    gs = jnp.sum(f32(gs_in), axis=0)
    return (
        output[None],
        grad_tokens[None],
        gs[:, EXPERTS],
        gc[:, :, : z.q_width].transpose(1, 0, 2).reshape(rs, D),
        join(gc[:, :, LANES : LANES + HEAD]),
        join(gc[:, :, LANES + HEAD :]),
        jnp.sum(f32(go_in), axis=0),
        gs[:, EXPERTS + 1],
        gs[:, :EXPERTS],
        jnp.sum(f32(gw_in[0]), axis=0),
        jnp.sum(f32(gw_in[1]), axis=0),
        jnp.sum(f32(gw_in[2]), axis=0).transpose(0, 2, 1),
    )


def solution(mesh):
    row = P(("ctx", "fsdp"), None)
    vec = P(("ctx", "fsdp"))
    seq = P("fsdp", "ctx", None)
    down = P("fsdp", None, "ctx")
    return jax.shard_map(
        functools.partial(local, Sizes(mesh)),
        mesh=mesh,
        in_specs=(seq, vec, row, row, row, row, vec, row, seq, seq, down, P("fsdp", "ctx"), seq, seq),
        out_specs=(seq, seq, vec, row, row, row, row, vec, row, seq, seq, down),
        check_vma=False,
    )
```

```python
import collections
import functools
import types

import jax
import jax.numpy as jnp
import numpy as np
from jax import lax
from jax.experimental import pallas as pl
from jax.experimental.pallas import tpu as pltpu
from jax.sharding import PartitionSpec as P

D = 1024
HEADS = 16
KV_HEADS = 8
HEAD = 64
EXPERTS = 32
TOP = 8
CAP = 48
LANES = 128

residual_scale = 0.22
score_scale = 0.015625
rope_base = 10000.0
norm_eps = 1e-06
masked_score = -1e30

MESH = pl.DeviceIdType.MESH
Place = collections.namedtuple("Place", ["c", "f", "m", "s", "h", "k", "p", "w"])


class Sizes:
    def __init__(self, mesh):
        self.C = mesh.shape["ctx"]
        self.F = mesh.shape["fsdp"]
        self.N = self.C * self.F
        self.G = EXPERTS // self.F
        self.S = self.C // self.G
        self.H = self.G // 2
        self.P = 2 * self.F
        self.J = self.C // 2
        self.q_heads = HEADS // self.C
        self.q_width = self.q_heads * HEAD
        self.share = self.C // KV_HEADS
        self.rows_w = D // self.N

    def place(self, c, f):
        k = lax.rem(c, 2)
        return Place(c, f, lax.rem(c, self.G), lax.div(c, self.G), lax.rem(lax.div(c, 2), self.H), k, f * 2 + k, c * self.F + f)

    def count(self, group):
        return {"ctx": self.C, "fsdp": self.F, "world": self.N, "col": self.H, "line": self.J, "plane": self.P}[group]

    def peer(self, group, me, n):
        if group == "ctx":
            return self.place(lax.rem(me.c + n, self.C), me.f)
        if group == "fsdp":
            return self.place(me.c, lax.rem(me.f + n, self.F))
        if group == "world":
            w = lax.rem(me.w + n, self.N)
            return self.place(lax.div(w, self.F), lax.rem(w, self.F))
        if group == "col":
            return self.place(me.s * self.G + 2 * lax.rem(me.h + n, self.H) + me.k, me.f)
        if group == "line":
            return self.place(2 * lax.rem(lax.div(me.c, 2) + n, self.J) + me.k, me.f)
        p = lax.rem(me.p + n, self.P)
        return self.place(me.s * self.G + 2 * me.h + lax.rem(p, 2), lax.div(p, 2))

    def expert(self, me, p):
        return lax.div(p, 2) * self.G + 2 * me.h + lax.rem(p, 2)


def bf(x):
    return x.astype(jnp.bfloat16)


def f32(x):
    return x.astype(jnp.float32)


def shape_of(shape, dtype=jnp.bfloat16):
    return jax.ShapeDtypeStruct(shape, dtype)


class Lane:
    def __init__(self, sizes, me, group, src, dst, sends, recvs):
        self.sizes, self.me, self.group, self.src, self.dst = sizes, me, group, src, dst
        self.sends, self.recvs, self.n = sends, recvs, sizes.count(group)

    def copy(self, k, to, source, landing):
        return pltpu.make_async_remote_copy(
            src_ref=source, dst_ref=landing, send_sem=self.sends.at[k], recv_sem=self.recvs.at[k],
            device_id=(to.c, to.f), device_id_type=MESH)

    def to(self, k):
        return self.sizes.peer(self.group, self.me, k)

    def start_one(self, k):
        to = self.to(k)
        self.copy(k, to, self.src(to), self.dst(self.me)).start()

    def wait_recv_one(self, k):
        landed = self.dst(self.sizes.peer(self.group, self.me, self.n - k))
        self.copy(k, self.to(k), landed, landed).wait_recv()

    def wait_send_one(self, k):
        to = self.to(k)
        self.copy(k, to, self.src(to), self.dst(self.me)).wait_send()

    def each(self, step):
        def one(k, carry):
            step(k)
            return carry
        lax.fori_loop(1, self.n, one, 0)

    def start(self):
        self.each(self.start_one)

    def wait_recv(self):
        self.each(self.wait_recv_one)

    def wait_send(self):
        self.each(self.wait_send_one)


class Chain:
    def __init__(self, sizes, me, group, own, landing, sends, recvs):
        self.col = group == "col"
        self.place, self.n = (me.h, sizes.H) if self.col else (lax.div(me.c, 2), sizes.J)
        self.sizes, self.me, self.own, self.landing, self.sends, self.recvs = sizes, me, own, landing, sends, recvs

    def copy(self, t, to, source, landing):
        c = self.me.s * self.sizes.G + 2 * to + self.me.k if self.col else 2 * to + self.me.k
        return pltpu.make_async_remote_copy(
            src_ref=source, dst_ref=landing, send_sem=self.sends.at[t], recv_sem=self.recvs.at[t],
            device_id=(c, self.me.f), device_id_type=MESH)

    def inside(self, place):
        return jnp.logical_and(place >= 0, place < self.n)

    def origin(self, t):
        return self.place - (1 - 2 * lax.rem(t, 2)) * (lax.div(t, 2) + 1)

    def start(self):
        for t, to in ((0, self.place + 1), (1, self.place - 1)):
            @pl.when(self.inside(to))
            def _(t=t, to=to):
                self.copy(t, to, self.own, self.landing(self.place)).start()

    def take(self, t):
        sign = 1 - 2 * lax.rem(t, 2)
        here = self.landing(self.origin(t))
        self.copy(t, self.place - sign, here, here).wait_recv()
        @pl.when(self.inside(self.place + sign))
        def _():
            self.copy(t + 2, self.place + sign, here, here).start()

    def wait_send(self):
        def one(t, carry):
            to = self.place + 1 - 2 * lax.rem(t, 2)
            origin = to - (1 - 2 * lax.rem(t, 2)) * (lax.div(t, 2) + 1)
            @pl.when(jnp.logical_and(self.inside(to), self.inside(origin)))
            def _():
                self.copy(t, to, self.landing(self.place), self.landing(self.place)).wait_send()
            return carry
        lax.fori_loop(0, 2 * (self.n - 1), one, 0)

    def visit_some(self, step, first, last):
        def one(t):
            @pl.when(self.inside(self.origin(t)))
            def _():
                self.take(t)
                step(self.origin(t))
        times(last, one, first)

    def visit(self, step, relay=None):
        each = 2 * self.n - 1

        def one(i):
            u = lax.rem(i, each)
            origin = jnp.where(u == 0, self.place, self.origin(jnp.maximum(u - 1, 0)))
            @pl.when(self.inside(origin))
            def _():
                @pl.when(jnp.logical_and(u > 0, i < each))
                def _():
                    self.take(u - 1)
                    if relay is not None:
                        relay.start(origin)
                if relay is None:
                    step(origin)
                else:
                    @pl.when(i >= each)
                    def _():
                        relay.wait_recv(origin)
                    step(origin, jnp.where(i < each, self.me.k, 1 - self.me.k))
        times(each if relay is None else 2 * each, one)


class Fold(Chain):
    def __init__(self, sizes, me, group, total, block, landing, sends, recvs):
        super().__init__(sizes, me, group, None, landing, sends, recvs)
        self.total, self.block = total, block

    def far_first(self, step):
        n = self.n
        flip = 2 * self.place >= n
        q = jnp.where(flip, n - 1 - self.place, self.place)

        def one(i):
            left = i - (n - 1 - 2 * q)
            near = q + (1 - 2 * lax.rem(jnp.maximum(left, 0), 2)) * (q - lax.div(jnp.maximum(left, 0), 2))
            dest = jnp.where(left < 0, n - 1 - i, near)
            step(jnp.where(flip, n - 1 - dest, dest))
        times(n, one)

    def index(self, dest):
        return jnp.where(dest > self.place, dest, self.n + dest)

    def add(self, index, slot):
        here = self.landing(slot)
        self.copy(index, self.place, here, here, self.place_of_peer()).wait_recv()
        self.total[...] += here[...].astype(jnp.float32)

    def place_of_peer(self):
        return jnp.where(self.place > 0, self.place - 1, self.place + 1)

    def copy(self, index, to, source, landing, peer=None):
        return super().copy(index, to if peer is None else peer, source, landing)

    def send(self, dest):
        up = dest > self.place
        @pl.when(jnp.where(up, self.place > 0, self.place < self.n - 1))
        def _():
            self.add(self.index(dest), dest)
        self.block(dest)[...] = self.total[...].astype(jnp.bfloat16)
        to = jnp.where(up, self.place + 1, self.place - 1)
        slot = jnp.where(jnp.logical_and(jnp.logical_not(up), dest == to), self.n, dest)
        self.copy(self.index(dest), to, self.block(dest), self.landing(slot)).start()

    def finish(self):
        @pl.when(self.place > 0)
        def _():
            self.add(self.place, self.place)
        @pl.when(self.place < self.n - 1)
        def _():
            self.add(self.n + self.place, self.n)

    def wait_send(self):
        def one(dest, carry):
            @pl.when(dest != self.place)
            def _():
                self.copy(self.index(dest), self.place_of_peer(), self.block(dest), self.landing(dest)).wait_send()
            return carry
        lax.fori_loop(0, self.n, one, 0)


class Relay:
    def __init__(self, sizes, me, own, landing, sends, recvs):
        self.J, self.me, self.own, self.landing, self.sends, self.recvs = sizes.J, me, own, landing, sends, recvs
        self.place = lax.div(me.c, 2)

    def copy(self, place, source, landing):
        return pltpu.make_async_remote_copy(
            src_ref=source, dst_ref=landing, send_sem=self.sends.at[place], recv_sem=self.recvs.at[place],
            device_id=(self.me.c + 1 - 2 * self.me.k, self.me.f), device_id_type=MESH)

    def start_own(self):
        self.copy(self.place, self.own, self.landing(self.me.c)).start()

    def start(self, place):
        here = self.landing(2 * place + self.me.k)
        self.copy(place, here, here).start()

    def wait_recv(self, place):
        there = self.landing(2 * place + 1 - self.me.k)
        self.copy(place, there, there).wait_recv()

    def wait_send(self):
        def one(place, carry):
            here = self.landing(2 * place + self.me.k)
            self.copy(place, here, here).wait_send()
            return carry
        lax.fori_loop(0, self.J, one, 0)


def meet(sizes, me, groups):
    barrier = pltpu.get_barrier_semaphore()
    total = 0
    for group in groups:
        def greet(k, carry, group=group):
            p = sizes.peer(group, me, k)
            pl.semaphore_signal(barrier, inc=1, device_id=(p.c, p.f), device_id_type=MESH)
            return carry
        lax.fori_loop(1, sizes.count(group), greet, 0)
        total += sizes.count(group) - 1
    pl.semaphore_wait(barrier, total)


def times(n, step, first=0):
    def one(i, carry):
        step(i)
        return carry
    lax.fori_loop(first, n, one, 0)


def column_lane(z, me, c, source, landing, sends, recvs):
    return Lane(z, me, "fsdp", lambda to: source(c, to), lambda p: landing(c, p), sends.at[c], recvs.at[c])


def nn(a, b):
    return lax.dot_general(a, b, (((1,), (0,)), ((), ())), preferred_element_type=jnp.float32)


def nt(a, b):
    return lax.dot_general(a, b, (((1,), (1,)), ((), ())), preferred_element_type=jnp.float32)


def tn(a, b):
    return lax.dot_general(a, b, (((0,), (0,)), ((), ())), preferred_element_type=jnp.float32)


def lane_of(shape):
    return lax.broadcasted_iota(jnp.int32, shape, 1)


def rope_tables(place_columns, frequency):
    angles = place_columns.astype(jnp.float32) * frequency
    return jnp.cos(angles), jnp.sin(angles)


def rope(x, cosine, sine):
    half = HEAD // 2
    mixed = jnp.where(lax.rem(lane_of(x.shape), HEAD) < half, -pltpu.roll(x, LANES - half, 1), pltpu.roll(x, half, 1))
    return x * cosine + mixed * sine


def rows_at(ref, i, n):
    return ref.at[pl.ds(pl.multiple_of(i * n, n), n), :]


def vmem(shape, dtype=jnp.bfloat16):
    return pltpu.VMEM(shape, dtype)


def frequencies():
    lanes = np.arange(LANES)
    steps = rope_base ** ((lanes % (HEAD // 2)) * (-2.0 / HEAD))
    return jnp.asarray(np.stack([steps, np.where(lanes < HEAD, steps, 0.0)] + [steps] * 6), jnp.float32)


def exact(kind, a, b):
    dims = {"nn": ((1,), (0,)), "nt": ((1,), (1,)), "tn": ((0,), (0,))}[kind]
    return lax.dot_general(a, b, (dims, ((), ())), precision=lax.Precision.HIGHEST, preferred_element_type=jnp.float32)


CHAIN_GROUPS = dict(tok="line", cot="col", rows="col", d_attn="line", part="col", mix="col", dn="line")
LANE_GROUPS = dict(
    place="ctx", wc="ctx", small="ctx", slot="col", gate_a="ctx", gate_b="ctx", up="ctx",
    down="ctx", att="ctx", gates="col", turn="col", gc="ctx", wo="line",
    gs="ctx", go="fsdp", grad0="ctx", grad1="ctx", grad2="ctx", grad3="ctx", grad4="ctx", grad5="ctx")
PLANE_LANES = ["cot", "row", "g", "back", "dg", "out"]
COLUMN_LANES = ["wc", "small", "wo", "gc", "gs"]
RELAYS = ["tok", "wo", "d_attn", "sib"]


def layer_kernel(z, R, dc, tile, names, *refs):
    r = types.SimpleNamespace(**dict(zip(names, refs)))
    me = z.place(lax.axis_index("ctx"), lax.axis_index("fsdp"))
    C, F, H, P, J, rs, qw = z.C, z.F, z.H, z.P, z.J, z.rows_w, z.q_width
    L = C * R
    half = dc // 2
    low, high = pl.ds(0, half), pl.ds(half, half)
    sems = lambda kind, name: (getattr(r, kind + name + "_send"), getattr(r, kind + name + "_recv"))

    def at_slot(ref, h, p):
        return rows_at(ref, h * P + p, CAP)

    def lane(name, source, landing):
        return Lane(z, me, LANE_GROUPS[name], source, landing, *sems("lane_", name))

    def chain(name, own, landing):
        return Chain(z, me, CHAIN_GROUPS[name], own, landing, *sems("chain_", name))

    def plane(name, source, landing):
        def at(h):
            send, recv = sems("plane_", name)
            land = lambda p: at_slot(landing, h, p.p) if len(landing.shape) == 2 else landing.at[h, p.p]
            return Lane(z, me, "plane", lambda to: source.at[h, to.p], land, send.at[h], recv.at[h])
        return at

    def column(name, source, landing):
        return lambda c: column_lane(z, me, c, source, landing, *sems("column_", name))

    def relay(name, own, landing):
        return Relay(z, me, own, landing, *sems("relay_", name))

    tok_chain = chain("tok", r.tok, lambda place: r.blocks.at[2 * place + me.k])
    tok_relay = relay("tok", r.tok, lambda c: r.blocks.at[c])
    place_lane = lane("place", lambda to: r.place, lambda p: r.place_all.at[p.c])
    wc_lane = lane("wc", lambda to: r.w_pack.at[to.c], lambda p: rows_at(r.wc_v, p.w, rs))
    small_lane = lane("small", lambda to: r.small, lambda p: rows_at(r.small_v, p.w, rs))
    wo_lane = lane("wo", lambda to: r.w_out, lambda p: rows_at(r.wo_v, p.w, rs))
    wo_relay = relay("wo", None, lambda c: rows_at(r.wo_v, c, qw))
    spread = lambda name, ref: column(
        name, lambda c, to: rows_at(ref, c * F + me.f, rs), lambda c, p: rows_at(ref, c * F + p.f, rs))
    wc_column, small_column, wo_column = spread("wc", r.wc_v), spread("small", r.small_v), spread("wo", r.wo_v)
    cot_chain = chain("cot", r.cot, lambda h: r.cot_all.at[h])
    slot_lane = lane("slot", lambda to: r.slot_t.at[pl.ds(0, EXPERTS), :], lambda p: r.slot_all.at[p.h])
    gate_a_lane = lane("gate_a", lambda to: r.w_gate.at[to.m, low], lambda p: r.wv.at[0, p.c, low])
    gate_b_lane = lane("gate_b", lambda to: r.w_gate.at[to.m, high], lambda p: r.wv.at[0, p.c, high])
    up_lane = lane("up", lambda to: r.w_up.at[to.m], lambda p: r.wv.at[1, p.c])
    down_lane = lane("down", lambda to: r.w_downt.at[to.m], lambda p: r.wv.at[2, p.c])
    att_lane = lane("att", lambda to: r.att_stage.at[to.c], lambda p: r.att_in.at[p.c])
    rows_chain = chain("rows", r.h2, lambda h: r.h_all.at[h])
    gates_lane = lane("gates", lambda to: r.gates_t.at[pl.ds(0, EXPERTS), :], lambda p: r.gate_all.at[p.h])
    turn_lane = lane("turn", lambda to: r.turn_stage.at[to.h], lambda p: r.turn_in.at[p.h])
    up_attn_chain = chain("d_attn", r.d_attn, lambda place: r.blocks.at[2 * place + me.k])
    up_attn_relay = relay("d_attn", r.d_attn, lambda c: r.blocks.at[c])
    dn_block = lambda c: rows_at(r.pool, c, R)
    dn_in = lambda j: rows_at(r.xin, j, R)
    sib_in = lambda j: rows_at(r.cot_v, j, R)
    fold = lambda name, block, landing: Fold(z, me, CHAIN_GROUPS[name], r.total, block, landing, *sems("chain_", name))
    part_fold = fold("part", lambda h: r.part_stage.at[h], lambda slot: r.part_in.at[slot])
    mix_fold = fold("mix", lambda h: r.part_stage.at[h], lambda slot: r.mix_in.at[slot])
    dn_fold = fold("dn", lambda place: dn_block(2 * place + me.k), dn_in)
    gc_lane = lane("gc", lambda to: r.gc_sum.at[to.c], lambda p: r.gc_in.at[p.c])
    gs_lane = lane("gs", lambda to: r.gs_sum.at[to.c], lambda p: r.gs_in.at[p.c])
    go_lane = lane("go", lambda to: rows_at(r.go_stage, to.f, rs), lambda p: r.go_in.at[p.f])
    gather = lambda name, stage, landing: column(
        name, lambda c, to: rows_at(stage, c * F + to.f, rs), lambda c, p: landing.at[p.f, c])
    gc_column, gs_column = gather("gc", r.gc_stage, r.gc_x), gather("gs", r.gs_stage, r.gs_x)
    grad_of = lambda j, c: rows_at(r.g_down, c, dc) if j == 2 else r.wv.at[j, c]
    grad_lanes = [
        lane("grad" + str(2 * j + i),
             lambda to, j=j, i=i: grad_of(j, to.c).at[(low, high)[i]],
             lambda p, j=j, i=i: r.gw_in.at[j, p.s, p.m, (low, high)[i]])
        for j in range(3) for i in range(2)
    ]
    cot_plane = plane("cot", r.d_rows, r.cot_v)
    row_plane = plane("row", r.stage, r.xin)
    g_plane = plane("g", r.g_stage, r.gin)
    back_plane = plane("back", r.d_rows, r.stage)
    dg_plane = plane("dg", r.dg_stage, r.dg_in)
    out_plane = plane("out", r.result, r.out_in)

    def sib_copy(j):
        send, recv = sems("relay_", "sib")
        return pltpu.make_async_remote_copy(
            src_ref=dn_block(2 * j + 1 - me.k), dst_ref=sib_in(j), send_sem=send.at[j], recv_sem=recv.at[j],
            device_id=(me.c + 1 - 2 * me.k, me.f), device_id_type=MESH)

    meet(z, me, ["ctx", "plane", "fsdp"])
    wc_lane.start()
    small_lane.start()
    place_lane.start()

    own = [
        pltpu.make_async_copy(r.w_pack.at[me.c], rows_at(r.wc_v, me.w, rs), r.own_sem.at[0]),
        pltpu.make_async_copy(r.small, rows_at(r.small_v, me.w, rs), r.own_sem.at[1]),
        pltpu.make_async_copy(r.w_out, rows_at(r.wo_v, me.w, rs), r.own_sem.at[2]),
    ]
    own_weights = [
        pltpu.make_async_copy(source.at[me.m], r.wv.at[j, me.c], r.own_sem.at[3 + j])
        for j, source in enumerate([r.w_gate, r.w_up, r.w_downt])
    ]
    for copy in own + own_weights:
        copy.start()
    r.blocks[me.c] = r.tok[...]
    r.place_all[me.c] = r.place[...]
    r.cot_all[me.h] = r.cot[...]

    named = jnp.zeros((R, LANES), jnp.float32)
    for j in range(TOP):
        named = jnp.where(r.routes[:, j : j + 1] == lane_of((R, LANES)), 1.0, named)
    row_id = lax.broadcasted_iota(jnp.int32, (R, R), 0)
    before = jnp.where(row_id > lane_of((R, R)), 1.0, 0.0).astype(jnp.bfloat16)
    slot = nn(before, named.astype(jnp.bfloat16))
    r.slot_t[...] = jnp.where(named > 0.5, slot, -1.0).T
    r.slot_all[me.h] = r.slot_t[0:EXPERTS, :]
    slot_lane.start()
    slot_id = lax.broadcasted_iota(jnp.int32, (CAP, R), 0).astype(jnp.float32)

    wc_lane.wait_recv()
    small_lane.wait_recv()
    wo_lane.start()
    tok_relay.start_own()
    tok_chain.start()
    cot_chain.start()
    for copy in own:
        copy.wait()
    times(C, lambda c: wc_column(c).start())
    times(C, lambda c: small_column(c).start())

    def choose(j):
        h = lax.rem(me.h + H - j, H)
        @pl.when(j > 0)
        def _():
            slot_lane.wait_recv_one(j)

        def for_expert(p):
            row = r.slot_all[h, pl.ds(z.expert(me, p), 1), :]
            r.pick[h, p] = jnp.where(row == slot_id, 1.0, 0.0).astype(jnp.bfloat16)
        times(P, for_expert)

    def dispatch_cot(h):
        def to_expert(n):
            p = lax.rem(me.p + n, P)
            r.d_rows[h, p] = nn(r.pick[h, p], r.cot_all[h]).astype(jnp.bfloat16)
            @pl.when(n > 0)
            def _():
                cot_plane(h).start_one(n)
        times(P, to_expert)
        at_slot(r.cot_v, h, me.p)[...] = r.d_rows[h, me.p]
    place_lane.wait_recv()
    times(C, lambda c: wc_column(c).wait_recv())
    times(C, lambda c: small_column(c).wait_recv())
    times(H, choose)
    gain_one = r.small_v[...].astype(jnp.float32).T[EXPERTS : EXPERTS + 1, :]
    gain_two = r.small_v[...].astype(jnp.float32).T[EXPERTS + 1 : EXPERTS + 2, :]
    head_of = lax.div(lane_of((R, LANES)), HEAD)

    def project(place, core):
        c = 2 * place + core
        x = r.blocks[c].astype(jnp.float32)
        inverse = lax.rsqrt(jnp.mean(x * x, axis=-1, keepdims=True) + norm_eps)
        h = (x * inverse * gain_one).astype(jnp.bfloat16)
        part = pl.ds(pl.multiple_of(c * R, R), R)
        r.h1[part, :] = h
        qkv = nn(h, r.wc_v[...])
        row = r.place_all[c][0:1, :].astype(jnp.float32)
        r.place_row[c] = jnp.broadcast_to(row, (8, R))
        places = jnp.broadcast_to(row, (R, R)).T
        r.place_col[part, :] = places
        r.q_all[part, :] = rope(qkv[:, :LANES], *rope_tables(places, r.freq[0:1, :])).astype(jnp.bfloat16)
        kv = rope(qkv[:, LANES:], *rope_tables(places, r.freq[1:2, :]))
        swapped = pltpu.roll(kv, HEAD, 1)
        r.k2[part, :] = jnp.where(head_of == 0, kv, swapped).astype(jnp.bfloat16)
        r.v2[part, :] = jnp.where(head_of == 0, swapped, kv).astype(jnp.bfloat16)
    tok_chain.visit(project, tok_relay)
    gate_a_lane.start()
    wo_lane.wait_recv()
    times(J, lambda j: wo_column(2 * j + me.k).start())
    dispatch_cot(me.h)
    cot_chain.visit_some(dispatch_cot, 0, 2)
    tok_relay.wait_send()

    def attend(c):
        part = pl.ds(pl.multiple_of(c * R, R), R)
        q = r.q_all[part, :]
        row = jnp.concatenate([r.place_row[i, 0:1, :] for i in range(C)], axis=1)
        allowed = row <= r.place_col[part, 0:1]
        total = jnp.zeros((R, LANES), jnp.float32)
        for h in range(z.q_heads):
            mine = head_of == h
            s = nt(jnp.where(mine, q, jnp.zeros_like(q)), r.k2[...]) * score_scale
            s = jnp.where(allowed, s, masked_score)
            top = jnp.max(s, axis=-1, keepdims=True)
            e = jnp.exp(s - top)
            weight = jnp.sum(e, axis=-1, keepdims=True)
            r.lse[h, part, :] = jnp.broadcast_to(top + jnp.log(weight), (R, LANES))
            total = jnp.where(mine, nn(e.astype(jnp.bfloat16), r.v2[...]) / weight, total)
        r.att_f[part, :] = total
        r.att_stage[c] = total.astype(jnp.bfloat16)
    times(C, attend)
    tok_chain.wait_send()
    att_lane.start()
    r.att_in[me.c] = r.att_stage[me.c]
    cot_chain.visit_some(dispatch_cot, 2, min(4, 2 * (H - 1)))
    times(J, lambda j: wo_column(2 * j + me.k).wait_recv())
    times(J, wo_relay.start)
    att_lane.wait_recv()
    times(J, wo_relay.wait_recv)
    x = r.tok[...].astype(jnp.float32)
    mixed = jnp.zeros((R, D), jnp.float32)
    for c in range(C):
        mixed = mixed + nn(r.att_in[c][:, :qw], r.wo_v[c * qw : (c + 1) * qw, :])
    mid = x + residual_scale * mixed
    r.middle[...] = mid
    inverse = lax.rsqrt(jnp.mean(mid * mid, axis=-1, keepdims=True) + norm_eps)
    hidden = (mid * inverse * gain_two).astype(jnp.bfloat16)
    r.h2[...] = hidden
    rows_chain.start()
    chosen = r.slot_t[...].T > -0.5
    logits = jnp.where(chosen, nn(hidden, r.small_v[...]), masked_score)
    raised = jnp.where(chosen, jnp.exp(logits - jnp.max(logits, axis=-1, keepdims=True)), 0.0)
    r.gates_t[...] = (raised / jnp.sum(raised, axis=-1, keepdims=True)).T
    gates_lane.start()
    r.h_all[me.h] = r.h2[...]
    r.gate_all[me.h] = r.gates_t[0:EXPERTS, :]

    def dispatch_rows(h):
        @pl.when(h != me.h)
        def _():
            gates_lane.wait_recv_one(lax.rem(me.h + H - h, H))

        def to_expert(n):
            p = lax.rem(me.p + n, P)
            hot = r.pick[h, p]
            r.stage[h, p] = nn(hot, r.h_all[h]).astype(jnp.bfloat16)
            g = jnp.broadcast_to(r.gate_all[h, pl.ds(z.expert(me, p), 1), :], (8, R))
            wide = jnp.concatenate([hot.astype(jnp.float32), jnp.zeros((LANES - CAP, R), jnp.float32)], axis=0)
            r.g_stage[h, p] = exact("nt", g, wide)
            @pl.when(n > 0)
            def _():
                row_plane(h).start_one(n)
        times(P, to_expert)
        at_slot(r.xin, h, me.p)[...] = r.stage[h, me.p]
        r.gin[h, me.p] = r.g_stage[h, me.p]
    rows_chain.visit(dispatch_rows)
    cot_chain.visit_some(dispatch_cot, 4, 2 * (H - 1))
    gate_b_lane.start()
    up_lane.start()
    down_lane.start()

    def send_gates(j):
        h = lax.rem(me.h + H - j, H)

        def to_expert(n):
            row_plane(h).wait_send_one(n)
            g_plane(h).start_one(n)
        times(P, to_expert, 1)
    times(H, send_gates)
    times(H, lambda h: cot_plane(h).wait_send())
    for copy in own_weights:
        copy.wait()
    for bulk in [gate_a_lane, gate_b_lane, up_lane]:
        bulk.wait_recv()
    times(H, lambda h: cot_plane(h).wait_recv())
    wg, wu, wd = [r.wv.at[j].reshape(D, r.wv.shape[3]) for j in range(3)]
    per = tile // CAP

    def forward(j):
        h = lax.rem(me.h + H - lax.rem(j + 1, H), H)
        row_plane(h).wait_recv()
        g_plane(h).wait_recv()

        def rows(t):
            part = pl.ds(pl.multiple_of((h * P + t * per) * CAP, CAP), tile)
            for p in range(per):
                turned = jnp.broadcast_to(r.gin[h, t * per + p, 0:1, :], (LANES, LANES)).T
                r.g_col[p * CAP : (p + 1) * CAP, :] = turned[0:CAP, :]
            x = r.xin[part, :]
            r.hid[part, :] = (jax.nn.silu(nn(x, wg[...])) * nn(x, wu[...])).astype(jnp.bfloat16)
            r.pool[part, :] = (residual_scale * r.g_col[:, 0:1] * r.cot_v[part, :].astype(jnp.float32)).astype(jnp.bfloat16)
        times(P // per, rows)
    times(H, forward)

    def cut_down(d):
        part = pl.ds(pl.multiple_of(d * 256, 256), 256)
        r.g_down[part, :] = tn(r.pool[pl.ds(0, H * P * CAP), part], r.hid[...]).astype(jnp.bfloat16)
    times(D // 256, cut_down)
    grad_lanes[4].start()
    grad_lanes[5].start()
    down_lane.wait_recv()

    def chunk(h):

        def rows(t):
            some = pl.ds(pl.multiple_of(t * per, per), per)
            part = pl.ds(pl.multiple_of((h * P + t * per) * CAP, CAP), tile)
            x = r.xin[part, :]
            gate = nn(x, wg[...])
            up = nn(x, wu[...])
            sig = jax.nn.sigmoid(gate)
            act = gate * sig
            out = nt(r.hid[part, :], wd[...]).astype(jnp.bfloat16)
            r.result[h, some] = out.reshape(per, CAP, D)
            upstream = r.cot_v[part, :].astype(jnp.float32)
            d_gates = residual_scale * jnp.sum(upstream * out.astype(jnp.float32), axis=-1, keepdims=True)
            d_hidden = nn(r.pool[part, :], wd[...])
            dg = (d_hidden * up * sig * (1.0 + gate * (1.0 - sig))).astype(jnp.bfloat16)
            du = (d_hidden * act).astype(jnp.bfloat16)
            r.d_gate[part, :] = dg
            r.d_up[part, :] = du
            r.d_rows[h, some] = (nt(dg, wg[...]) + nt(du, wu[...])).astype(jnp.bfloat16).reshape(per, CAP, D)
            r.g_col[...] = jnp.broadcast_to(d_gates, (tile, LANES))
            for p in range(per):
                turned = jnp.concatenate(
                    [r.g_col[p * CAP : (p + 1) * CAP, :], jnp.zeros((LANES - CAP, LANES), jnp.float32)], axis=0)
                r.dg_stage[h, t * per + p] = turned.T[0:8, :]
        times(P // per, rows)
        back_plane(h).start()
        dg_plane(h).start()
        r.stage[h, me.p] = r.d_rows[h, me.p]
        r.dg_in[h, me.p] = r.dg_stage[h, me.p]
    part_fold.far_first(chunk)

    def cut(d):
        part = pl.ds(pl.multiple_of(d * 256, 256), 256)
        x = r.xin[:, part]
        wg[part, :] = tn(x, r.d_gate[...]).astype(jnp.bfloat16)
        wu[part, :] = tn(x, r.d_up[...]).astype(jnp.bfloat16)
    times(D // 256, cut)
    grad_lanes[0].start()
    own_grads = [
        pltpu.make_async_copy(grad_of(j, me.c), r.gw_in.at[j, me.s, me.m], r.own_sem.at[8 + j]) for j in range(3)
    ]
    for copy in own_grads:
        copy.start()

    def collect(h):
        back_plane(h).wait_recv()
        dg_plane(h).wait_recv()
        r.total[...] = tn(r.pick[h].reshape(P * CAP, R), r.stage[h].reshape(P * CAP, D))
        r.turn_stage[h] = jnp.zeros((EXPERTS, R), jnp.float32)

        def gates_of(p):
            row = jnp.broadcast_to(r.dg_in[h, p, 0:1, 0:CAP], (8, CAP))
            r.turn_stage[h, pl.ds(z.expert(me, p), 1), :] = exact("nn", row, r.pick[h, p].astype(jnp.float32))[0:1, :]
        times(P, gates_of)
        @pl.when(h != me.h)
        def _():
            part_fold.send(h)
            turn_lane.start_one(lax.rem(h + H - me.h, H))
    part_fold.far_first(collect)
    r.turn_v[...] = jnp.zeros((LANES, R), jnp.float32)
    r.turn_v[0:EXPERTS, :] = r.turn_stage[me.h]
    times(H, lambda h: out_plane(h).start())
    own_out = pltpu.make_async_copy(r.result.at[:, me.p], r.out_in.at[:, me.p], r.own_sem.at[7])
    own_out.start()
    part_fold.finish()
    turn_lane.wait_recv()

    def add_part(n):
        h = lax.rem(me.h + n + 1, H)
        r.turn_v[0:EXPERTS, :] += r.turn_in[h]
    times(H - 1, add_part)
    gts = r.gates_t[...].T
    dgs = r.turn_v[...].T
    d_log = gts * (dgs - jnp.sum(gts * dgs, axis=-1, keepdims=True))
    d_h2 = r.total[...] + exact("nt", d_log, r.small_v[...].astype(jnp.float32))
    mid = r.middle[...]
    inverse = lax.rsqrt(jnp.mean(mid * mid, axis=-1, keepdims=True) + norm_eps)
    n2 = mid * inverse
    g = d_h2 * gain_two
    dm = r.cot[...].astype(jnp.float32) + inverse * (g - n2 * jnp.mean(g * n2, axis=-1, keepdims=True))
    r.d_mid[...] = dm
    r.d_attn[...] = (residual_scale * dm).astype(jnp.bfloat16)
    up_attn_relay.start_own()
    up_attn_chain.start()
    r.gain_v[...] = jnp.zeros((LANES, D), jnp.float32)
    r.gain_v[EXPERTS + 1 : EXPERTS + 2, :] = jnp.sum(d_h2 * n2, axis=0, keepdims=True)
    r.g_small[...] = exact("tn", r.h2[...].astype(jnp.float32), d_log)

    r.blocks[me.c] = r.d_attn[...]
    r.dk_acc[...] = jnp.zeros((L, LANES), jnp.float32)
    r.dv_acc[...] = jnp.zeros((L, LANES), jnp.float32)
    wo_c = rows_at(r.wo_v, me.c, qw)

    def attend_back(place, core):
        c = 2 * place + core
        part = pl.ds(pl.multiple_of(c * R, R), R)
        q = r.q_all[part, :]
        d_mix = nt(r.blocks[c], wo_c[...])
        if qw < LANES:
            d_mix = jnp.concatenate([d_mix, jnp.zeros((R, LANES - qw), jnp.float32)], axis=1)
        d_mix = d_mix.astype(jnp.bfloat16)
        row = jnp.concatenate([r.place_row[i, 0:1, :] for i in range(C)], axis=1)
        places = r.place_col[part, :]
        allowed = row <= places[:, 0:1]
        dq = jnp.zeros((R, LANES), jnp.float32)
        for h in range(z.q_heads):
            mine = head_of == h
            rows = pl.ds(h * R, R)
            q_h = jnp.where(mine, q, jnp.zeros_like(q))
            dm_h = jnp.where(mine, d_mix, jnp.zeros_like(d_mix))
            r.q_v[rows, :] = q_h
            r.dm_v[rows, :] = dm_h
            s = jnp.where(allowed, nt(q_h, r.k2[...]) * score_scale, masked_score)
            p = jnp.exp(s - r.lse[h, part, 0:1])
            r.p_v[rows, :] = p.astype(jnp.bfloat16)
            delta = jnp.sum(dm_h.astype(jnp.float32) * r.att_f[part, :], axis=-1, keepdims=True)
            ds = (p * (nt(dm_h, r.v2[...]) - delta)).astype(jnp.bfloat16)
            r.ds_v[rows, :] = ds
            dq = jnp.where(mine, nn(ds, r.k2[...]) * score_scale, dq)
        r.dk_acc[...] += tn(r.ds_v[...], r.q_v[...])
        r.dv_acc[...] += tn(r.p_v[...], r.dm_v[...])
        cosine, sine = rope_tables(places, r.freq[0:1, :])
        r.d_qkv[part, 0:LANES] = rope(dq, cosine, -sine).astype(jnp.bfloat16)
    up_attn_chain.visit(attend_back, up_attn_relay)
    grad_lanes[1].start()

    def finish_kv(c):
        part = pl.ds(pl.multiple_of(c * R, R), R)
        dk = r.dk_acc[part, :] * score_scale
        dv = r.dv_acc[part, :]
        dk = dk + pltpu.roll(dk, HEAD, 1)
        dv = dv + pltpu.roll(dv, HEAD, 1)
        cosine, sine = rope_tables(r.place_col[part, :], r.freq[1:2, :])
        r.d_qkv[part, LANES : 2 * LANES] = rope(jnp.where(head_of == 0, dk, dv), cosine, -sine).astype(jnp.bfloat16)
    times(C, finish_kv)

    def down_tokens(c):
        return nt(r.d_qkv[pl.ds(pl.multiple_of(c * R, R), R), :], r.wc_v[...])

    def for_sibling(place):
        c = 2 * place + 1 - me.k
        dn_block(c)[...] = down_tokens(c).astype(jnp.bfloat16)
        sib_copy(place).start()
    dn_fold.far_first(for_sibling)

    def for_line(place):
        dn = down_tokens(2 * place + me.k)
        sib_copy(place).wait_recv()
        r.total[...] = dn + sib_in(place)[...].astype(jnp.float32)
        @pl.when(place != dn_fold.place)
        def _():
            dn_fold.send(place)
        @pl.when(place == dn_fold.place)
        def _():
            r.grad_tokens[...] = r.total[...]
    dn_fold.far_first(for_line)

    own_out.wait()
    part_fold.wait_send()

    def mix(h):
        out_plane(h).wait_recv()
        load = pltpu.make_async_copy(r.out_in.at[h], r.stage.at[h], r.own_sem.at[12])
        load.start()

        def weigh(p):
            g = r.gate_all[h, pl.ds(z.expert(me, p), 1), :] * r.pick[h, p].astype(jnp.float32)
            high = g.astype(jnp.bfloat16)
            r.mix_hi[p] = high
            r.mix_lo[p] = (g - high.astype(jnp.float32)).astype(jnp.bfloat16)
        times(P, weigh)
        load.wait()
        rows = r.stage[h].reshape(P * CAP, D)
        total = tn(r.mix_hi[...].reshape(P * CAP, R), rows) + tn(r.mix_lo[...].reshape(P * CAP, R), rows)
        r.total[...] = total
        @pl.when(h != me.h)
        def _():
            mix_fold.send(h)
    mix_fold.far_first(mix)
    grad_lanes[2].start()
    grad_lanes[3].start()

    def weights(d):
        part = pl.ds(pl.multiple_of(d * 256, 256), 256)
        total = tn(r.h1[:, part], r.d_qkv[...])
        r.gc_stage[part, :] = total.astype(jnp.bfloat16)
        gain = jnp.sum(total * r.wc_v[part, :].astype(jnp.float32), axis=-1, keepdims=True)
        gain = gain / r.small_v[part, EXPERTS : EXPERTS + 1].astype(jnp.float32)
        r.g_small[part, :] = jnp.where(lane_of((256, LANES)) == EXPERTS, gain, r.g_small[part, :])
    times(D // 256, weights)
    times(C, lambda c: gc_column(c).start())
    r.gs_stage[...] = (r.g_small[...] + r.gain_v[...].T).astype(jnp.bfloat16)
    times(C, lambda c: gs_column(c).start())
    own_last = [
        pltpu.make_async_copy(rows_at(stage, c * F + me.f, rs), landing.at[me.f, c], r.own_cols.at[i, c])
        for i, (stage, landing) in enumerate([(r.gc_stage, r.gc_x), (r.gs_stage, r.gs_x)]) for c in range(C)
    ]
    for copy in own_last:
        copy.start()
    r.go_stage[...] = tn(r.att_f[...].astype(jnp.bfloat16), r.blocks[...].reshape(L, D)).astype(jnp.bfloat16)
    go_lane.start()
    own_go = pltpu.make_async_copy(rows_at(r.go_stage, me.f, rs), r.go_in.at[me.f], r.own_sem.at[13])
    own_go.start()
    for copy in own_last:
        copy.wait()
    times(C, lambda c: gc_column(c).wait_recv())
    times(C, lambda c: gs_column(c).wait_recv())
    gc_total = r.gc_x[0].astype(jnp.float32)
    gs_total = r.gs_x[0].astype(jnp.float32)
    for f in range(1, F):
        gc_total = gc_total + r.gc_x[f].astype(jnp.float32)
        gs_total = gs_total + r.gs_x[f].astype(jnp.float32)
    r.gc_sum[...] = gc_total.astype(jnp.bfloat16)
    r.gs_sum[...] = gs_total.astype(jnp.bfloat16)
    gc_lane.start()
    gs_lane.start()
    own_sums = [
        pltpu.make_async_copy(r.gc_sum.at[me.c], r.gc_in.at[me.c], r.own_sem.at[14]),
        pltpu.make_async_copy(r.gs_sum.at[me.c], r.gs_in.at[me.c], r.own_sem.at[15]),
    ]
    for copy in own_sums:
        copy.start()
    mix_fold.finish()
    r.output[...] = (r.middle[...] + residual_scale * r.total[...]).astype(jnp.bfloat16)

    r.total[...] = r.grad_tokens[...]
    dn_fold.finish()
    d_h1 = r.total[...]
    x = r.tok[...].astype(jnp.float32)
    inverse = lax.rsqrt(jnp.mean(x * x, axis=-1, keepdims=True) + norm_eps)
    n1 = x * inverse
    g = d_h1 * gain_one
    r.grad_tokens[...] = r.d_mid[...] + inverse * (g - n1 * jnp.mean(g * n1, axis=-1, keepdims=True))
    for last in [gc_lane, gs_lane, go_lane]:
        last.wait_recv()
    for last in grad_lanes:
        last.wait_recv()
    for last in [place_lane, wc_lane, small_lane, slot_lane, gate_a_lane, gate_b_lane, up_lane, down_lane, att_lane, gates_lane,
                 turn_lane, wo_lane, gc_lane, gs_lane, go_lane] + grad_lanes:
        last.wait_send()
    for last in [cot_chain, rows_chain, up_attn_chain, mix_fold, dn_fold]:
        last.wait_send()
    for last in [wo_relay, up_attn_relay]:
        last.wait_send()
    times(J, lambda j: sib_copy(j).wait_send())
    for last in [g_plane, back_plane, dg_plane, out_plane]:
        times(H, lambda h, last=last: last(h).wait_send())
    times(J, lambda j: wo_column(2 * j + me.k).wait_send())
    for last in [wc_column, small_column, gc_column, gs_column]:
        times(C, lambda c, last=last: last(c).wait_send())
    for copy in own_grads + own_sums + [own_go]:
        copy.wait()


def layer_call(z, R, ff, dc, tok, place, routes, cot, w_pack, small, w_out, w_gate, w_up, w_downt):
    C, F, N, H, P, J, S, rs = z.C, z.F, z.N, z.H, z.P, z.J, z.S, z.rows_w
    L, f, f16 = C * R, jnp.float32, jnp.bfloat16
    rows, heads, tile = H * P * CAP, z.q_heads * R, 8 * CAP
    ins = dict(tok=(tok, 1), place=(place, 1), routes=(routes, 1), cot=(cot, 1), freq=(frequencies(), 1), w_pack=(w_pack, 0),
               small=(small, 0), w_out=(w_out, 0), w_gate=(w_gate, 0), w_up=(w_up, 0), w_downt=(w_downt, 0))
    outs = dict(
        output=(shape_of((R, D)), 1), grad_tokens=(shape_of((R, D), f), 1), gc_in=(shape_of((C, rs, 2 * LANES)), 0),
        gs_in=(shape_of((C, rs, LANES)), 0), go_in=(shape_of((F, rs, D)), 0), gw_in=(shape_of((3, S, z.G, dc, ff)), 0),
        out_in=(shape_of((H, P, CAP, D)), 0))
    scratch = dict(
        blocks=vmem((C, R, D)), place_all=vmem((C, 8, R), jnp.int32), wc_v=vmem((D, 2 * LANES)), small_v=vmem((D, LANES)),
        wo_v=vmem((D, D)), cot_all=vmem((H, R, D)), slot_all=vmem((H, EXPERTS, R), f), slot_t=vmem((LANES, R), f),
        place_col=vmem((L, R), f), place_row=vmem((C, 8, R), f), h1=vmem((L, D)), q_all=vmem((L, LANES)), k2=vmem((L, LANES)),
        v2=vmem((L, LANES)), lse=vmem((z.q_heads, L, LANES), f), att_f=vmem((L, LANES), f), att_stage=vmem((C, R, LANES)),
        att_in=vmem((C, R, LANES)), middle=vmem((R, D), f), h2=vmem((R, D)), gates_t=vmem((LANES, R), f),
        gate_all=vmem((H, EXPERTS, R), f), h_all=vmem((H, R, D)), pick=vmem((H, P, CAP, R)), stage=vmem((H, P, CAP, D)),
        xin=vmem((rows, D)), g_stage=vmem((H, P, 8, LANES), f), gin=vmem((H, P, 8, LANES), f), wv=vmem((3, C, dc, ff)),
        cot_v=vmem((rows, D)), d_rows=vmem((H, P, CAP, D)), dg_stage=vmem((H, P, 8, LANES), f),
        dg_in=vmem((H, P, 8, LANES), f), hid=vmem((rows, ff)), d_gate=vmem((rows, ff)), d_up=vmem((rows, ff)),
        pool=vmem((max(rows, L), D)), g_col=vmem((tile, LANES), f), result=vmem((H, P, CAP, D)),
        part_stage=vmem((H, R, D)), part_in=vmem((H + 1, R, D)), turn_stage=vmem((H, EXPERTS, R), f),
        turn_in=vmem((H, EXPERTS, R), f), turn_v=vmem((LANES, R), f), d_mid=vmem((R, D), f), d_attn=vmem((R, D)),
        g_small=vmem((D, LANES), f), g_down=vmem((D, ff)), gain_v=vmem((LANES, D), f), ds_v=vmem((heads, L)), p_v=vmem((heads, L)),
        q_v=vmem((heads, LANES)), dm_v=vmem((heads, LANES)), dk_acc=vmem((L, LANES), f), dv_acc=vmem((L, LANES), f),
        d_qkv=vmem((L, 2 * LANES)),
        gc_stage=vmem((D, 2 * LANES)), go_stage=vmem((LANES, D)), gs_stage=vmem((D, LANES)), gc_x=vmem((F, C, rs, 2 * LANES)),
        gs_x=vmem((F, C, rs, LANES)), gc_sum=vmem((C, rs, 2 * LANES)), gs_sum=vmem((C, rs, LANES)), mix_hi=vmem((P, CAP, R)),
        mix_lo=vmem((P, CAP, R)), mix_in=vmem((H + 1, R, D)), total=vmem((R, D), f), own_sem=pltpu.SemaphoreType.DMA((16,)),
        own_cols=pltpu.SemaphoreType.DMA((2, C)))
    both = ("_send", "_recv")
    scratch |= {"lane_" + n + b: pltpu.SemaphoreType.DMA((z.count(g),)) for n, g in LANE_GROUPS.items() for b in both}
    steps = {"col": 2 * H, "line": 2 * J}
    scratch |= {"chain_" + n + b: pltpu.SemaphoreType.DMA((steps[g],)) for n, g in CHAIN_GROUPS.items() for b in both}
    scratch |= {"plane_" + n + b: pltpu.SemaphoreType.DMA((H, P)) for n in PLANE_LANES for b in both}
    scratch |= {"column_" + n + b: pltpu.SemaphoreType.DMA((C, F)) for n in COLUMN_LANES for b in both}
    scratch |= {"relay_" + n + b: pltpu.SemaphoreType.DMA((J,)) for n in RELAYS for b in both}
    names = list(ins) + list(outs) + list(scratch)
    space = lambda fast: pl.BlockSpec(memory_space=pltpu.VMEM if fast else pl.ANY)
    results = pl.pallas_call(
        functools.partial(layer_kernel, z, R, dc, tile, names), name="layer",
        out_shape=[o for o, _ in outs.values()], in_specs=[space(fast) for _, fast in ins.values()],
        out_specs=[space(fast) for _, fast in outs.values()], scratch_shapes=list(scratch.values()),
        compiler_params=pltpu.CompilerParams(collective_id=0, has_side_effects=True, vmem_limit_bytes=67043328),
    )(*[a for a, _ in ins.values()])
    return results[:6]


def local(z, tokens, norm_first, w_query, w_key, w_value, w_out, norm_second, w_router,
          w_gate, w_up, w_down, positions, routes, cotangent):
    C, F = z.C, z.F
    R = tokens.shape[1]
    rs = z.rows_w
    ff = w_gate.shape[2]
    dc = D // C

    heads_q = jnp.pad(w_query.reshape(rs, C, z.q_width), ((0, 0), (0, 0), (0, LANES - z.q_width)))
    heads_k = jnp.repeat(w_key.reshape(rs, KV_HEADS, HEAD), z.share, axis=1)
    heads_v = jnp.repeat(w_value.reshape(rs, KV_HEADS, HEAD), z.share, axis=1)
    w_pack = jnp.concatenate([heads_q, heads_k, heads_v], axis=2).transpose(1, 0, 2)
    small = jnp.concatenate(
        [w_router, norm_first[:, None], norm_second[:, None], jnp.zeros((rs, 128 - EXPERTS - 2), jnp.bfloat16)], axis=1)
    place_pack = jnp.broadcast_to(positions[0][None, :], (8, R))
    w_downt = w_down.transpose(0, 2, 1)
    output, grad_tokens, gc_in, gs_in, go_in, gw_in = layer_call(
        z, R, ff, dc, tokens[0], place_pack, routes[0], cotangent[0], w_pack, small, w_out, w_gate, w_up, w_downt)
    gc = f32(gc_in)
    join = lambda a: a.reshape(KV_HEADS, z.share, rs, HEAD).sum(axis=1).transpose(1, 0, 2).reshape(rs, KV_HEADS * HEAD)
    gs = jnp.sum(f32(gs_in), axis=0)
    return (
        output[None],
        grad_tokens[None],
        gs[:, EXPERTS],
        gc[:, :, : z.q_width].transpose(1, 0, 2).reshape(rs, D),
        join(gc[:, :, LANES : LANES + HEAD]),
        join(gc[:, :, LANES + HEAD :]),
        jnp.sum(f32(go_in), axis=0),
        gs[:, EXPERTS + 1],
        gs[:, :EXPERTS],
        jnp.sum(f32(gw_in[0]), axis=0),
        jnp.sum(f32(gw_in[1]), axis=0),
        jnp.sum(f32(gw_in[2]), axis=0).transpose(0, 2, 1),
    )


def solution(mesh):
    row = P(("ctx", "fsdp"), None)
    vec = P(("ctx", "fsdp"))
    seq = P("fsdp", "ctx", None)
    down = P("fsdp", None, "ctx")
    return jax.shard_map(
        functools.partial(local, Sizes(mesh)),
        mesh=mesh,
        in_specs=(seq, vec, row, row, row, row, vec, row, seq, seq, down, P("fsdp", "ctx"), seq, seq),
        out_specs=(seq, seq, vec, row, row, row, row, vec, row, seq, seq, down),
        check_vma=False,
    )
```

```python
import collections
import functools
import types

import jax
import jax.numpy as jnp
import numpy as np
from jax import lax
from jax.experimental import pallas as pl
from jax.experimental.pallas import tpu as pltpu
from jax.sharding import PartitionSpec as P

D = 1024
HEADS = 16
KV_HEADS = 8
HEAD = 64
EXPERTS = 32
TOP = 8
CAP = 48
LANES = 128

residual_scale = 0.22
score_scale = 0.015625
rope_base = 10000.0
norm_eps = 1e-06
masked_score = -1e30

MESH = pl.DeviceIdType.MESH
Place = collections.namedtuple("Place", ["c", "f", "m", "s", "h", "k", "p", "w"])


class Sizes:
    def __init__(self, mesh):
        self.C = mesh.shape["ctx"]
        self.F = mesh.shape["fsdp"]
        self.N = self.C * self.F
        self.G = EXPERTS // self.F
        self.S = self.C // self.G
        self.H = self.G // 2
        self.P = 2 * self.F
        self.J = self.C // 2
        self.q_heads = HEADS // self.C
        self.q_width = self.q_heads * HEAD
        self.share = self.C // KV_HEADS
        self.rows_w = D // self.N

    def place(self, c, f):
        k = lax.rem(c, 2)
        return Place(c, f, lax.rem(c, self.G), lax.div(c, self.G), lax.rem(lax.div(c, 2), self.H), k, f * 2 + k, c * self.F + f)

    def count(self, group):
        return {"ctx": self.C, "fsdp": self.F, "world": self.N, "col": self.H, "line": self.J, "plane": self.P}[group]

    def peer(self, group, me, n):
        if group == "ctx":
            return self.place(lax.rem(me.c + n, self.C), me.f)
        if group == "fsdp":
            return self.place(me.c, lax.rem(me.f + n, self.F))
        if group == "world":
            w = lax.rem(me.w + n, self.N)
            return self.place(lax.div(w, self.F), lax.rem(w, self.F))
        if group == "col":
            return self.place(me.s * self.G + 2 * lax.rem(me.h + n, self.H) + me.k, me.f)
        if group == "line":
            return self.place(2 * lax.rem(lax.div(me.c, 2) + n, self.J) + me.k, me.f)
        p = lax.rem(me.p + n, self.P)
        return self.place(me.s * self.G + 2 * me.h + lax.rem(p, 2), lax.div(p, 2))

    def expert(self, me, p):
        return lax.div(p, 2) * self.G + 2 * me.h + lax.rem(p, 2)


def bf(x):
    return x.astype(jnp.bfloat16)


def f32(x):
    return x.astype(jnp.float32)


def shape_of(shape, dtype=jnp.bfloat16):
    return jax.ShapeDtypeStruct(shape, dtype)


class Lane:
    def __init__(self, sizes, me, group, src, dst, sends, recvs):
        self.sizes, self.me, self.group, self.src, self.dst = sizes, me, group, src, dst
        self.sends, self.recvs, self.n = sends, recvs, sizes.count(group)

    def copy(self, k, to, source, landing):
        return pltpu.make_async_remote_copy(
            src_ref=source, dst_ref=landing, send_sem=self.sends.at[k], recv_sem=self.recvs.at[k],
            device_id=(to.c, to.f), device_id_type=MESH)

    def to(self, k):
        return self.sizes.peer(self.group, self.me, k)

    def start_one(self, k):
        to = self.to(k)
        self.copy(k, to, self.src(to), self.dst(self.me)).start()

    def wait_recv_one(self, k):
        landed = self.dst(self.sizes.peer(self.group, self.me, self.n - k))
        self.copy(k, self.to(k), landed, landed).wait_recv()

    def wait_send_one(self, k):
        to = self.to(k)
        self.copy(k, to, self.src(to), self.dst(self.me)).wait_send()

    def each(self, step):
        def one(k, carry):
            step(k)
            return carry
        lax.fori_loop(1, self.n, one, 0)

    def start(self):
        self.each(self.start_one)

    def wait_recv(self):
        self.each(self.wait_recv_one)

    def wait_send(self):
        self.each(self.wait_send_one)


class Chain:
    def __init__(self, sizes, me, group, own, landing, sends, recvs):
        self.col = group == "col"
        self.place, self.n = (me.h, sizes.H) if self.col else (lax.div(me.c, 2), sizes.J)
        self.sizes, self.me, self.own, self.landing, self.sends, self.recvs = sizes, me, own, landing, sends, recvs

    def copy(self, t, to, source, landing):
        c = self.me.s * self.sizes.G + 2 * to + self.me.k if self.col else 2 * to + self.me.k
        return pltpu.make_async_remote_copy(
            src_ref=source, dst_ref=landing, send_sem=self.sends.at[t], recv_sem=self.recvs.at[t],
            device_id=(c, self.me.f), device_id_type=MESH)

    def inside(self, place):
        return jnp.logical_and(place >= 0, place < self.n)

    def origin(self, t):
        return self.place - (1 - 2 * lax.rem(t, 2)) * (lax.div(t, 2) + 1)

    def start(self):
        for t, to in ((0, self.place + 1), (1, self.place - 1)):
            @pl.when(self.inside(to))
            def _(t=t, to=to):
                self.copy(t, to, self.own, self.landing(self.place)).start()

    def take(self, t):
        sign = 1 - 2 * lax.rem(t, 2)
        here = self.landing(self.origin(t))
        self.copy(t, self.place - sign, here, here).wait_recv()
        @pl.when(self.inside(self.place + sign))
        def _():
            self.copy(t + 2, self.place + sign, here, here).start()

    def wait_send(self):
        def one(t, carry):
            to = self.place + 1 - 2 * lax.rem(t, 2)
            origin = to - (1 - 2 * lax.rem(t, 2)) * (lax.div(t, 2) + 1)
            @pl.when(jnp.logical_and(self.inside(to), self.inside(origin)))
            def _():
                self.copy(t, to, self.landing(self.place), self.landing(self.place)).wait_send()
            return carry
        lax.fori_loop(0, 2 * (self.n - 1), one, 0)

    def visit_some(self, step, first, last):
        def one(t):
            @pl.when(self.inside(self.origin(t)))
            def _():
                self.take(t)
                step(self.origin(t))
        times(last, one, first)

    def visit(self, step, relay=None):
        each = 2 * self.n - 1

        def one(i):
            u = lax.rem(i, each)
            origin = jnp.where(u == 0, self.place, self.origin(jnp.maximum(u - 1, 0)))
            @pl.when(self.inside(origin))
            def _():
                @pl.when(jnp.logical_and(u > 0, i < each))
                def _():
                    self.take(u - 1)
                    if relay is not None:
                        relay.start(origin)
                if relay is None:
                    step(origin)
                else:
                    @pl.when(i >= each)
                    def _():
                        relay.wait_recv(origin)
                    step(origin, jnp.where(i < each, self.me.k, 1 - self.me.k))
        times(each if relay is None else 2 * each, one)


class Fold(Chain):
    def __init__(self, sizes, me, group, total, block, landing, sends, recvs):
        super().__init__(sizes, me, group, None, landing, sends, recvs)
        self.total, self.block = total, block

    def far_first(self, step):
        n = self.n
        flip = 2 * self.place >= n
        q = jnp.where(flip, n - 1 - self.place, self.place)

        def one(i):
            left = i - (n - 1 - 2 * q)
            near = q + (1 - 2 * lax.rem(jnp.maximum(left, 0), 2)) * (q - lax.div(jnp.maximum(left, 0), 2))
            dest = jnp.where(left < 0, n - 1 - i, near)
            step(jnp.where(flip, n - 1 - dest, dest))
        times(n, one)

    def index(self, dest):
        return jnp.where(dest > self.place, dest, self.n + dest)

    def add(self, index, slot):
        here = self.landing(slot)
        self.copy(index, self.place, here, here, self.place_of_peer()).wait_recv()
        self.total[...] += here[...].astype(jnp.float32)

    def place_of_peer(self):
        return jnp.where(self.place > 0, self.place - 1, self.place + 1)

    def copy(self, index, to, source, landing, peer=None):
        return super().copy(index, to if peer is None else peer, source, landing)

    def send(self, dest):
        up = dest > self.place
        @pl.when(jnp.where(up, self.place > 0, self.place < self.n - 1))
        def _():
            self.add(self.index(dest), dest)
        self.block(dest)[...] = self.total[...].astype(jnp.bfloat16)
        to = jnp.where(up, self.place + 1, self.place - 1)
        slot = jnp.where(jnp.logical_and(jnp.logical_not(up), dest == to), self.n, dest)
        self.copy(self.index(dest), to, self.block(dest), self.landing(slot)).start()

    def finish(self):
        @pl.when(self.place > 0)
        def _():
            self.add(self.place, self.place)
        @pl.when(self.place < self.n - 1)
        def _():
            self.add(self.n + self.place, self.n)

    def wait_send(self):
        def one(dest, carry):
            @pl.when(dest != self.place)
            def _():
                self.copy(self.index(dest), self.place_of_peer(), self.block(dest), self.landing(dest)).wait_send()
            return carry
        lax.fori_loop(0, self.n, one, 0)


class Relay:
    def __init__(self, sizes, me, own, landing, sends, recvs):
        self.J, self.me, self.own, self.landing, self.sends, self.recvs = sizes.J, me, own, landing, sends, recvs
        self.place = lax.div(me.c, 2)

    def copy(self, place, source, landing):
        return pltpu.make_async_remote_copy(
            src_ref=source, dst_ref=landing, send_sem=self.sends.at[place], recv_sem=self.recvs.at[place],
            device_id=(self.me.c + 1 - 2 * self.me.k, self.me.f), device_id_type=MESH)

    def start_own(self):
        self.copy(self.place, self.own, self.landing(self.me.c)).start()

    def start(self, place):
        here = self.landing(2 * place + self.me.k)
        self.copy(place, here, here).start()

    def wait_recv(self, place):
        there = self.landing(2 * place + 1 - self.me.k)
        self.copy(place, there, there).wait_recv()

    def wait_send(self):
        def one(place, carry):
            here = self.landing(2 * place + self.me.k)
            self.copy(place, here, here).wait_send()
            return carry
        lax.fori_loop(0, self.J, one, 0)


def meet(sizes, me, groups):
    barrier = pltpu.get_barrier_semaphore()
    total = 0
    for group in groups:
        def greet(k, carry, group=group):
            p = sizes.peer(group, me, k)
            pl.semaphore_signal(barrier, inc=1, device_id=(p.c, p.f), device_id_type=MESH)
            return carry
        lax.fori_loop(1, sizes.count(group), greet, 0)
        total += sizes.count(group) - 1
    pl.semaphore_wait(barrier, total)


def times(n, step, first=0):
    def one(i, carry):
        step(i)
        return carry
    lax.fori_loop(first, n, one, 0)


def column_lane(z, me, c, source, landing, sends, recvs):
    return Lane(z, me, "fsdp", lambda to: source(c, to), lambda p: landing(c, p), sends.at[c], recvs.at[c])


def nn(a, b):
    return lax.dot_general(a, b, (((1,), (0,)), ((), ())), preferred_element_type=jnp.float32)


def nt(a, b):
    return lax.dot_general(a, b, (((1,), (1,)), ((), ())), preferred_element_type=jnp.float32)


def tn(a, b):
    return lax.dot_general(a, b, (((0,), (0,)), ((), ())), preferred_element_type=jnp.float32)


def lane_of(shape):
    return lax.broadcasted_iota(jnp.int32, shape, 1)


def rope_tables(place_columns, frequency):
    angles = place_columns.astype(jnp.float32) * frequency
    return jnp.cos(angles), jnp.sin(angles)


def rope(x, cosine, sine):
    half = HEAD // 2
    mixed = jnp.where(lax.rem(lane_of(x.shape), HEAD) < half, -pltpu.roll(x, LANES - half, 1), pltpu.roll(x, half, 1))
    return x * cosine + mixed * sine


def rows_at(ref, i, n):
    return ref.at[pl.ds(pl.multiple_of(i * n, n), n), :]


def vmem(shape, dtype=jnp.bfloat16):
    return pltpu.VMEM(shape, dtype)


def frequencies():
    lanes = np.arange(LANES)
    steps = rope_base ** ((lanes % (HEAD // 2)) * (-2.0 / HEAD))
    return jnp.asarray(np.stack([steps, np.where(lanes < HEAD, steps, 0.0)] + [steps] * 6), jnp.float32)


def exact(kind, a, b):
    dims = {"nn": ((1,), (0,)), "nt": ((1,), (1,)), "tn": ((0,), (0,))}[kind]
    return lax.dot_general(a, b, (dims, ((), ())), precision=lax.Precision.HIGHEST, preferred_element_type=jnp.float32)


CHAIN_GROUPS = dict(tok="line", cot="col", rows="col", d_attn="line", part="col", mix="col", dn="line")
LANE_GROUPS = dict(
    place="ctx", wc="ctx", small="ctx", slot="col", gate_a="ctx", gate_b="ctx", up="ctx",
    down="ctx", att="ctx", gates="col", turn="col", gc="ctx", wo="line",
    gs="ctx", go="fsdp", grad0="ctx", grad1="ctx", grad2="ctx", grad3="ctx", grad4="ctx", grad5="ctx")
PLANE_LANES = ["cot", "row", "g", "back", "dg", "out"]
COLUMN_LANES = ["wc", "small", "wo", "gc", "gs"]
RELAYS = ["tok", "wo", "d_attn", "sib"]


def layer_kernel(z, R, dc, tile, names, *refs):
    r = types.SimpleNamespace(**dict(zip(names, refs)))
    me = z.place(lax.axis_index("ctx"), lax.axis_index("fsdp"))
    C, F, H, P, J, rs, qw = z.C, z.F, z.H, z.P, z.J, z.rows_w, z.q_width
    L = C * R
    half = dc // 2
    low, high = pl.ds(0, half), pl.ds(half, half)
    sems = lambda kind, name: (getattr(r, kind + name + "_send"), getattr(r, kind + name + "_recv"))

    def at_slot(ref, h, p):
        return rows_at(ref, h * P + p, CAP)

    def lane(name, source, landing):
        return Lane(z, me, LANE_GROUPS[name], source, landing, *sems("lane_", name))

    def chain(name, own, landing):
        return Chain(z, me, CHAIN_GROUPS[name], own, landing, *sems("chain_", name))

    def plane(name, source, landing):
        def at(h):
            send, recv = sems("plane_", name)
            land = lambda p: at_slot(landing, h, p.p) if len(landing.shape) == 2 else landing.at[h, p.p]
            return Lane(z, me, "plane", lambda to: source.at[h, to.p], land, send.at[h], recv.at[h])
        return at

    def column(name, source, landing):
        return lambda c: column_lane(z, me, c, source, landing, *sems("column_", name))

    def relay(name, own, landing):
        return Relay(z, me, own, landing, *sems("relay_", name))

    tok_chain = chain("tok", r.tok, lambda place: r.blocks.at[2 * place + me.k])
    tok_relay = relay("tok", r.tok, lambda c: r.blocks.at[c])
    place_lane = lane("place", lambda to: r.place_all.at[me.c], lambda p: r.place_all.at[p.c])
    wc_lane = lane("wc", lambda to: r.w_pack.at[to.c], lambda p: rows_at(r.wc_v, p.w, rs))
    small_lane = lane("small", lambda to: r.small, lambda p: rows_at(r.small_v, p.w, rs))
    wo_lane = lane("wo", lambda to: r.w_out, lambda p: rows_at(r.wo_v, p.w, rs))
    wo_relay = relay("wo", None, lambda c: rows_at(r.wo_v, c, qw))
    spread = lambda name, ref: column(
        name, lambda c, to: rows_at(ref, c * F + me.f, rs), lambda c, p: rows_at(ref, c * F + p.f, rs))
    wc_column, small_column, wo_column = spread("wc", r.wc_v), spread("small", r.small_v), spread("wo", r.wo_v)
    cot_chain = chain("cot", r.cot, lambda h: r.cot_all.at[h])
    slot_lane = lane("slot", lambda to: r.slot_t.at[pl.ds(0, EXPERTS), :], lambda p: r.slot_all.at[p.h])
    gate_a_lane = lane("gate_a", lambda to: r.w_gate.at[to.m, low], lambda p: r.wv.at[0, p.c, low])
    gate_b_lane = lane("gate_b", lambda to: r.w_gate.at[to.m, high], lambda p: r.wv.at[0, p.c, high])
    up_lane = lane("up", lambda to: r.w_up.at[to.m], lambda p: r.wv.at[1, p.c])
    down_lane = lane("down", lambda to: r.w_downt.at[to.m], lambda p: r.wv.at[2, p.c])
    att_lane = lane("att", lambda to: r.att_stage.at[to.c], lambda p: r.att_in.at[p.c])
    rows_chain = chain("rows", r.h2, lambda h: r.h_all.at[h])
    gates_lane = lane("gates", lambda to: r.gates_t.at[pl.ds(0, EXPERTS), :], lambda p: r.gate_all.at[p.h])
    turn_lane = lane("turn", lambda to: r.turn_stage.at[to.h], lambda p: r.turn_in.at[p.h])
    up_attn_chain = chain("d_attn", r.d_attn, lambda place: r.blocks.at[2 * place + me.k])
    up_attn_relay = relay("d_attn", r.d_attn, lambda c: r.blocks.at[c])
    dn_block = lambda c: rows_at(r.pool, c, R)
    dn_in = lambda j: rows_at(r.xin, j, R)
    sib_in = lambda j: rows_at(r.cot_v, j, R)
    fold = lambda name, block, landing: Fold(z, me, CHAIN_GROUPS[name], r.total, block, landing, *sems("chain_", name))
    part_fold = fold("part", lambda h: r.part_stage.at[h], lambda slot: r.part_in.at[slot])
    mix_fold = fold("mix", lambda h: r.part_stage.at[h], lambda slot: r.mix_in.at[slot])
    dn_fold = fold("dn", lambda place: dn_block(2 * place + me.k), dn_in)
    gc_lane = lane("gc", lambda to: r.gc_sum.at[to.c], lambda p: r.gc_in.at[p.c])
    gs_lane = lane("gs", lambda to: r.gs_sum.at[to.c], lambda p: r.gs_in.at[p.c])
    go_lane = lane("go", lambda to: rows_at(r.go_stage, to.f, rs), lambda p: r.go_in.at[p.f])
    gather = lambda name, stage, landing: column(
        name, lambda c, to: rows_at(stage, c * F + to.f, rs), lambda c, p: landing.at[p.f, c])
    gc_column, gs_column = gather("gc", r.gc_stage, r.gc_x), gather("gs", r.gs_stage, r.gs_x)
    grad_of = lambda j, c: rows_at(r.g_down, c, dc) if j == 2 else r.wv.at[j, c]
    grad_lanes = [
        lane("grad" + str(2 * j + i),
             lambda to, j=j, i=i: grad_of(j, to.c).at[(low, high)[i]],
             lambda p, j=j, i=i: r.gw_in.at[j, p.s, p.m, (low, high)[i]])
        for j in range(3) for i in range(2)
    ]
    cot_plane = plane("cot", r.d_rows, r.cot_v)
    row_plane = plane("row", r.stage, r.xin)
    g_plane = plane("g", r.g_stage, r.gin)
    back_plane = plane("back", r.d_rows, r.stage)
    dg_plane = plane("dg", r.dg_stage, r.dg_in)
    out_plane = plane("out", r.result, r.out_in)

    def sib_copy(j):
        send, recv = sems("relay_", "sib")
        return pltpu.make_async_remote_copy(
            src_ref=dn_block(2 * j + 1 - me.k), dst_ref=sib_in(j), send_sem=send.at[j], recv_sem=recv.at[j],
            device_id=(me.c + 1 - 2 * me.k, me.f), device_id_type=MESH)

    meet(z, me, ["ctx", "plane", "fsdp"])
    r.place_all[me.c] = jnp.broadcast_to(r.place[...], (8, R))
    wc_lane.start()
    small_lane.start()
    place_lane.start()

    own = [
        pltpu.make_async_copy(r.w_pack.at[me.c], rows_at(r.wc_v, me.w, rs), r.own_sem.at[0]),
        pltpu.make_async_copy(r.small, rows_at(r.small_v, me.w, rs), r.own_sem.at[1]),
        pltpu.make_async_copy(r.w_out, rows_at(r.wo_v, me.w, rs), r.own_sem.at[2]),
    ]
    own_weights = [
        pltpu.make_async_copy(source.at[me.m], r.wv.at[j, me.c], r.own_sem.at[3 + j])
        for j, source in enumerate([r.w_gate, r.w_up, r.w_downt])
    ]
    for copy in own + own_weights:
        copy.start()
    r.blocks[me.c] = r.tok[...]
    r.cot_all[me.h] = r.cot[...]

    row_id = lax.broadcasted_iota(jnp.int32, (LANES, R), 0)
    named = jnp.zeros((LANES, R), jnp.float32)
    for j in range(TOP):
        named = jnp.where(r.routes[j : j + 1, :] == row_id, 1.0, named)
    before = jnp.where(row_id < lane_of((R, R)), 1.0, 0.0).astype(jnp.bfloat16)
    slot = nn(named.astype(jnp.bfloat16), before)
    r.slot_t[...] = jnp.where(named > 0.5, slot, -1.0)
    r.slot_all[me.h] = r.slot_t[0:EXPERTS, :]
    slot_lane.start()
    slot_id = lax.broadcasted_iota(jnp.int32, (CAP, R), 0).astype(jnp.float32)

    wc_lane.wait_recv()
    small_lane.wait_recv()
    wo_lane.start()
    tok_relay.start_own()
    tok_chain.start()
    cot_chain.start()
    for copy in own:
        copy.wait()
    times(C, lambda c: wc_column(c).start())
    times(C, lambda c: small_column(c).start())

    def choose(j):
        h = lax.rem(me.h + H - j, H)
        @pl.when(j > 0)
        def _():
            slot_lane.wait_recv_one(j)

        def for_expert(p):
            row = r.slot_all[h, pl.ds(z.expert(me, p), 1), :]
            r.pick[h, p] = jnp.where(row == slot_id, 1.0, 0.0).astype(jnp.bfloat16)
        times(P, for_expert)

    def dispatch_cot(h):
        def to_expert(n):
            p = lax.rem(me.p + n, P)
            r.d_rows[h, p] = nn(r.pick[h, p], r.cot_all[h]).astype(jnp.bfloat16)
            @pl.when(n > 0)
            def _():
                cot_plane(h).start_one(n)
        times(P, to_expert)
        at_slot(r.cot_v, h, me.p)[...] = r.d_rows[h, me.p]
    place_lane.wait_recv()
    times(C, lambda c: wc_column(c).wait_recv())
    times(C, lambda c: small_column(c).wait_recv())
    times(H, choose)
    gain_one = r.small_v[...].astype(jnp.float32).T[EXPERTS : EXPERTS + 1, :]
    gain_two = r.small_v[...].astype(jnp.float32).T[EXPERTS + 1 : EXPERTS + 2, :]
    head_of = lax.div(lane_of((R, LANES)), HEAD)

    def project(place, core):
        c = 2 * place + core
        x = r.blocks[c].astype(jnp.float32)
        inverse = lax.rsqrt(jnp.mean(x * x, axis=-1, keepdims=True) + norm_eps)
        h = (x * inverse * gain_one).astype(jnp.bfloat16)
        part = pl.ds(pl.multiple_of(c * R, R), R)
        r.h1[part, :] = h
        qkv = nn(h, r.wc_v[...])
        row = r.place_all[c][0:1, :].astype(jnp.float32)
        r.place_row[c] = jnp.broadcast_to(row, (8, R))
        places = jnp.broadcast_to(row, (R, R)).T
        r.place_col[part, :] = places
        r.q_all[part, :] = rope(qkv[:, :LANES], *rope_tables(places, r.freq[0:1, :])).astype(jnp.bfloat16)
        kv = rope(qkv[:, LANES:], *rope_tables(places, r.freq[1:2, :]))
        swapped = pltpu.roll(kv, HEAD, 1)
        r.k2[part, :] = jnp.where(head_of == 0, kv, swapped).astype(jnp.bfloat16)
        r.v2[part, :] = jnp.where(head_of == 0, swapped, kv).astype(jnp.bfloat16)
    dispatch_cot(me.h)
    wo_lane.wait_recv()
    times(J, lambda j: wo_column(2 * j + me.k).start())
    tok_chain.visit(project, tok_relay)
    gate_a_lane.start()
    cot_chain.visit_some(dispatch_cot, 0, 2)
    tok_relay.wait_send()

    def attend(c):
        part = pl.ds(pl.multiple_of(c * R, R), R)
        q = r.q_all[part, :]
        row = jnp.concatenate([r.place_row[i, 0:1, :] for i in range(C)], axis=1)
        allowed = row <= r.place_col[part, 0:1]
        total = jnp.zeros((R, LANES), jnp.float32)
        for h in range(z.q_heads):
            mine = head_of == h
            s = nt(jnp.where(mine, q, jnp.zeros_like(q)), r.k2[...]) * score_scale
            s = jnp.where(allowed, s, masked_score)
            top = jnp.max(s, axis=-1, keepdims=True)
            e = jnp.exp(s - top)
            weight = jnp.sum(e, axis=-1, keepdims=True)
            r.lse[h, part, :] = jnp.broadcast_to(top + jnp.log(weight), (R, LANES))
            total = jnp.where(mine, nn(e.astype(jnp.bfloat16), r.v2[...]) / weight, total)
        r.att_f[part, :] = total
        r.att_stage[c] = total.astype(jnp.bfloat16)
    times(C, attend)
    tok_chain.wait_send()
    att_lane.start()
    r.att_in[me.c] = r.att_stage[me.c]
    cot_chain.visit_some(dispatch_cot, 2, min(4, 2 * (H - 1)))
    times(J, lambda j: wo_column(2 * j + me.k).wait_recv())
    times(J, wo_relay.start)
    att_lane.wait_recv()
    times(J, wo_relay.wait_recv)
    x = r.tok[...].astype(jnp.float32)
    mixed = jnp.zeros((R, D), jnp.float32)
    for c in range(C):
        mixed = mixed + nn(r.att_in[c][:, :qw], r.wo_v[c * qw : (c + 1) * qw, :])
    mid = x + residual_scale * mixed
    r.middle[...] = mid
    inverse = lax.rsqrt(jnp.mean(mid * mid, axis=-1, keepdims=True) + norm_eps)
    hidden = (mid * inverse * gain_two).astype(jnp.bfloat16)
    r.h2[...] = hidden
    rows_chain.start()
    chosen = r.slot_t[...].T > -0.5
    logits = jnp.where(chosen, nn(hidden, r.small_v[...]), masked_score)
    raised = jnp.where(chosen, jnp.exp(logits - jnp.max(logits, axis=-1, keepdims=True)), 0.0)
    r.gates_t[...] = (raised / jnp.sum(raised, axis=-1, keepdims=True)).T
    gates_lane.start()
    r.h_all[me.h] = r.h2[...]
    r.gate_all[me.h] = r.gates_t[0:EXPERTS, :]

    def dispatch_rows(h):
        @pl.when(h != me.h)
        def _():
            gates_lane.wait_recv_one(lax.rem(me.h + H - h, H))

        def to_expert(n):
            p = lax.rem(me.p + n, P)
            hot = r.pick[h, p]
            r.stage[h, p] = nn(hot, r.h_all[h]).astype(jnp.bfloat16)
            g = jnp.broadcast_to(r.gate_all[h, pl.ds(z.expert(me, p), 1), :], (8, R))
            wide = jnp.concatenate([hot.astype(jnp.float32), jnp.zeros((LANES - CAP, R), jnp.float32)], axis=0)
            r.g_stage[h, p] = exact("nt", g, wide)
            @pl.when(n > 0)
            def _():
                row_plane(h).start_one(n)
        times(P, to_expert)
        at_slot(r.xin, h, me.p)[...] = r.stage[h, me.p]
        r.gin[h, me.p] = r.g_stage[h, me.p]
    rows_chain.visit(dispatch_rows)
    cot_chain.visit_some(dispatch_cot, 4, 2 * (H - 1))
    gate_b_lane.start()
    up_lane.start()
    down_lane.start()

    def send_gates(j):
        h = lax.rem(me.h + H - j, H)

        def to_expert(n):
            row_plane(h).wait_send_one(n)
            g_plane(h).start_one(n)
        times(P, to_expert, 1)
    times(H, send_gates)
    times(H, lambda h: cot_plane(h).wait_send())
    for copy in own_weights:
        copy.wait()
    for bulk in [gate_a_lane, gate_b_lane, up_lane]:
        bulk.wait_recv()
    times(H, lambda h: cot_plane(h).wait_recv())
    wg, wu, wd = [r.wv.at[j].reshape(D, r.wv.shape[3]) for j in range(3)]
    per = tile // CAP

    def forward(j):
        h = lax.rem(me.h + H - lax.rem(j + 1, H), H)
        row_plane(h).wait_recv()
        g_plane(h).wait_recv()

        def rows(t):
            part = pl.ds(pl.multiple_of((h * P + t * per) * CAP, CAP), tile)
            for p in range(per):
                turned = jnp.broadcast_to(r.gin[h, t * per + p, 0:1, :], (LANES, LANES)).T
                r.g_col[p * CAP : (p + 1) * CAP, :] = turned[0:CAP, :]
            x = r.xin[part, :]
            r.hid[part, :] = (jax.nn.silu(nn(x, wg[...])) * nn(x, wu[...])).astype(jnp.bfloat16)
            r.pool[part, :] = (residual_scale * r.g_col[:, 0:1] * r.cot_v[part, :].astype(jnp.float32)).astype(jnp.bfloat16)
        times(P // per, rows)
    times(H, forward)

    def cut_down(d):
        part = pl.ds(pl.multiple_of(d * 256, 256), 256)
        r.g_down[part, :] = tn(r.pool[pl.ds(0, H * P * CAP), part], r.hid[...]).astype(jnp.bfloat16)
    times(D // 256, cut_down)
    grad_lanes[4].start()
    grad_lanes[5].start()
    down_lane.wait_recv()

    def chunk(h):

        def rows(t):
            some = pl.ds(pl.multiple_of(t * per, per), per)
            part = pl.ds(pl.multiple_of((h * P + t * per) * CAP, CAP), tile)
            x = r.xin[part, :]
            gate = nn(x, wg[...])
            up = nn(x, wu[...])
            sig = jax.nn.sigmoid(gate)
            act = gate * sig
            out = nt(r.hid[part, :], wd[...]).astype(jnp.bfloat16)
            r.result[h, some] = out.reshape(per, CAP, D)
            upstream = r.cot_v[part, :].astype(jnp.float32)
            d_gates = residual_scale * jnp.sum(upstream * out.astype(jnp.float32), axis=-1, keepdims=True)
            d_hidden = nn(r.pool[part, :], wd[...])
            dg = (d_hidden * up * sig * (1.0 + gate * (1.0 - sig))).astype(jnp.bfloat16)
            du = (d_hidden * act).astype(jnp.bfloat16)
            r.d_gate[part, :] = dg
            r.d_up[part, :] = du
            r.d_rows[h, some] = (nt(dg, wg[...]) + nt(du, wu[...])).astype(jnp.bfloat16).reshape(per, CAP, D)
            r.g_col[...] = jnp.broadcast_to(d_gates, (tile, LANES))
            for p in range(per):
                turned = jnp.concatenate(
                    [r.g_col[p * CAP : (p + 1) * CAP, :], jnp.zeros((LANES - CAP, LANES), jnp.float32)], axis=0)
                r.dg_stage[h, t * per + p] = turned.T[0:8, :]
        times(P // per, rows)
        back_plane(h).start()
        dg_plane(h).start()
        r.stage[h, me.p] = r.d_rows[h, me.p]
        r.dg_in[h, me.p] = r.dg_stage[h, me.p]
    part_fold.far_first(chunk)

    def cut(d):
        part = pl.ds(pl.multiple_of(d * 256, 256), 256)
        x = r.xin[:, part]
        wg[part, :] = tn(x, r.d_gate[...]).astype(jnp.bfloat16)
        wu[part, :] = tn(x, r.d_up[...]).astype(jnp.bfloat16)
    times(D // 256, cut)
    grad_lanes[0].start()
    own_grads = [
        pltpu.make_async_copy(grad_of(j, me.c), r.gw_in.at[j, me.s, me.m], r.own_sem.at[8 + j]) for j in range(3)
    ]
    for copy in own_grads:
        copy.start()

    def trickle(q):
        for i, bulk in enumerate(grad_lanes[1:4]):
            n = q - i * (C - 1) + 1
            @pl.when(jnp.logical_and(n > 0, n < C))
            def _(bulk=bulk, n=n):
                bulk.start_one(n)

    def collect(h):
        back_plane(h).wait_recv()
        dg_plane(h).wait_recv()
        r.total[...] = tn(r.pick[h].reshape(P * CAP, R), r.stage[h].reshape(P * CAP, D))
        r.turn_stage[h] = jnp.zeros((EXPERTS, R), jnp.float32)

        def gates_of(p):
            row = jnp.broadcast_to(r.dg_in[h, p, 0:1, 0:CAP], (8, CAP))
            r.turn_stage[h, pl.ds(z.expert(me, p), 1), :] = exact("nn", row, r.pick[h, p].astype(jnp.float32))[0:1, :]
        times(P, gates_of)
        @pl.when(h != me.h)
        def _():
            part_fold.send(h)
            turn_lane.start_one(lax.rem(h + H - me.h, H))
    part_fold.far_first(collect)
    r.turn_v[...] = jnp.zeros((LANES, R), jnp.float32)
    r.turn_v[0:EXPERTS, :] = r.turn_stage[me.h]
    times(H, lambda h: out_plane(h).start())
    own_out = pltpu.make_async_copy(r.result.at[:, me.p], r.out_in.at[:, me.p], r.own_sem.at[7])
    own_out.start()
    part_fold.finish()
    turn_lane.wait_recv()

    def add_part(n):
        h = lax.rem(me.h + n + 1, H)
        r.turn_v[0:EXPERTS, :] += r.turn_in[h]
    times(H - 1, add_part)
    gts = r.gates_t[...].T
    dgs = r.turn_v[...].T
    d_log = gts * (dgs - jnp.sum(gts * dgs, axis=-1, keepdims=True))
    d_h2 = r.total[...] + exact("nt", d_log, r.small_v[...].astype(jnp.float32))
    mid = r.middle[...]
    inverse = lax.rsqrt(jnp.mean(mid * mid, axis=-1, keepdims=True) + norm_eps)
    n2 = mid * inverse
    g = d_h2 * gain_two
    dm = r.cot[...].astype(jnp.float32) + inverse * (g - n2 * jnp.mean(g * n2, axis=-1, keepdims=True))
    r.d_mid[...] = dm
    r.d_attn[...] = (residual_scale * dm).astype(jnp.bfloat16)
    up_attn_relay.start_own()
    up_attn_chain.start()
    r.gain_v[...] = jnp.zeros((LANES, D), jnp.float32)
    r.gain_v[EXPERTS + 1 : EXPERTS + 2, :] = jnp.sum(d_h2 * n2, axis=0, keepdims=True)
    r.g_small[...] = exact("tn", r.h2[...].astype(jnp.float32), d_log)

    r.blocks[me.c] = r.d_attn[...]
    r.dk_acc[...] = jnp.zeros((L, LANES), jnp.float32)
    r.dv_acc[...] = jnp.zeros((L, LANES), jnp.float32)
    wo_c = rows_at(r.wo_v, me.c, qw)

    def attend_back(place, core):
        c = 2 * place + core
        trickle(2 * H + c)
        part = pl.ds(pl.multiple_of(c * R, R), R)
        q = r.q_all[part, :]
        d_mix = nt(r.blocks[c], wo_c[...])
        if qw < LANES:
            d_mix = jnp.concatenate([d_mix, jnp.zeros((R, LANES - qw), jnp.float32)], axis=1)
        d_mix = d_mix.astype(jnp.bfloat16)
        row = jnp.concatenate([r.place_row[i, 0:1, :] for i in range(C)], axis=1)
        places = r.place_col[part, :]
        allowed = row <= places[:, 0:1]
        dq = jnp.zeros((R, LANES), jnp.float32)
        for h in range(z.q_heads):
            mine = head_of == h
            rows = pl.ds(h * R, R)
            q_h = jnp.where(mine, q, jnp.zeros_like(q))
            dm_h = jnp.where(mine, d_mix, jnp.zeros_like(d_mix))
            r.q_v[rows, :] = q_h
            r.dm_v[rows, :] = dm_h
            s = jnp.where(allowed, nt(q_h, r.k2[...]) * score_scale, masked_score)
            p = jnp.exp(s - r.lse[h, part, 0:1])
            r.p_v[rows, :] = p.astype(jnp.bfloat16)
            delta = jnp.sum(dm_h.astype(jnp.float32) * r.att_f[part, :], axis=-1, keepdims=True)
            ds = (p * (nt(dm_h, r.v2[...]) - delta)).astype(jnp.bfloat16)
            r.ds_v[rows, :] = ds
            dq = jnp.where(mine, nn(ds, r.k2[...]) * score_scale, dq)
        r.dk_acc[...] += tn(r.ds_v[...], r.q_v[...])
        r.dv_acc[...] += tn(r.p_v[...], r.dm_v[...])
        cosine, sine = rope_tables(places, r.freq[0:1, :])
        r.d_qkv[part, 0:LANES] = rope(dq, cosine, -sine).astype(jnp.bfloat16)
    up_attn_chain.visit(attend_back, up_attn_relay)

    def finish_kv(c):
        part = pl.ds(pl.multiple_of(c * R, R), R)
        dk = r.dk_acc[part, :] * score_scale
        dv = r.dv_acc[part, :]
        dk = dk + pltpu.roll(dk, HEAD, 1)
        dv = dv + pltpu.roll(dv, HEAD, 1)
        cosine, sine = rope_tables(r.place_col[part, :], r.freq[1:2, :])
        r.d_qkv[part, LANES : 2 * LANES] = rope(jnp.where(head_of == 0, dk, dv), cosine, -sine).astype(jnp.bfloat16)
    times(C, finish_kv)

    def down_tokens(c):
        return nt(r.d_qkv[pl.ds(pl.multiple_of(c * R, R), R), :], r.wc_v[...])

    def for_sibling(place):
        c = 2 * place + 1 - me.k
        dn_block(c)[...] = down_tokens(c).astype(jnp.bfloat16)
        sib_copy(place).start()
    dn_fold.far_first(for_sibling)

    def for_line(place):
        dn = down_tokens(2 * place + me.k)
        sib_copy(place).wait_recv()
        r.total[...] = dn + sib_in(place)[...].astype(jnp.float32)
        @pl.when(place != dn_fold.place)
        def _():
            dn_fold.send(place)
        @pl.when(place == dn_fold.place)
        def _():
            r.grad_tokens[...] = r.total[...]
    dn_fold.far_first(for_line)

    own_out.wait()
    part_fold.wait_send()

    def mix(h):
        out_plane(h).wait_recv()
        load = pltpu.make_async_copy(r.out_in.at[h], r.stage.at[h], r.own_sem.at[12])
        load.start()

        def weigh(p):
            g = r.gate_all[h, pl.ds(z.expert(me, p), 1), :] * r.pick[h, p].astype(jnp.float32)
            high = g.astype(jnp.bfloat16)
            r.mix_hi[p] = high
            r.mix_lo[p] = (g - high.astype(jnp.float32)).astype(jnp.bfloat16)
        times(P, weigh)
        load.wait()
        rows = r.stage[h].reshape(P * CAP, D)
        total = tn(r.mix_hi[...].reshape(P * CAP, R), rows) + tn(r.mix_lo[...].reshape(P * CAP, R), rows)
        r.total[...] = total
        @pl.when(h != me.h)
        def _():
            mix_fold.send(h)
    mix_fold.far_first(mix)
    times(3 * (C - 1), trickle, 2 * H + C)
    times(2 * H, trickle)

    def weights(d):
        part = pl.ds(pl.multiple_of(d * 256, 256), 256)
        total = tn(r.h1[:, part], r.d_qkv[...])
        r.gc_stage[part, :] = total.astype(jnp.bfloat16)
        gain = jnp.sum(total * r.wc_v[part, :].astype(jnp.float32), axis=-1, keepdims=True)
        gain = gain / r.small_v[part, EXPERTS : EXPERTS + 1].astype(jnp.float32)
        r.g_small[part, :] = jnp.where(lane_of((256, LANES)) == EXPERTS, gain, r.g_small[part, :])
    times(D // 256, weights)
    times(C, lambda c: gc_column(c).start())
    r.gs_stage[...] = (r.g_small[...] + r.gain_v[...].T).astype(jnp.bfloat16)
    times(C, lambda c: gs_column(c).start())
    own_last = [
        pltpu.make_async_copy(rows_at(stage, c * F + me.f, rs), landing.at[me.f, c], r.own_cols.at[i, c])
        for i, (stage, landing) in enumerate([(r.gc_stage, r.gc_x), (r.gs_stage, r.gs_x)]) for c in range(C)
    ]
    for copy in own_last:
        copy.start()
    r.go_stage[...] = tn(r.att_f[...].astype(jnp.bfloat16), r.blocks[...].reshape(L, D)).astype(jnp.bfloat16)
    go_lane.start()
    own_go = pltpu.make_async_copy(rows_at(r.go_stage, me.f, rs), r.go_in.at[me.f], r.own_sem.at[13])
    own_go.start()
    for copy in own_last:
        copy.wait()
    times(C, lambda c: gc_column(c).wait_recv())
    times(C, lambda c: gs_column(c).wait_recv())
    gc_total = r.gc_x[0].astype(jnp.float32)
    gs_total = r.gs_x[0].astype(jnp.float32)
    for f in range(1, F):
        gc_total = gc_total + r.gc_x[f].astype(jnp.float32)
        gs_total = gs_total + r.gs_x[f].astype(jnp.float32)
    r.gc_sum[...] = gc_total.astype(jnp.bfloat16)
    r.gs_sum[...] = gs_total.astype(jnp.bfloat16)
    gc_lane.start()
    gs_lane.start()
    own_sums = [
        pltpu.make_async_copy(r.gc_sum.at[me.c], r.gc_in.at[me.c], r.own_sem.at[14]),
        pltpu.make_async_copy(r.gs_sum.at[me.c], r.gs_in.at[me.c], r.own_sem.at[15]),
    ]
    for copy in own_sums:
        copy.start()
    for last in [place_lane, wc_lane, small_lane, slot_lane, gate_a_lane, gate_b_lane, up_lane, down_lane, att_lane, gates_lane,
                 turn_lane, wo_lane, *grad_lanes[4:]]:
        last.wait_send()
    for last in [cot_chain, rows_chain, up_attn_chain, wo_relay, up_attn_relay]:
        last.wait_send()
    times(J, lambda j: sib_copy(j).wait_send())
    for last in [g_plane, back_plane, dg_plane, out_plane]:
        times(H, lambda h, last=last: last(h).wait_send())
    times(J, lambda j: wo_column(2 * j + me.k).wait_send())
    for last in [wc_column, small_column, gc_column, gs_column]:
        times(C, lambda c, last=last: last(c).wait_send())
    mix_fold.finish()
    r.output[...] = (r.middle[...] + residual_scale * r.total[...]).astype(jnp.bfloat16)

    r.total[...] = r.grad_tokens[...]
    dn_fold.finish()
    d_h1 = r.total[...]
    x = r.tok[...].astype(jnp.float32)
    inverse = lax.rsqrt(jnp.mean(x * x, axis=-1, keepdims=True) + norm_eps)
    n1 = x * inverse
    g = d_h1 * gain_one
    r.grad_tokens[...] = r.d_mid[...] + inverse * (g - n1 * jnp.mean(g * n1, axis=-1, keepdims=True))
    for last in [gc_lane, gs_lane, go_lane]:
        last.wait_recv()
    for last in grad_lanes:
        last.wait_recv()
    for last in [gc_lane, gs_lane, go_lane] + grad_lanes[:4]:
        last.wait_send()
    for last in [mix_fold, dn_fold]:
        last.wait_send()
    for copy in own_grads + own_sums + [own_go]:
        copy.wait()


def layer_call(z, R, ff, dc, tok, place, routes, cot, w_pack, small, w_out, w_gate, w_up, w_downt):
    C, F, N, H, P, J, S, rs = z.C, z.F, z.N, z.H, z.P, z.J, z.S, z.rows_w
    L, f, f16 = C * R, jnp.float32, jnp.bfloat16
    rows, heads, tile = H * P * CAP, z.q_heads * R, 8 * CAP
    ins = dict(tok=(tok, 1), place=(place, 1), routes=(routes, 1), cot=(cot, 1), freq=(frequencies(), 1), w_pack=(w_pack, 0),
               small=(small, 0), w_out=(w_out, 0), w_gate=(w_gate, 0), w_up=(w_up, 0), w_downt=(w_downt, 0))
    outs = dict(
        output=(shape_of((R, D)), 1), grad_tokens=(shape_of((R, D), f), 1), gc_in=(shape_of((C, rs, 2 * LANES)), 0),
        gs_in=(shape_of((C, rs, LANES)), 0), go_in=(shape_of((F, rs, D)), 0), gw_in=(shape_of((3, S, z.G, dc, ff)), 0),
        out_in=(shape_of((H, P, CAP, D)), 0))
    scratch = dict(
        blocks=vmem((C, R, D)), place_all=vmem((C, 8, R), jnp.int32), wc_v=vmem((D, 2 * LANES)), small_v=vmem((D, LANES)),
        wo_v=vmem((D, D)), cot_all=vmem((H, R, D)), slot_all=vmem((H, EXPERTS, R), f), slot_t=vmem((LANES, R), f),
        place_col=vmem((L, R), f), place_row=vmem((C, 8, R), f), h1=vmem((L, D)), q_all=vmem((L, LANES)), k2=vmem((L, LANES)),
        v2=vmem((L, LANES)), lse=vmem((z.q_heads, L, LANES), f), att_f=vmem((L, LANES), f), att_stage=vmem((C, R, LANES)),
        att_in=vmem((C, R, LANES)), middle=vmem((R, D), f), h2=vmem((R, D)), gates_t=vmem((LANES, R), f),
        gate_all=vmem((H, EXPERTS, R), f), h_all=vmem((H, R, D)), pick=vmem((H, P, CAP, R)), stage=vmem((H, P, CAP, D)),
        xin=vmem((rows, D)), g_stage=vmem((H, P, 8, LANES), f), gin=vmem((H, P, 8, LANES), f), wv=vmem((3, C, dc, ff)),
        cot_v=vmem((rows, D)), d_rows=vmem((H, P, CAP, D)), dg_stage=vmem((H, P, 8, LANES), f),
        dg_in=vmem((H, P, 8, LANES), f), hid=vmem((rows, ff)), d_gate=vmem((rows, ff)), d_up=vmem((rows, ff)),
        pool=vmem((max(rows, L), D)), g_col=vmem((tile, LANES), f), result=vmem((H, P, CAP, D)),
        part_stage=vmem((H, R, D)), part_in=vmem((H + 1, R, D)), turn_stage=vmem((H, EXPERTS, R), f),
        turn_in=vmem((H, EXPERTS, R), f), turn_v=vmem((LANES, R), f), d_mid=vmem((R, D), f), d_attn=vmem((R, D)),
        g_small=vmem((D, LANES), f), g_down=vmem((D, ff)), gain_v=vmem((LANES, D), f), ds_v=vmem((heads, L)), p_v=vmem((heads, L)),
        q_v=vmem((heads, LANES)), dm_v=vmem((heads, LANES)), dk_acc=vmem((L, LANES), f), dv_acc=vmem((L, LANES), f),
        d_qkv=vmem((L, 2 * LANES)),
        gc_stage=vmem((D, 2 * LANES)), go_stage=vmem((LANES, D)), gs_stage=vmem((D, LANES)), gc_x=vmem((F, C, rs, 2 * LANES)),
        gs_x=vmem((F, C, rs, LANES)), gc_sum=vmem((C, rs, 2 * LANES)), gs_sum=vmem((C, rs, LANES)), mix_hi=vmem((P, CAP, R)),
        mix_lo=vmem((P, CAP, R)), mix_in=vmem((H + 1, R, D)), total=vmem((R, D), f), own_sem=pltpu.SemaphoreType.DMA((16,)),
        own_cols=pltpu.SemaphoreType.DMA((2, C)))
    both = ("_send", "_recv")
    scratch |= {"lane_" + n + b: pltpu.SemaphoreType.DMA((z.count(g),)) for n, g in LANE_GROUPS.items() for b in both}
    steps = {"col": 2 * H, "line": 2 * J}
    scratch |= {"chain_" + n + b: pltpu.SemaphoreType.DMA((steps[g],)) for n, g in CHAIN_GROUPS.items() for b in both}
    scratch |= {"plane_" + n + b: pltpu.SemaphoreType.DMA((H, P)) for n in PLANE_LANES for b in both}
    scratch |= {"column_" + n + b: pltpu.SemaphoreType.DMA((C, F)) for n in COLUMN_LANES for b in both}
    scratch |= {"relay_" + n + b: pltpu.SemaphoreType.DMA((J,)) for n in RELAYS for b in both}
    names = list(ins) + list(outs) + list(scratch)
    space = lambda fast: pl.BlockSpec(memory_space=pltpu.VMEM if fast else pl.ANY)
    results = pl.pallas_call(
        functools.partial(layer_kernel, z, R, dc, tile, names), name="layer",
        out_shape=[o for o, _ in outs.values()], in_specs=[space(fast) for _, fast in ins.values()],
        out_specs=[space(fast) for _, fast in outs.values()], scratch_shapes=list(scratch.values()),
        compiler_params=pltpu.CompilerParams(collective_id=0, has_side_effects=True, vmem_limit_bytes=67043328),
    )(*[a for a, _ in ins.values()])
    return results[:6]


def local(z, tokens, norm_first, w_query, w_key, w_value, w_out, norm_second, w_router,
          w_gate, w_up, w_down, positions, routes, cotangent):
    C, F = z.C, z.F
    R = tokens.shape[1]
    rs = z.rows_w
    ff = w_gate.shape[2]
    dc = D // C

    heads_q = jnp.pad(w_query.reshape(rs, C, z.q_width), ((0, 0), (0, 0), (0, LANES - z.q_width)))
    heads_k = jnp.repeat(w_key.reshape(rs, KV_HEADS, HEAD), z.share, axis=1)
    heads_v = jnp.repeat(w_value.reshape(rs, KV_HEADS, HEAD), z.share, axis=1)
    w_pack = jnp.concatenate([heads_q, heads_k, heads_v], axis=2).transpose(1, 0, 2)
    small = jnp.concatenate(
        [w_router, norm_first[:, None], norm_second[:, None], jnp.zeros((rs, 128 - EXPERTS - 2), jnp.bfloat16)], axis=1)
    w_downt = w_down.transpose(0, 2, 1)
    output, grad_tokens, gc_in, gs_in, go_in, gw_in = layer_call(
        z, R, ff, dc, tokens[0], positions, routes[0].T, cotangent[0], w_pack, small, w_out, w_gate, w_up, w_downt)
    gc = f32(gc_in)
    join = lambda a: a.reshape(KV_HEADS, z.share, rs, HEAD).sum(axis=1).transpose(1, 0, 2).reshape(rs, KV_HEADS * HEAD)
    gs = jnp.sum(f32(gs_in), axis=0)
    return (
        output[None],
        grad_tokens[None],
        gs[:, EXPERTS],
        gc[:, :, : z.q_width].transpose(1, 0, 2).reshape(rs, D),
        join(gc[:, :, LANES : LANES + HEAD]),
        join(gc[:, :, LANES + HEAD :]),
        jnp.sum(f32(go_in), axis=0),
        gs[:, EXPERTS + 1],
        gs[:, :EXPERTS],
        jnp.sum(f32(gw_in[0]), axis=0),
        jnp.sum(f32(gw_in[1]), axis=0),
        jnp.sum(f32(gw_in[2]), axis=0).transpose(0, 2, 1),
    )


def solution(mesh):
    row = P(("ctx", "fsdp"), None)
    vec = P(("ctx", "fsdp"))
    seq = P("fsdp", "ctx", None)
    down = P("fsdp", None, "ctx")
    return jax.shard_map(
        functools.partial(local, Sizes(mesh)),
        mesh=mesh,
        in_specs=(seq, vec, row, row, row, row, vec, row, seq, seq, down, P("fsdp", "ctx"), seq, seq),
        out_specs=(seq, seq, vec, row, row, row, row, vec, row, seq, seq, down),
        check_vma=False,
    )
```

```python
import collections
import functools
import types

import jax
import jax.numpy as jnp
import numpy as np
from jax import lax
from jax.experimental import pallas as pl
from jax.experimental.pallas import tpu as pltpu
from jax.sharding import PartitionSpec as P

D = 1024
HEADS = 16
KV_HEADS = 8
HEAD = 64
EXPERTS = 32
TOP = 8
CAP = 48
LANES = 128

residual_scale = 0.22
score_scale = 0.015625
rope_base = 10000.0
norm_eps = 1e-06
masked_score = -1e30

MESH = pl.DeviceIdType.MESH
Place = collections.namedtuple("Place", ["c", "f", "m", "s", "h", "k", "p", "w"])


class Sizes:
    def __init__(self, mesh):
        self.C = mesh.shape["ctx"]
        self.F = mesh.shape["fsdp"]
        self.N = self.C * self.F
        self.G = EXPERTS // self.F
        self.S = self.C // self.G
        self.H = self.G // 2
        self.P = 2 * self.F
        self.J = self.C // 2
        self.q_heads = HEADS // self.C
        self.q_width = self.q_heads * HEAD
        self.share = self.C // KV_HEADS
        self.rows_w = D // self.N

    def place(self, c, f):
        k = lax.rem(c, 2)
        return Place(c, f, lax.rem(c, self.G), lax.div(c, self.G), lax.rem(lax.div(c, 2), self.H), k, f * 2 + k, c * self.F + f)

    def count(self, group):
        return {"ctx": self.C, "fsdp": self.F, "world": self.N, "col": self.H, "line": self.J, "plane": self.P}[group]

    def peer(self, group, me, n):
        if group == "ctx":
            return self.place(lax.rem(me.c + n, self.C), me.f)
        if group == "fsdp":
            return self.place(me.c, lax.rem(me.f + n, self.F))
        if group == "world":
            w = lax.rem(me.w + n, self.N)
            return self.place(lax.div(w, self.F), lax.rem(w, self.F))
        if group == "col":
            return self.place(me.s * self.G + 2 * lax.rem(me.h + n, self.H) + me.k, me.f)
        if group == "line":
            return self.place(2 * lax.rem(lax.div(me.c, 2) + n, self.J) + me.k, me.f)
        p = lax.rem(me.p + n, self.P)
        return self.place(me.s * self.G + 2 * me.h + lax.rem(p, 2), lax.div(p, 2))

    def expert(self, me, p):
        return lax.div(p, 2) * self.G + 2 * me.h + lax.rem(p, 2)


def bf(x):
    return x.astype(jnp.bfloat16)


def f32(x):
    return x.astype(jnp.float32)


def shape_of(shape, dtype=jnp.bfloat16):
    return jax.ShapeDtypeStruct(shape, dtype)


class Lane:
    def __init__(self, sizes, me, group, src, dst, sends, recvs):
        self.sizes, self.me, self.group, self.src, self.dst = sizes, me, group, src, dst
        self.sends, self.recvs, self.n = sends, recvs, sizes.count(group)

    def copy(self, k, to, source, landing):
        return pltpu.make_async_remote_copy(
            src_ref=source, dst_ref=landing, send_sem=self.sends.at[k], recv_sem=self.recvs.at[k],
            device_id=(to.c, to.f), device_id_type=MESH)

    def to(self, k):
        return self.sizes.peer(self.group, self.me, k)

    def start_one(self, k):
        to = self.to(k)
        self.copy(k, to, self.src(to), self.dst(self.me)).start()

    def wait_recv_one(self, k):
        landed = self.dst(self.sizes.peer(self.group, self.me, self.n - k))
        self.copy(k, self.to(k), landed, landed).wait_recv()

    def wait_send_one(self, k):
        to = self.to(k)
        self.copy(k, to, self.src(to), self.dst(self.me)).wait_send()

    def each(self, step):
        def one(k, carry):
            step(k)
            return carry
        lax.fori_loop(1, self.n, one, 0)

    def start(self):
        self.each(self.start_one)

    def wait_recv(self):
        self.each(self.wait_recv_one)

    def wait_send(self):
        self.each(self.wait_send_one)


class Chain:
    def __init__(self, sizes, me, group, own, landing, sends, recvs):
        self.col = group == "col"
        self.place, self.n = (me.h, sizes.H) if self.col else (lax.div(me.c, 2), sizes.J)
        self.sizes, self.me, self.own, self.landing, self.sends, self.recvs = sizes, me, own, landing, sends, recvs

    def copy(self, t, to, source, landing):
        c = self.me.s * self.sizes.G + 2 * to + self.me.k if self.col else 2 * to + self.me.k
        return pltpu.make_async_remote_copy(
            src_ref=source, dst_ref=landing, send_sem=self.sends.at[t], recv_sem=self.recvs.at[t],
            device_id=(c, self.me.f), device_id_type=MESH)

    def inside(self, place):
        return jnp.logical_and(place >= 0, place < self.n)

    def origin(self, t):
        return self.place - (1 - 2 * lax.rem(t, 2)) * (lax.div(t, 2) + 1)

    def start(self):
        for t, to in ((0, self.place + 1), (1, self.place - 1)):
            @pl.when(self.inside(to))
            def _(t=t, to=to):
                self.copy(t, to, self.own, self.landing(self.place)).start()

    def take(self, t):
        sign = 1 - 2 * lax.rem(t, 2)
        here = self.landing(self.origin(t))
        self.copy(t, self.place - sign, here, here).wait_recv()
        @pl.when(self.inside(self.place + sign))
        def _():
            self.copy(t + 2, self.place + sign, here, here).start()

    def wait_send(self):
        def one(t, carry):
            to = self.place + 1 - 2 * lax.rem(t, 2)
            origin = to - (1 - 2 * lax.rem(t, 2)) * (lax.div(t, 2) + 1)
            @pl.when(jnp.logical_and(self.inside(to), self.inside(origin)))
            def _():
                self.copy(t, to, self.landing(self.place), self.landing(self.place)).wait_send()
            return carry
        lax.fori_loop(0, 2 * (self.n - 1), one, 0)

    def visit_some(self, step, first, last):
        def one(t):
            @pl.when(self.inside(self.origin(t)))
            def _():
                self.take(t)
                step(self.origin(t))
        times(last, one, first)

    def visit(self, step, relay=None):
        each = 2 * self.n - 1

        def one(i):
            u = lax.rem(i, each)
            origin = jnp.where(u == 0, self.place, self.origin(jnp.maximum(u - 1, 0)))
            @pl.when(self.inside(origin))
            def _():
                @pl.when(jnp.logical_and(u > 0, i < each))
                def _():
                    self.take(u - 1)
                    if relay is not None:
                        relay.start(origin)
                if relay is None:
                    step(origin)
                else:
                    @pl.when(i >= each)
                    def _():
                        relay.wait_recv(origin)
                    step(origin, jnp.where(i < each, self.me.k, 1 - self.me.k))
        times(each if relay is None else 2 * each, one)


class Fold(Chain):
    def __init__(self, sizes, me, group, total, block, landing, sends, recvs):
        super().__init__(sizes, me, group, None, landing, sends, recvs)
        self.total, self.block = total, block

    def far_first(self, step):
        n = self.n
        flip = 2 * self.place >= n
        q = jnp.where(flip, n - 1 - self.place, self.place)

        def one(i):
            left = i - (n - 1 - 2 * q)
            near = q + (1 - 2 * lax.rem(jnp.maximum(left, 0), 2)) * (q - lax.div(jnp.maximum(left, 0), 2))
            dest = jnp.where(left < 0, n - 1 - i, near)
            step(jnp.where(flip, n - 1 - dest, dest))
        times(n, one)

    def index(self, dest):
        return jnp.where(dest > self.place, dest, self.n + dest)

    def add(self, index, slot):
        here = self.landing(slot)
        self.copy(index, self.place, here, here, self.place_of_peer()).wait_recv()
        self.total[...] += here[...].astype(jnp.float32)

    def place_of_peer(self):
        return jnp.where(self.place > 0, self.place - 1, self.place + 1)

    def copy(self, index, to, source, landing, peer=None):
        return super().copy(index, to if peer is None else peer, source, landing)

    def send(self, dest):
        up = dest > self.place
        @pl.when(jnp.where(up, self.place > 0, self.place < self.n - 1))
        def _():
            self.add(self.index(dest), dest)
        self.block(dest)[...] = self.total[...].astype(jnp.bfloat16)
        to = jnp.where(up, self.place + 1, self.place - 1)
        slot = jnp.where(jnp.logical_and(jnp.logical_not(up), dest == to), self.n, dest)
        self.copy(self.index(dest), to, self.block(dest), self.landing(slot)).start()

    def finish(self):
        @pl.when(self.place > 0)
        def _():
            self.add(self.place, self.place)
        @pl.when(self.place < self.n - 1)
        def _():
            self.add(self.n + self.place, self.n)

    def wait_send(self):
        def one(dest, carry):
            @pl.when(dest != self.place)
            def _():
                self.copy(self.index(dest), self.place_of_peer(), self.block(dest), self.landing(dest)).wait_send()
            return carry
        lax.fori_loop(0, self.n, one, 0)


class Relay:
    def __init__(self, sizes, me, own, landing, sends, recvs):
        self.J, self.me, self.own, self.landing, self.sends, self.recvs = sizes.J, me, own, landing, sends, recvs
        self.place = lax.div(me.c, 2)

    def copy(self, place, source, landing):
        return pltpu.make_async_remote_copy(
            src_ref=source, dst_ref=landing, send_sem=self.sends.at[place], recv_sem=self.recvs.at[place],
            device_id=(self.me.c + 1 - 2 * self.me.k, self.me.f), device_id_type=MESH)

    def start_own(self):
        self.copy(self.place, self.own, self.landing(self.me.c)).start()

    def start(self, place):
        here = self.landing(2 * place + self.me.k)
        self.copy(place, here, here).start()

    def wait_recv(self, place):
        there = self.landing(2 * place + 1 - self.me.k)
        self.copy(place, there, there).wait_recv()

    def wait_send(self):
        def one(place, carry):
            here = self.landing(2 * place + self.me.k)
            self.copy(place, here, here).wait_send()
            return carry
        lax.fori_loop(0, self.J, one, 0)


def meet(sizes, me, groups):
    barrier = pltpu.get_barrier_semaphore()
    total = 0
    for group in groups:
        def greet(k, carry, group=group):
            p = sizes.peer(group, me, k)
            pl.semaphore_signal(barrier, inc=1, device_id=(p.c, p.f), device_id_type=MESH)
            return carry
        lax.fori_loop(1, sizes.count(group), greet, 0)
        total += sizes.count(group) - 1
    pl.semaphore_wait(barrier, total)


def times(n, step, first=0):
    def one(i, carry):
        step(i)
        return carry
    lax.fori_loop(first, n, one, 0)


def column_lane(z, me, c, source, landing, sends, recvs):
    return Lane(z, me, "fsdp", lambda to: source(c, to), lambda p: landing(c, p), sends.at[c], recvs.at[c])


def nn(a, b):
    return lax.dot_general(a, b, (((1,), (0,)), ((), ())), preferred_element_type=jnp.float32)


def nt(a, b):
    return lax.dot_general(a, b, (((1,), (1,)), ((), ())), preferred_element_type=jnp.float32)


def tn(a, b):
    return lax.dot_general(a, b, (((0,), (0,)), ((), ())), preferred_element_type=jnp.float32)


def lane_of(shape):
    return lax.broadcasted_iota(jnp.int32, shape, 1)


def rope_tables(place_columns, frequency):
    angles = place_columns.astype(jnp.float32) * frequency
    return jnp.cos(angles), jnp.sin(angles)


def rope(x, cosine, sine):
    half = HEAD // 2
    mixed = jnp.where(lax.rem(lane_of(x.shape), HEAD) < half, -pltpu.roll(x, LANES - half, 1), pltpu.roll(x, half, 1))
    return x * cosine + mixed * sine


def rows_at(ref, i, n):
    return ref.at[pl.ds(pl.multiple_of(i * n, n), n), :]


def vmem(shape, dtype=jnp.bfloat16):
    return pltpu.VMEM(shape, dtype)


def frequencies():
    lanes = np.arange(LANES)
    steps = rope_base ** ((lanes % (HEAD // 2)) * (-2.0 / HEAD))
    return jnp.asarray(np.stack([steps, np.where(lanes < HEAD, steps, 0.0)] + [steps] * 6), jnp.float32)


def exact(kind, a, b):
    dims = {"nn": ((1,), (0,)), "nt": ((1,), (1,)), "tn": ((0,), (0,))}[kind]
    return lax.dot_general(a, b, (dims, ((), ())), precision=lax.Precision.HIGHEST, preferred_element_type=jnp.float32)


CHAIN_GROUPS = dict(tok="line", cot="col", rows="col", d_attn="line", part="col", mix="col", dn="line")
LANE_GROUPS = dict(
    place="ctx", wc="ctx", small="ctx", slot="col", gate_a="ctx", gate_b="ctx", up="ctx",
    down="ctx", att="ctx", gates="col", turn="col", gc="ctx", wo="line",
    gs="ctx", go="fsdp", grad0="ctx", grad1="ctx", grad2="ctx", grad3="ctx", grad4="ctx", grad5="ctx")
PLANE_LANES = ["cot", "row", "g", "back", "dg", "out"]
COLUMN_LANES = ["wc", "small", "wo", "gc", "gs"]
RELAYS = ["tok", "wo", "d_attn", "sib"]


def layer_kernel(z, R, dc, tile, names, *refs):
    r = types.SimpleNamespace(**dict(zip(names, refs)))
    me = z.place(lax.axis_index("ctx"), lax.axis_index("fsdp"))
    C, F, H, P, J, rs, qw = z.C, z.F, z.H, z.P, z.J, z.rows_w, z.q_width
    L = C * R
    half = dc // 2
    low, high = pl.ds(0, half), pl.ds(half, half)
    sems = lambda kind, name: (getattr(r, kind + name + "_send"), getattr(r, kind + name + "_recv"))

    def at_slot(ref, h, p):
        return rows_at(ref, h * P + p, CAP)

    def lane(name, source, landing):
        return Lane(z, me, LANE_GROUPS[name], source, landing, *sems("lane_", name))

    def chain(name, own, landing):
        return Chain(z, me, CHAIN_GROUPS[name], own, landing, *sems("chain_", name))

    def plane(name, source, landing):
        def at(h):
            send, recv = sems("plane_", name)
            land = lambda p: at_slot(landing, h, p.p) if len(landing.shape) == 2 else landing.at[h, p.p]
            return Lane(z, me, "plane", lambda to: source.at[h, to.p], land, send.at[h], recv.at[h])
        return at

    def column(name, source, landing):
        return lambda c: column_lane(z, me, c, source, landing, *sems("column_", name))

    def relay(name, own, landing):
        return Relay(z, me, own, landing, *sems("relay_", name))

    tok_chain = chain("tok", r.tok, lambda place: r.blocks.at[2 * place + me.k])
    tok_relay = relay("tok", r.tok, lambda c: r.blocks.at[c])
    place_lane = lane("place", lambda to: r.place_all.at[me.c], lambda p: r.place_all.at[p.c])
    wc_lane = lane("wc", lambda to: r.w_pack.at[to.c], lambda p: rows_at(r.wc_v, p.w, rs))
    small_lane = lane("small", lambda to: r.small, lambda p: rows_at(r.small_v, p.w, rs))
    wo_lane = lane("wo", lambda to: r.w_out, lambda p: rows_at(r.wo_v, p.w, rs))
    wo_relay = relay("wo", None, lambda c: rows_at(r.wo_v, c, qw))
    spread = lambda name, ref: column(
        name, lambda c, to: rows_at(ref, c * F + me.f, rs), lambda c, p: rows_at(ref, c * F + p.f, rs))
    wc_column, small_column, wo_column = spread("wc", r.wc_v), spread("small", r.small_v), spread("wo", r.wo_v)
    cot_chain = chain("cot", r.cot, lambda h: r.cot_all.at[h])
    slot_lane = lane("slot", lambda to: r.slot_t.at[pl.ds(0, EXPERTS), :], lambda p: r.slot_all.at[p.h])
    gate_a_lane = lane("gate_a", lambda to: r.w_gate.at[to.m, low], lambda p: r.wv.at[0, p.c, low])
    gate_b_lane = lane("gate_b", lambda to: r.w_gate.at[to.m, high], lambda p: r.wv.at[0, p.c, high])
    up_lane = lane("up", lambda to: r.w_up.at[to.m], lambda p: r.wv.at[1, p.c])
    down_lane = lane("down", lambda to: r.w_downt.at[to.m], lambda p: r.wv.at[2, p.c])
    att_lane = lane("att", lambda to: r.att_stage.at[to.c], lambda p: r.att_in.at[p.c])
    rows_chain = chain("rows", r.h2, lambda h: r.h_all.at[h])
    gates_lane = lane("gates", lambda to: r.gates_t.at[pl.ds(0, EXPERTS), :], lambda p: r.gate_all.at[p.h])
    turn_lane = lane("turn", lambda to: r.turn_stage.at[to.h], lambda p: r.turn_in.at[p.h])
    up_attn_chain = chain("d_attn", r.d_attn, lambda place: r.blocks.at[2 * place + me.k])
    up_attn_relay = relay("d_attn", r.d_attn, lambda c: r.blocks.at[c])
    dn_block = lambda c: rows_at(r.pool, c, R)
    dn_in = lambda j: rows_at(r.xin, j, R)
    sib_in = lambda j: rows_at(r.cot_v, j, R)
    fold = lambda name, block, landing: Fold(z, me, CHAIN_GROUPS[name], r.total, block, landing, *sems("chain_", name))
    part_fold = fold("part", lambda h: r.part_stage.at[h], lambda slot: r.part_in.at[slot])
    mix_fold = fold("mix", lambda h: r.part_stage.at[h], lambda slot: r.mix_in.at[slot])
    dn_fold = fold("dn", lambda place: dn_block(2 * place + me.k), dn_in)
    gc_lane = lane("gc", lambda to: r.gc_sum.at[to.c], lambda p: r.gc_in.at[p.c])
    gs_lane = lane("gs", lambda to: r.gs_sum.at[to.c], lambda p: r.gs_in.at[p.c])
    go_lane = lane("go", lambda to: rows_at(r.go_stage, to.f, rs), lambda p: r.go_in.at[p.f])
    gather = lambda name, stage, landing: column(
        name, lambda c, to: rows_at(stage, c * F + to.f, rs), lambda c, p: landing.at[p.f, c])
    gc_column, gs_column = gather("gc", r.gc_stage, r.gc_x), gather("gs", r.gs_stage, r.gs_x)
    halves = (pl.ds(0, r.g_down.shape[1] // 2), pl.ds(r.g_down.shape[1] // 2, r.g_down.shape[1] // 2))
    grad_lanes = [
        lane("grad" + str(2 * j + i),
             lambda to, j=j, i=i: r.wv.at[j, to.c, (low, high)[i]],
             lambda p, j=j, i=i: r.gw_in.at[j, p.s, p.m, (low, high)[i]])
        for j in range(2) for i in range(2)
    ] + [
        lane("grad" + str(4 + i), lambda to, i=i: r.g_down.at[to.c, halves[i]], lambda p, i=i: r.gd_in.at[p.s, p.m, halves[i]])
        for i in range(2)
    ]
    cot_plane = plane("cot", r.d_rows, r.cot_v)
    row_plane = plane("row", r.stage, r.xin)
    g_plane = plane("g", r.g_stage, r.gin)
    back_plane = plane("back", r.d_rows, r.stage)
    dg_plane = plane("dg", r.dg_stage, r.dg_in)
    out_plane = plane("out", r.result, r.out_in)

    def sib_copy(j):
        send, recv = sems("relay_", "sib")
        return pltpu.make_async_remote_copy(
            src_ref=dn_block(2 * j + 1 - me.k), dst_ref=sib_in(j), send_sem=send.at[j], recv_sem=recv.at[j],
            device_id=(me.c + 1 - 2 * me.k, me.f), device_id_type=MESH)

    meet(z, me, ["ctx", "plane", "fsdp"])
    r.place_all[me.c] = jnp.broadcast_to(r.place[...], (8, R))
    wc_lane.start()
    small_lane.start()
    place_lane.start()

    own = [
        pltpu.make_async_copy(r.w_pack.at[me.c], rows_at(r.wc_v, me.w, rs), r.own_sem.at[0]),
        pltpu.make_async_copy(r.small, rows_at(r.small_v, me.w, rs), r.own_sem.at[1]),
        pltpu.make_async_copy(r.w_out, rows_at(r.wo_v, me.w, rs), r.own_sem.at[2]),
    ]
    own_weights = [
        pltpu.make_async_copy(source.at[me.m], r.wv.at[j, me.c], r.own_sem.at[3 + j])
        for j, source in enumerate([r.w_gate, r.w_up, r.w_downt])
    ]
    for copy in own + own_weights:
        copy.start()
    r.blocks[me.c] = r.tok[...]
    r.cot_all[me.h] = r.cot[...]

    row_id = lax.broadcasted_iota(jnp.int32, (LANES, R), 0)
    named = jnp.zeros((LANES, R), jnp.float32)
    for j in range(TOP):
        named = jnp.where(r.routes[j : j + 1, :] == row_id, 1.0, named)
    before = jnp.where(row_id < lane_of((R, R)), 1.0, 0.0).astype(jnp.bfloat16)
    slot = nn(named.astype(jnp.bfloat16), before)
    r.slot_t[...] = jnp.where(named > 0.5, slot, -1.0)
    r.slot_all[me.h] = r.slot_t[0:EXPERTS, :]
    slot_lane.start()
    slot_id = lax.broadcasted_iota(jnp.int32, (CAP, R), 0).astype(jnp.float32)

    wc_lane.wait_recv()
    small_lane.wait_recv()
    wo_lane.start()
    tok_relay.start_own()
    tok_chain.start()
    cot_chain.start()
    for copy in own:
        copy.wait()
    times(C, lambda c: wc_column(c).start())
    times(C, lambda c: small_column(c).start())

    def choose(j):
        h = lax.rem(me.h + H - j, H)
        @pl.when(j > 0)
        def _():
            slot_lane.wait_recv_one(j)

        def for_expert(p):
            row = r.slot_all[h, pl.ds(z.expert(me, p), 1), :]
            r.pick[h, p] = jnp.where(row == slot_id, 1.0, 0.0).astype(jnp.bfloat16)
        times(P, for_expert)

    def dispatch_cot(h):
        def to_expert(n):
            p = lax.rem(me.p + n, P)
            r.d_rows[h, p] = nn(r.pick[h, p], r.cot_all[h]).astype(jnp.bfloat16)
            @pl.when(n > 0)
            def _():
                cot_plane(h).start_one(n)
        times(P, to_expert)
        at_slot(r.cot_v, h, me.p)[...] = r.d_rows[h, me.p]
    place_lane.wait_recv()
    times(C, lambda c: wc_column(c).wait_recv())
    times(C, lambda c: small_column(c).wait_recv())
    times(H, choose)
    gain_one = r.small_v[...].astype(jnp.float32).T[EXPERTS : EXPERTS + 1, :]
    gain_two = r.small_v[...].astype(jnp.float32).T[EXPERTS + 1 : EXPERTS + 2, :]
    head_of = lax.div(lane_of((R, LANES)), HEAD)

    def project(place, core):
        c = 2 * place + core
        x = r.blocks[c].astype(jnp.float32)
        inverse = lax.rsqrt(jnp.mean(x * x, axis=-1, keepdims=True) + norm_eps)
        h = (x * inverse * gain_one).astype(jnp.bfloat16)
        part = pl.ds(pl.multiple_of(c * R, R), R)
        r.h1[part, :] = h
        qkv = nn(h, r.wc_v[...])
        row = r.place_all[c][0:1, :].astype(jnp.float32)
        r.place_row[c] = jnp.broadcast_to(row, (8, R))
        places = jnp.broadcast_to(row, (R, R)).T
        r.place_col[part, :] = places
        r.q_all[part, :] = rope(qkv[:, :LANES], *rope_tables(places, r.freq[0:1, :])).astype(jnp.bfloat16)
        kv = rope(qkv[:, LANES:], *rope_tables(places, r.freq[1:2, :]))
        swapped = pltpu.roll(kv, HEAD, 1)
        r.k2[part, :] = jnp.where(head_of == 0, kv, swapped).astype(jnp.bfloat16)
        r.v2[part, :] = jnp.where(head_of == 0, swapped, kv).astype(jnp.bfloat16)
    dispatch_cot(me.h)
    wo_lane.wait_recv()
    times(J, lambda j: wo_column(2 * j + me.k).start())
    tok_chain.visit(project, tok_relay)
    gate_a_lane.start()
    cot_chain.visit_some(dispatch_cot, 0, 2)
    tok_relay.wait_send()

    def attend(c):
        part = pl.ds(pl.multiple_of(c * R, R), R)
        q = r.q_all[part, :]
        row = jnp.concatenate([r.place_row[i, 0:1, :] for i in range(C)], axis=1)
        allowed = row <= r.place_col[part, 0:1]
        total = jnp.zeros((R, LANES), jnp.float32)
        for h in range(z.q_heads):
            mine = head_of == h
            s = nt(jnp.where(mine, q, jnp.zeros_like(q)), r.k2[...]) * score_scale
            s = jnp.where(allowed, s, masked_score)
            top = jnp.max(s, axis=-1, keepdims=True)
            e = jnp.exp(s - top)
            weight = jnp.sum(e, axis=-1, keepdims=True)
            r.lse[h, part, :] = jnp.broadcast_to(top + jnp.log(weight), (R, LANES))
            total = jnp.where(mine, nn(e.astype(jnp.bfloat16), r.v2[...]) / weight, total)
        r.att_f[part, :] = total
        r.att_stage[c] = total.astype(jnp.bfloat16)
    times(C, attend)
    tok_chain.wait_send()
    att_lane.start()
    r.att_in[me.c] = r.att_stage[me.c]
    cot_chain.visit_some(dispatch_cot, 2, min(4, 2 * (H - 1)))
    times(J, lambda j: wo_column(2 * j + me.k).wait_recv())
    times(J, wo_relay.start)
    att_lane.wait_recv()
    times(J, wo_relay.wait_recv)
    x = r.tok[...].astype(jnp.float32)
    mixed = jnp.zeros((R, D), jnp.float32)
    for c in range(C):
        mixed = mixed + nn(r.att_in[c][:, :qw], r.wo_v[c * qw : (c + 1) * qw, :])
    mid = x + residual_scale * mixed
    r.middle[...] = mid
    inverse = lax.rsqrt(jnp.mean(mid * mid, axis=-1, keepdims=True) + norm_eps)
    hidden = (mid * inverse * gain_two).astype(jnp.bfloat16)
    r.h2[...] = hidden
    rows_chain.start()
    chosen = r.slot_t[...].T > -0.5
    logits = jnp.where(chosen, nn(hidden, r.small_v[...]), masked_score)
    raised = jnp.where(chosen, jnp.exp(logits - jnp.max(logits, axis=-1, keepdims=True)), 0.0)
    r.gates_t[...] = (raised / jnp.sum(raised, axis=-1, keepdims=True)).T
    gates_lane.start()
    r.h_all[me.h] = r.h2[...]
    r.gate_all[me.h] = r.gates_t[0:EXPERTS, :]

    def dispatch_rows(h):
        @pl.when(h != me.h)
        def _():
            gates_lane.wait_recv_one(lax.rem(me.h + H - h, H))

        def to_expert(n):
            p = lax.rem(me.p + n, P)
            hot = r.pick[h, p]
            r.stage[h, p] = nn(hot, r.h_all[h]).astype(jnp.bfloat16)
            g = jnp.broadcast_to(r.gate_all[h, pl.ds(z.expert(me, p), 1), :], (8, R))
            wide = jnp.concatenate([hot.astype(jnp.float32), jnp.zeros((LANES - CAP, R), jnp.float32)], axis=0)
            r.g_stage[h, p] = exact("nt", g, wide)
            @pl.when(n > 0)
            def _():
                row_plane(h).start_one(n)
        times(P, to_expert)
        at_slot(r.xin, h, me.p)[...] = r.stage[h, me.p]
        r.gin[h, me.p] = r.g_stage[h, me.p]
    rows_chain.visit(dispatch_rows)
    cot_chain.visit_some(dispatch_cot, 4, 2 * (H - 1))
    gate_b_lane.start()
    up_lane.start()
    down_lane.start()

    def send_gates(j):
        h = lax.rem(me.h + H - j, H)

        def to_expert(n):
            row_plane(h).wait_send_one(n)
            g_plane(h).start_one(n)
        times(P, to_expert, 1)
    times(H, send_gates)
    times(H, lambda h: cot_plane(h).wait_send())
    for copy in own_weights:
        copy.wait()
    for bulk in [gate_a_lane, gate_b_lane, up_lane]:
        bulk.wait_recv()
    times(H, lambda h: cot_plane(h).wait_recv())
    wg, wu, wd = [r.wv.at[j].reshape(D, r.wv.shape[3]) for j in range(3)]
    per = tile // CAP

    def forward(j):
        h = lax.rem(me.h + H - lax.rem(j + 1, H), H)
        row_plane(h).wait_recv()
        g_plane(h).wait_recv()

        def rows(t):
            part = pl.ds(pl.multiple_of((h * P + t * per) * CAP, CAP), tile)
            for p in range(per):
                turned = jnp.broadcast_to(r.gin[h, t * per + p, 0:1, :], (LANES, LANES)).T
                r.g_col[p * CAP : (p + 1) * CAP, :] = turned[0:CAP, :]
            x = r.xin[part, :]
            r.hid[part, :] = (jax.nn.silu(nn(x, wg[...])) * nn(x, wu[...])).astype(jnp.bfloat16)
            r.pool[part, :] = (residual_scale * r.g_col[:, 0:1] * r.cot_v[part, :].astype(jnp.float32)).astype(jnp.bfloat16)
        times(P // per, rows)
    times(H, forward)

    def cut_down(d):
        part = pl.ds(pl.multiple_of(d * 256, 256), 256)
        total = tn(r.hid[...], r.pool[pl.ds(0, H * P * CAP), part]).astype(jnp.bfloat16)
        for i in range(256 // dc):
            r.g_down[d * (256 // dc) + i] = total[:, i * dc : (i + 1) * dc]
    times(D // 256, cut_down)
    grad_lanes[4].start()
    grad_lanes[5].start()
    down_lane.wait_recv()

    def chunk(h):

        def rows(t):
            some = pl.ds(pl.multiple_of(t * per, per), per)
            part = pl.ds(pl.multiple_of((h * P + t * per) * CAP, CAP), tile)
            x = r.xin[part, :]
            gate = nn(x, wg[...])
            up = nn(x, wu[...])
            sig = jax.nn.sigmoid(gate)
            act = gate * sig
            out = nt(r.hid[part, :], wd[...]).astype(jnp.bfloat16)
            r.result[h, some] = out.reshape(per, CAP, D)
            upstream = r.cot_v[part, :].astype(jnp.float32)
            d_gates = residual_scale * jnp.sum(upstream * out.astype(jnp.float32), axis=-1, keepdims=True)
            d_hidden = nn(r.pool[part, :], wd[...])
            dg = (d_hidden * up * sig * (1.0 + gate * (1.0 - sig))).astype(jnp.bfloat16)
            du = (d_hidden * act).astype(jnp.bfloat16)
            r.d_gate[part, :] = dg
            r.d_up[part, :] = du
            r.d_rows[h, some] = (nt(dg, wg[...]) + nt(du, wu[...])).astype(jnp.bfloat16).reshape(per, CAP, D)
            r.g_col[...] = jnp.broadcast_to(d_gates, (tile, LANES))
            for p in range(per):
                turned = jnp.concatenate(
                    [r.g_col[p * CAP : (p + 1) * CAP, :], jnp.zeros((LANES - CAP, LANES), jnp.float32)], axis=0)
                r.dg_stage[h, t * per + p] = turned.T[0:8, :]
        times(P // per, rows)
        back_plane(h).start()
        dg_plane(h).start()
        r.stage[h, me.p] = r.d_rows[h, me.p]
        r.dg_in[h, me.p] = r.dg_stage[h, me.p]
    part_fold.far_first(chunk)

    def cut(d):
        part = pl.ds(pl.multiple_of(d * 256, 256), 256)
        x = r.xin[:, part]
        wg[part, :] = tn(x, r.d_gate[...]).astype(jnp.bfloat16)
        wu[part, :] = tn(x, r.d_up[...]).astype(jnp.bfloat16)
    times(D // 256, cut)
    grad_lanes[0].start()
    own_grads = [
        pltpu.make_async_copy(source, landing, r.own_sem.at[8 + j]) for j, (source, landing) in enumerate([
            (r.wv.at[0, me.c], r.gw_in.at[0, me.s, me.m]), (r.wv.at[1, me.c], r.gw_in.at[1, me.s, me.m]),
            (r.g_down.at[me.c], r.gd_in.at[me.s, me.m])])
    ]
    for copy in own_grads:
        copy.start()

    def trickle(q):
        for i, bulk in enumerate(grad_lanes[1:4]):
            n = q - i * (C - 1) + 1
            @pl.when(jnp.logical_and(n > 0, n < C))
            def _(bulk=bulk, n=n):
                bulk.start_one(n)

    def collect(h):
        back_plane(h).wait_recv()
        dg_plane(h).wait_recv()
        r.total[...] = tn(r.pick[h].reshape(P * CAP, R), r.stage[h].reshape(P * CAP, D))
        r.turn_stage[h] = jnp.zeros((EXPERTS, R), jnp.float32)

        def gates_of(p):
            row = jnp.broadcast_to(r.dg_in[h, p, 0:1, 0:CAP], (8, CAP))
            r.turn_stage[h, pl.ds(z.expert(me, p), 1), :] = exact("nn", row, r.pick[h, p].astype(jnp.float32))[0:1, :]
        times(P, gates_of)
        @pl.when(h != me.h)
        def _():
            part_fold.send(h)
            turn_lane.start_one(lax.rem(h + H - me.h, H))
    part_fold.far_first(collect)
    r.turn_v[...] = jnp.zeros((LANES, R), jnp.float32)
    r.turn_v[0:EXPERTS, :] = r.turn_stage[me.h]
    times(H, lambda h: out_plane(h).start())
    own_out = pltpu.make_async_copy(r.result.at[:, me.p], r.out_in.at[:, me.p], r.own_sem.at[7])
    own_out.start()
    part_fold.finish()
    turn_lane.wait_recv()

    def add_part(n):
        h = lax.rem(me.h + n + 1, H)
        r.turn_v[0:EXPERTS, :] += r.turn_in[h]
    times(H - 1, add_part)
    gts = r.gates_t[...].T
    dgs = r.turn_v[...].T
    d_log = gts * (dgs - jnp.sum(gts * dgs, axis=-1, keepdims=True))
    d_h2 = r.total[...] + exact("nt", d_log, r.small_v[...].astype(jnp.float32))
    mid = r.middle[...]
    inverse = lax.rsqrt(jnp.mean(mid * mid, axis=-1, keepdims=True) + norm_eps)
    n2 = mid * inverse
    g = d_h2 * gain_two
    dm = r.cot[...].astype(jnp.float32) + inverse * (g - n2 * jnp.mean(g * n2, axis=-1, keepdims=True))
    r.d_mid[...] = dm
    r.d_attn[...] = (residual_scale * dm).astype(jnp.bfloat16)
    up_attn_relay.start_own()
    up_attn_chain.start()
    r.gain_v[...] = jnp.zeros((LANES, D), jnp.float32)
    r.gain_v[EXPERTS + 1 : EXPERTS + 2, :] = jnp.sum(d_h2 * n2, axis=0, keepdims=True)
    r.g_small[...] = exact("tn", r.h2[...].astype(jnp.float32), d_log)

    r.blocks[me.c] = r.d_attn[...]
    r.dk_acc[...] = jnp.zeros((L, LANES), jnp.float32)
    r.dv_acc[...] = jnp.zeros((L, LANES), jnp.float32)
    wo_c = rows_at(r.wo_v, me.c, qw)

    def attend_back(place, core):
        c = 2 * place + core
        trickle(2 * H + c)
        part = pl.ds(pl.multiple_of(c * R, R), R)
        q = r.q_all[part, :]
        d_mix = nt(r.blocks[c], wo_c[...])
        if qw < LANES:
            d_mix = jnp.concatenate([d_mix, jnp.zeros((R, LANES - qw), jnp.float32)], axis=1)
        d_mix = d_mix.astype(jnp.bfloat16)
        row = jnp.concatenate([r.place_row[i, 0:1, :] for i in range(C)], axis=1)
        places = r.place_col[part, :]
        allowed = row <= places[:, 0:1]
        dq = jnp.zeros((R, LANES), jnp.float32)
        for h in range(z.q_heads):
            mine = head_of == h
            rows = pl.ds(h * R, R)
            q_h = jnp.where(mine, q, jnp.zeros_like(q))
            dm_h = jnp.where(mine, d_mix, jnp.zeros_like(d_mix))
            r.q_v[rows, :] = q_h
            r.dm_v[rows, :] = dm_h
            s = jnp.where(allowed, nt(q_h, r.k2[...]) * score_scale, masked_score)
            p = jnp.exp(s - r.lse[h, part, 0:1])
            r.p_v[rows, :] = p.astype(jnp.bfloat16)
            delta = jnp.sum(dm_h.astype(jnp.float32) * r.att_f[part, :], axis=-1, keepdims=True)
            ds = (p * (nt(dm_h, r.v2[...]) - delta)).astype(jnp.bfloat16)
            r.ds_v[rows, :] = ds
            dq = jnp.where(mine, nn(ds, r.k2[...]) * score_scale, dq)
        r.dk_acc[...] += tn(r.ds_v[...], r.q_v[...])
        r.dv_acc[...] += tn(r.p_v[...], r.dm_v[...])
        cosine, sine = rope_tables(places, r.freq[0:1, :])
        r.d_qkv[part, 0:LANES] = rope(dq, cosine, -sine).astype(jnp.bfloat16)
    up_attn_chain.visit(attend_back, up_attn_relay)

    def finish_kv(c):
        part = pl.ds(pl.multiple_of(c * R, R), R)
        dk = r.dk_acc[part, :] * score_scale
        dv = r.dv_acc[part, :]
        dk = dk + pltpu.roll(dk, HEAD, 1)
        dv = dv + pltpu.roll(dv, HEAD, 1)
        cosine, sine = rope_tables(r.place_col[part, :], r.freq[1:2, :])
        r.d_qkv[part, LANES : 2 * LANES] = rope(jnp.where(head_of == 0, dk, dv), cosine, -sine).astype(jnp.bfloat16)
    times(C, finish_kv)

    def down_tokens(c):
        return nt(r.d_qkv[pl.ds(pl.multiple_of(c * R, R), R), :], r.wc_v[...])

    def for_sibling(place):
        c = 2 * place + 1 - me.k
        dn_block(c)[...] = down_tokens(c).astype(jnp.bfloat16)
        sib_copy(place).start()
    dn_fold.far_first(for_sibling)

    def for_line(place):
        dn = down_tokens(2 * place + me.k)
        sib_copy(place).wait_recv()
        r.total[...] = dn + sib_in(place)[...].astype(jnp.float32)
        @pl.when(place != dn_fold.place)
        def _():
            dn_fold.send(place)
        @pl.when(place == dn_fold.place)
        def _():
            r.grad_tokens[...] = r.total[...]
    dn_fold.far_first(for_line)

    own_out.wait()
    part_fold.wait_send()

    def mix(h):
        out_plane(h).wait_recv()
        load = pltpu.make_async_copy(r.out_in.at[h], r.stage.at[h], r.own_sem.at[12])
        load.start()

        def weigh(p):
            g = r.gate_all[h, pl.ds(z.expert(me, p), 1), :] * r.pick[h, p].astype(jnp.float32)
            high = g.astype(jnp.bfloat16)
            r.mix_hi[p] = high
            r.mix_lo[p] = (g - high.astype(jnp.float32)).astype(jnp.bfloat16)
        times(P, weigh)
        load.wait()
        rows = r.stage[h].reshape(P * CAP, D)
        total = tn(r.mix_hi[...].reshape(P * CAP, R), rows) + tn(r.mix_lo[...].reshape(P * CAP, R), rows)
        r.total[...] = total
        @pl.when(h != me.h)
        def _():
            mix_fold.send(h)
    mix_fold.far_first(mix)
    times(3 * (C - 1), trickle, 2 * H + C)
    times(2 * H, trickle)

    def weights(d):
        part = pl.ds(pl.multiple_of(d * 256, 256), 256)
        total = tn(r.h1[:, part], r.d_qkv[...])
        r.gc_stage[part, :] = total.astype(jnp.bfloat16)
        gain = jnp.sum(total * r.wc_v[part, :].astype(jnp.float32), axis=-1, keepdims=True)
        gain = gain / r.small_v[part, EXPERTS : EXPERTS + 1].astype(jnp.float32)
        r.g_small[part, :] = jnp.where(lane_of((256, LANES)) == EXPERTS, gain, r.g_small[part, :])
    times(D // 256, weights)
    times(C, lambda c: gc_column(c).start())
    r.gs_stage[...] = (r.g_small[...] + r.gain_v[...].T).astype(jnp.bfloat16)
    times(C, lambda c: gs_column(c).start())
    own_last = [
        pltpu.make_async_copy(rows_at(stage, c * F + me.f, rs), landing.at[me.f, c], r.own_cols.at[i, c])
        for i, (stage, landing) in enumerate([(r.gc_stage, r.gc_x), (r.gs_stage, r.gs_x)]) for c in range(C)
    ]
    for copy in own_last:
        copy.start()
    r.go_stage[...] = tn(r.att_f[...].astype(jnp.bfloat16), r.blocks[...].reshape(L, D)).astype(jnp.bfloat16)
    go_lane.start()
    own_go = pltpu.make_async_copy(rows_at(r.go_stage, me.f, rs), r.go_in.at[me.f], r.own_sem.at[13])
    own_go.start()
    for copy in own_last:
        copy.wait()
    times(C, lambda c: gc_column(c).wait_recv())
    times(C, lambda c: gs_column(c).wait_recv())
    gc_total = r.gc_x[0].astype(jnp.float32)
    gs_total = r.gs_x[0].astype(jnp.float32)
    for f in range(1, F):
        gc_total = gc_total + r.gc_x[f].astype(jnp.float32)
        gs_total = gs_total + r.gs_x[f].astype(jnp.float32)
    r.gc_sum[...] = gc_total.astype(jnp.bfloat16)
    r.gs_sum[...] = gs_total.astype(jnp.bfloat16)
    gc_lane.start()
    gs_lane.start()
    own_sums = [
        pltpu.make_async_copy(r.gc_sum.at[me.c], r.gc_in.at[me.c], r.own_sem.at[14]),
        pltpu.make_async_copy(r.gs_sum.at[me.c], r.gs_in.at[me.c], r.own_sem.at[15]),
    ]
    for copy in own_sums:
        copy.start()
    for last in [place_lane, wc_lane, small_lane, slot_lane, gate_a_lane, gate_b_lane, up_lane, down_lane, att_lane, gates_lane,
                 turn_lane, wo_lane, *grad_lanes[4:]]:
        last.wait_send()
    for last in [cot_chain, rows_chain, up_attn_chain, wo_relay, up_attn_relay]:
        last.wait_send()
    times(J, lambda j: sib_copy(j).wait_send())
    for last in [g_plane, back_plane, dg_plane, out_plane]:
        times(H, lambda h, last=last: last(h).wait_send())
    times(J, lambda j: wo_column(2 * j + me.k).wait_send())
    for last in [wc_column, small_column, gc_column, gs_column]:
        times(C, lambda c, last=last: last(c).wait_send())
    mix_fold.finish()
    r.output[...] = (r.middle[...] + residual_scale * r.total[...]).astype(jnp.bfloat16)

    r.total[...] = r.grad_tokens[...]
    dn_fold.finish()
    d_h1 = r.total[...]
    x = r.tok[...].astype(jnp.float32)
    inverse = lax.rsqrt(jnp.mean(x * x, axis=-1, keepdims=True) + norm_eps)
    n1 = x * inverse
    g = d_h1 * gain_one
    r.grad_tokens[...] = r.d_mid[...] + inverse * (g - n1 * jnp.mean(g * n1, axis=-1, keepdims=True))
    for last in [gc_lane, gs_lane, go_lane]:
        last.wait_recv()
    for last in grad_lanes:
        last.wait_recv()
    for last in [gc_lane, gs_lane, go_lane] + grad_lanes[:4]:
        last.wait_send()
    for last in [mix_fold, dn_fold]:
        last.wait_send()
    for copy in own_grads + own_sums + [own_go]:
        copy.wait()


def layer_call(z, R, ff, dc, tok, place, routes, cot, w_pack, small, w_out, w_gate, w_up, w_downt):
    C, F, N, H, P, J, S, rs = z.C, z.F, z.N, z.H, z.P, z.J, z.S, z.rows_w
    L, f, f16 = C * R, jnp.float32, jnp.bfloat16
    rows, heads, tile = H * P * CAP, z.q_heads * R, 8 * CAP
    ins = dict(tok=(tok, 1), place=(place, 1), routes=(routes, 1), cot=(cot, 1), freq=(frequencies(), 1), w_pack=(w_pack, 0),
               small=(small, 0), w_out=(w_out, 0), w_gate=(w_gate, 0), w_up=(w_up, 0), w_downt=(w_downt, 0))
    outs = dict(
        output=(shape_of((R, D)), 1), grad_tokens=(shape_of((R, D), f), 1), gc_in=(shape_of((C, rs, 2 * LANES)), 0),
        gs_in=(shape_of((C, rs, LANES)), 0), go_in=(shape_of((F, rs, D)), 0), gw_in=(shape_of((2, S, z.G, dc, ff)), 0),
        gd_in=(shape_of((S, z.G, ff, dc)), 0),
        out_in=(shape_of((H, P, CAP, D)), 0))
    scratch = dict(
        blocks=vmem((C, R, D)), place_all=vmem((C, 8, R), jnp.int32), wc_v=vmem((D, 2 * LANES)), small_v=vmem((D, LANES)),
        wo_v=vmem((D, D)), cot_all=vmem((H, R, D)), slot_all=vmem((H, EXPERTS, R), f), slot_t=vmem((LANES, R), f),
        place_col=vmem((L, R), f), place_row=vmem((C, 8, R), f), h1=vmem((L, D)), q_all=vmem((L, LANES)), k2=vmem((L, LANES)),
        v2=vmem((L, LANES)), lse=vmem((z.q_heads, L, LANES), f), att_f=vmem((L, LANES), f), att_stage=vmem((C, R, LANES)),
        att_in=vmem((C, R, LANES)), middle=vmem((R, D), f), h2=vmem((R, D)), gates_t=vmem((LANES, R), f),
        gate_all=vmem((H, EXPERTS, R), f), h_all=vmem((H, R, D)), pick=vmem((H, P, CAP, R)), stage=vmem((H, P, CAP, D)),
        xin=vmem((rows, D)), g_stage=vmem((H, P, 8, LANES), f), gin=vmem((H, P, 8, LANES), f), wv=vmem((3, C, dc, ff)),
        cot_v=vmem((rows, D)), d_rows=vmem((H, P, CAP, D)), dg_stage=vmem((H, P, 8, LANES), f),
        dg_in=vmem((H, P, 8, LANES), f), hid=vmem((rows, ff)), d_gate=vmem((rows, ff)), d_up=vmem((rows, ff)),
        pool=vmem((max(rows, L), D)), g_col=vmem((tile, LANES), f), result=vmem((H, P, CAP, D)),
        part_stage=vmem((H, R, D)), part_in=vmem((H + 1, R, D)), turn_stage=vmem((H, EXPERTS, R), f),
        turn_in=vmem((H, EXPERTS, R), f), turn_v=vmem((LANES, R), f), d_mid=vmem((R, D), f), d_attn=vmem((R, D)),
        g_small=vmem((D, LANES), f), g_down=vmem((C, ff, dc)), gain_v=vmem((LANES, D), f), ds_v=vmem((heads, L)), p_v=vmem((heads, L)),
        q_v=vmem((heads, LANES)), dm_v=vmem((heads, LANES)), dk_acc=vmem((L, LANES), f), dv_acc=vmem((L, LANES), f),
        d_qkv=vmem((L, 2 * LANES)),
        gc_stage=vmem((D, 2 * LANES)), go_stage=vmem((LANES, D)), gs_stage=vmem((D, LANES)), gc_x=vmem((F, C, rs, 2 * LANES)),
        gs_x=vmem((F, C, rs, LANES)), gc_sum=vmem((C, rs, 2 * LANES)), gs_sum=vmem((C, rs, LANES)), mix_hi=vmem((P, CAP, R)),
        mix_lo=vmem((P, CAP, R)), mix_in=vmem((H + 1, R, D)), total=vmem((R, D), f), own_sem=pltpu.SemaphoreType.DMA((16,)),
        own_cols=pltpu.SemaphoreType.DMA((2, C)))
    both = ("_send", "_recv")
    scratch |= {"lane_" + n + b: pltpu.SemaphoreType.DMA((z.count(g),)) for n, g in LANE_GROUPS.items() for b in both}
    steps = {"col": 2 * H, "line": 2 * J}
    scratch |= {"chain_" + n + b: pltpu.SemaphoreType.DMA((steps[g],)) for n, g in CHAIN_GROUPS.items() for b in both}
    scratch |= {"plane_" + n + b: pltpu.SemaphoreType.DMA((H, P)) for n in PLANE_LANES for b in both}
    scratch |= {"column_" + n + b: pltpu.SemaphoreType.DMA((C, F)) for n in COLUMN_LANES for b in both}
    scratch |= {"relay_" + n + b: pltpu.SemaphoreType.DMA((J,)) for n in RELAYS for b in both}
    names = list(ins) + list(outs) + list(scratch)
    space = lambda fast: pl.BlockSpec(memory_space=pltpu.VMEM if fast else pl.ANY)
    results = pl.pallas_call(
        functools.partial(layer_kernel, z, R, dc, tile, names), name="layer",
        out_shape=[o for o, _ in outs.values()], in_specs=[space(fast) for _, fast in ins.values()],
        out_specs=[space(fast) for _, fast in outs.values()], scratch_shapes=list(scratch.values()),
        compiler_params=pltpu.CompilerParams(collective_id=0, has_side_effects=True, vmem_limit_bytes=67043328),
    )(*[a for a, _ in ins.values()])
    return results[:7]


def local(z, tokens, norm_first, w_query, w_key, w_value, w_out, norm_second, w_router,
          w_gate, w_up, w_down, positions, routes, cotangent):
    C, F = z.C, z.F
    R = tokens.shape[1]
    rs = z.rows_w
    ff = w_gate.shape[2]
    dc = D // C

    heads_q = jnp.pad(w_query.reshape(rs, C, z.q_width), ((0, 0), (0, 0), (0, LANES - z.q_width)))
    heads_k = jnp.repeat(w_key.reshape(rs, KV_HEADS, HEAD), z.share, axis=1)
    heads_v = jnp.repeat(w_value.reshape(rs, KV_HEADS, HEAD), z.share, axis=1)
    w_pack = jnp.concatenate([heads_q, heads_k, heads_v], axis=2).transpose(1, 0, 2)
    small = jnp.concatenate(
        [w_router, norm_first[:, None], norm_second[:, None], jnp.zeros((rs, 128 - EXPERTS - 2), jnp.bfloat16)], axis=1)
    w_downt = w_down.transpose(0, 2, 1)
    output, grad_tokens, gc_in, gs_in, go_in, gw_in, gd_in = layer_call(
        z, R, ff, dc, tokens[0], positions, routes[0].T, cotangent[0], w_pack, small, w_out, w_gate, w_up, w_downt)
    gc = f32(gc_in)
    join = lambda a: a.reshape(KV_HEADS, z.share, rs, HEAD).sum(axis=1).transpose(1, 0, 2).reshape(rs, KV_HEADS * HEAD)
    gs = jnp.sum(f32(gs_in), axis=0)
    return (
        output[None],
        grad_tokens[None],
        gs[:, EXPERTS],
        gc[:, :, : z.q_width].transpose(1, 0, 2).reshape(rs, D),
        join(gc[:, :, LANES : LANES + HEAD]),
        join(gc[:, :, LANES + HEAD :]),
        jnp.sum(f32(go_in), axis=0),
        gs[:, EXPERTS + 1],
        gs[:, :EXPERTS],
        jnp.sum(f32(gw_in[0]), axis=0),
        jnp.sum(f32(gw_in[1]), axis=0),
        jnp.sum(f32(gd_in), axis=0),
    )


def solution(mesh):
    row = P(("ctx", "fsdp"), None)
    vec = P(("ctx", "fsdp"))
    seq = P("fsdp", "ctx", None)
    down = P("fsdp", None, "ctx")
    return jax.shard_map(
        functools.partial(local, Sizes(mesh)),
        mesh=mesh,
        in_specs=(seq, vec, row, row, row, row, vec, row, seq, seq, down, P("fsdp", "ctx"), seq, seq),
        out_specs=(seq, seq, vec, row, row, row, row, vec, row, seq, seq, down),
        check_vma=False,
    )
```
